32 devices in a mesh: dp: 8 (over z, y), ep: 4 (over x, core).
Axes of the slice: x: 2, y: 2, z: 4, core: 2. Of those that a mesh axis runs over, the one named last changes fastest.
Arguments:
- hidden_in: bfloat16 [4096, 2048], P(('dp', 'ep')), may hold values from -6 to 6
- cotangent: bfloat16 [4096, 2048], P(('dp', 'ep')), may hold values from -6 to 6
- deal_order: int32 [4096], P(('dp', 'ep')), may hold values from 0 to 4095, as said below
- seq_lengths: int32 [32, 3], P(('dp', 'ep')), may hold values from 1 to 80, 112 in all within a row
- expert_ids: int32 [4096, 8], P(('dp', 'ep')), may hold values from 0 to 15, all different within a row; in each aligned block of 128 rows (0 to 127, 128 to 255, ...) at most 80 rows name the same one
- w_query: bfloat16 [2048, 4096], P(('dp', 'ep')), may hold values from -0.125 to 0.125
- w_key: bfloat16 [2048, 512], P(('dp', 'ep')), may hold values from -0.125 to 0.125
- w_value: bfloat16 [2048, 512], P(('dp', 'ep')), may hold values from -0.125 to 0.125
- w_out: bfloat16 [4096, 2048], P(('dp', 'ep')), may hold values from -0.375 to 0.375
- w_router: bfloat16 [2048, 16], P(('dp', 'ep')), may hold values from -0.0625 to 0.0625
- gain_attn: bfloat16 [2048], P(('dp', 'ep')), may hold values from 0.5 to 1.5
- gain_moe: bfloat16 [2048], P(('dp', 'ep')), may hold values from 0.5 to 1.5
- gain_query: bfloat16 [128], replicated, may hold values from 0.5 to 1.5
- gain_key: bfloat16 [128], replicated, may hold values from 0.5 to 1.5
- w_gate: bfloat16 [16, 2048, 768], P('ep', 'dp'), may hold values from -0.125 to 0.125
- w_up: bfloat16 [16, 2048, 768], P('ep', 'dp'), may hold values from -0.125 to 0.125
- w_down: bfloat16 [16, 768, 2048], P('ep', None, 'dp'), may hold values from -0.875 to 0.875
- clip_threshold: float32 [32], replicated, may hold values from 0.1 to 1
Outputs:
- block_out: bfloat16 [4096, 2048], P(('dp', 'ep'))
- grad_input: float32 [4096, 2048], P(('dp', 'ep'))
- grad_query: float32 [2048, 4096], P(('dp', 'ep'))
- grad_key: float32 [2048, 512], P(('dp', 'ep'))
- grad_value: float32 [2048, 512], P(('dp', 'ep'))
- grad_out: float32 [4096, 2048], P(('dp', 'ep'))
- grad_router: float32 [2048, 16], P(('dp', 'ep'))
- grad_gain_attn: float32 [2048], P(('dp', 'ep'))
- grad_gain_moe: float32 [2048], P(('dp', 'ep'))
- grad_gain_query: float32 [128], replicated
- grad_gain_key: float32 [128], replicated
- grad_gate: float32 [16, 2048, 768], P('ep', 'dp')
- grad_up: float32 [16, 2048, 768], P('ep', 'dp')
- grad_down: float32 [16, 768, 2048], P('ep', None, 'dp')
- clip_factor: float32 [32], replicated
The draws below stay inside these ranges and needn't reach their ends.
Inputs may be any that keep to these rules, and one draw needn't show every extreme that they name: `deal_order`: each aligned block of 128 entries is a permutation of that block's own row numbers. `seq_lengths`: each device's 3 lengths sum to 112, and the longest is exactly 80. `expert_ids`: A row names 8 different experts; within the rows of one device no expert is named more than 80 times, a bound that some block reaches.
All inputs are finite; a program needn't handle non-finite values.
Results may differ from the reference program's by a relative error of at most 0.017.
Values may be sent and summed in bfloat16 or wider, within the bound.
A program may use at most 320 MiB of HBM per device.

```python
import math
import jax
import jax.numpy as jnp
import numpy as np
from jax import lax

D = 2048
HEADS = 32
KV_HEADS = 4
HEAD_DIM = 128
FF = 768
TOPK = 8
TOK_DEV = 128
SEQ_DEV = 3
VALID_DEV = 112
MAXLEN = 80
EXPERTS = 16
CAP = 80
TOKENS = 4096
N_DP = 8
N_EP = 4


def draw_deal_order(key, part):
    block_count = TOKENS // TOK_DEV
    block_keys = jax.random.split(jax.random.fold_in(key, 17), block_count)
    shuffled = jax.vmap(lambda block_key: jax.random.permutation(block_key, TOK_DEV))(block_keys)
    offsets = jnp.arange(block_count, dtype=jnp.int32)[:, None] * TOK_DEV
    return (shuffled.astype(jnp.int32) + offsets).reshape(-1).astype(jnp.int32)


def block_levels(own_key, extent, shards, smallest, top_value):
    def one(axis_at, blocks):
        steps = jax.random.uniform(jax.random.fold_in(jax.random.fold_in(own_key, 6), axis_at), (blocks,), jnp.float32, smallest / len(shards), top_value / len(shards))
        return jnp.repeat(jnp.exp(steps), extent[axis_at] // blocks).reshape((-1,) + (1,) * (len(extent) - axis_at - 1))

    loudness = one(*shards[0])
    for cut in shards[1:]:
        loudness = loudness * one(*cut)
    return loudness


def length_profile(count, total, most, lean):
    portions = [(1 << 20) // math.isqrt(grade ** lean) + 1 for grade in range(2, count + 1)]
    spare, given = total - most - (count - 1), [1] * (count - 1)
    while spare > 0:
        candidates = [i for i in range(count - 1) if given[i] < most]
        mass, remaining = sum([portions[i] for i in candidates]), spare
        for i in candidates:
            extra = min(most - given[i], max(1, remaining * portions[i] // mass), spare)
            given[i] = given[i] + extra
            spare = spare - extra
    return np.array([most] + given)


def ragged(rng, amount, total, limit, slope):
    if amount == 2:
        one = jax.random.randint(rng, (), max(1, total - limit), min(limit, total - 1) + 1)
        return jnp.stack([one, total - one])
    tallies = jnp.asarray(length_profile(amount, total, limit, slope), jnp.int32)
    couples = (amount - 1) // 2
    source_of, receiver = tallies[1:1 + 2 * couples:2], tallies[2:2 + 2 * couples:2]
    margin = jnp.minimum(source_of - 1, limit - receiver)
    passed = jax.random.randint(jax.random.fold_in(rng, 1), (couples,), 0, 1 << 20) % (margin + 1)
    tallies = tallies.at[1:1 + 2 * couples:2].set(source_of - passed).at[2:2 + 2 * couples:2].set(receiver + passed)
    return tallies[jax.random.permutation(jax.random.fold_in(rng, 2), amount)]


def assign_block(key, own, number, rows, number_of, top, reach, skew):
    sequence = jax.random.permutation(key, number_of)
    heavy_load, usual = shares(number_of, rows * top, reach, skew, True), shares(number_of, rows * top, reach, skew, False)
    places = jnp.arange(number_of)

    def named(sizes, rotation):
        used = int((sizes > 0).sum())
        fixed = max(1, used // 4)
        shifted = fixed + (places - fixed + rotation * (used - fixed)) % max(1, number_of - fixed)
        return jnp.zeros((number_of,), jnp.int32).at[sequence[jnp.where(places < fixed, places, shifted)]].set(jnp.asarray(sizes, jnp.int32))

    sizes = jnp.where(number % 4 == 0, named(heavy_load, number // 4), named(usual, number - number // 4 - 1))
    mixed = jax.random.permutation(jax.random.fold_in(own, 3), number_of)
    giver, receiver = mixed[0:number_of // 2 * 2:2], mixed[1:number_of // 2 * 2:2]
    room = jnp.minimum(sizes[giver] - 1, reach - sizes[receiver]) // 2
    room = jnp.where((giver == sequence[0]) | (receiver == sequence[0]) | (sizes[receiver] == 0), 0, jnp.maximum(room, 0))
    shifted = jax.random.randint(jax.random.fold_in(own, 4), (number_of // 2,), 0, 1 << 20) % (room + 1)
    sizes = sizes.at[giver].add(-shifted).at[receiver].add(shifted)
    labels = jnp.searchsorted(jnp.cumsum(sizes), jnp.arange(rows * top), side="right").astype(jnp.int32)
    grid = labels.reshape(top, rows).T
    grid = grid[jax.random.permutation(jax.random.fold_in(own, 1), rows)]
    rotation = jax.random.randint(jax.random.fold_in(own, 2), (rows, 1), 0, top)
    return jnp.take_along_axis(grid, (jnp.arange(top)[None, :] + rotation) % top, axis=1)


def shares(amount, total, limit, slope, full):
    weights = [(1 << 20) // math.isqrt(grade ** slope) + 1 for grade in range(1, amount + 1)]
    largest = limit if full else min(limit, max(-(-total // amount), total * weights[0] // sum(weights)))
    least = 1 if total - largest >= amount - 1 else 0
    given, surplus = [largest] + [least] * (amount - 1), total - largest - least * (amount - 1)
    while surplus > 0:
        free = [i for i in range(1, amount) if given[i] < largest] or [i for i in range(1, amount) if given[i] < limit]
        whole, left = sum([weights[i] for i in free]), surplus
        for i in free:
            addition = min(limit - given[i], max(1, left * weights[i] // whole), surplus)
            given[i] = given[i] + addition
            surplus = surplus - addition
    return np.array(given)


def scatter_about(key, dims, deviation, bound, cuts=(), held_as=jnp.bfloat16):
    loudness = block_levels(key, dims, cuts, -0.22, 0.18) if cuts else 1.0
    values = jax.random.normal(key, dims, jnp.float32) * deviation * loudness
    return jnp.minimum(jnp.maximum(values, -bound), bound).astype(held_as)


def setup_inputs(seed: int = 0) -> dict:
    seeds = jax.random.split(jax.random.key(seed), 19)
    hidden_in = scatter_about(seeds[0], (TOKENS, D), 1.0, 6.0, ((0, 32),))
    cotangent = scatter_about(seeds[1], (TOKENS, D), 1.0, 6.0, ((0, 32),))
    deal_order = draw_deal_order(jax.random.fold_in(seeds[18], 71), 0)
    seq_lengths = jax.vmap(lambda own: ragged(own, SEQ_DEV, VALID_DEV, MAXLEN, 2))(jax.random.split(seeds[3], (N_DP * N_EP))).reshape((N_DP * N_EP, SEQ_DEV)).astype(jnp.int32)
    expert_ids_keys = jax.random.split(jax.random.fold_in(seeds[4], 1), TOKENS // TOK_DEV)
    expert_ids_turns = jax.random.permutation(jax.random.fold_in(seeds[4], 3), TOKENS // TOK_DEV)
    expert_ids = jax.vmap(lambda own, number: assign_block(jax.random.fold_in(seeds[4], 2), own, number, TOK_DEV, EXPERTS, TOPK, CAP, 2))(expert_ids_keys, expert_ids_turns).reshape((TOKENS, TOPK))
    w_query = scatter_about(seeds[5], (D, HEADS * HEAD_DIM), D ** -0.5, 0.125, ((0, 32),))
    w_key = scatter_about(seeds[6], (D, KV_HEADS * HEAD_DIM), D ** -0.5, 0.125, ((0, 32),))
    w_value = scatter_about(seeds[7], (D, KV_HEADS * HEAD_DIM), D ** -0.5, 0.125, ((0, 32),))
    w_out = scatter_about(seeds[8], (HEADS * HEAD_DIM, D), (HEADS * HEAD_DIM // 16) ** -0.5, 0.375, ((0, 32),))
    w_router = scatter_about(seeds[9], (D, EXPERTS), (4 * D) ** -0.5, 0.0625, ((0, 32),))
    gain_attn = jnp.clip(1.0 + 0.1 * jax.random.normal(seeds[10], (D,), jnp.float32), 0.5, 1.5).astype(jnp.bfloat16)
    gain_moe = jnp.clip(1.0 + 0.1 * jax.random.normal(seeds[11], (D,), jnp.float32), 0.5, 1.5).astype(jnp.bfloat16)
    gain_query = jnp.clip(1.0 + 0.1 * jax.random.normal(seeds[12], (HEAD_DIM,), jnp.float32), 0.5, 1.5).astype(jnp.bfloat16)
    gain_key = jnp.clip(1.0 + 0.1 * jax.random.normal(seeds[13], (HEAD_DIM,), jnp.float32), 0.5, 1.5).astype(jnp.bfloat16)
    w_gate = scatter_about(seeds[14], (EXPERTS, D, FF), D ** -0.5, 0.125, ((0, 4), (1, 8)))
    w_up = scatter_about(seeds[15], (EXPERTS, D, FF), D ** -0.5, 0.125, ((0, 4), (1, 8)))
    w_down = scatter_about(seeds[16], (EXPERTS, FF, D), (FF // 16) ** -0.5, 0.875, ((0, 4), (2, 8)))
    clip_threshold = jnp.clip(jax.random.uniform(seeds[17], (HEADS,), jnp.float32, 0.1, 1.0), 0.1, 1.0)
    return {"hidden_in": hidden_in, "cotangent": cotangent, "deal_order": deal_order, "seq_lengths": seq_lengths, "expert_ids": expert_ids, "w_query": w_query, "w_key": w_key, "w_value": w_value, "w_out": w_out, "w_router": w_router, "gain_attn": gain_attn, "gain_moe": gain_moe, "gain_query": gain_query, "gain_key": gain_key, "w_gate": w_gate, "w_up": w_up, "w_down": w_down, "clip_threshold": clip_threshold}


highest = lax.Precision.HIGHEST
epsilon = 1e-06
theta_base = 1000000.0
masked_fill = -1e+30

@jax.custom_vjp
def low(v):
    return lax.optimization_barrier(v.astype(jnp.bfloat16)).astype(jnp.float32)

@jax.custom_vjp
def low_back(v):
    return v

def low_keep(v):
    return (low(v), None)

def low_pass(kept, grad):
    return (grad,)

def back_keep(v):
    return (v, None)

def back_low(kept, grad):
    return (low(grad),)
low.defvjp(low_keep, low_pass)
low_back.defvjp(back_keep, back_low)

def product(left_side, right_side):
    return jnp.dot(left_side, right_side, precision=highest, preferred_element_type=jnp.float32)

def rms_scale(values):
    return lax.rsqrt(lax.optimization_barrier(jnp.mean(values * values, axis=-1, keepdims=True)) + epsilon)

def rotate_half(values):
    half_dim = values.shape[-1] // 2
    return jnp.concatenate([-values[..., half_dim:], values[..., :half_dim]], axis=-1)

def rotate(values, cosine_table, sine_table):
    return values * cosine_table + rotate_half(values) * sine_table

def layout(lens_row, tok_count):
    seq_ends = jnp.cumsum(lens_row).astype(jnp.int32)
    row_index = jnp.arange(tok_count, dtype=jnp.int32)
    segment = lax.optimization_barrier(jnp.sum((row_index[:, None] >= seq_ends[None, :]).astype(jnp.int32), axis=1)).astype(jnp.int32)
    starts_all = jnp.concatenate([jnp.zeros((1,), jnp.int32), seq_ends])
    seg_hot = segment[:, None] == jnp.arange(starts_all.shape[0], dtype=jnp.int32)[None, :]
    first_row = lax.optimization_barrier(jnp.sum(jnp.where(seg_hot, starts_all[None, :], 0), axis=1)).astype(jnp.int32)
    position = row_index - first_row
    valid_row = segment < lens_row.shape[0]
    allowed = (segment[:, None] == segment[None, :]) & (row_index[None, :] <= row_index[:, None])
    return (position, valid_row, allowed)

def rotary_tables(position, head_dim):
    half_dim = head_dim // 2
    frequency = theta_base ** (-(jnp.arange(half_dim, dtype=jnp.float32) * 2.0) / head_dim)
    angles = position.astype(jnp.float32)[:, None] * frequency[None, :]
    angles = jnp.concatenate([angles, angles], axis=-1)
    return (jnp.cos(angles), jnp.sin(angles))

def attention_block(block_rows, lens_row, weights):
    w_query, w_key, w_value, w_out, gain_attn, gain_query, gain_key = weights
    tok_count = block_rows.shape[0]
    group_size = HEADS // KV_HEADS
    position, valid_row, allowed = layout(lens_row, tok_count)
    cosine_table, sine_table = rotary_tables(position, HEAD_DIM)
    normed_in = low(block_rows * rms_scale(block_rows) * gain_attn)
    query_raw = low_back(product(normed_in, w_query)).reshape(tok_count, KV_HEADS, group_size, HEAD_DIM)
    key_raw = low_back(product(normed_in, w_key)).reshape(tok_count, KV_HEADS, HEAD_DIM)
    value_rows = low(low_back(product(normed_in, w_value))).reshape(tok_count, KV_HEADS, HEAD_DIM)
    query_rot = low(rotate(query_raw * rms_scale(query_raw) * gain_query, cosine_table[:, None, None, :], sine_table[:, None, None, :]))
    key_rot = low(rotate(key_raw * rms_scale(key_raw) * gain_key, cosine_table[:, None, :], sine_table[:, None, :]))
    score_scale = HEAD_DIM ** (-0.5)
    scores = low_back(jnp.einsum('tkgd,ukd->kgtu', query_rot, key_rot, precision=highest) * score_scale)
    masked = jnp.where(allowed, scores, masked_fill)
    row_top = lax.optimization_barrier(jnp.max(masked, axis=-1, keepdims=True))
    exponent = jnp.exp(masked - row_top)
    probs_low = low(exponent / lax.optimization_barrier(jnp.sum(exponent, axis=-1, keepdims=True)))
    mixed_heads = low(low_back(jnp.einsum('kgtu,ukd->tkgd', probs_low, value_rows, precision=highest)))
    branch = low_back(product(mixed_heads.reshape(tok_count, HEADS * HEAD_DIM), w_out))
    largest = lax.optimization_barrier(jnp.max(jnp.where(allowed & valid_row[:, None], scores, masked_fill), axis=(2, 3))).reshape(HEADS)
    return (block_rows + branch, largest, valid_row.astype(jnp.float32))

def expert_term(normed_mid, pieces):
    gate_mat, up_mat, down_mat, weight_col = pieces
    sent_rows = low_back(normed_mid)
    gate_part = low_back(product(sent_rows, gate_mat))
    up_part = low_back(product(sent_rows, up_mat))
    hidden = low(jax.nn.silu(gate_part) * up_part)
    returned = low(low_back(product(hidden, down_mat)))
    return weight_col[:, None] * returned

def forward(hidden_in, w_query, w_key, w_value, w_out, w_router, gain_attn, gain_moe, gain_query, gain_key, w_gate, w_up, w_down, deal_order, seq_lengths, expert_ids):
    dealt_rows = hidden_in[deal_order]
    blocks = dealt_rows.reshape(-1, TOK_DEV, D)
    attn_weights = (w_query, w_key, w_value, w_out, gain_attn, gain_query, gain_key)

    def one_block(pieces):
        return jax.checkpoint(attention_block)(pieces[0], pieces[1], attn_weights)
    after_attn, largest, valid_rows = lax.map(one_block, (blocks, seq_lengths))
    resid_mid = after_attn.reshape(-1, D)
    valid_all = valid_rows.reshape(-1)
    normed_mid = low(resid_mid * rms_scale(resid_mid) * gain_moe)
    logits = low_back(product(normed_mid, w_router))
    picked = jnp.take_along_axis(logits, expert_ids, axis=1)
    gate_weights = jax.nn.softmax(picked, axis=-1)
    expert_hot = (expert_ids[:, :, None] == jnp.arange(EXPERTS, dtype=jnp.int32)[None, None, :]).astype(jnp.float32)
    route_weights = lax.optimization_barrier(jnp.sum(gate_weights[:, :, None] * expert_hot, axis=1))

    def expert_step(running, pieces):
        return (running + jax.checkpoint(expert_term)(normed_mid, pieces), None)
    moe_out, ignored = lax.scan(expert_step, jnp.zeros_like(resid_mid), (w_gate, w_up, w_down, route_weights.T))
    resid_out = resid_mid + moe_out
    out_rows = jnp.where(valid_all[:, None] > 0.5, resid_out, 0.0)
    result = jnp.zeros_like(out_rows).at[deal_order].set(out_rows)
    return (result, lax.optimization_barrier(jnp.max(largest, axis=0)))

def reference(hidden_in, cotangent, deal_order, seq_lengths, expert_ids, w_query, w_key, w_value, w_out, w_router, gain_attn, gain_moe, gain_query, gain_key, w_gate, w_up, w_down, clip_threshold):
    floats = tuple((array_in.astype(jnp.float32) for array_in in (hidden_in, w_query, w_key, w_value, w_out, w_router, gain_attn, gain_moe, gain_query, gain_key, w_gate, w_up, w_down)))

    def wrapped(*params):
        return forward(*params, deal_order, seq_lengths, expert_ids)
    outputs, pullback, largest = jax.vjp(wrapped, *floats, has_aux=True)
    gradients = pullback(cotangent.astype(jnp.float32))
    clip_factor = jnp.sqrt(clip_threshold / jnp.maximum(largest, clip_threshold))
    return (outputs.astype(jnp.bfloat16), gradients[0], gradients[1], gradients[2], gradients[3], gradients[4], gradients[5], gradients[6], gradients[7], gradients[8], gradients[9], gradients[10], gradients[11], gradients[12], clip_factor)
```

```python
import functools

import jax
import jax.numpy as jnp
from jax import lax
from jax.experimental import pallas as pl
from jax.experimental.pallas import tpu as pltpu
from jax.sharding import PartitionSpec as P

epsilon = 1e-06
theta_base = 1000000.0
masked_fill = -1e30


def rms_scale(values):
    return lax.rsqrt(jnp.mean(values * values, axis=-1, keepdims=True) + epsilon)


def rotate_half(values):
    half_dim = values.shape[-1] // 2
    return jnp.concatenate([-values[..., half_dim:], values[..., :half_dim]], axis=-1)


def rotate(values, cosine_table, sine_table):
    return values * cosine_table + rotate_half(values) * sine_table


def rotate_back(values, cosine_table, sine_table):
    scaled = values * sine_table
    half_dim = values.shape[-1] // 2
    turned = jnp.concatenate([scaled[..., half_dim:], -scaled[..., :half_dim]], axis=-1)
    return values * cosine_table + turned


def norm_back(grad_unit, unit_rows, inv_root):
    return inv_root * (
        grad_unit - unit_rows * jnp.mean(grad_unit * unit_rows, axis=-1, keepdims=True)
    )


def contract(left_side, right_side, pattern):
    return jnp.einsum(pattern, left_side, right_side, preferred_element_type=jnp.float32)


def layout(lens_row, tok_count):
    seq_ends = jnp.cumsum(lens_row)
    row_index = jnp.arange(tok_count, dtype=jnp.int32)
    segment = jnp.sum((row_index[:, None] >= seq_ends[None, :]).astype(jnp.int32), axis=1)
    starts_all = jnp.concatenate([jnp.zeros((1,), jnp.int32), seq_ends])
    seg_hot = segment[:, None] == jnp.arange(starts_all.shape[0], dtype=jnp.int32)[None, :]
    first_row = jnp.sum(jnp.where(seg_hot, starts_all[None, :], 0), axis=1)
    position = row_index - first_row
    valid_row = segment < lens_row.shape[0]
    allowed = (segment[:, None] == segment[None, :]) & (row_index[None, :] <= row_index[:, None])
    return (position, valid_row, allowed)


def rotary_tables(position, head_dim):
    half_dim = head_dim // 2
    frequency = theta_base ** (-(jnp.arange(half_dim, dtype=jnp.float32) * 2.0) / head_dim)
    angles = position.astype(jnp.float32)[:, None] * frequency[None, :]
    angles = jnp.concatenate([angles, angles], axis=-1)
    return (jnp.cos(angles), jnp.sin(angles))


def per_device(
    hidden_in,
    cotangent,
    deal_order,
    seq_lengths,
    expert_ids,
    w_query,
    w_key,
    w_value,
    w_out,
    w_router,
    gain_attn,
    gain_moe,
    gain_query,
    gain_key,
    w_gate,
    w_up,
    w_down,
    clip_threshold,
):
    tok_count = hidden_in.shape[0]
    model_width = hidden_in.shape[1]
    head_dim = gain_query.shape[0]
    local_order = deal_order % tok_count
    position, valid_row, allowed = layout(seq_lengths[0], tok_count)
    valid_col = valid_row.astype(jnp.float32)[:, None]
    cosine_table, sine_table = rotary_tables(position, head_dim)
    cosine_query = cosine_table[:, None, None, :]
    sine_query = sine_table[:, None, None, :]
    cosine_key = cosine_table[:, None, :]
    sine_key = sine_table[:, None, :]
    attn_params = (
        lax.all_gather(w_query, ("dp", "ep"), axis=0, tiled=True),
        lax.all_gather(w_key, ("dp", "ep"), axis=0, tiled=True),
        lax.all_gather(w_value, ("dp", "ep"), axis=0, tiled=True),
        lax.all_gather(w_out, ("dp", "ep"), axis=0, tiled=True),
        lax.all_gather(w_router, ("dp", "ep"), axis=0, tiled=True),
        lax.all_gather(gain_attn, ("dp", "ep"), axis=0, tiled=True),
        lax.all_gather(gain_moe, ("dp", "ep"), axis=0, tiled=True),
    )
    expert_params = (
        lax.all_gather(w_gate, "dp", axis=1, tiled=True),
        lax.all_gather(w_up, "dp", axis=1, tiled=True),
        lax.all_gather(w_down, "dp", axis=2, tiled=True),
    )
    query_full, key_full, value_full, out_full, router_full, gain_attn_full, gain_moe_full = (
        attn_params
    )
    gate_full, up_full, down_full = expert_params
    head_count = query_full.shape[1] // head_dim
    kv_count = key_full.shape[1] // head_dim
    group_size = head_count // kv_count
    experts = router_full.shape[1]
    top_count = expert_ids.shape[1]
    exp_local = w_gate.shape[0]
    ep_count = lax.axis_size("ep")
    capacity = (tok_count * top_count * 5 + 4 * experts - 1) // (4 * experts)
    score_scale = head_dim ** (-0.5)
    resid_in = hidden_in[local_order].astype(jnp.float32)
    inv_one = rms_scale(resid_in)
    unit_one = resid_in * inv_one
    gain_one = gain_attn_full.astype(jnp.float32)
    normed_in = (unit_one * gain_one).astype(jnp.bfloat16)
    query_raw = jnp.dot(normed_in, query_full, preferred_element_type=jnp.float32).reshape(
        tok_count, kv_count, group_size, head_dim
    )
    key_raw = jnp.dot(normed_in, key_full, preferred_element_type=jnp.float32).reshape(
        tok_count, kv_count, head_dim
    )
    value_rows = (
        jnp.dot(normed_in, value_full, preferred_element_type=jnp.float32)
        .astype(jnp.bfloat16)
        .reshape(tok_count, kv_count, head_dim)
    )
    inv_query = rms_scale(query_raw)
    unit_query = query_raw * inv_query
    gain_query_f = gain_query.astype(jnp.float32)
    query_rot = rotate(unit_query * gain_query_f, cosine_query, sine_query).astype(jnp.bfloat16)
    inv_key = rms_scale(key_raw)
    unit_key = key_raw * inv_key
    gain_key_f = gain_key.astype(jnp.float32)
    key_rot = rotate(unit_key * gain_key_f, cosine_key, sine_key).astype(jnp.bfloat16)
    scores = contract(query_rot, key_rot, "tkgd,ukd->kgtu") * score_scale
    masked = jnp.where(allowed, scores, masked_fill)
    row_top = jnp.max(masked, axis=-1, keepdims=True)
    exponent = jnp.exp(masked - row_top)
    row_total = jnp.sum(exponent, axis=-1, keepdims=True)
    log_total = row_top + jnp.log(row_total)
    probs_low = (exponent / row_total).astype(jnp.bfloat16)
    mixed_heads = (
        contract(probs_low, value_rows, "kgtu,ukd->tkgd")
        .astype(jnp.bfloat16)
        .reshape(tok_count, head_count * head_dim)
    )
    resid_mid = resid_in + jnp.dot(mixed_heads, out_full, preferred_element_type=jnp.float32)
    largest_local = jnp.max(
        jnp.where(allowed & valid_row[:, None], scores, masked_fill), axis=(2, 3)
    ).reshape(head_count)
    largest = lax.pmax(largest_local, ("dp", "ep"))
    clip_factor = jnp.sqrt(clip_threshold / jnp.maximum(largest, clip_threshold))
    inv_two = rms_scale(resid_mid)
    unit_two = resid_mid * inv_two
    gain_two = gain_moe_full.astype(jnp.float32)
    normed_mid = (unit_two * gain_two).astype(jnp.bfloat16)
    logits = jnp.dot(normed_mid, router_full, preferred_element_type=jnp.float32)
    choose = expert_ids[:, :, None] == jnp.arange(experts, dtype=jnp.int32)[None, None, :]
    picked = jnp.sum(jnp.where(choose, logits[:, None, :], 0.0), axis=2)
    gate_weights = jax.nn.softmax(picked, axis=-1)
    flat_ids = expert_ids.reshape(-1)
    flat_hot = (flat_ids[:, None] == jnp.arange(experts, dtype=jnp.int32)[None, :]).astype(
        jnp.int32
    )
    slot_rank = jnp.sum((jnp.cumsum(flat_hot, axis=0) - 1) * flat_hot, axis=1)
    slot_index = flat_ids * capacity + slot_rank
    pair_token = jnp.arange(tok_count * top_count, dtype=jnp.int32) // top_count
    send_rows = (
        jnp.zeros((experts * capacity, model_width), jnp.bfloat16)
        .at[slot_index]
        .set(normed_mid[pair_token])
    )
    send_rows = send_rows.reshape(ep_count, exp_local, capacity, model_width)
    arrived = lax.all_to_all(send_rows, "ep", split_axis=0, concat_axis=0, tiled=True)
    gate_part = contract(arrived, gate_full, "secd,edf->secf")
    up_part = contract(arrived, up_full, "secd,edf->secf")
    hidden_mid = (jax.nn.silu(gate_part) * up_part).astype(jnp.bfloat16)
    produced = contract(hidden_mid, down_full, "secf,efd->secd").astype(jnp.bfloat16)
    returned = lax.all_to_all(produced, "ep", split_axis=0, concat_axis=0, tiled=True)
    returned, arrived, gate_part, up_part = (returned, arrived, gate_part, up_part)
    pair_out = (
        returned.reshape(experts * capacity, model_width)[slot_index]
        .reshape(tok_count, top_count, model_width)
        .astype(jnp.float32)
    )
    resid_out = resid_mid + jnp.sum(gate_weights[:, :, None] * pair_out, axis=1)
    out_rows = (resid_out * valid_col).astype(jnp.bfloat16)
    block_out = jnp.zeros_like(out_rows).at[local_order].set(out_rows)
    attn_params = (
        lax.all_gather(w_query, ("dp", "ep"), axis=0, tiled=True),
        lax.all_gather(w_key, ("dp", "ep"), axis=0, tiled=True),
        lax.all_gather(w_value, ("dp", "ep"), axis=0, tiled=True),
        lax.all_gather(w_out, ("dp", "ep"), axis=0, tiled=True),
        lax.all_gather(w_router, ("dp", "ep"), axis=0, tiled=True),
        lax.all_gather(gain_attn, ("dp", "ep"), axis=0, tiled=True),
        lax.all_gather(gain_moe, ("dp", "ep"), axis=0, tiled=True),
    )
    expert_params = (
        lax.all_gather(w_gate, "dp", axis=1, tiled=True),
        lax.all_gather(w_up, "dp", axis=1, tiled=True),
        lax.all_gather(w_down, "dp", axis=2, tiled=True),
    )
    query_full, key_full, value_full, out_full, router_full, gain_attn_full, gain_moe_full = (
        attn_params
    )
    gate_full, up_full, down_full = expert_params
    grad_mid_out = cotangent[local_order].astype(jnp.float32) * valid_col
    grad_gates = jnp.sum(grad_mid_out[:, None, :] * pair_out, axis=2)
    grad_pair = (gate_weights[:, :, None] * grad_mid_out[:, None, :]).astype(jnp.bfloat16)
    send_grads = (
        jnp.zeros((experts * capacity, model_width), jnp.bfloat16)
        .at[slot_index]
        .set(grad_pair.reshape(-1, model_width))
    )
    send_grads = send_grads.reshape(ep_count, exp_local, capacity, model_width)
    grad_arrived = lax.all_to_all(send_grads, "ep", split_axis=0, concat_axis=0, tiled=True)
    grad_hidden = contract(grad_arrived, down_full, "secd,efd->secf")
    sigmoid_gate = jax.nn.sigmoid(gate_part)
    silu_gate = jax.nn.silu(gate_part)
    grad_gate_part = (
        grad_hidden * up_part * sigmoid_gate * (1.0 + gate_part * (1.0 - sigmoid_gate))
    ).astype(jnp.bfloat16)
    grad_up_part = (grad_hidden * silu_gate).astype(jnp.bfloat16)
    grad_rows = (
        contract(grad_gate_part, gate_full, "secf,edf->secd")
        + contract(grad_up_part, up_full, "secf,edf->secd")
    ).astype(jnp.bfloat16)
    grad_back = lax.all_to_all(grad_rows, "ep", split_axis=0, concat_axis=0, tiled=True)
    hidden_mid = (silu_gate * up_part).astype(jnp.bfloat16)
    grad_gate_w = contract(arrived, grad_gate_part, "secd,secf->edf")
    grad_up_w = contract(arrived, grad_up_part, "secd,secf->edf")
    grad_down_w = contract(hidden_mid, grad_arrived, "secf,secd->efd")
    grad_gate, grad_up, grad_down = (
        lax.psum_scatter(
            grad_gate_w.astype(jnp.bfloat16), "dp", scatter_dimension=1, tiled=True
        ).astype(jnp.float32),
        lax.psum_scatter(
            grad_up_w.astype(jnp.bfloat16), "dp", scatter_dimension=1, tiled=True
        ).astype(jnp.float32),
        lax.psum_scatter(
            grad_down_w.astype(jnp.bfloat16), "dp", scatter_dimension=2, tiled=True
        ).astype(jnp.float32),
    )
    mean_term = jnp.sum(gate_weights * grad_gates, axis=1, keepdims=True)
    grad_picked = gate_weights * (grad_gates - mean_term)
    grad_logits = jnp.sum(jnp.where(choose, grad_picked[:, :, None], 0.0), axis=1).astype(
        jnp.bfloat16
    )
    grad_router_w = contract(normed_mid, grad_logits, "td,te->de")
    pair_grads = (
        grad_back.reshape(experts * capacity, model_width)[slot_index]
        .reshape(tok_count, top_count, model_width)
        .astype(jnp.float32)
    )
    grad_normed_mid = jnp.sum(pair_grads, axis=1) + contract(grad_logits, router_full, "te,de->td")
    grad_gain_moe_w = jnp.sum(grad_normed_mid * unit_two, axis=0)
    grad_mid = grad_mid_out + norm_back(grad_normed_mid * gain_two, unit_two, inv_two)
    grad_branch = grad_mid.astype(jnp.bfloat16)
    grad_out_w = contract(mixed_heads, grad_branch, "tq,td->qd")
    grad_mixed = (
        contract(grad_branch, out_full, "td,qd->tq")
        .astype(jnp.bfloat16)
        .reshape(tok_count, kv_count, group_size, head_dim)
    )
    scores_again = contract(query_rot, key_rot, "tkgd,ukd->kgtu") * score_scale
    probs_back = jnp.exp(jnp.where(allowed, scores_again, masked_fill) - log_total)
    grad_value_rows = contract(
        probs_back.astype(jnp.bfloat16), grad_mixed, "kgtu,tkgd->ukd"
    ).astype(jnp.bfloat16)
    grad_probs = contract(grad_mixed, value_rows, "tkgd,ukd->kgtu")
    grad_scores = (
        probs_back * (grad_probs - jnp.sum(probs_back * grad_probs, axis=-1, keepdims=True))
    ).astype(jnp.bfloat16)
    grad_query_rot = contract(grad_scores, key_rot, "kgtu,ukd->tkgd") * score_scale
    grad_key_rot = contract(grad_scores, query_rot, "kgtu,tkgd->ukd") * score_scale
    grad_query_normed = rotate_back(grad_query_rot, cosine_query, sine_query)
    grad_key_normed = rotate_back(grad_key_rot, cosine_key, sine_key)
    grad_gain_q = jnp.sum(grad_query_normed * unit_query, axis=(0, 1, 2))
    grad_gain_k = jnp.sum(grad_key_normed * unit_key, axis=(0, 1))
    grad_query_raw = (
        norm_back(grad_query_normed * gain_query_f, unit_query, inv_query)
        .astype(jnp.bfloat16)
        .reshape(tok_count, head_count * head_dim)
    )
    grad_key_raw = (
        norm_back(grad_key_normed * gain_key_f, unit_key, inv_key)
        .astype(jnp.bfloat16)
        .reshape(tok_count, kv_count * head_dim)
    )
    grad_value_flat = grad_value_rows.reshape(tok_count, kv_count * head_dim)
    grad_query_w = contract(normed_in, grad_query_raw, "td,tq->dq")
    grad_key_w = contract(normed_in, grad_key_raw, "td,tq->dq")
    grad_value_w = contract(normed_in, grad_value_flat, "td,tq->dq")
    grad_normed_in = (
        contract(grad_query_raw, query_full, "tq,dq->td")
        + contract(grad_key_raw, key_full, "tq,dq->td")
        + contract(grad_value_flat, value_full, "tq,dq->td")
    )
    grad_gain_attn_w = jnp.sum(grad_normed_in * unit_one, axis=0)
    grad_resid_in = grad_mid + norm_back(grad_normed_in * gain_one, unit_one, inv_one)
    grad_input = jnp.zeros_like(grad_resid_in).at[local_order].set(grad_resid_in)
    grad_sums = (
        lax.psum_scatter(grad_query_w, ("dp", "ep"), scatter_dimension=0, tiled=True),
        lax.psum_scatter(grad_key_w, ("dp", "ep"), scatter_dimension=0, tiled=True),
        lax.psum_scatter(grad_value_w, ("dp", "ep"), scatter_dimension=0, tiled=True),
        lax.psum_scatter(grad_out_w, ("dp", "ep"), scatter_dimension=0, tiled=True),
        lax.psum_scatter(grad_router_w, ("dp", "ep"), scatter_dimension=0, tiled=True),
        lax.psum_scatter(grad_gain_attn_w, ("dp", "ep"), scatter_dimension=0, tiled=True),
        lax.psum_scatter(grad_gain_moe_w, ("dp", "ep"), scatter_dimension=0, tiled=True),
    )
    gain_sums = lax.psum((grad_gain_q, grad_gain_k), ("dp", "ep"))
    return (
        block_out,
        grad_input,
        grad_sums[0],
        grad_sums[1],
        grad_sums[2],
        grad_sums[3],
        grad_sums[4],
        grad_sums[5],
        grad_sums[6],
        gain_sums[0],
        gain_sums[1],
        grad_gate,
        grad_up,
        grad_down,
        clip_factor,
    )


MESH = pl.DeviceIdType.MESH


def place():
    dp = lax.axis_index("dp")
    ep = lax.axis_index("ep")
    z, y = dp // 2, dp % 2
    x, c = ep // 2, ep % 2
    first = (1 - c) * y + c * x
    second = (1 - c) * x + c * y
    return dp, ep, z, y, x, c, first, second


def targets(dp, ep, z, y, x, c, nz):
    up = (jnp.where(z < nz - 1, dp + 2, dp), ep)
    down = (jnp.where(z > 0, dp - 2, dp), ep)
    turn_y, turn_x = 1 - 2 * y, 2 - 4 * x
    near = (dp + (1 - c) * turn_y, ep + c * turn_x)
    far = (dp + c * turn_y, ep + (1 - c) * turn_x)
    twin = (dp, ep + 1 - 2 * c)
    return up, down, near, far, twin


def slot(z, first, second, c):
    return z * 8 + first * (4 - 2 * c) + second * (2 + 2 * c) + c


def greet(nz, z, up, down, near, far, twin):
    barrier = pltpu.get_barrier_semaphore()

    @pl.when(z < nz - 1)
    def _():
        pl.semaphore_signal(barrier, inc=1, device_id=up, device_id_type=MESH)

    @pl.when(z > 0)
    def _():
        pl.semaphore_signal(barrier, inc=1, device_id=down, device_id_type=MESH)

    for other in (near, far, twin):
        pl.semaphore_signal(barrier, inc=1, device_id=other, device_id_type=MESH)
    peers = 3 + jnp.where(z < nz - 1, 1, 0) + jnp.where(z > 0, 1, 0)
    pl.semaphore_wait(barrier, peers)


def gather_kernel(nz, count, *refs):
    ins = refs[:count]
    outs = refs[count : 2 * count]
    send_sem, recv_sem, own_sem = refs[2 * count :]
    dp, ep, z, y, x, c, a, b = place()
    up, down, near, far, twin = targets(dp, ep, z, y, x, c, nz)
    ways = (up, down, near, far, twin)
    greet(nz, z, up, down, near, far, twin)
    mine = slot(z, a, b, c)
    pending = []

    def push(way, where, allowed=None, own=False):
        for k in range(count):
            copy = pltpu.make_async_remote_copy(
                src_ref=ins[k] if own else outs[k].at[where],
                dst_ref=outs[k].at[where],
                send_sem=send_sem.at[k, way, where],
                recv_sem=recv_sem.at[k, where],
                device_id=ways[way],
                device_id_type=MESH,
            )
            if allowed is None:
                copy.start()
            else:
                pl.when(allowed)(copy.start)
            pending.append((allowed, copy))

    def arrive(where):
        for k in range(count):
            pltpu.make_async_remote_copy(
                src_ref=outs[k].at[where],
                dst_ref=outs[k].at[where],
                send_sem=send_sem.at[k, 0, where],
                recv_sem=recv_sem.at[k, where],
                device_id=twin,
                device_id_type=MESH,
            ).wait_recv()

    own_copies = [pltpu.make_async_copy(ins[k], outs[k].at[mine], own_sem.at[k]) for k in range(count)]
    push(0, mine, z < nz - 1, True)
    push(1, mine, z > 0, True)
    push(2, mine, None, True)
    push(3, mine, None, True)
    push(4, mine, None, True)
    for copy in own_copies:
        copy.start()

    def along(step):
        if step == 0:
            yield None, z
        else:
            yield z >= step, jnp.maximum(z - step, 0)
            yield z + step < nz, jnp.minimum(z + step, nz - 1)

    def on(allowed, action):
        if allowed is None:
            action()
        else:
            pl.when(allowed)(action)

    for turn in range(1, nz + 2):
        if turn < nz:
            for index, (allowed, zz) in enumerate(along(turn)):
                where = slot(zz, a, b, c)
                on(allowed, functools.partial(arrive, where))
                if index == 0:
                    push(0, where, allowed & (z < nz - 1))
                else:
                    push(1, where, allowed & (z > 0))
                for way in (2, 3, 4):
                    push(way, where, allowed)
        if turn - 1 < nz:
            for allowed, zz in along(turn - 1):
                where = slot(zz, 1 - a, b, c)
                on(allowed, functools.partial(arrive, where))
                for way in (3, 4):
                    push(way, where, allowed)
            for allowed, zz in along(turn - 1):
                where = slot(zz, a, 1 - b, c)
                on(allowed, functools.partial(arrive, where))
                push(4, where, allowed)
        if turn >= 2:
            for allowed, zz in along(turn - 2):
                where = slot(zz, 1 - a, 1 - b, c)
                on(allowed, functools.partial(arrive, where))
                push(4, where, allowed)
    for zz in range(nz):
        for aa in range(2):
            for bb in range(2):
                arrive(slot(zz, aa, bb, 1 - c))
    for allowed, copy in pending:
        on(allowed, copy.wait_send)
    for copy in own_copies:
        copy.wait()


def gather_rows(arrays, devices, ident):
    count = len(arrays)
    nz = devices // 8
    return pl.pallas_call(
        functools.partial(gather_kernel, nz, count),
        out_shape=tuple(jax.ShapeDtypeStruct((devices,) + v.shape, v.dtype) for v in arrays),
        in_specs=[pl.BlockSpec(memory_space=pltpu.VMEM)] * count,
        out_specs=tuple(pl.BlockSpec(memory_space=pl.ANY) for v in arrays),
        scratch_shapes=[
            pltpu.SemaphoreType.DMA((count, 5, devices)),
            pltpu.SemaphoreType.DMA((count, devices)),
            pltpu.SemaphoreType.DMA((count,)),
        ],
        compiler_params=pltpu.CompilerParams(collective_id=ident, has_side_effects=True),
        name="gather_rows_%d" % ident,
    )(*arrays)


def scatter_kernel(nz, left_ref, right_ref, out_ref, sent, got, from_far, from_near, rising, falling,
                   twin_send, twin_recv, far_send, far_recv, near_send, near_recv, line_send, up_recv, down_recv):
    dp, ep, z, y, x, c, a, b = place()
    up, down, near, far, twin = targets(dp, ep, z, y, x, c, nz)
    greet(nz, z, up, down, near, far, twin)
    per = 4 * nz

    def zed(step):
        if nz == 4:
            far_one = jnp.where(z < 2, 3, 0)
            second = jnp.where(z < 2, 2 - 2 * z, 7 - 2 * z)
            third = 1 + z % 2
            return jnp.where(step == 0, far_one, jnp.where(step == 1, second, jnp.where(step == 2, third, z)))
        return (z + 1 + step) % nz

    def term(where):
        return jnp.dot(left_ref[where], right_ref[...], preferred_element_type=jnp.float32)

    def order(index, aa, bb, cc):
        part = index // nz
        flip_b = 1 - part // 2
        flip_a = 1 - part % 2
        return slot(zed(index % nz), aa + flip_a * (1 - 2 * aa), bb + flip_b * (1 - 2 * bb), cc)

    def twin_copy(index):
        return pltpu.make_async_remote_copy(
            src_ref=sent.at[index], dst_ref=got.at[index], send_sem=twin_send.at[index],
            recv_sem=twin_recv.at[index], device_id=twin, device_id_type=MESH)

    def far_copy(index):
        return pltpu.make_async_remote_copy(
            src_ref=got.at[index], dst_ref=from_far.at[index], send_sem=far_send.at[index],
            recv_sem=far_recv.at[index], device_id=far, device_id_type=MESH)

    def near_copy(index):
        return pltpu.make_async_remote_copy(
            src_ref=got.at[2 * nz + index], dst_ref=from_near.at[index], send_sem=near_send.at[index],
            recv_sem=near_recv.at[index], device_id=near, device_id_type=MESH)

    def up_copy(index, zz):
        return pltpu.make_async_remote_copy(
            src_ref=got.at[3 * nz + index], dst_ref=rising.at[zz], send_sem=line_send.at[index],
            recv_sem=up_recv.at[zz], device_id=up, device_id_type=MESH)

    def down_copy(index, zz):
        return pltpu.make_async_remote_copy(
            src_ref=got.at[3 * nz + index], dst_ref=falling.at[zz], send_sem=line_send.at[index],
            recv_sem=down_recv.at[zz], device_id=down, device_id_type=MESH)

    def give(index):
        sent[index] = term(order(index, b, a, 1 - c)).astype(sent.dtype)
        twin_copy(index).start()

    def taken(index):
        value = term(order(index, a, b, c))
        twin_copy(index).wait_recv()
        return value + got[index].astype(jnp.float32)

    def far_step(step, carry):
        give(2 * step)
        give(2 * step + 1)
        got[step] = taken(step).astype(got.dtype)
        far_copy(step).start()
        return carry

    lax.fori_loop(0, 2 * nz, far_step, 0)

    def near_step(step, carry):
        value = taken(2 * nz + step)
        far_copy(step).wait_recv()
        value = value + from_far[step].astype(jnp.float32)
        got[2 * nz + step] = value.astype(got.dtype)
        near_copy(step).start()
        return carry

    lax.fori_loop(0, nz, near_step, 0)

    def line_step(step, carry):
        zz = zed(step)
        value = taken(3 * nz + step)
        far_copy(nz + step).wait_recv()
        near_copy(step).wait_recv()
        out_ref[...] = value + from_far[nz + step].astype(jnp.float32) + from_near[step].astype(jnp.float32)

        @pl.when((zz >= z) & (z > 0))
        def _():
            up_copy(step, zz).wait_recv()
            out_ref[...] += rising[zz].astype(jnp.float32)

        @pl.when((zz <= z) & (z < nz - 1))
        def _():
            down_copy(step, zz).wait_recv()
            out_ref[...] += falling[zz].astype(jnp.float32)

        @pl.when(zz > z)
        def _():
            got[3 * nz + step] = out_ref[...].astype(got.dtype)
            up_copy(step, zz).start()

        @pl.when(zz < z)
        def _():
            got[3 * nz + step] = out_ref[...].astype(got.dtype)
            down_copy(step, zz).start()

        return carry

    lax.fori_loop(0, nz, line_step, 0)

    def finish(step, carry):
        twin_copy(step).wait_send()
        return carry

    lax.fori_loop(0, per, finish, 0)

    def finish_far(step, carry):
        far_copy(step).wait_send()
        return carry

    lax.fori_loop(0, 2 * nz, finish_far, 0)

    def finish_near(step, carry):
        near_copy(step).wait_send()

        @pl.when(step < nz - 1)
        def _():
            up_copy(step, 0).wait_send()

        return carry

    lax.fori_loop(0, nz, finish_near, 0)


def scatter_sum(left, right, devices, ident):
    nz = devices // 8
    rows = left.shape[0] // devices
    depth, wide = right.shape
    block = (rows, wide)
    low = jnp.bfloat16
    dma = pltpu.SemaphoreType.DMA
    return pl.pallas_call(
        functools.partial(scatter_kernel, nz),
        out_shape=jax.ShapeDtypeStruct(block, jnp.float32),
        in_specs=[pl.BlockSpec(memory_space=pltpu.VMEM)] * 2,
        out_specs=pl.BlockSpec(memory_space=pltpu.VMEM),
        scratch_shapes=[
            pltpu.VMEM((4 * nz,) + block, low),
            pltpu.VMEM((4 * nz,) + block, low),
            pltpu.VMEM((2 * nz,) + block, low),
            pltpu.VMEM((nz,) + block, low),
            pltpu.VMEM((nz,) + block, low),
            pltpu.VMEM((nz,) + block, low),
            dma((4 * nz,)), dma((4 * nz,)), dma((2 * nz,)), dma((2 * nz,)),
            dma((nz,)), dma((nz,)), dma((nz,)), dma((nz,)), dma((nz,)),
        ],
        compiler_params=pltpu.CompilerParams(
            collective_id=ident, has_side_effects=True, vmem_limit_bytes=58 * 2**20),
        name="scatter_sum_%d" % ident,
    )(left.reshape(devices, rows, depth), right)


def whole_rows(mesh):
    return mesh.shape["ep"] == 4 and mesh.shape["dp"] % 2 == 0 and mesh.shape["dp"] <= 8


def exact_dot(left_side, right_side):
    return jnp.dot(
        left_side, right_side, precision=lax.Precision.HIGHEST, preferred_element_type=jnp.float32
    )


def block_layout(lens, tok_count):
    ends = [lens[:, :1]]
    for at in range(1, lens.shape[1]):
        ends.append(ends[-1] + lens[:, at : at + 1])
    row_index = lax.broadcasted_iota(jnp.int32, (lens.shape[0], tok_count), 1)
    segment = jnp.zeros_like(row_index)
    first_row = jnp.zeros_like(row_index)
    for end in ends:
        passed = row_index >= end
        segment = segment + passed.astype(jnp.int32)
        first_row = jnp.where(passed, end, first_row)
    return (segment, row_index - first_row, segment < lens.shape[1])


def by_experts(
    hidden_in,
    cotangent,
    deal_order,
    seq_lengths,
    expert_ids,
    w_query,
    w_key,
    w_value,
    w_out,
    w_router,
    gain_attn,
    gain_moe,
    gain_query,
    gain_key,
    w_gate,
    w_up,
    w_down,
    clip_threshold,
):
    f32, low = jnp.float32, jnp.bfloat16
    everyone = ("dp", "ep")
    dp_count, ep_count = lax.axis_size("dp"), lax.axis_size("ep")
    devices = dp_count * ep_count
    dp, ep = lax.axis_index("dp"), lax.axis_index("ep")
    me = dp * ep_count + ep
    tok_count, width = hidden_in.shape
    all_count = devices * tok_count
    head_dim = gain_query.shape[0]
    half_dim = head_dim // 2
    rows_own = w_query.shape[0]
    head_count = w_query.shape[1] // head_dim
    kv_count = w_key.shape[1] // head_dim
    group_size = head_count // kv_count
    experts = w_router.shape[1]
    exp_local, wide_own, hidden = w_gate.shape
    parts = dp_count // exp_local
    piece = hidden // parts
    score_scale = head_dim ** (-0.5)

    gain_col = gain_attn.astype(f32)[:, None]
    heads_in = (w_query.astype(f32) * gain_col).astype(low).reshape(rows_own, head_count, head_dim)
    keys_in = (w_key.astype(f32) * gain_col).astype(low).reshape(rows_own, kv_count, head_dim)
    values_in = (w_value.astype(f32) * gain_col).astype(low).reshape(rows_own, kv_count, head_dim)
    sent_heads = jnp.concatenate(
        [heads_in, jnp.repeat(keys_in, group_size, axis=1), jnp.repeat(values_in, group_size, axis=1)],
        axis=2,
    ).transpose(1, 0, 2)
    w_heads = lax.all_to_all(sent_heads, everyone, 0, 0, tiled=True).reshape(width, 3 * head_dim)

    def by_part(weights):
        return weights.reshape(exp_local, wide_own, parts, piece).transpose(0, 2, 1, 3)

    sent_rise = jnp.concatenate([by_part(w_gate), by_part(w_up)], axis=3).reshape(
        dp_count, wide_own, 2 * piece
    )
    w_rise = lax.all_to_all(sent_rise, "dp", 0, 0, tiled=True).reshape(width, 2 * piece)
    w_fall = lax.all_to_all(w_down.reshape(dp_count, piece, wide_own), "dp", 0, 0, tiled=True)
    w_fall = w_fall.transpose(1, 0, 2).reshape(piece, width)

    local_order = deal_order % tok_count
    deal = (local_order[:, None] == jnp.arange(tok_count, dtype=jnp.int32)[None, :]).astype(low)
    resid_in = jnp.dot(deal, hidden_in, preferred_element_type=f32)
    own_segment, own_position, own_valid = block_layout(seq_lengths, tok_count)
    valid_col = own_valid[0].astype(f32)[:, None]
    grad_mid_out = jnp.dot(deal, cotangent, preferred_element_type=f32) * valid_col
    inv_one = rms_scale(resid_in)
    unit_one = resid_in * inv_one
    lens_row = jnp.pad(seq_lengths.astype(f32), ((0, 0), (0, 128 - seq_lengths.shape[1])))
    gain_row = jnp.pad(gain_moe.astype(f32)[None, :], ((0, 0), (0, 128 - rows_own)))
    router_rows = w_router.astype(f32).reshape(-1, 128)
    note_one = jnp.concatenate([lens_row, gain_row, router_rows], axis=0)
    note_one = jnp.pad(note_one, ((0, -note_one.shape[0] % 8), (0, 0)))
    unit_all, grad_all, notes = gather_rows(
        (unit_one.astype(low), grad_mid_out.astype(low), note_one), devices, 1
    )
    lens_all = notes[:, 0, : seq_lengths.shape[1]].astype(jnp.int32)
    gain_two = notes[:, 1, :rows_own].reshape(1, width)
    router_full = notes[:, 2 : 2 + router_rows.shape[0]].reshape(width, experts)

    segment, position, valid_row = block_layout(lens_all, tok_count)
    step_down = lax.broadcasted_iota(jnp.int32, (1, tok_count, tok_count), 1)
    step_across = lax.broadcasted_iota(jnp.int32, (1, tok_count, tok_count), 2)
    allowed = (segment[:, :, None] == segment[:, None, :]) & (step_across <= step_down)
    cosine_rows, sine_rows = rotary_tables(jnp.arange(tok_count, dtype=jnp.int32), head_dim)
    place_hot = (position.reshape(-1)[:, None] == jnp.arange(tok_count)[None, :]).astype(f32)
    cosine_all = exact_dot(place_hot, cosine_rows).reshape(devices, tok_count, head_dim)
    sine_all = exact_dot(place_hot, sine_rows).reshape(devices, tok_count, head_dim)
    flat_unit = unit_all.reshape(all_count, width)
    projected = jnp.dot(flat_unit, w_heads, preferred_element_type=f32).reshape(
        devices, tok_count, 3 * head_dim
    )
    query_raw = projected[..., :head_dim]
    key_raw = projected[..., head_dim : 2 * head_dim]
    value_rows = projected[..., 2 * head_dim :].astype(low)
    gain_query_f = gain_query.astype(f32)
    gain_key_f = gain_key.astype(f32)
    inv_query = rms_scale(query_raw)
    unit_query = query_raw * inv_query
    query_rot = rotate(unit_query * gain_query_f, cosine_all, sine_all).astype(low)
    inv_key = rms_scale(key_raw)
    unit_key = key_raw * inv_key
    key_rot = rotate(unit_key * gain_key_f, cosine_all, sine_all).astype(low)
    scores = contract(query_rot, key_rot, "btd,bud->btu") * score_scale
    masked = jnp.where(allowed, scores, masked_fill)
    row_top = jnp.max(masked, axis=-1, keepdims=True)
    exponent = jnp.exp(masked - row_top)
    probs = exponent / jnp.sum(exponent, axis=-1, keepdims=True)
    probs_low = probs.astype(low)
    mixed = contract(probs_low, value_rows, "btu,bud->btd").astype(low).reshape(all_count, head_dim)
    largest_own = jnp.max(jnp.where(valid_row[:, :, None], row_top, masked_fill))
    resid_mid = resid_in + scatter_sum(mixed, w_out, devices, 2)

    inv_two = rms_scale(resid_mid)
    unit_two = resid_mid * inv_two
    normed_mid = (unit_two * gain_two).astype(low)
    logits = jnp.dot(normed_mid, router_full.astype(low), preferred_element_type=f32)
    choose = (expert_ids[:, :, None] == jnp.arange(experts, dtype=jnp.int32)[None, None, :]).any(axis=1)
    picked = jnp.where(choose, logits, masked_fill)
    gate_power = jnp.where(choose, jnp.exp(picked - jnp.max(picked, axis=1, keepdims=True)), 0.0)
    route = gate_power / jnp.sum(gate_power, axis=1, keepdims=True)
    note_two = jnp.concatenate([route.T, jnp.full((8, tok_count), largest_own, f32)], axis=0)
    normed_all, notes = gather_rows((normed_mid, note_two), devices, 3)
    clip_factor = jnp.sqrt(clip_threshold / jnp.maximum(notes[:, experts, 0], clip_threshold))

    mine = ep * exp_local + dp // parts
    weight = lax.dynamic_slice_in_dim(notes, mine, 1, axis=1).reshape(all_count, 1)
    flat_mid = normed_all.reshape(all_count, width)
    flat_grad = grad_all.reshape(all_count, width)
    risen = jnp.dot(flat_mid, w_rise, preferred_element_type=f32)
    gate_part, up_part = risen[:, :piece], risen[:, piece:]
    grad_plain = contract(flat_grad, w_fall, "td,fd->tf")
    sigmoid_gate = jax.nn.sigmoid(gate_part)
    silu_gate = gate_part * sigmoid_gate
    hidden_mid = silu_gate * up_part
    grad_route = jnp.sum(hidden_mid * grad_plain, axis=1, keepdims=True)
    weighted_mid = (hidden_mid * weight).astype(low)
    grad_hidden = grad_plain * weight
    grad_gate_part = (
        grad_hidden * up_part * sigmoid_gate * (1.0 + gate_part * (1.0 - sigmoid_gate))
    ).astype(low)
    grad_up_part = (grad_hidden * silu_gate).astype(low)
    route_high = grad_route.astype(low)
    route_rest = (grad_route - route_high.astype(f32)).astype(low)
    both = jnp.concatenate([grad_gate_part, grad_up_part], axis=1)
    lane = lax.broadcasted_iota(jnp.int32, (1, 128), 1)
    tail = jnp.where(lane == 0, route_high, jnp.where(lane == 1, route_rest, jnp.zeros((), low)))
    left = jnp.concatenate([both, tail], axis=1)
    spot = lax.broadcasted_iota(jnp.int32, (128, 128), 0)
    across = lax.broadcasted_iota(jnp.int32, (128, 128), 1)
    spread = ((spot < 2) & (across == mine)).astype(low)
    right = jnp.concatenate(
        [
            jnp.concatenate([w_rise.T, jnp.zeros((2 * piece, 128), low)], axis=1),
            jnp.concatenate([jnp.zeros((128, width), low), spread], axis=1),
        ],
        axis=0,
    )
    summed = scatter_sum(left, right, devices, 4)
    grad_rise_w = contract(flat_mid, both, "td,tf->df").astype(low)
    grad_fall_w = contract(weighted_mid, flat_grad, "tf,td->fd").astype(low)
    back_rise = lax.all_to_all(
        grad_rise_w.reshape(dp_count, wide_own, 2 * piece), "dp", 0, 0, tiled=True
    )
    back_fall = lax.all_to_all(
        grad_fall_w.reshape(piece, dp_count, wide_own).transpose(1, 0, 2), "dp", 0, 0, tiled=True
    )
    resid_out = resid_mid + scatter_sum(weighted_mid, w_fall, devices, 5)
    undeal = (jnp.arange(tok_count, dtype=jnp.int32)[:, None] == local_order[None, :]).astype(low)
    block_out = jnp.dot(
        undeal, (resid_out * valid_col).astype(low), preferred_element_type=f32
    ).astype(low)

    def from_part(grads):
        grads = grads.reshape(exp_local, parts, wide_own, piece).transpose(0, 2, 1, 3)
        return grads.reshape(exp_local, wide_own, hidden).astype(f32)

    grad_gate = from_part(back_rise[..., :piece])
    grad_up = from_part(back_rise[..., piece:])
    grad_down = back_fall.reshape(exp_local, hidden, wide_own).astype(f32)

    grad_gates = summed[:, width : width + experts]
    mean_term = jnp.sum(route * grad_gates, axis=1, keepdims=True)
    grad_logits = (route * (grad_gates - mean_term)).astype(low)
    grad_normed_mid = summed[:, :width] + contract(grad_logits, router_full.astype(low), "te,de->td")
    gain_part = jnp.sum(grad_normed_mid * unit_two, axis=0)
    grad_mid = grad_mid_out + norm_back(grad_normed_mid * gain_two, unit_two, inv_two)
    grad_branch = grad_mid.astype(low)
    note_three = jnp.concatenate([grad_logits.T.astype(f32), gain_part.reshape(-1, 128)], axis=0)
    branch_all, notes = gather_rows((grad_branch, note_three), devices, 6)
    logits_all = notes[:, :experts].astype(low)
    normed_own = lax.dynamic_slice_in_dim(normed_all, me * rows_own, rows_own, axis=2)
    grad_router = contract(normed_own, logits_all, "btd,bet->de")
    gain_sum = jnp.sum(notes[:, experts:], axis=0).reshape(-1)
    grad_gain_moe = lax.dynamic_slice_in_dim(gain_sum, me * rows_own, rows_own)

    flat_branch = branch_all.reshape(all_count, width)
    grad_out = contract(mixed, flat_branch, "tq,td->qd")
    grad_mixed = (
        contract(flat_branch, w_out, "td,qd->tq").astype(low).reshape(devices, tok_count, head_dim)
    )
    grad_value = contract(probs_low, grad_mixed, "btu,btd->bud").astype(low)
    grad_probs = contract(grad_mixed, value_rows, "btd,bud->btu")
    grad_scores = (
        probs * (grad_probs - jnp.sum(probs * grad_probs, axis=-1, keepdims=True))
    ).astype(low)
    grad_query_rot = contract(grad_scores, key_rot, "btu,bud->btd") * score_scale
    grad_key_rot = contract(grad_scores, query_rot, "btu,btd->bud") * score_scale
    grad_query_normed = rotate_back(grad_query_rot, cosine_all, sine_all)
    grad_key_normed = rotate_back(grad_key_rot, cosine_all, sine_all)
    gain_pair = jnp.stack(
        [
            jnp.sum(grad_query_normed * unit_query, axis=(0, 1)),
            jnp.sum(grad_key_normed * unit_key, axis=(0, 1)),
        ]
    )
    grad_query_raw = norm_back(grad_query_normed * gain_query_f, unit_query, inv_query).astype(low)
    grad_key_raw = norm_back(grad_key_normed * gain_key_f, unit_key, inv_key).astype(low)
    grad_heads = jnp.concatenate([grad_query_raw, grad_key_raw, grad_value], axis=2).reshape(
        all_count, 3 * head_dim
    )
    grad_heads_w = contract(flat_unit, grad_heads, "td,tq->dq").astype(low)
    back_heads = lax.all_to_all(
        grad_heads_w.reshape(devices, rows_own, 3 * head_dim), everyone, 0, 0, tiled=True
    ).astype(f32)
    grad_unit_one = scatter_sum(grad_heads, w_heads.T, devices, 7)
    (gain_pairs,) = gather_rows((jnp.pad(gain_pair, ((0, 6), (0, 0))),), devices, 8)
    gain_pair = jnp.sum(gain_pairs, axis=0)
    plain_query = back_heads[..., :head_dim].transpose(1, 0, 2).reshape(rows_own, -1)

    def of_group(grads):
        grads = jnp.sum(grads.reshape(kv_count, group_size, rows_own, head_dim), axis=1)
        return grads.transpose(1, 0, 2).reshape(rows_own, -1)

    plain_key = of_group(back_heads[..., head_dim : 2 * head_dim])
    plain_value = of_group(back_heads[..., 2 * head_dim :])
    grad_gain_attn = (
        jnp.sum(plain_query * w_query.astype(f32), axis=1)
        + jnp.sum(plain_key * w_key.astype(f32), axis=1)
        + jnp.sum(plain_value * w_value.astype(f32), axis=1)
    )
    grad_resid_in = grad_mid + norm_back(grad_unit_one, unit_one, inv_one)
    grad_input = exact_dot(undeal.astype(f32), grad_resid_in)
    return (
        block_out,
        grad_input,
        plain_query * gain_col,
        plain_key * gain_col,
        plain_value * gain_col,
        grad_out,
        grad_router,
        grad_gain_attn,
        grad_gain_moe,
        gain_pair[0],
        gain_pair[1],
        grad_gate,
        grad_up,
        grad_down,
        clip_factor,
    )


def solution(mesh):
    placed = (
        P(("dp", "ep"), None),
        P(("dp", "ep"), None),
        P(("dp", "ep")),
        P(("dp", "ep"), None),
        P(("dp", "ep"), None),
        P(("dp", "ep"), None),
        P(("dp", "ep"), None),
        P(("dp", "ep"), None),
        P(("dp", "ep"), None),
        P(("dp", "ep"), None),
        P(("dp", "ep")),
        P(("dp", "ep")),
        P(),
        P(),
        P("ep", "dp", None),
        P("ep", "dp", None),
        P("ep", None, "dp"),
        P(),
    )
    return jax.shard_map(
        per_device if not whole_rows(mesh) else by_experts,
        mesh=mesh,
        in_specs=placed,
        out_specs=(
            P(("dp", "ep"), None),
            P(("dp", "ep"), None),
            P(("dp", "ep"), None),
            P(("dp", "ep"), None),
            P(("dp", "ep"), None),
            P(("dp", "ep"), None),
            P(("dp", "ep"), None),
            P(("dp", "ep")),
            P(("dp", "ep")),
            P(),
            P(),
            P("ep", "dp", None),
            P("ep", "dp", None),
            P("ep", None, "dp"),
            P(),
        ),
        check_vma=False,
    )
```

```python
import functools

import jax
import jax.numpy as jnp
from jax import lax
from jax.experimental import pallas as pl
from jax.experimental.pallas import tpu as pltpu
from jax.sharding import PartitionSpec as P

epsilon = 1e-06
theta_base = 1000000.0
masked_fill = -1e30


def rms_scale(values):
    return lax.rsqrt(jnp.mean(values * values, axis=-1, keepdims=True) + epsilon)


def rotate_half(values):
    half_dim = values.shape[-1] // 2
    return jnp.concatenate([-values[..., half_dim:], values[..., :half_dim]], axis=-1)


def rotate(values, cosine_table, sine_table):
    return values * cosine_table + rotate_half(values) * sine_table


def rotate_back(values, cosine_table, sine_table):
    scaled = values * sine_table
    half_dim = values.shape[-1] // 2
    turned = jnp.concatenate([scaled[..., half_dim:], -scaled[..., :half_dim]], axis=-1)
    return values * cosine_table + turned


def norm_back(grad_unit, unit_rows, inv_root):
    return inv_root * (
        grad_unit - unit_rows * jnp.mean(grad_unit * unit_rows, axis=-1, keepdims=True)
    )


def contract(left_side, right_side, pattern):
    return jnp.einsum(pattern, left_side, right_side, preferred_element_type=jnp.float32)


def layout(lens_row, tok_count):
    seq_ends = jnp.cumsum(lens_row)
    row_index = jnp.arange(tok_count, dtype=jnp.int32)
    segment = jnp.sum((row_index[:, None] >= seq_ends[None, :]).astype(jnp.int32), axis=1)
    starts_all = jnp.concatenate([jnp.zeros((1,), jnp.int32), seq_ends])
    seg_hot = segment[:, None] == jnp.arange(starts_all.shape[0], dtype=jnp.int32)[None, :]
    first_row = jnp.sum(jnp.where(seg_hot, starts_all[None, :], 0), axis=1)
    position = row_index - first_row
    valid_row = segment < lens_row.shape[0]
    allowed = (segment[:, None] == segment[None, :]) & (row_index[None, :] <= row_index[:, None])
    return (position, valid_row, allowed)


def rotary_tables(position, head_dim):
    half_dim = head_dim // 2
    frequency = theta_base ** (-(jnp.arange(half_dim, dtype=jnp.float32) * 2.0) / head_dim)
    angles = position.astype(jnp.float32)[:, None] * frequency[None, :]
    angles = jnp.concatenate([angles, angles], axis=-1)
    return (jnp.cos(angles), jnp.sin(angles))


def per_device(
    hidden_in,
    cotangent,
    deal_order,
    seq_lengths,
    expert_ids,
    w_query,
    w_key,
    w_value,
    w_out,
    w_router,
    gain_attn,
    gain_moe,
    gain_query,
    gain_key,
    w_gate,
    w_up,
    w_down,
    clip_threshold,
):
    tok_count = hidden_in.shape[0]
    model_width = hidden_in.shape[1]
    head_dim = gain_query.shape[0]
    local_order = deal_order % tok_count
    position, valid_row, allowed = layout(seq_lengths[0], tok_count)
    valid_col = valid_row.astype(jnp.float32)[:, None]
    cosine_table, sine_table = rotary_tables(position, head_dim)
    cosine_query = cosine_table[:, None, None, :]
    sine_query = sine_table[:, None, None, :]
    cosine_key = cosine_table[:, None, :]
    sine_key = sine_table[:, None, :]
    attn_params = (
        lax.all_gather(w_query, ("dp", "ep"), axis=0, tiled=True),
        lax.all_gather(w_key, ("dp", "ep"), axis=0, tiled=True),
        lax.all_gather(w_value, ("dp", "ep"), axis=0, tiled=True),
        lax.all_gather(w_out, ("dp", "ep"), axis=0, tiled=True),
        lax.all_gather(w_router, ("dp", "ep"), axis=0, tiled=True),
        lax.all_gather(gain_attn, ("dp", "ep"), axis=0, tiled=True),
        lax.all_gather(gain_moe, ("dp", "ep"), axis=0, tiled=True),
    )
    expert_params = (
        lax.all_gather(w_gate, "dp", axis=1, tiled=True),
        lax.all_gather(w_up, "dp", axis=1, tiled=True),
        lax.all_gather(w_down, "dp", axis=2, tiled=True),
    )
    query_full, key_full, value_full, out_full, router_full, gain_attn_full, gain_moe_full = (
        attn_params
    )
    gate_full, up_full, down_full = expert_params
    head_count = query_full.shape[1] // head_dim
    kv_count = key_full.shape[1] // head_dim
    group_size = head_count // kv_count
    experts = router_full.shape[1]
    top_count = expert_ids.shape[1]
    exp_local = w_gate.shape[0]
    ep_count = lax.axis_size("ep")
    capacity = (tok_count * top_count * 5 + 4 * experts - 1) // (4 * experts)
    score_scale = head_dim ** (-0.5)
    resid_in = hidden_in[local_order].astype(jnp.float32)
    inv_one = rms_scale(resid_in)
    unit_one = resid_in * inv_one
    gain_one = gain_attn_full.astype(jnp.float32)
    normed_in = (unit_one * gain_one).astype(jnp.bfloat16)
    query_raw = jnp.dot(normed_in, query_full, preferred_element_type=jnp.float32).reshape(
        tok_count, kv_count, group_size, head_dim
    )
    key_raw = jnp.dot(normed_in, key_full, preferred_element_type=jnp.float32).reshape(
        tok_count, kv_count, head_dim
    )
    value_rows = (
        jnp.dot(normed_in, value_full, preferred_element_type=jnp.float32)
        .astype(jnp.bfloat16)
        .reshape(tok_count, kv_count, head_dim)
    )
    inv_query = rms_scale(query_raw)
    unit_query = query_raw * inv_query
    gain_query_f = gain_query.astype(jnp.float32)
    query_rot = rotate(unit_query * gain_query_f, cosine_query, sine_query).astype(jnp.bfloat16)
    inv_key = rms_scale(key_raw)
    unit_key = key_raw * inv_key
    gain_key_f = gain_key.astype(jnp.float32)
    key_rot = rotate(unit_key * gain_key_f, cosine_key, sine_key).astype(jnp.bfloat16)
    scores = contract(query_rot, key_rot, "tkgd,ukd->kgtu") * score_scale
    masked = jnp.where(allowed, scores, masked_fill)
    row_top = jnp.max(masked, axis=-1, keepdims=True)
    exponent = jnp.exp(masked - row_top)
    row_total = jnp.sum(exponent, axis=-1, keepdims=True)
    log_total = row_top + jnp.log(row_total)
    probs_low = (exponent / row_total).astype(jnp.bfloat16)
    mixed_heads = (
        contract(probs_low, value_rows, "kgtu,ukd->tkgd")
        .astype(jnp.bfloat16)
        .reshape(tok_count, head_count * head_dim)
    )
    resid_mid = resid_in + jnp.dot(mixed_heads, out_full, preferred_element_type=jnp.float32)
    largest_local = jnp.max(
        jnp.where(allowed & valid_row[:, None], scores, masked_fill), axis=(2, 3)
    ).reshape(head_count)
    largest = lax.pmax(largest_local, ("dp", "ep"))
    clip_factor = jnp.sqrt(clip_threshold / jnp.maximum(largest, clip_threshold))
    inv_two = rms_scale(resid_mid)
    unit_two = resid_mid * inv_two
    gain_two = gain_moe_full.astype(jnp.float32)
    normed_mid = (unit_two * gain_two).astype(jnp.bfloat16)
    logits = jnp.dot(normed_mid, router_full, preferred_element_type=jnp.float32)
    choose = expert_ids[:, :, None] == jnp.arange(experts, dtype=jnp.int32)[None, None, :]
    picked = jnp.sum(jnp.where(choose, logits[:, None, :], 0.0), axis=2)
    gate_weights = jax.nn.softmax(picked, axis=-1)
    flat_ids = expert_ids.reshape(-1)
    flat_hot = (flat_ids[:, None] == jnp.arange(experts, dtype=jnp.int32)[None, :]).astype(
        jnp.int32
    )
    slot_rank = jnp.sum((jnp.cumsum(flat_hot, axis=0) - 1) * flat_hot, axis=1)
    slot_index = flat_ids * capacity + slot_rank
    pair_token = jnp.arange(tok_count * top_count, dtype=jnp.int32) // top_count
    send_rows = (
        jnp.zeros((experts * capacity, model_width), jnp.bfloat16)
        .at[slot_index]
        .set(normed_mid[pair_token])
    )
    send_rows = send_rows.reshape(ep_count, exp_local, capacity, model_width)
    arrived = lax.all_to_all(send_rows, "ep", split_axis=0, concat_axis=0, tiled=True)
    gate_part = contract(arrived, gate_full, "secd,edf->secf")
    up_part = contract(arrived, up_full, "secd,edf->secf")
    hidden_mid = (jax.nn.silu(gate_part) * up_part).astype(jnp.bfloat16)
    produced = contract(hidden_mid, down_full, "secf,efd->secd").astype(jnp.bfloat16)
    returned = lax.all_to_all(produced, "ep", split_axis=0, concat_axis=0, tiled=True)
    returned, arrived, gate_part, up_part = (returned, arrived, gate_part, up_part)
    pair_out = (
        returned.reshape(experts * capacity, model_width)[slot_index]
        .reshape(tok_count, top_count, model_width)
        .astype(jnp.float32)
    )
    resid_out = resid_mid + jnp.sum(gate_weights[:, :, None] * pair_out, axis=1)
    out_rows = (resid_out * valid_col).astype(jnp.bfloat16)
    block_out = jnp.zeros_like(out_rows).at[local_order].set(out_rows)
    attn_params = (
        lax.all_gather(w_query, ("dp", "ep"), axis=0, tiled=True),
        lax.all_gather(w_key, ("dp", "ep"), axis=0, tiled=True),
        lax.all_gather(w_value, ("dp", "ep"), axis=0, tiled=True),
        lax.all_gather(w_out, ("dp", "ep"), axis=0, tiled=True),
        lax.all_gather(w_router, ("dp", "ep"), axis=0, tiled=True),
        lax.all_gather(gain_attn, ("dp", "ep"), axis=0, tiled=True),
        lax.all_gather(gain_moe, ("dp", "ep"), axis=0, tiled=True),
    )
    expert_params = (
        lax.all_gather(w_gate, "dp", axis=1, tiled=True),
        lax.all_gather(w_up, "dp", axis=1, tiled=True),
        lax.all_gather(w_down, "dp", axis=2, tiled=True),
    )
    query_full, key_full, value_full, out_full, router_full, gain_attn_full, gain_moe_full = (
        attn_params
    )
    gate_full, up_full, down_full = expert_params
    grad_mid_out = cotangent[local_order].astype(jnp.float32) * valid_col
    grad_gates = jnp.sum(grad_mid_out[:, None, :] * pair_out, axis=2)
    grad_pair = (gate_weights[:, :, None] * grad_mid_out[:, None, :]).astype(jnp.bfloat16)
    send_grads = (
        jnp.zeros((experts * capacity, model_width), jnp.bfloat16)
        .at[slot_index]
        .set(grad_pair.reshape(-1, model_width))
    )
    send_grads = send_grads.reshape(ep_count, exp_local, capacity, model_width)
    grad_arrived = lax.all_to_all(send_grads, "ep", split_axis=0, concat_axis=0, tiled=True)
    grad_hidden = contract(grad_arrived, down_full, "secd,efd->secf")
    sigmoid_gate = jax.nn.sigmoid(gate_part)
    silu_gate = jax.nn.silu(gate_part)
    grad_gate_part = (
        grad_hidden * up_part * sigmoid_gate * (1.0 + gate_part * (1.0 - sigmoid_gate))
    ).astype(jnp.bfloat16)
    grad_up_part = (grad_hidden * silu_gate).astype(jnp.bfloat16)
    grad_rows = (
        contract(grad_gate_part, gate_full, "secf,edf->secd")
        + contract(grad_up_part, up_full, "secf,edf->secd")
    ).astype(jnp.bfloat16)
    grad_back = lax.all_to_all(grad_rows, "ep", split_axis=0, concat_axis=0, tiled=True)
    hidden_mid = (silu_gate * up_part).astype(jnp.bfloat16)
    grad_gate_w = contract(arrived, grad_gate_part, "secd,secf->edf")
    grad_up_w = contract(arrived, grad_up_part, "secd,secf->edf")
    grad_down_w = contract(hidden_mid, grad_arrived, "secf,secd->efd")
    grad_gate, grad_up, grad_down = (
        lax.psum_scatter(
            grad_gate_w.astype(jnp.bfloat16), "dp", scatter_dimension=1, tiled=True
        ).astype(jnp.float32),
        lax.psum_scatter(
            grad_up_w.astype(jnp.bfloat16), "dp", scatter_dimension=1, tiled=True
        ).astype(jnp.float32),
        lax.psum_scatter(
            grad_down_w.astype(jnp.bfloat16), "dp", scatter_dimension=2, tiled=True
        ).astype(jnp.float32),
    )
    mean_term = jnp.sum(gate_weights * grad_gates, axis=1, keepdims=True)
    grad_picked = gate_weights * (grad_gates - mean_term)
    grad_logits = jnp.sum(jnp.where(choose, grad_picked[:, :, None], 0.0), axis=1).astype(
        jnp.bfloat16
    )
    grad_router_w = contract(normed_mid, grad_logits, "td,te->de")
    pair_grads = (
        grad_back.reshape(experts * capacity, model_width)[slot_index]
        .reshape(tok_count, top_count, model_width)
        .astype(jnp.float32)
    )
    grad_normed_mid = jnp.sum(pair_grads, axis=1) + contract(grad_logits, router_full, "te,de->td")
    grad_gain_moe_w = jnp.sum(grad_normed_mid * unit_two, axis=0)
    grad_mid = grad_mid_out + norm_back(grad_normed_mid * gain_two, unit_two, inv_two)
    grad_branch = grad_mid.astype(jnp.bfloat16)
    grad_out_w = contract(mixed_heads, grad_branch, "tq,td->qd")
    grad_mixed = (
        contract(grad_branch, out_full, "td,qd->tq")
        .astype(jnp.bfloat16)
        .reshape(tok_count, kv_count, group_size, head_dim)
    )
    scores_again = contract(query_rot, key_rot, "tkgd,ukd->kgtu") * score_scale
    probs_back = jnp.exp(jnp.where(allowed, scores_again, masked_fill) - log_total)
    grad_value_rows = contract(
        probs_back.astype(jnp.bfloat16), grad_mixed, "kgtu,tkgd->ukd"
    ).astype(jnp.bfloat16)
    grad_probs = contract(grad_mixed, value_rows, "tkgd,ukd->kgtu")
    grad_scores = (
        probs_back * (grad_probs - jnp.sum(probs_back * grad_probs, axis=-1, keepdims=True))
    ).astype(jnp.bfloat16)
    grad_query_rot = contract(grad_scores, key_rot, "kgtu,ukd->tkgd") * score_scale
    grad_key_rot = contract(grad_scores, query_rot, "kgtu,tkgd->ukd") * score_scale
    grad_query_normed = rotate_back(grad_query_rot, cosine_query, sine_query)
    grad_key_normed = rotate_back(grad_key_rot, cosine_key, sine_key)
    grad_gain_q = jnp.sum(grad_query_normed * unit_query, axis=(0, 1, 2))
    grad_gain_k = jnp.sum(grad_key_normed * unit_key, axis=(0, 1))
    grad_query_raw = (
        norm_back(grad_query_normed * gain_query_f, unit_query, inv_query)
        .astype(jnp.bfloat16)
        .reshape(tok_count, head_count * head_dim)
    )
    grad_key_raw = (
        norm_back(grad_key_normed * gain_key_f, unit_key, inv_key)
        .astype(jnp.bfloat16)
        .reshape(tok_count, kv_count * head_dim)
    )
    grad_value_flat = grad_value_rows.reshape(tok_count, kv_count * head_dim)
    grad_query_w = contract(normed_in, grad_query_raw, "td,tq->dq")
    grad_key_w = contract(normed_in, grad_key_raw, "td,tq->dq")
    grad_value_w = contract(normed_in, grad_value_flat, "td,tq->dq")
    grad_normed_in = (
        contract(grad_query_raw, query_full, "tq,dq->td")
        + contract(grad_key_raw, key_full, "tq,dq->td")
        + contract(grad_value_flat, value_full, "tq,dq->td")
    )
    grad_gain_attn_w = jnp.sum(grad_normed_in * unit_one, axis=0)
    grad_resid_in = grad_mid + norm_back(grad_normed_in * gain_one, unit_one, inv_one)
    grad_input = jnp.zeros_like(grad_resid_in).at[local_order].set(grad_resid_in)
    grad_sums = (
        lax.psum_scatter(grad_query_w, ("dp", "ep"), scatter_dimension=0, tiled=True),
        lax.psum_scatter(grad_key_w, ("dp", "ep"), scatter_dimension=0, tiled=True),
        lax.psum_scatter(grad_value_w, ("dp", "ep"), scatter_dimension=0, tiled=True),
        lax.psum_scatter(grad_out_w, ("dp", "ep"), scatter_dimension=0, tiled=True),
        lax.psum_scatter(grad_router_w, ("dp", "ep"), scatter_dimension=0, tiled=True),
        lax.psum_scatter(grad_gain_attn_w, ("dp", "ep"), scatter_dimension=0, tiled=True),
        lax.psum_scatter(grad_gain_moe_w, ("dp", "ep"), scatter_dimension=0, tiled=True),
    )
    gain_sums = lax.psum((grad_gain_q, grad_gain_k), ("dp", "ep"))
    return (
        block_out,
        grad_input,
        grad_sums[0],
        grad_sums[1],
        grad_sums[2],
        grad_sums[3],
        grad_sums[4],
        grad_sums[5],
        grad_sums[6],
        gain_sums[0],
        gain_sums[1],
        grad_gate,
        grad_up,
        grad_down,
        clip_factor,
    )


MESH = pl.DeviceIdType.MESH


def place():
    dp = lax.axis_index("dp")
    ep = lax.axis_index("ep")
    z, y = dp // 2, dp % 2
    x, c = ep // 2, ep % 2
    first = (1 - c) * y + c * x
    second = (1 - c) * x + c * y
    return dp, ep, z, y, x, c, first, second


def targets(dp, ep, z, y, x, c, nz):
    up = (jnp.where(z < nz - 1, dp + 2, dp), ep)
    down = (jnp.where(z > 0, dp - 2, dp), ep)
    turn_y, turn_x = 1 - 2 * y, 2 - 4 * x
    near = (dp + (1 - c) * turn_y, ep + c * turn_x)
    far = (dp + c * turn_y, ep + (1 - c) * turn_x)
    twin = (dp, ep + 1 - 2 * c)
    return up, down, near, far, twin


def slot(z, first, second, c):
    return z * 8 + first * (4 - 2 * c) + second * (2 + 2 * c) + c


def greet(nz, z, dp, ep, ways, everyone):
    barrier = pltpu.get_barrier_semaphore()
    if everyone:
        total = nz * 8
        me = dp * 4 + ep

        def hello(step, carry):
            other = (me + step) % total
            pl.semaphore_signal(
                barrier, inc=1, device_id=(other // 4, other % 4), device_id_type=MESH
            )
            return carry

        lax.fori_loop(1, total, hello, 0)
        pl.semaphore_wait(barrier, total - 1)
        return
    up, down, near, far, twin = ways

    @pl.when(z < nz - 1)
    def _():
        pl.semaphore_signal(barrier, inc=1, device_id=up, device_id_type=MESH)

    @pl.when(z > 0)
    def _():
        pl.semaphore_signal(barrier, inc=1, device_id=down, device_id_type=MESH)

    for other in (near, far, twin):
        pl.semaphore_signal(barrier, inc=1, device_id=other, device_id_type=MESH)
    peers = 3 + jnp.where(z < nz - 1, 1, 0) + jnp.where(z > 0, 1, 0)
    pl.semaphore_wait(barrier, peers)


class Riders:
    def __init__(self, kinds, nz, dp, ep, refs):
        count = len(kinds)
        self.kinds, self.dp, self.ep = kinds, dp, ep
        self.ins, self.outs = refs[:count], refs[count : 2 * count]
        self.send, self.recv, self.own = refs[2 * count :] if count else (None, None, None)
        self.sizes = [2 * nz if kind == "dp" else 8 * nz for kind in kinds]
        self.at = [dp if kind == "dp" else dp * 4 + ep for kind in kinds]
        self.steps = [(r, k) for r in range(count) for k in range(1, self.sizes[r])]
        self.steps.sort(key=lambda step: step[1] / self.sizes[step[0]])

    def device(self, r, other):
        if self.kinds[r] == "dp":
            return (other, self.ep)
        return (other // 4, other % 4)

    def copy(self, r, step):
        other = (self.at[r] + step) % self.sizes[r]
        return pltpu.make_async_remote_copy(
            src_ref=self.ins[r] if self.kinds[r] == "same" else self.ins[r].at[other],
            dst_ref=self.outs[r].at[self.at[r]],
            send_sem=self.send.at[r, step],
            recv_sem=self.recv.at[r, self.at[r]],
            device_id=self.device(r, other),
            device_id_type=MESH,
        )

    def arrival(self, r, step):
        other = (self.at[r] + step) % self.sizes[r]
        return pltpu.make_async_remote_copy(
            src_ref=self.outs[r].at[other],
            dst_ref=self.outs[r].at[other],
            send_sem=self.send.at[r, step],
            recv_sem=self.recv.at[r, other],
            device_id=self.device(r, other),
            device_id_type=MESH,
        )

    def own_copy(self, r):
        here = self.ins[r] if self.kinds[r] == "same" else self.ins[r].at[self.at[r]]
        return pltpu.make_async_copy(here, self.outs[r].at[self.at[r]], self.own.at[r])

    def begin(self):
        for r in range(len(self.kinds)):
            self.own_copy(r).start()

    def some(self, share, shares):
        total = len(self.steps)
        for r, k in self.steps[total * share // shares : total * (share + 1) // shares]:
            self.copy(r, k).start()

    def looped(self, step, steps):
        for r in range(len(self.kinds)):
            per = -(-(self.sizes[r] - 1) // steps)
            for k in range(per):
                piece = 1 + step * per + k

                @pl.when(piece < self.sizes[r])
                def _():
                    self.copy(r, piece).start()

    def finish(self):
        for r in range(len(self.kinds)):

            def settle(step, carry):
                self.arrival(r, step).wait_recv()
                self.copy(r, step).wait_send()
                return carry

            lax.fori_loop(1, self.sizes[r], settle, 0)
            self.own_copy(r).wait()


def rider_shapes(riders, devices):
    kinds = tuple(kind for kind, _ in riders)
    arrays = tuple(array for _, array in riders)
    outs = tuple(
        jax.ShapeDtypeStruct(((devices,) + v.shape) if kind == "same" else v.shape, v.dtype)
        for kind, v in riders
    )
    dma = pltpu.SemaphoreType.DMA
    count = len(riders)
    sems = [dma((count, devices)), dma((count, devices)), dma((count,))] if count else []
    return kinds, arrays, outs, sems


def gather_kernel(nz, count, kinds, *refs):
    extra = len(kinds)
    ins = refs[:count]
    outs = refs[count + extra : 2 * count + extra]
    send_sem, recv_sem, own_sem = refs[2 * (count + extra) : 2 * (count + extra) + 3]
    dp, ep, z, y, x, c, a, b = place()
    ways = targets(dp, ep, z, y, x, c, nz)
    twin = ways[4]
    riders = Riders(
        kinds, nz, dp, ep,
        refs[count : count + extra]
        + refs[2 * count + extra : 2 * (count + extra)]
        + refs[2 * (count + extra) + 3 :],
    )
    greet(nz, z, dp, ep, ways, extra > 0)
    mine = slot(z, a, b, c)
    pending = []

    def push(way, where, allowed=None, own=False):
        for k in range(count):
            copy = pltpu.make_async_remote_copy(
                src_ref=ins[k] if own else outs[k].at[where],
                dst_ref=outs[k].at[where],
                send_sem=send_sem.at[k, way, where],
                recv_sem=recv_sem.at[k, where],
                device_id=ways[way],
                device_id_type=MESH,
            )
            if allowed is None:
                copy.start()
            else:
                pl.when(allowed)(copy.start)
            pending.append((allowed, copy))

    def arrive(where):
        for k in range(count):
            pltpu.make_async_remote_copy(
                src_ref=outs[k].at[where],
                dst_ref=outs[k].at[where],
                send_sem=send_sem.at[k, 0, where],
                recv_sem=recv_sem.at[k, where],
                device_id=twin,
                device_id_type=MESH,
            ).wait_recv()

    own_copies = [pltpu.make_async_copy(ins[k], outs[k].at[mine], own_sem.at[k]) for k in range(count)]
    push(0, mine, z < nz - 1, True)
    push(1, mine, z > 0, True)
    push(2, mine, None, True)
    push(3, mine, None, True)
    push(4, mine, None, True)
    for copy in own_copies:
        copy.start()
    riders.begin()

    def along(step):
        if step == 0:
            yield None, z
        else:
            yield z >= step, jnp.maximum(z - step, 0)
            yield z + step < nz, jnp.minimum(z + step, nz - 1)

    def on(allowed, action):
        if allowed is None:
            action()
        else:
            pl.when(allowed)(action)

    for turn in range(1, nz + 2):
        if turn <= nz:
            riders.some(turn - 1, nz)
        if turn < nz:
            for index, (allowed, zz) in enumerate(along(turn)):
                where = slot(zz, a, b, c)
                on(allowed, functools.partial(arrive, where))
                if index == 0:
                    push(0, where, allowed & (z < nz - 1))
                else:
                    push(1, where, allowed & (z > 0))
                for way in (2, 3, 4):
                    push(way, where, allowed)
        if turn - 1 < nz:
            for allowed, zz in along(turn - 1):
                where = slot(zz, 1 - a, b, c)
                on(allowed, functools.partial(arrive, where))
                for way in (3, 4):
                    push(way, where, allowed)
            for allowed, zz in along(turn - 1):
                where = slot(zz, a, 1 - b, c)
                on(allowed, functools.partial(arrive, where))
                push(4, where, allowed)
        if turn >= 2:
            for allowed, zz in along(turn - 2):
                where = slot(zz, 1 - a, 1 - b, c)
                on(allowed, functools.partial(arrive, where))
                push(4, where, allowed)
    for zz in range(nz):
        for aa in range(2):
            for bb in range(2):
                arrive(slot(zz, aa, bb, 1 - c))
    for allowed, copy in pending:
        on(allowed, copy.wait_send)
    for copy in own_copies:
        copy.wait()
    riders.finish()


def gather_rows(arrays, devices, ident, riders=()):
    count = len(arrays)
    nz = devices // 8
    kinds, ridden, rider_outs, rider_sems = rider_shapes(riders, devices)
    return pl.pallas_call(
        functools.partial(gather_kernel, nz, count, kinds),
        out_shape=tuple(jax.ShapeDtypeStruct((devices,) + v.shape, v.dtype) for v in arrays)
        + rider_outs,
        in_specs=[pl.BlockSpec(memory_space=pltpu.VMEM)] * (count + len(riders)),
        out_specs=tuple(pl.BlockSpec(memory_space=pl.ANY) for v in arrays + ridden),
        scratch_shapes=[
            pltpu.SemaphoreType.DMA((count, 5, devices)),
            pltpu.SemaphoreType.DMA((count, devices)),
            pltpu.SemaphoreType.DMA((count,)),
        ]
        + rider_sems,
        compiler_params=pltpu.CompilerParams(collective_id=ident, has_side_effects=True),
        name="gather_rows_%d" % ident,
    )(*arrays, *ridden)


def scatter_kernel(nz, turned, beside, kinds, *refs):
    extra = len(kinds)
    left_ref, right_ref = refs[:2]
    beside_ref = refs[2] if beside else None
    refs = refs[2 + beside :]
    out_ref = refs[extra]
    sent, got, from_far, from_near, rising, falling = refs[2 * extra + 1 : 2 * extra + 7]
    (twin_send, twin_recv, far_send, far_recv, near_send, near_recv, line_send, up_recv,
     down_recv) = refs[2 * extra + 7 : 2 * extra + 16]
    dp, ep, z, y, x, c, a, b = place()
    ways = targets(dp, ep, z, y, x, c, nz)
    up, down, near, far, twin = ways
    riders = Riders(
        kinds, nz, dp, ep, refs[:extra] + refs[extra + 1 : 2 * extra + 1] + refs[2 * extra + 16 :]
    )
    greet(nz, z, dp, ep, ways, extra > 0)
    riders.begin()
    per = 4 * nz

    def zed(step):
        if nz == 4:
            far_one = jnp.where(z < 2, 3, 0)
            second = jnp.where(z < 2, 2 - 2 * z, 7 - 2 * z)
            third = 1 + z % 2
            return jnp.where(step == 0, far_one, jnp.where(step == 1, second, jnp.where(step == 2, third, z)))
        return (z + 1 + step) % nz

    def term(where):
        sides = (((1,), (1 if turned else 0,)), ((), ()))
        value = lax.dot_general(
            left_ref[where], right_ref[...], sides, preferred_element_type=jnp.float32
        )
        if beside:
            value = jnp.concatenate([value, beside_ref[where].astype(jnp.float32)], axis=1)
        return value

    def order(index, aa, bb, cc):
        part = index // nz
        flip_b = 1 - part // 2
        flip_a = 1 - part % 2
        return slot(zed(index % nz), aa + flip_a * (1 - 2 * aa), bb + flip_b * (1 - 2 * bb), cc)

    def twin_copy(index):
        return pltpu.make_async_remote_copy(
            src_ref=sent.at[index], dst_ref=got.at[index], send_sem=twin_send.at[index],
            recv_sem=twin_recv.at[index], device_id=twin, device_id_type=MESH)

    def far_copy(index):
        return pltpu.make_async_remote_copy(
            src_ref=got.at[index], dst_ref=from_far.at[index], send_sem=far_send.at[index],
            recv_sem=far_recv.at[index], device_id=far, device_id_type=MESH)

    def near_copy(index):
        return pltpu.make_async_remote_copy(
            src_ref=got.at[2 * nz + index], dst_ref=from_near.at[index], send_sem=near_send.at[index],
            recv_sem=near_recv.at[index], device_id=near, device_id_type=MESH)

    def up_copy(index, zz):
        return pltpu.make_async_remote_copy(
            src_ref=got.at[3 * nz + index], dst_ref=rising.at[zz], send_sem=line_send.at[index],
            recv_sem=up_recv.at[zz], device_id=up, device_id_type=MESH)

    def down_copy(index, zz):
        return pltpu.make_async_remote_copy(
            src_ref=got.at[3 * nz + index], dst_ref=falling.at[zz], send_sem=line_send.at[index],
            recv_sem=down_recv.at[zz], device_id=down, device_id_type=MESH)

    def give(index):
        sent[index] = term(order(index, b, a, 1 - c)).astype(sent.dtype)
        twin_copy(index).start()

    def taken(index):
        value = term(order(index, a, b, c))
        twin_copy(index).wait_recv()
        return value + got[index].astype(jnp.float32)

    def far_step(step, carry):
        give(2 * step)
        give(2 * step + 1)
        got[step] = taken(step).astype(got.dtype)
        far_copy(step).start()
        riders.looped(step, 2 * nz)
        return carry

    lax.fori_loop(0, 2 * nz, far_step, 0)

    def near_step(step, carry):
        value = taken(2 * nz + step)
        far_copy(step).wait_recv()
        value = value + from_far[step].astype(jnp.float32)
        got[2 * nz + step] = value.astype(got.dtype)
        near_copy(step).start()
        return carry

    lax.fori_loop(0, nz, near_step, 0)

    def line_step(step, carry):
        zz = zed(step)
        value = taken(3 * nz + step)
        far_copy(nz + step).wait_recv()
        near_copy(step).wait_recv()
        out_ref[...] = value + from_far[nz + step].astype(jnp.float32) + from_near[step].astype(jnp.float32)

        @pl.when((zz >= z) & (z > 0))
        def _():
            up_copy(step, zz).wait_recv()
            out_ref[...] += rising[zz].astype(jnp.float32)

        @pl.when((zz <= z) & (z < nz - 1))
        def _():
            down_copy(step, zz).wait_recv()
            out_ref[...] += falling[zz].astype(jnp.float32)

        @pl.when(zz > z)
        def _():
            got[3 * nz + step] = out_ref[...].astype(got.dtype)
            up_copy(step, zz).start()

        @pl.when(zz < z)
        def _():
            got[3 * nz + step] = out_ref[...].astype(got.dtype)
            down_copy(step, zz).start()

        return carry

    lax.fori_loop(0, nz, line_step, 0)

    def finish(step, carry):
        twin_copy(step).wait_send()
        return carry

    lax.fori_loop(0, per, finish, 0)

    def finish_far(step, carry):
        far_copy(step).wait_send()
        return carry

    lax.fori_loop(0, 2 * nz, finish_far, 0)

    def finish_near(step, carry):
        near_copy(step).wait_send()

        @pl.when(step < nz - 1)
        def _():
            up_copy(step, 0).wait_send()

        return carry

    lax.fori_loop(0, nz, finish_near, 0)
    riders.finish()


def scatter_sum(left, right, devices, ident, turned=False, beside=None, riders=()):
    nz = devices // 8
    rows = left.shape[0] // devices
    depth, wide = right.shape[::-1] if turned else right.shape
    held = () if beside is None else (beside.reshape(devices, rows, -1),)
    wide = wide + sum(v.shape[2] for v in held)
    kinds, ridden, rider_outs, rider_sems = rider_shapes(riders, devices)
    block = (rows, wide)
    low = jnp.bfloat16
    dma = pltpu.SemaphoreType.DMA
    result = pl.pallas_call(
        functools.partial(scatter_kernel, nz, turned, len(held), kinds),
        out_shape=(jax.ShapeDtypeStruct(block, jnp.float32),) + rider_outs,
        in_specs=[pl.BlockSpec(memory_space=pltpu.VMEM)] * (2 + len(held) + len(riders)),
        out_specs=(pl.BlockSpec(memory_space=pltpu.VMEM),)
        + (pl.BlockSpec(memory_space=pl.ANY),) * len(riders),
        scratch_shapes=[
            pltpu.VMEM((4 * nz,) + block, low),
            pltpu.VMEM((4 * nz,) + block, low),
            pltpu.VMEM((2 * nz,) + block, low),
            pltpu.VMEM((nz,) + block, low),
            pltpu.VMEM((nz,) + block, low),
            pltpu.VMEM((nz,) + block, low),
            dma((4 * nz,)), dma((4 * nz,)), dma((2 * nz,)), dma((2 * nz,)),
            dma((nz,)), dma((nz,)), dma((nz,)), dma((nz,)), dma((nz,)),
        ]
        + rider_sems,
        compiler_params=pltpu.CompilerParams(
            collective_id=ident, has_side_effects=True, vmem_limit_bytes=58 * 2**20),
        name="scatter_sum_%d" % ident,
    )(left.reshape(devices, rows, depth), right, *held, *ridden)
    return result if riders else result[0]


def whole_rows(mesh):
    return mesh.shape["ep"] == 4 and mesh.shape["dp"] % 2 == 0 and mesh.shape["dp"] <= 8


def exact_dot(left_side, right_side):
    return jnp.dot(
        left_side, right_side, precision=lax.Precision.HIGHEST, preferred_element_type=jnp.float32
    )


def block_layout(lens, tok_count):
    ends = [lens[:, :1]]
    for at in range(1, lens.shape[1]):
        ends.append(ends[-1] + lens[:, at : at + 1])
    row_index = lax.broadcasted_iota(jnp.int32, (lens.shape[0], tok_count), 1)
    segment = jnp.zeros_like(row_index)
    first_row = jnp.zeros_like(row_index)
    for end in ends:
        passed = row_index >= end
        segment = segment + passed.astype(jnp.int32)
        first_row = jnp.where(passed, end, first_row)
    return (segment, row_index - first_row)


def by_experts(
    hidden_in,
    cotangent,
    deal_order,
    seq_lengths,
    expert_ids,
    w_query,
    w_key,
    w_value,
    w_out,
    w_router,
    gain_attn,
    gain_moe,
    gain_query,
    gain_key,
    w_gate,
    w_up,
    w_down,
    clip_threshold,
):
    f32, low = jnp.float32, jnp.bfloat16
    dp_count, ep_count = lax.axis_size("dp"), lax.axis_size("ep")
    devices = dp_count * ep_count
    dp, ep = lax.axis_index("dp"), lax.axis_index("ep")
    me = dp * ep_count + ep
    tok_count, width = hidden_in.shape
    row_count = tok_count * 7 // 8
    all_count = devices * row_count
    head_dim = gain_query.shape[0]
    half_dim = head_dim // 2
    rows_own = w_query.shape[0]
    head_count = w_query.shape[1] // head_dim
    kv_count = w_key.shape[1] // head_dim
    group_size = head_count // kv_count
    experts = w_router.shape[1]
    exp_local, wide_own, hidden = w_gate.shape
    parts = dp_count // exp_local
    piece = hidden // parts
    score_scale = head_dim ** (-0.5)

    gain_col = gain_attn.astype(f32)[:, None]
    heads_in = (w_query.astype(f32) * gain_col).astype(low).reshape(rows_own, head_count, head_dim)
    keys_in = (w_key.astype(f32) * gain_col).astype(low).reshape(rows_own, kv_count, head_dim)
    values_in = (w_value.astype(f32) * gain_col).astype(low).reshape(rows_own, kv_count, head_dim)
    sent_heads = jnp.concatenate(
        [heads_in, jnp.repeat(keys_in, group_size, axis=1), jnp.repeat(values_in, group_size, axis=1)],
        axis=2,
    ).transpose(1, 0, 2)
    def by_part(weights):
        weights = weights.reshape(exp_local, wide_own, parts, piece).transpose(0, 2, 1, 3)
        return weights.reshape(dp_count, wide_own, piece)

    local_order = deal_order % tok_count
    deal = (local_order[:, None] == jnp.arange(tok_count, dtype=jnp.int32)[None, :]).astype(low)
    deal = deal[:row_count]
    resid_in = jnp.dot(deal, hidden_in, preferred_element_type=f32)
    grad_mid_out = jnp.dot(deal, cotangent, preferred_element_type=f32)
    inv_one = rms_scale(resid_in)
    unit_one = resid_in * inv_one
    lens_row = jnp.pad(seq_lengths.astype(f32), ((0, 0), (0, 128 - seq_lengths.shape[1])))
    gain_row = jnp.pad(gain_moe.astype(f32)[None, :], ((0, 0), (0, 128 - rows_own)))
    router_rows = w_router.astype(f32).reshape(-1, 128)
    note_one = jnp.concatenate([lens_row, gain_row, router_rows], axis=0)
    note_one = jnp.pad(note_one, ((0, -note_one.shape[0] % 8), (0, 0)))
    unit_all, notes, w_heads, w_fall = gather_rows(
        (unit_one.astype(low), note_one),
        devices,
        1,
        (("all", sent_heads), ("dp", w_down.reshape(dp_count, piece, wide_own))),
    )
    w_heads = w_heads.reshape(width, 3 * head_dim)
    w_fall = w_fall.transpose(1, 0, 2).reshape(piece, width)
    grad_all, w_rise_up = gather_rows(
        (grad_mid_out.astype(low),), devices, 9, (("dp", by_part(w_up)),)
    )
    lens_all = notes[:, 0, : seq_lengths.shape[1]].astype(jnp.int32)
    gain_two = notes[:, 1, :rows_own].reshape(1, width)
    router_full = notes[:, 2 : 2 + router_rows.shape[0]].reshape(width, experts)

    segment, position = block_layout(lens_all, row_count)
    step_down = lax.broadcasted_iota(jnp.int32, (1, row_count, row_count), 1)
    step_across = lax.broadcasted_iota(jnp.int32, (1, row_count, row_count), 2)
    allowed = (segment[:, :, None] == segment[:, None, :]) & (step_across <= step_down)
    cosine_rows, sine_rows = rotary_tables(jnp.arange(tok_count, dtype=jnp.int32), head_dim)
    place_hot = (position.reshape(-1)[:, None] == jnp.arange(tok_count)[None, :]).astype(f32)
    cosine_all = exact_dot(place_hot, cosine_rows).reshape(devices, row_count, head_dim)
    sine_all = exact_dot(place_hot, sine_rows).reshape(devices, row_count, head_dim)
    flat_unit = unit_all.reshape(all_count, width)
    projected = jnp.dot(flat_unit, w_heads, preferred_element_type=f32).reshape(
        devices, row_count, 3 * head_dim
    )
    query_raw = projected[..., :head_dim]
    key_raw = projected[..., head_dim : 2 * head_dim]
    value_rows = projected[..., 2 * head_dim :].astype(low)
    gain_query_f = gain_query.astype(f32)
    gain_key_f = gain_key.astype(f32)
    inv_query = rms_scale(query_raw)
    unit_query = query_raw * inv_query
    query_rot = rotate(unit_query * gain_query_f, cosine_all, sine_all).astype(low)
    inv_key = rms_scale(key_raw)
    unit_key = key_raw * inv_key
    key_rot = rotate(unit_key * gain_key_f, cosine_all, sine_all).astype(low)
    scores = contract(query_rot, key_rot, "btd,bud->btu") * score_scale
    masked = jnp.where(allowed, scores, masked_fill)
    row_top = jnp.max(masked, axis=-1, keepdims=True)
    exponent = jnp.exp(masked - row_top)
    probs = exponent / jnp.sum(exponent, axis=-1, keepdims=True)
    probs_low = probs.astype(low)
    mixed = contract(probs_low, value_rows, "btu,bud->btd").astype(low).reshape(all_count, head_dim)
    largest_own = jnp.max(row_top)
    branch, w_rise_gate = scatter_sum(
        mixed, w_out, devices, 2, riders=(("dp", by_part(w_gate)),)
    )
    resid_mid = resid_in + branch
    w_rise = jnp.concatenate([w_rise_gate, w_rise_up], axis=2).reshape(width, 2 * piece)

    inv_two = rms_scale(resid_mid)
    unit_two = resid_mid * inv_two
    normed_mid = (unit_two * gain_two).astype(low)
    logits = jnp.dot(normed_mid, router_full.astype(low), preferred_element_type=f32)
    choose = (expert_ids[:row_count, :, None] == jnp.arange(experts, dtype=jnp.int32)[None, None, :]).any(axis=1)
    picked = jnp.where(choose, logits, masked_fill)
    gate_power = jnp.where(choose, jnp.exp(picked - jnp.max(picked, axis=1, keepdims=True)), 0.0)
    route = gate_power / jnp.sum(gate_power, axis=1, keepdims=True)
    note_two = jnp.concatenate([route.T, jnp.full((8, row_count), largest_own, f32)], axis=0)
    note_two = jnp.pad(note_two, ((0, 0), (0, 128 - row_count)))
    normed_all, notes = gather_rows((normed_mid, note_two), devices, 3)
    clip_factor = jnp.sqrt(clip_threshold / jnp.maximum(notes[:, experts, 0], clip_threshold))

    mine = ep * exp_local + dp // parts
    weight = lax.dynamic_slice_in_dim(notes, mine, 1, axis=1)[..., :row_count].reshape(all_count, 1)
    flat_mid = normed_all.reshape(all_count, width)
    flat_grad = grad_all.reshape(all_count, width)
    risen = jnp.dot(flat_mid, w_rise, preferred_element_type=f32)
    gate_part, up_part = risen[:, :piece], risen[:, piece:]
    grad_plain = contract(flat_grad, w_fall, "td,fd->tf")
    sigmoid_gate = jax.nn.sigmoid(gate_part)
    silu_gate = gate_part * sigmoid_gate
    hidden_mid = silu_gate * up_part
    grad_route = jnp.sum(hidden_mid * grad_plain, axis=1, keepdims=True)
    weighted_mid = (hidden_mid * weight).astype(low)
    grad_hidden = grad_plain * weight
    grad_gate_part = (
        grad_hidden * up_part * sigmoid_gate * (1.0 + gate_part * (1.0 - sigmoid_gate))
    ).astype(low)
    grad_up_part = (grad_hidden * silu_gate).astype(low)
    both = jnp.concatenate([grad_gate_part, grad_up_part], axis=1)
    lane = lax.broadcasted_iota(jnp.int32, (1, 128), 1)
    beside = jnp.where(lane == mine, grad_route, 0.0).astype(low)
    summed = scatter_sum(both, w_rise, devices, 4, turned=True, beside=beside)
    grad_rise_w = contract(flat_mid, both, "td,tf->df").astype(low)
    grad_fall_w = contract(weighted_mid, flat_grad, "tf,td->fd").astype(low)
    def from_part(grads):
        grads = grads.reshape(exp_local, parts, wide_own, piece).transpose(0, 2, 1, 3)
        return grads.reshape(exp_local, wide_own, hidden).astype(f32)

    grad_gates = summed[:, width : width + experts]
    mean_term = jnp.sum(route * grad_gates, axis=1, keepdims=True)
    grad_logits = (route * (grad_gates - mean_term)).astype(low)
    grad_normed_mid = summed[:, :width] + contract(grad_logits, router_full.astype(low), "te,de->td")
    gain_part = jnp.sum(grad_normed_mid * unit_two, axis=0)
    grad_mid = grad_mid_out + norm_back(grad_normed_mid * gain_two, unit_two, inv_two)
    grad_branch = grad_mid.astype(low)
    note_three = jnp.concatenate(
        [
            jnp.pad(grad_logits.T.astype(f32), ((0, 0), (0, 128 - row_count))),
            gain_part.reshape(-1, 128),
        ],
        axis=0,
    )
    branch_all, notes, back_gate = gather_rows(
        (grad_branch, note_three),
        devices,
        6,
        (("dp", grad_rise_w[:, :piece].reshape(dp_count, wide_own, piece)),),
    )
    logits_all = notes[:, :experts, :row_count].astype(low)
    normed_own = lax.dynamic_slice_in_dim(normed_all, me * rows_own, rows_own, axis=2)
    grad_router = contract(normed_own, logits_all, "btd,bet->de")
    gain_sum = jnp.sum(notes[:, experts:], axis=0).reshape(-1)
    grad_gain_moe = lax.dynamic_slice_in_dim(gain_sum, me * rows_own, rows_own)

    flat_branch = branch_all.reshape(all_count, width)
    grad_out = contract(mixed, flat_branch, "tq,td->qd")
    grad_mixed = (
        contract(flat_branch, w_out, "td,qd->tq").astype(low).reshape(devices, row_count, head_dim)
    )
    grad_value = contract(probs_low, grad_mixed, "btu,btd->bud").astype(low)
    grad_probs = contract(grad_mixed, value_rows, "btd,bud->btu")
    grad_scores = (
        probs * (grad_probs - jnp.sum(probs * grad_probs, axis=-1, keepdims=True))
    ).astype(low)
    grad_query_rot = contract(grad_scores, key_rot, "btu,bud->btd") * score_scale
    grad_key_rot = contract(grad_scores, query_rot, "btu,btd->bud") * score_scale
    grad_query_normed = rotate_back(grad_query_rot, cosine_all, sine_all)
    grad_key_normed = rotate_back(grad_key_rot, cosine_all, sine_all)
    gain_pair = jnp.stack(
        [
            jnp.sum(grad_query_normed * unit_query, axis=(0, 1)),
            jnp.sum(grad_key_normed * unit_key, axis=(0, 1)),
        ]
    )
    grad_query_raw = norm_back(grad_query_normed * gain_query_f, unit_query, inv_query).astype(low)
    grad_key_raw = norm_back(grad_key_normed * gain_key_f, unit_key, inv_key).astype(low)
    grad_heads = jnp.concatenate([grad_query_raw, grad_key_raw, grad_value], axis=2).reshape(
        all_count, 3 * head_dim
    )
    grad_heads_w = contract(flat_unit, grad_heads, "td,tq->dq").astype(low)
    moe_rows, back_up = scatter_sum(
        weighted_mid,
        w_fall,
        devices,
        5,
        riders=(("dp", grad_rise_w[:, piece:].reshape(dp_count, wide_own, piece)),),
    )
    resid_out = resid_mid + moe_rows
    undeal = (jnp.arange(tok_count, dtype=jnp.int32)[:, None] == local_order[None, :]).astype(low)
    undeal = undeal[:, :row_count]
    block_out = jnp.dot(undeal, resid_out.astype(low), preferred_element_type=f32).astype(low)
    grad_unit_one, back_heads, back_fall, gain_pairs = scatter_sum(
        grad_heads,
        w_heads,
        devices,
        7,
        turned=True,
        riders=(
            ("all", grad_heads_w.reshape(devices, rows_own, 3 * head_dim)),
            ("dp", grad_fall_w.reshape(piece, dp_count, wide_own).transpose(1, 0, 2)),
            ("same", jnp.pad(gain_pair, ((0, 6), (0, 0)))),
        ),
    )
    back_heads = back_heads.astype(f32)
    grad_gate = from_part(back_gate)
    grad_up = from_part(back_up)
    grad_down = back_fall.reshape(exp_local, hidden, wide_own).astype(f32)
    gain_pair = jnp.sum(gain_pairs, axis=0)
    plain_query = back_heads[..., :head_dim].transpose(1, 0, 2).reshape(rows_own, -1)

    def of_group(grads):
        grads = jnp.sum(grads.reshape(kv_count, group_size, rows_own, head_dim), axis=1)
        return grads.transpose(1, 0, 2).reshape(rows_own, -1)

    plain_key = of_group(back_heads[..., head_dim : 2 * head_dim])
    plain_value = of_group(back_heads[..., 2 * head_dim :])
    grad_gain_attn = (
        jnp.sum(plain_query * w_query.astype(f32), axis=1)
        + jnp.sum(plain_key * w_key.astype(f32), axis=1)
        + jnp.sum(plain_value * w_value.astype(f32), axis=1)
    )
    grad_resid_in = grad_mid + norm_back(grad_unit_one, unit_one, inv_one)
    grad_input = exact_dot(undeal.astype(f32), grad_resid_in)
    return (
        block_out,
        grad_input,
        plain_query * gain_col,
        plain_key * gain_col,
        plain_value * gain_col,
        grad_out,
        grad_router,
        grad_gain_attn,
        grad_gain_moe,
        gain_pair[0],
        gain_pair[1],
        grad_gate,
        grad_up,
        grad_down,
        clip_factor,
    )


def solution(mesh):
    placed = (
        P(("dp", "ep"), None),
        P(("dp", "ep"), None),
        P(("dp", "ep")),
        P(("dp", "ep"), None),
        P(("dp", "ep"), None),
        P(("dp", "ep"), None),
        P(("dp", "ep"), None),
        P(("dp", "ep"), None),
        P(("dp", "ep"), None),
        P(("dp", "ep"), None),
        P(("dp", "ep")),
        P(("dp", "ep")),
        P(),
        P(),
        P("ep", "dp", None),
        P("ep", "dp", None),
        P("ep", None, "dp"),
        P(),
    )
    return jax.shard_map(
        per_device if not whole_rows(mesh) else by_experts,
        mesh=mesh,
        in_specs=placed,
        out_specs=(
            P(("dp", "ep"), None),
            P(("dp", "ep"), None),
            P(("dp", "ep"), None),
            P(("dp", "ep"), None),
            P(("dp", "ep"), None),
            P(("dp", "ep"), None),
            P(("dp", "ep"), None),
            P(("dp", "ep")),
            P(("dp", "ep")),
            P(),
            P(),
            P("ep", "dp", None),
            P("ep", "dp", None),
            P("ep", None, "dp"),
            P(),
        ),
        check_vma=False,
    )
```

```python
import functools

import jax
import jax.numpy as jnp
from jax import lax
from jax.experimental import pallas as pl
from jax.experimental.pallas import tpu as pltpu
from jax.sharding import PartitionSpec as P

epsilon = 1e-06
theta_base = 1000000.0
masked_fill = -1e30


def rms_scale(values):
    return lax.rsqrt(jnp.mean(values * values, axis=-1, keepdims=True) + epsilon)


def rotate_half(values):
    half_dim = values.shape[-1] // 2
    return jnp.concatenate([-values[..., half_dim:], values[..., :half_dim]], axis=-1)


def rotate(values, cosine_table, sine_table):
    return values * cosine_table + rotate_half(values) * sine_table


def rotate_back(values, cosine_table, sine_table):
    scaled = values * sine_table
    half_dim = values.shape[-1] // 2
    turned = jnp.concatenate([scaled[..., half_dim:], -scaled[..., :half_dim]], axis=-1)
    return values * cosine_table + turned


def norm_back(grad_unit, unit_rows, inv_root):
    return inv_root * (
        grad_unit - unit_rows * jnp.mean(grad_unit * unit_rows, axis=-1, keepdims=True)
    )


def contract(left_side, right_side, pattern):
    return jnp.einsum(pattern, left_side, right_side, preferred_element_type=jnp.float32)


def layout(lens_row, tok_count):
    seq_ends = jnp.cumsum(lens_row)
    row_index = jnp.arange(tok_count, dtype=jnp.int32)
    segment = jnp.sum((row_index[:, None] >= seq_ends[None, :]).astype(jnp.int32), axis=1)
    starts_all = jnp.concatenate([jnp.zeros((1,), jnp.int32), seq_ends])
    seg_hot = segment[:, None] == jnp.arange(starts_all.shape[0], dtype=jnp.int32)[None, :]
    first_row = jnp.sum(jnp.where(seg_hot, starts_all[None, :], 0), axis=1)
    position = row_index - first_row
    valid_row = segment < lens_row.shape[0]
    allowed = (segment[:, None] == segment[None, :]) & (row_index[None, :] <= row_index[:, None])
    return (position, valid_row, allowed)


def rotary_tables(position, head_dim):
    half_dim = head_dim // 2
    frequency = theta_base ** (-(jnp.arange(half_dim, dtype=jnp.float32) * 2.0) / head_dim)
    angles = position.astype(jnp.float32)[:, None] * frequency[None, :]
    angles = jnp.concatenate([angles, angles], axis=-1)
    return (jnp.cos(angles), jnp.sin(angles))


def per_device(
    hidden_in,
    cotangent,
    deal_order,
    seq_lengths,
    expert_ids,
    w_query,
    w_key,
    w_value,
    w_out,
    w_router,
    gain_attn,
    gain_moe,
    gain_query,
    gain_key,
    w_gate,
    w_up,
    w_down,
    clip_threshold,
):
    tok_count = hidden_in.shape[0]
    model_width = hidden_in.shape[1]
    head_dim = gain_query.shape[0]
    local_order = deal_order % tok_count
    position, valid_row, allowed = layout(seq_lengths[0], tok_count)
    valid_col = valid_row.astype(jnp.float32)[:, None]
    cosine_table, sine_table = rotary_tables(position, head_dim)
    cosine_query = cosine_table[:, None, None, :]
    sine_query = sine_table[:, None, None, :]
    cosine_key = cosine_table[:, None, :]
    sine_key = sine_table[:, None, :]
    attn_params = (
        lax.all_gather(w_query, ("dp", "ep"), axis=0, tiled=True),
        lax.all_gather(w_key, ("dp", "ep"), axis=0, tiled=True),
        lax.all_gather(w_value, ("dp", "ep"), axis=0, tiled=True),
        lax.all_gather(w_out, ("dp", "ep"), axis=0, tiled=True),
        lax.all_gather(w_router, ("dp", "ep"), axis=0, tiled=True),
        lax.all_gather(gain_attn, ("dp", "ep"), axis=0, tiled=True),
        lax.all_gather(gain_moe, ("dp", "ep"), axis=0, tiled=True),
    )
    expert_params = (
        lax.all_gather(w_gate, "dp", axis=1, tiled=True),
        lax.all_gather(w_up, "dp", axis=1, tiled=True),
        lax.all_gather(w_down, "dp", axis=2, tiled=True),
    )
    query_full, key_full, value_full, out_full, router_full, gain_attn_full, gain_moe_full = (
        attn_params
    )
    gate_full, up_full, down_full = expert_params
    head_count = query_full.shape[1] // head_dim
    kv_count = key_full.shape[1] // head_dim
    group_size = head_count // kv_count
    experts = router_full.shape[1]
    top_count = expert_ids.shape[1]
    exp_local = w_gate.shape[0]
    ep_count = lax.axis_size("ep")
    capacity = (tok_count * top_count * 5 + 4 * experts - 1) // (4 * experts)
    score_scale = head_dim ** (-0.5)
    resid_in = hidden_in[local_order].astype(jnp.float32)
    inv_one = rms_scale(resid_in)
    unit_one = resid_in * inv_one
    gain_one = gain_attn_full.astype(jnp.float32)
    normed_in = (unit_one * gain_one).astype(jnp.bfloat16)
    query_raw = jnp.dot(normed_in, query_full, preferred_element_type=jnp.float32).reshape(
        tok_count, kv_count, group_size, head_dim
    )
    key_raw = jnp.dot(normed_in, key_full, preferred_element_type=jnp.float32).reshape(
        tok_count, kv_count, head_dim
    )
    value_rows = (
        jnp.dot(normed_in, value_full, preferred_element_type=jnp.float32)
        .astype(jnp.bfloat16)
        .reshape(tok_count, kv_count, head_dim)
    )
    inv_query = rms_scale(query_raw)
    unit_query = query_raw * inv_query
    gain_query_f = gain_query.astype(jnp.float32)
    query_rot = rotate(unit_query * gain_query_f, cosine_query, sine_query).astype(jnp.bfloat16)
    inv_key = rms_scale(key_raw)
    unit_key = key_raw * inv_key
    gain_key_f = gain_key.astype(jnp.float32)
    key_rot = rotate(unit_key * gain_key_f, cosine_key, sine_key).astype(jnp.bfloat16)
    scores = contract(query_rot, key_rot, "tkgd,ukd->kgtu") * score_scale
    masked = jnp.where(allowed, scores, masked_fill)
    row_top = jnp.max(masked, axis=-1, keepdims=True)
    exponent = jnp.exp(masked - row_top)
    row_total = jnp.sum(exponent, axis=-1, keepdims=True)
    log_total = row_top + jnp.log(row_total)
    probs_low = (exponent / row_total).astype(jnp.bfloat16)
    mixed_heads = (
        contract(probs_low, value_rows, "kgtu,ukd->tkgd")
        .astype(jnp.bfloat16)
        .reshape(tok_count, head_count * head_dim)
    )
    resid_mid = resid_in + jnp.dot(mixed_heads, out_full, preferred_element_type=jnp.float32)
    largest_local = jnp.max(
        jnp.where(allowed & valid_row[:, None], scores, masked_fill), axis=(2, 3)
    ).reshape(head_count)
    largest = lax.pmax(largest_local, ("dp", "ep"))
    clip_factor = jnp.sqrt(clip_threshold / jnp.maximum(largest, clip_threshold))
    inv_two = rms_scale(resid_mid)
    unit_two = resid_mid * inv_two
    gain_two = gain_moe_full.astype(jnp.float32)
    normed_mid = (unit_two * gain_two).astype(jnp.bfloat16)
    logits = jnp.dot(normed_mid, router_full, preferred_element_type=jnp.float32)
    choose = expert_ids[:, :, None] == jnp.arange(experts, dtype=jnp.int32)[None, None, :]
    picked = jnp.sum(jnp.where(choose, logits[:, None, :], 0.0), axis=2)
    gate_weights = jax.nn.softmax(picked, axis=-1)
    flat_ids = expert_ids.reshape(-1)
    flat_hot = (flat_ids[:, None] == jnp.arange(experts, dtype=jnp.int32)[None, :]).astype(
        jnp.int32
    )
    slot_rank = jnp.sum((jnp.cumsum(flat_hot, axis=0) - 1) * flat_hot, axis=1)
    slot_index = flat_ids * capacity + slot_rank
    pair_token = jnp.arange(tok_count * top_count, dtype=jnp.int32) // top_count
    send_rows = (
        jnp.zeros((experts * capacity, model_width), jnp.bfloat16)
        .at[slot_index]
        .set(normed_mid[pair_token])
    )
    send_rows = send_rows.reshape(ep_count, exp_local, capacity, model_width)
    arrived = lax.all_to_all(send_rows, "ep", split_axis=0, concat_axis=0, tiled=True)
    gate_part = contract(arrived, gate_full, "secd,edf->secf")
    up_part = contract(arrived, up_full, "secd,edf->secf")
    hidden_mid = (jax.nn.silu(gate_part) * up_part).astype(jnp.bfloat16)
    produced = contract(hidden_mid, down_full, "secf,efd->secd").astype(jnp.bfloat16)
    returned = lax.all_to_all(produced, "ep", split_axis=0, concat_axis=0, tiled=True)
    returned, arrived, gate_part, up_part = (returned, arrived, gate_part, up_part)
    pair_out = (
        returned.reshape(experts * capacity, model_width)[slot_index]
        .reshape(tok_count, top_count, model_width)
        .astype(jnp.float32)
    )
    resid_out = resid_mid + jnp.sum(gate_weights[:, :, None] * pair_out, axis=1)
    out_rows = (resid_out * valid_col).astype(jnp.bfloat16)
    block_out = jnp.zeros_like(out_rows).at[local_order].set(out_rows)
    attn_params = (
        lax.all_gather(w_query, ("dp", "ep"), axis=0, tiled=True),
        lax.all_gather(w_key, ("dp", "ep"), axis=0, tiled=True),
        lax.all_gather(w_value, ("dp", "ep"), axis=0, tiled=True),
        lax.all_gather(w_out, ("dp", "ep"), axis=0, tiled=True),
        lax.all_gather(w_router, ("dp", "ep"), axis=0, tiled=True),
        lax.all_gather(gain_attn, ("dp", "ep"), axis=0, tiled=True),
        lax.all_gather(gain_moe, ("dp", "ep"), axis=0, tiled=True),
    )
    expert_params = (
        lax.all_gather(w_gate, "dp", axis=1, tiled=True),
        lax.all_gather(w_up, "dp", axis=1, tiled=True),
        lax.all_gather(w_down, "dp", axis=2, tiled=True),
    )
    query_full, key_full, value_full, out_full, router_full, gain_attn_full, gain_moe_full = (
        attn_params
    )
    gate_full, up_full, down_full = expert_params
    grad_mid_out = cotangent[local_order].astype(jnp.float32) * valid_col
    grad_gates = jnp.sum(grad_mid_out[:, None, :] * pair_out, axis=2)
    grad_pair = (gate_weights[:, :, None] * grad_mid_out[:, None, :]).astype(jnp.bfloat16)
    send_grads = (
        jnp.zeros((experts * capacity, model_width), jnp.bfloat16)
        .at[slot_index]
        .set(grad_pair.reshape(-1, model_width))
    )
    send_grads = send_grads.reshape(ep_count, exp_local, capacity, model_width)
    grad_arrived = lax.all_to_all(send_grads, "ep", split_axis=0, concat_axis=0, tiled=True)
    grad_hidden = contract(grad_arrived, down_full, "secd,efd->secf")
    sigmoid_gate = jax.nn.sigmoid(gate_part)
    silu_gate = jax.nn.silu(gate_part)
    grad_gate_part = (
        grad_hidden * up_part * sigmoid_gate * (1.0 + gate_part * (1.0 - sigmoid_gate))
    ).astype(jnp.bfloat16)
    grad_up_part = (grad_hidden * silu_gate).astype(jnp.bfloat16)
    grad_rows = (
        contract(grad_gate_part, gate_full, "secf,edf->secd")
        + contract(grad_up_part, up_full, "secf,edf->secd")
    ).astype(jnp.bfloat16)
    grad_back = lax.all_to_all(grad_rows, "ep", split_axis=0, concat_axis=0, tiled=True)
    hidden_mid = (silu_gate * up_part).astype(jnp.bfloat16)
    grad_gate_w = contract(arrived, grad_gate_part, "secd,secf->edf")
    grad_up_w = contract(arrived, grad_up_part, "secd,secf->edf")
    grad_down_w = contract(hidden_mid, grad_arrived, "secf,secd->efd")
    grad_gate, grad_up, grad_down = (
        lax.psum_scatter(
            grad_gate_w.astype(jnp.bfloat16), "dp", scatter_dimension=1, tiled=True
        ).astype(jnp.float32),
        lax.psum_scatter(
            grad_up_w.astype(jnp.bfloat16), "dp", scatter_dimension=1, tiled=True
        ).astype(jnp.float32),
        lax.psum_scatter(
            grad_down_w.astype(jnp.bfloat16), "dp", scatter_dimension=2, tiled=True
        ).astype(jnp.float32),
    )
    mean_term = jnp.sum(gate_weights * grad_gates, axis=1, keepdims=True)
    grad_picked = gate_weights * (grad_gates - mean_term)
    grad_logits = jnp.sum(jnp.where(choose, grad_picked[:, :, None], 0.0), axis=1).astype(
        jnp.bfloat16
    )
    grad_router_w = contract(normed_mid, grad_logits, "td,te->de")
    pair_grads = (
        grad_back.reshape(experts * capacity, model_width)[slot_index]
        .reshape(tok_count, top_count, model_width)
        .astype(jnp.float32)
    )
    grad_normed_mid = jnp.sum(pair_grads, axis=1) + contract(grad_logits, router_full, "te,de->td")
    grad_gain_moe_w = jnp.sum(grad_normed_mid * unit_two, axis=0)
    grad_mid = grad_mid_out + norm_back(grad_normed_mid * gain_two, unit_two, inv_two)
    grad_branch = grad_mid.astype(jnp.bfloat16)
    grad_out_w = contract(mixed_heads, grad_branch, "tq,td->qd")
    grad_mixed = (
        contract(grad_branch, out_full, "td,qd->tq")
        .astype(jnp.bfloat16)
        .reshape(tok_count, kv_count, group_size, head_dim)
    )
    scores_again = contract(query_rot, key_rot, "tkgd,ukd->kgtu") * score_scale
    probs_back = jnp.exp(jnp.where(allowed, scores_again, masked_fill) - log_total)
    grad_value_rows = contract(
        probs_back.astype(jnp.bfloat16), grad_mixed, "kgtu,tkgd->ukd"
    ).astype(jnp.bfloat16)
    grad_probs = contract(grad_mixed, value_rows, "tkgd,ukd->kgtu")
    grad_scores = (
        probs_back * (grad_probs - jnp.sum(probs_back * grad_probs, axis=-1, keepdims=True))
    ).astype(jnp.bfloat16)
    grad_query_rot = contract(grad_scores, key_rot, "kgtu,ukd->tkgd") * score_scale
    grad_key_rot = contract(grad_scores, query_rot, "kgtu,tkgd->ukd") * score_scale
    grad_query_normed = rotate_back(grad_query_rot, cosine_query, sine_query)
    grad_key_normed = rotate_back(grad_key_rot, cosine_key, sine_key)
    grad_gain_q = jnp.sum(grad_query_normed * unit_query, axis=(0, 1, 2))
    grad_gain_k = jnp.sum(grad_key_normed * unit_key, axis=(0, 1))
    grad_query_raw = (
        norm_back(grad_query_normed * gain_query_f, unit_query, inv_query)
        .astype(jnp.bfloat16)
        .reshape(tok_count, head_count * head_dim)
    )
    grad_key_raw = (
        norm_back(grad_key_normed * gain_key_f, unit_key, inv_key)
        .astype(jnp.bfloat16)
        .reshape(tok_count, kv_count * head_dim)
    )
    grad_value_flat = grad_value_rows.reshape(tok_count, kv_count * head_dim)
    grad_query_w = contract(normed_in, grad_query_raw, "td,tq->dq")
    grad_key_w = contract(normed_in, grad_key_raw, "td,tq->dq")
    grad_value_w = contract(normed_in, grad_value_flat, "td,tq->dq")
    grad_normed_in = (
        contract(grad_query_raw, query_full, "tq,dq->td")
        + contract(grad_key_raw, key_full, "tq,dq->td")
        + contract(grad_value_flat, value_full, "tq,dq->td")
    )
    grad_gain_attn_w = jnp.sum(grad_normed_in * unit_one, axis=0)
    grad_resid_in = grad_mid + norm_back(grad_normed_in * gain_one, unit_one, inv_one)
    grad_input = jnp.zeros_like(grad_resid_in).at[local_order].set(grad_resid_in)
    grad_sums = (
        lax.psum_scatter(grad_query_w, ("dp", "ep"), scatter_dimension=0, tiled=True),
        lax.psum_scatter(grad_key_w, ("dp", "ep"), scatter_dimension=0, tiled=True),
        lax.psum_scatter(grad_value_w, ("dp", "ep"), scatter_dimension=0, tiled=True),
        lax.psum_scatter(grad_out_w, ("dp", "ep"), scatter_dimension=0, tiled=True),
        lax.psum_scatter(grad_router_w, ("dp", "ep"), scatter_dimension=0, tiled=True),
        lax.psum_scatter(grad_gain_attn_w, ("dp", "ep"), scatter_dimension=0, tiled=True),
        lax.psum_scatter(grad_gain_moe_w, ("dp", "ep"), scatter_dimension=0, tiled=True),
    )
    gain_sums = lax.psum((grad_gain_q, grad_gain_k), ("dp", "ep"))
    return (
        block_out,
        grad_input,
        grad_sums[0],
        grad_sums[1],
        grad_sums[2],
        grad_sums[3],
        grad_sums[4],
        grad_sums[5],
        grad_sums[6],
        gain_sums[0],
        gain_sums[1],
        grad_gate,
        grad_up,
        grad_down,
        clip_factor,
    )


MESH = pl.DeviceIdType.MESH


def place():
    dp = lax.axis_index("dp")
    ep = lax.axis_index("ep")
    z, y = dp // 2, dp % 2
    x, c = ep // 2, ep % 2
    first = (1 - c) * y + c * x
    second = (1 - c) * x + c * y
    return dp, ep, z, y, x, c, first, second


def targets(dp, ep, z, y, x, c, nz):
    up = (jnp.where(z < nz - 1, dp + 2, dp), ep)
    down = (jnp.where(z > 0, dp - 2, dp), ep)
    turn_y, turn_x = 1 - 2 * y, 2 - 4 * x
    near = (dp + (1 - c) * turn_y, ep + c * turn_x)
    far = (dp + c * turn_y, ep + (1 - c) * turn_x)
    twin = (dp, ep + 1 - 2 * c)
    return up, down, near, far, twin


def slot(z, first, second, c):
    return z * 8 + first * (4 - 2 * c) + second * (2 + 2 * c) + c


def greet(nz, z, dp, ep, ways, everyone):
    barrier = pltpu.get_barrier_semaphore()
    if everyone:
        total = nz * 8
        me = dp * 4 + ep

        def hello(step, carry):
            other = (me + step) % total
            pl.semaphore_signal(
                barrier, inc=1, device_id=(other // 4, other % 4), device_id_type=MESH
            )
            return carry

        lax.fori_loop(1, total, hello, 0)
        pl.semaphore_wait(barrier, total - 1)
        return
    for step in range(1, nz):
        other = ((z + step) % nz) * 2 + dp % 2
        pl.semaphore_signal(barrier, inc=1, device_id=(other, ep), device_id_type=MESH)
    for other in ways[2:]:
        pl.semaphore_signal(barrier, inc=1, device_id=other, device_id_type=MESH)
    pl.semaphore_wait(barrier, nz + 2)


class Riders:
    def __init__(self, kinds, nz, spot, refs):
        count = len(kinds)
        self.kinds, self.nz = kinds, nz
        self.dp, self.ep, self.z, self.y = spot
        self.me = self.dp * 4 + self.ep
        self.over_y = (self.dp + 1 - 2 * self.y, self.ep)
        self.ins, self.outs = refs[:count], refs[count : 2 * count]
        self.send, self.onward, self.recv, self.own = refs[2 * count :] if count else (None,) * 4
        self.spans = []
        for kind in kinds:
            if kind in ("all", "same"):
                self.spans.append((1, 8 * nz))
            else:
                self.spans.append((1 if kind in ("line", "cube") else 0, nz))
        self.steps = [(r, k) for r in range(count) for k in range(*self.spans[r])]
        self.steps.sort(key=lambda step: step[1] / self.spans[step[0]][1])
        self.cubes = [r for r in range(count) if kinds[r] == "cube"]

    def remote(self, source, target, send, recv, device):
        return pltpu.make_async_remote_copy(
            src_ref=source, dst_ref=target, send_sem=send, recv_sem=recv,
            device_id=device, device_id_type=MESH)

    def copy(self, r, step):
        kind, source, target = self.kinds[r], self.ins[r], self.outs[r]
        if kind in ("all", "same"):
            other = (self.me + step) % (8 * self.nz)
            source = source if kind == "same" else source.at[other]
            target, key, device = target.at[self.me], self.me, (other // 4, other % 4)
        elif kind in ("line", "cube"):
            other = (self.z + step) % self.nz
            source, key, device = source.at[other], self.z, (other * 2 + self.y, self.ep)
            target = target.at[self.z] if kind == "line" else target.at[self.z, self.y]
        else:
            source = source.at[step, 1 - self.y] if kind == "half" else source.at[step]
            target, key, device = target.at[step], step, self.over_y
        return self.remote(source, target, self.send.at[r, step], self.recv.at[r, key], device)

    def arrival(self, r, step):
        kind, target = self.kinds[r], self.outs[r]
        if kind in ("all", "same"):
            key = (self.me + step) % (8 * self.nz)
            target = target.at[key]
        elif kind in ("line", "cube"):
            key = (self.z + self.nz - step) % self.nz
            target = target.at[key] if kind == "line" else target.at[key, self.y]
        else:
            key, target = step, target.at[step]
        return self.remote(target, target, self.send.at[r, step], self.recv.at[r, key], self.over_y)

    def passing(self, r, step, first=False):
        key = (self.z + self.nz - step) % self.nz
        target = self.outs[r].at[key, self.y]
        source = self.ins[r].at[key] if first else target
        return self.remote(
            source, target, self.onward.at[r, step], self.recv.at[r, self.nz + key], self.over_y)

    def passed(self, r, step):
        key = (self.z + self.nz - step) % self.nz
        target = self.outs[r].at[key, 1 - self.y]
        return self.remote(
            target, target, self.onward.at[r, step], self.recv.at[r, self.nz + key], self.over_y)

    def own_copy(self, r):
        kind, source, target = self.kinds[r], self.ins[r], self.outs[r]
        if kind in ("all", "same"):
            source = source if kind == "same" else source.at[self.me]
            target = target.at[self.me]
        else:
            source = source.at[self.z]
            target = target.at[self.z] if kind == "line" else target.at[self.z, self.y]
        return pltpu.make_async_copy(source, target, self.own.at[r])

    def begin(self):
        for r, kind in enumerate(self.kinds):
            if kind not in ("half", "across"):
                self.own_copy(r).start()
            if kind == "cube":
                self.passing(r, 0, True).start()

    def some(self, share, shares):
        total = len(self.steps)
        for r, k in self.steps[total * share // shares : total * (share + 1) // shares]:
            self.copy(r, k).start()

    def onwards(self, step):
        for r in self.cubes:
            self.arrival(r, step).wait_recv()
            self.passing(r, step).start()

    def looped(self, step, steps):
        for r in range(len(self.kinds)):
            first, last = self.spans[r]
            per = -(-(last - first) // steps)
            for k in range(per):
                piece = first + step * per + k

                @pl.when(piece < last)
                def _():
                    self.copy(r, piece).start()

    def finish(self):
        for r, kind in enumerate(self.kinds):

            def settle(step, carry):
                if kind != "cube":
                    self.arrival(r, step).wait_recv()
                self.copy(r, step).wait_send()
                return carry

            lax.fori_loop(*self.spans[r], settle, 0)
            if kind == "cube":

                def settle_y(step, carry):
                    self.passed(r, step).wait_recv()
                    self.passing(r, step).wait_send()
                    return carry

                lax.fori_loop(0, self.nz, settle_y, 0)
            if kind not in ("half", "across"):
                self.own_copy(r).wait()


def rider_shapes(riders, devices):
    kinds = tuple(kind for kind, _ in riders)
    arrays = tuple(array for _, array in riders)
    outs = []
    for kind, v in riders:
        shape = v.shape
        if kind == "same":
            shape = (devices,) + shape
        elif kind == "cube":
            shape = shape[:1] + (2,) + shape[1:]
        elif kind == "half":
            shape = shape[:1] + shape[2:]
        outs.append(jax.ShapeDtypeStruct(shape, v.dtype))
    dma = pltpu.SemaphoreType.DMA
    count = len(riders)
    sems = [dma((count, devices))] * 3 + [dma((count,))] if count else []
    return kinds, arrays, tuple(outs), sems


def rider_specs(kinds):
    return [
        pl.BlockSpec(memory_space=pl.ANY if kind in ("half", "across") else pltpu.VMEM)
        for kind in kinds
    ]


def wide_greeting(kinds):
    return "all" in kinds or "same" in kinds


def gather_kernel(nz, count, kinds, *refs):
    extra = len(kinds)
    ins = refs[:count]
    outs = refs[count + extra : 2 * count + extra]
    send_sem, recv_sem, own_sem = refs[2 * (count + extra) : 2 * (count + extra) + 3]
    dp, ep, z, y, x, c, a, b = place()
    ways = targets(dp, ep, z, y, x, c, nz)
    twin = ways[4]
    riders = Riders(
        kinds, nz, (dp, ep, z, y),
        refs[count : count + extra]
        + refs[2 * count + extra : 2 * (count + extra)]
        + refs[2 * (count + extra) + 3 :],
    )
    greet(nz, z, dp, ep, ways, wide_greeting(kinds))
    mine = slot(z, a, b, c)
    pending = []

    def push(way, where, allowed=None, own=False):
        for k in range(count):
            copy = pltpu.make_async_remote_copy(
                src_ref=ins[k] if own else outs[k].at[where],
                dst_ref=outs[k].at[where],
                send_sem=send_sem.at[k, way, where],
                recv_sem=recv_sem.at[k, where],
                device_id=ways[way],
                device_id_type=MESH,
            )
            if allowed is None:
                copy.start()
            else:
                pl.when(allowed)(copy.start)
            pending.append((allowed, copy))

    def arrive(where):
        for k in range(count):
            pltpu.make_async_remote_copy(
                src_ref=outs[k].at[where],
                dst_ref=outs[k].at[where],
                send_sem=send_sem.at[k, 0, where],
                recv_sem=recv_sem.at[k, where],
                device_id=twin,
                device_id_type=MESH,
            ).wait_recv()

    own_copies = [pltpu.make_async_copy(ins[k], outs[k].at[mine], own_sem.at[k]) for k in range(count)]
    push(0, mine, z < nz - 1, True)
    push(1, mine, z > 0, True)
    push(2, mine, None, True)
    push(3, mine, None, True)
    push(4, mine, None, True)
    for copy in own_copies:
        copy.start()
    riders.begin()

    def along(step):
        if step == 0:
            yield None, z
        else:
            yield z >= step, jnp.maximum(z - step, 0)
            yield z + step < nz, jnp.minimum(z + step, nz - 1)

    def on(allowed, action):
        if allowed is None:
            action()
        else:
            pl.when(allowed)(action)

    for turn in range(1, nz + 2):
        if turn <= nz:
            riders.some(turn - 1, nz)
        if turn < nz:
            for index, (allowed, zz) in enumerate(along(turn)):
                where = slot(zz, a, b, c)
                on(allowed, functools.partial(arrive, where))
                if index == 0:
                    push(0, where, allowed & (z < nz - 1))
                else:
                    push(1, where, allowed & (z > 0))
                for way in (2, 3, 4):
                    push(way, where, allowed)
        if turn - 1 < nz:
            for allowed, zz in along(turn - 1):
                where = slot(zz, 1 - a, b, c)
                on(allowed, functools.partial(arrive, where))
                for way in (3, 4):
                    push(way, where, allowed)
            for allowed, zz in along(turn - 1):
                where = slot(zz, a, 1 - b, c)
                on(allowed, functools.partial(arrive, where))
                push(4, where, allowed)
        if turn >= 2:
            for allowed, zz in along(turn - 2):
                where = slot(zz, 1 - a, 1 - b, c)
                on(allowed, functools.partial(arrive, where))
                push(4, where, allowed)
    for zz in range(nz):
        for aa in range(2):
            for bb in range(2):
                arrive(slot(zz, aa, bb, 1 - c))
    for allowed, copy in pending:
        on(allowed, copy.wait_send)
    for copy in own_copies:
        copy.wait()
    riders.finish()


def gather_rows(arrays, devices, ident, riders=()):
    count = len(arrays)
    nz = devices // 8
    kinds, ridden, rider_outs, rider_sems = rider_shapes(riders, devices)
    return pl.pallas_call(
        functools.partial(gather_kernel, nz, count, kinds),
        out_shape=tuple(jax.ShapeDtypeStruct((devices,) + v.shape, v.dtype) for v in arrays)
        + rider_outs,
        in_specs=[pl.BlockSpec(memory_space=pltpu.VMEM)] * count + rider_specs(kinds),
        out_specs=tuple(pl.BlockSpec(memory_space=pl.ANY) for v in arrays + ridden),
        scratch_shapes=[
            pltpu.SemaphoreType.DMA((count, 5, devices)),
            pltpu.SemaphoreType.DMA((count, devices)),
            pltpu.SemaphoreType.DMA((count,)),
        ]
        + rider_sems,
        compiler_params=pltpu.CompilerParams(collective_id=ident, has_side_effects=True),
        name="gather_rows_%d" % ident,
    )(*arrays, *ridden)


def scatter_kernel(nz, turned, kinds, *refs):
    extra = len(kinds)
    left_ref, right_ref = refs[:2]
    refs = refs[2:]
    out_ref = refs[extra]
    sent, got, from_far, from_near, rising, falling = refs[2 * extra + 1 : 2 * extra + 7]
    (twin_send, twin_recv, far_send, far_recv, near_send, near_recv, line_send, up_recv,
     down_recv) = refs[2 * extra + 7 : 2 * extra + 16]
    dp, ep, z, y, x, c, a, b = place()
    ways = targets(dp, ep, z, y, x, c, nz)
    up, down, near, far, twin = ways
    riders = Riders(
        kinds, nz, (dp, ep, z, y),
        refs[:extra] + refs[extra + 1 : 2 * extra + 1] + refs[2 * extra + 16 :]
    )
    greet(nz, z, dp, ep, ways, wide_greeting(kinds))
    riders.begin()
    per = 4 * nz

    def zed(step):
        if nz == 4:
            far_one = jnp.where(z < 2, 3, 0)
            second = jnp.where(z < 2, 2 - 2 * z, 7 - 2 * z)
            third = 1 + z % 2
            return jnp.where(step == 0, far_one, jnp.where(step == 1, second, jnp.where(step == 2, third, z)))
        return (z + 1 + step) % nz

    def term(where):
        sides = (((1,), (1 if turned else 0,)), ((), ()))
        return lax.dot_general(
            left_ref[where], right_ref[...], sides, preferred_element_type=jnp.float32
        )

    def order(index, aa, bb, cc):
        part = index // nz
        flip_b = 1 - part // 2
        flip_a = 1 - part % 2
        return slot(zed(index % nz), aa + flip_a * (1 - 2 * aa), bb + flip_b * (1 - 2 * bb), cc)

    def twin_copy(index):
        return pltpu.make_async_remote_copy(
            src_ref=sent.at[index], dst_ref=got.at[index], send_sem=twin_send.at[index],
            recv_sem=twin_recv.at[index], device_id=twin, device_id_type=MESH)

    def far_copy(index):
        return pltpu.make_async_remote_copy(
            src_ref=got.at[index], dst_ref=from_far.at[index], send_sem=far_send.at[index],
            recv_sem=far_recv.at[index], device_id=far, device_id_type=MESH)

    def near_copy(index):
        return pltpu.make_async_remote_copy(
            src_ref=got.at[2 * nz + index], dst_ref=from_near.at[index], send_sem=near_send.at[index],
            recv_sem=near_recv.at[index], device_id=near, device_id_type=MESH)

    def up_copy(index, zz):
        return pltpu.make_async_remote_copy(
            src_ref=got.at[3 * nz + index], dst_ref=rising.at[zz], send_sem=line_send.at[index],
            recv_sem=up_recv.at[zz], device_id=up, device_id_type=MESH)

    def down_copy(index, zz):
        return pltpu.make_async_remote_copy(
            src_ref=got.at[3 * nz + index], dst_ref=falling.at[zz], send_sem=line_send.at[index],
            recv_sem=down_recv.at[zz], device_id=down, device_id_type=MESH)

    def give(index):
        sent[index] = term(order(index, b, a, 1 - c)).astype(sent.dtype)
        twin_copy(index).start()

    def taken(index):
        value = term(order(index, a, b, c))
        twin_copy(index).wait_recv()
        return value + got[index].astype(jnp.float32)

    def far_step(step, carry):
        give(2 * step)
        give(2 * step + 1)
        got[step] = taken(step).astype(got.dtype)
        far_copy(step).start()
        riders.looped(step, 2 * nz)
        return carry

    lax.fori_loop(0, 2 * nz, far_step, 0)

    def near_step(step, carry):
        value = taken(2 * nz + step)
        far_copy(step).wait_recv()
        value = value + from_far[step].astype(jnp.float32)
        got[2 * nz + step] = value.astype(got.dtype)
        near_copy(step).start()
        return carry

    lax.fori_loop(0, nz, near_step, 0)

    def line_step(step, carry):
        zz = zed(step)
        value = taken(3 * nz + step)
        far_copy(nz + step).wait_recv()
        near_copy(step).wait_recv()
        out_ref[...] = value + from_far[nz + step].astype(jnp.float32) + from_near[step].astype(jnp.float32)

        @pl.when((zz >= z) & (z > 0))
        def _():
            up_copy(step, zz).wait_recv()
            out_ref[...] += rising[zz].astype(jnp.float32)

        @pl.when((zz <= z) & (z < nz - 1))
        def _():
            down_copy(step, zz).wait_recv()
            out_ref[...] += falling[zz].astype(jnp.float32)

        @pl.when(zz > z)
        def _():
            got[3 * nz + step] = out_ref[...].astype(got.dtype)
            up_copy(step, zz).start()

        @pl.when(zz < z)
        def _():
            got[3 * nz + step] = out_ref[...].astype(got.dtype)
            down_copy(step, zz).start()

        return carry

    lax.fori_loop(0, nz, line_step, 0)

    def finish(step, carry):
        twin_copy(step).wait_send()
        return carry

    lax.fori_loop(0, per, finish, 0)

    def finish_far(step, carry):
        far_copy(step).wait_send()
        return carry

    lax.fori_loop(0, 2 * nz, finish_far, 0)

    def finish_near(step, carry):
        near_copy(step).wait_send()

        @pl.when(step < nz - 1)
        def _():
            up_copy(step, 0).wait_send()

        return carry

    lax.fori_loop(0, nz, finish_near, 0)
    riders.finish()


def scatter_sum(left, right, devices, ident, turned=False, riders=()):
    nz = devices // 8
    rows = left.shape[0] // devices
    depth, wide = right.shape[::-1] if turned else right.shape
    kinds, ridden, rider_outs, rider_sems = rider_shapes(riders, devices)
    block = (rows, wide)
    low = jnp.bfloat16
    dma = pltpu.SemaphoreType.DMA
    result = pl.pallas_call(
        functools.partial(scatter_kernel, nz, turned, kinds),
        out_shape=(jax.ShapeDtypeStruct(block, jnp.float32),) + rider_outs,
        in_specs=[pl.BlockSpec(memory_space=pltpu.VMEM)] * 2 + rider_specs(kinds),
        out_specs=(pl.BlockSpec(memory_space=pltpu.VMEM),)
        + (pl.BlockSpec(memory_space=pl.ANY),) * len(riders),
        scratch_shapes=[
            pltpu.VMEM((4 * nz,) + block, low),
            pltpu.VMEM((4 * nz,) + block, low),
            pltpu.VMEM((2 * nz,) + block, low),
            pltpu.VMEM((nz,) + block, low),
            pltpu.VMEM((nz,) + block, low),
            pltpu.VMEM((nz,) + block, low),
            dma((4 * nz,)), dma((4 * nz,)), dma((2 * nz,)), dma((2 * nz,)),
            dma((nz,)), dma((nz,)), dma((nz,)), dma((nz,)), dma((nz,)),
        ]
        + rider_sems,
        compiler_params=pltpu.CompilerParams(
            collective_id=ident, has_side_effects=True, vmem_limit_bytes=58 * 2**20),
        name="scatter_sum_%d" % ident,
    )(left.reshape(devices, rows, depth), right, *ridden)
    return result if riders else result[0]


def slab_gather_kernel(nz, count, kinds, *refs):
    extra = len(kinds)
    ins = refs[:count]
    outs = refs[count + extra : 2 * count + extra]
    send_sem, recv_sem, own_sem = refs[2 * (count + extra) : 2 * (count + extra) + 3]
    dp, ep, z, y, x, c, _, _ = place()
    ways = targets(dp, ep, z, y, x, c, nz)
    side = (dp, ep + 2 - 4 * x)
    ways = (ways[0], ways[1], side, ways[4])
    riders = Riders(
        kinds, nz, (dp, ep, z, y),
        refs[count : count + extra]
        + refs[2 * count + extra : 2 * (count + extra)]
        + refs[2 * (count + extra) + 3 :],
    )
    greet(nz, z, dp, ep, (None, None, riders.over_y, side, ways[3]), False)
    mine = z * 4 + ep
    pending = []

    def push(way, where, allowed=None, own=False):
        for k in range(count):
            copy = pltpu.make_async_remote_copy(
                src_ref=ins[k] if own else outs[k].at[where],
                dst_ref=outs[k].at[where],
                send_sem=send_sem.at[k, way, where],
                recv_sem=recv_sem.at[k, where],
                device_id=ways[way],
                device_id_type=MESH,
            )
            on(allowed, copy.start)
            pending.append((allowed, copy))

    def arrive(where):
        for k in range(count):
            pltpu.make_async_remote_copy(
                src_ref=outs[k].at[where],
                dst_ref=outs[k].at[where],
                send_sem=send_sem.at[k, 0, where],
                recv_sem=recv_sem.at[k, where],
                device_id=side,
                device_id_type=MESH,
            ).wait_recv()

    def on(allowed, action):
        if allowed is None:
            action()
        else:
            pl.when(allowed)(action)

    own_copies = [pltpu.make_async_copy(ins[k], outs[k].at[mine], own_sem.at[k]) for k in range(count)]
    push(0, mine, z < nz - 1, True)
    push(1, mine, z > 0, True)
    push(2, mine, None, True)
    push(3, mine, None, True)
    for copy in own_copies:
        copy.start()
    riders.begin()
    riders.some(0, 1)

    def along(step):
        if step == 0:
            yield None, z
        else:
            yield z >= step, jnp.maximum(z - step, 0)
            yield z + step < nz, jnp.minimum(z + step, nz - 1)

    for turn in range(1, nz + 1):
        if turn < nz:
            for index, (allowed, zz) in enumerate(along(turn)):
                where = zz * 4 + ep
                on(allowed, functools.partial(arrive, where))
                if index == 0:
                    push(0, where, allowed & (z < nz - 1))
                else:
                    push(1, where, allowed & (z > 0))
                push(2, where, allowed)
                push(3, where, allowed)
        for allowed, zz in along(turn - 1):
            where = zz * 4 + ep + 2 - 4 * x
            on(allowed, functools.partial(arrive, where))
            push(3, where, allowed)
        if turn >= 2:
            riders.onwards(turn - 1)
    for where in range(4 * nz):
        pl.when(where % 2 != c)(functools.partial(arrive, where))
    for allowed, copy in pending:
        on(allowed, copy.wait_send)
    for copy in own_copies:
        copy.wait()
    riders.finish()


def slab_gather(arrays, devices, ident, riders=()):
    count = len(arrays)
    nz = devices // 8
    kinds, ridden, rider_outs, rider_sems = rider_shapes(riders, devices)
    return pl.pallas_call(
        functools.partial(slab_gather_kernel, nz, count, kinds),
        out_shape=tuple(jax.ShapeDtypeStruct((4 * nz,) + v.shape, v.dtype) for v in arrays)
        + rider_outs,
        in_specs=[pl.BlockSpec(memory_space=pltpu.VMEM)] * count + rider_specs(kinds),
        out_specs=tuple(pl.BlockSpec(memory_space=pl.ANY) for v in arrays + ridden),
        scratch_shapes=[
            pltpu.SemaphoreType.DMA((count, 4, 4 * nz)),
            pltpu.SemaphoreType.DMA((count, 4 * nz)),
            pltpu.SemaphoreType.DMA((count,)),
        ]
        + rider_sems,
        compiler_params=pltpu.CompilerParams(collective_id=ident, has_side_effects=True),
        name="slab_gather_%d" % ident,
    )(*arrays, *ridden)


def slab_scatter_kernel(nz, pairs, turned, beside, kinds, *refs):
    extra = len(kinds)
    lefts, rights = refs[:pairs], refs[pairs : 2 * pairs]
    beside_ref = refs[2 * pairs] if beside else None
    refs = refs[2 * pairs + beside :]
    out_ref = refs[extra]
    sent, got, from_side, rising, falling = refs[2 * extra + 1 : 2 * extra + 6]
    (twin_send, twin_recv, side_send, side_recv, line_send, up_recv,
     down_recv) = refs[2 * extra + 6 : 2 * extra + 13]
    dp, ep, z, y, x, c, _, _ = place()
    up, down, _, _, twin = targets(dp, ep, z, y, x, c, nz)
    side = (dp, ep + 2 - 4 * x)
    riders = Riders(
        kinds, nz, (dp, ep, z, y),
        refs[:extra] + refs[extra + 1 : 2 * extra + 1] + refs[2 * extra + 13 :],
    )
    greet(nz, z, dp, ep, (None, None, riders.over_y, side, twin), False)
    riders.begin()
    plain = rights[0].shape[0 if turned else 1]
    span = 512 if plain % 512 == 0 else plain

    def zed(step):
        if nz == 4:
            far_one = jnp.where(z < 2, 3, 0)
            second = jnp.where(z < 2, 2 - 2 * z, 7 - 2 * z)
            third = 1 + z % 2
            return jnp.where(step == 0, far_one, jnp.where(step == 1, second, jnp.where(step == 2, third, z)))
        return (z + 1 + step) % nz

    def order(index, cc):
        flip = 1 - index // nz
        return zed(index % nz) * 4 + (x + flip * (1 - 2 * x)) * 2 + cc

    def combine(target, where, added):
        def fill(chunk, carry):
            at = pl.ds(pl.multiple_of(chunk * span, span), span)
            total = None
            for left_ref, right_ref in zip(lefts, rights):
                value = lax.dot_general(
                    left_ref[where],
                    right_ref[at, :] if turned else right_ref[:, at],
                    (((1,), (1 if turned else 0,)), ((), ())),
                    preferred_element_type=jnp.float32,
                )
                total = value if total is None else total + value
            for ref in added:
                total = total + ref[:, at].astype(jnp.float32)
            target[:, at] = total.astype(target.dtype)
            return carry

        lax.fori_loop(0, plain // span, fill, 0)
        if beside:
            at = pl.ds(plain, beside_ref.shape[2])
            total = beside_ref[where].astype(jnp.float32)
            for ref in added:
                total = total + ref[:, at].astype(jnp.float32)
            target[:, at] = total.astype(target.dtype)

    def twin_copy(index):
        return pltpu.make_async_remote_copy(
            src_ref=sent.at[index], dst_ref=got.at[index], send_sem=twin_send.at[index],
            recv_sem=twin_recv.at[index], device_id=twin, device_id_type=MESH)

    def side_copy(index):
        return pltpu.make_async_remote_copy(
            src_ref=got.at[index], dst_ref=from_side.at[index], send_sem=side_send.at[index],
            recv_sem=side_recv.at[index], device_id=side, device_id_type=MESH)

    def up_copy(index, zz):
        return pltpu.make_async_remote_copy(
            src_ref=got.at[nz + index], dst_ref=rising.at[zz], send_sem=line_send.at[index],
            recv_sem=up_recv.at[zz], device_id=up, device_id_type=MESH)

    def down_copy(index, zz):
        return pltpu.make_async_remote_copy(
            src_ref=got.at[nz + index], dst_ref=falling.at[zz], send_sem=line_send.at[index],
            recv_sem=down_recv.at[zz], device_id=down, device_id_type=MESH)

    def give(index, carry):
        combine(sent.at[index], order(index, 1 - c), ())
        twin_copy(index).start()
        return carry

    def side_step(step, carry):
        lax.fori_loop(2 * step, 2 * step + 2, give, 0)
        twin_copy(step).wait_recv()
        combine(got.at[step], order(step, c), (got.at[step],))
        side_copy(step).start()
        riders.looped(step, nz)
        return carry

    lax.fori_loop(0, nz, side_step, 0)

    def line_step(step, carry):
        zz = zed(step)
        twin_copy(nz + step).wait_recv()
        side_copy(step).wait_recv()
        combine(out_ref, order(nz + step, c), (got.at[nz + step], from_side.at[step]))

        @pl.when((zz >= z) & (z > 0))
        def _():
            up_copy(step, zz).wait_recv()
            out_ref[...] += rising[zz].astype(jnp.float32)

        @pl.when((zz <= z) & (z < nz - 1))
        def _():
            down_copy(step, zz).wait_recv()
            out_ref[...] += falling[zz].astype(jnp.float32)

        @pl.when(zz > z)
        def _():
            got[nz + step] = out_ref[...].astype(got.dtype)
            up_copy(step, zz).start()

        @pl.when(zz < z)
        def _():
            got[nz + step] = out_ref[...].astype(got.dtype)
            down_copy(step, zz).start()

        return carry

    lax.fori_loop(0, nz, line_step, 0)

    def finish(step, carry):
        twin_copy(step).wait_send()
        return carry

    lax.fori_loop(0, 2 * nz, finish, 0)

    def finish_side(step, carry):
        side_copy(step).wait_send()

        @pl.when(step < nz - 1)
        def _():
            up_copy(step, 0).wait_send()

        return carry

    lax.fori_loop(0, nz, finish_side, 0)
    riders.finish()


def slab_scatter(lefts, rights, devices, ident, turned=False, beside=None, riders=()):
    nz = devices // 8
    blocks = 4 * nz
    rows = lefts[0].shape[0] // blocks
    wide = rights[0].shape[0 if turned else 1]
    held = () if beside is None else (beside.reshape(blocks, rows, -1),)
    wide = wide + sum(v.shape[2] for v in held)
    kinds, ridden, rider_outs, rider_sems = rider_shapes(riders, devices)
    block = (rows, wide)
    low = jnp.bfloat16
    dma = pltpu.SemaphoreType.DMA
    pairs = len(lefts)
    result = pl.pallas_call(
        functools.partial(slab_scatter_kernel, nz, pairs, turned, len(held), kinds),
        out_shape=(jax.ShapeDtypeStruct(block, jnp.float32),) + rider_outs,
        in_specs=[pl.BlockSpec(memory_space=pltpu.VMEM)] * (2 * pairs + len(held))
        + rider_specs(kinds),
        out_specs=(pl.BlockSpec(memory_space=pltpu.VMEM),)
        + (pl.BlockSpec(memory_space=pl.ANY),) * len(riders),
        scratch_shapes=[
            pltpu.VMEM((2 * nz,) + block, low),
            pltpu.VMEM((2 * nz,) + block, low),
            pltpu.VMEM((nz,) + block, low),
            pltpu.VMEM((nz,) + block, low),
            pltpu.VMEM((nz,) + block, low),
            dma((2 * nz,)), dma((2 * nz,)), dma((nz,)), dma((nz,)), dma((nz,)), dma((nz,)), dma((nz,)),
        ]
        + rider_sems,
        compiler_params=pltpu.CompilerParams(
            collective_id=ident, has_side_effects=True, vmem_limit_bytes=58 * 2**20),
        name="slab_scatter_%d" % ident,
    )(*(v.reshape(blocks, rows, -1) for v in lefts), *rights, *held, *ridden)
    return result if riders else result[0]


def whole_rows(mesh):
    return mesh.shape["ep"] == 4 and mesh.shape["dp"] % 2 == 0 and mesh.shape["dp"] <= 8


def exact_dot(left_side, right_side):
    return jnp.dot(
        left_side, right_side, precision=lax.Precision.HIGHEST, preferred_element_type=jnp.float32
    )


def block_layout(lens, tok_count):
    ends = [lens[:, :1]]
    for at in range(1, lens.shape[1]):
        ends.append(ends[-1] + lens[:, at : at + 1])
    row_index = lax.broadcasted_iota(jnp.int32, (lens.shape[0], tok_count), 1)
    segment = jnp.zeros_like(row_index)
    first_row = jnp.zeros_like(row_index)
    for end in ends:
        passed = row_index >= end
        segment = segment + passed.astype(jnp.int32)
        first_row = jnp.where(passed, end, first_row)
    return (segment, row_index - first_row)


def by_experts(
    hidden_in,
    cotangent,
    deal_order,
    seq_lengths,
    expert_ids,
    w_query,
    w_key,
    w_value,
    w_out,
    w_router,
    gain_attn,
    gain_moe,
    gain_query,
    gain_key,
    w_gate,
    w_up,
    w_down,
    clip_threshold,
):
    f32, low = jnp.float32, jnp.bfloat16
    dp_count, ep_count = lax.axis_size("dp"), lax.axis_size("ep")
    devices = dp_count * ep_count
    dp, ep = lax.axis_index("dp"), lax.axis_index("ep")
    me = dp * ep_count + ep
    tok_count, width = hidden_in.shape
    row_count = tok_count * 7 // 8
    all_count = devices * row_count
    head_dim = gain_query.shape[0]
    half_dim = head_dim // 2
    rows_own = w_query.shape[0]
    head_count = w_query.shape[1] // head_dim
    kv_count = w_key.shape[1] // head_dim
    group_size = head_count // kv_count
    experts = w_router.shape[1]
    exp_local, wide_own, hidden = w_gate.shape
    lines = dp_count // 2
    slab = lines * ep_count
    z, y = dp // 2, dp % 2
    score_scale = head_dim ** (-0.5)

    gain_col = gain_attn.astype(f32)[:, None]
    heads_in = (w_query.astype(f32) * gain_col).astype(low).reshape(rows_own, head_count, head_dim)
    keys_in = (w_key.astype(f32) * gain_col).astype(low).reshape(rows_own, kv_count, head_dim)
    values_in = (w_value.astype(f32) * gain_col).astype(low).reshape(rows_own, kv_count, head_dim)
    sent_heads = jnp.concatenate(
        [heads_in, jnp.repeat(keys_in, group_size, axis=1), jnp.repeat(values_in, group_size, axis=1)],
        axis=2,
    ).transpose(1, 0, 2)

    local_order = deal_order % tok_count
    deal = (local_order[:, None] == jnp.arange(tok_count, dtype=jnp.int32)[None, :]).astype(low)
    deal = deal[:row_count]
    resid_in = jnp.dot(deal, hidden_in, preferred_element_type=f32)
    grad_mid_out = jnp.dot(deal, cotangent, preferred_element_type=f32)
    inv_one = rms_scale(resid_in)
    unit_one = resid_in * inv_one
    lens_row = jnp.pad(seq_lengths.astype(f32), ((0, 0), (0, 128 - seq_lengths.shape[1])))
    gain_row = jnp.pad(gain_moe.astype(f32)[None, :], ((0, 0), (0, 128 - rows_own)))
    router_rows = w_router.astype(f32).reshape(-1, 128)
    note_one = jnp.concatenate([lens_row, gain_row, router_rows], axis=0)
    note_one = jnp.pad(note_one, ((0, -note_one.shape[0] % 8), (0, 0)))
    unit_all, notes, w_heads = gather_rows(
        (unit_one.astype(low), note_one), devices, 1, (("all", sent_heads),)
    )
    w_heads = w_heads.reshape(width, 3 * head_dim)
    grad_all, w_rise_up = slab_gather(
        (grad_mid_out.astype(low),), devices, 9, (("cube", w_up),)
    )
    w_rise_up = w_rise_up.reshape(width, hidden)
    lens_all = notes[:, 0, : seq_lengths.shape[1]].astype(jnp.int32)
    gain_two = notes[:, 1, :rows_own].reshape(1, width)
    router_full = notes[:, 2 : 2 + router_rows.shape[0]].reshape(width, experts)

    segment, position = block_layout(lens_all, row_count)
    step_down = lax.broadcasted_iota(jnp.int32, (1, row_count, row_count), 1)
    step_across = lax.broadcasted_iota(jnp.int32, (1, row_count, row_count), 2)
    allowed = (segment[:, :, None] == segment[:, None, :]) & (step_across <= step_down)
    cosine_rows, sine_rows = rotary_tables(jnp.arange(tok_count, dtype=jnp.int32), head_dim)
    place_hot = (position.reshape(-1)[:, None] == jnp.arange(tok_count)[None, :]).astype(f32)
    cosine_all = exact_dot(place_hot, cosine_rows).reshape(devices, row_count, head_dim)
    sine_all = exact_dot(place_hot, sine_rows).reshape(devices, row_count, head_dim)
    flat_unit = unit_all.reshape(all_count, width)
    projected = jnp.dot(flat_unit, w_heads, preferred_element_type=f32).reshape(
        devices, row_count, 3 * head_dim
    )
    query_raw = projected[..., :head_dim]
    key_raw = projected[..., head_dim : 2 * head_dim]
    value_rows = projected[..., 2 * head_dim :].astype(low)
    gain_query_f = gain_query.astype(f32)
    gain_key_f = gain_key.astype(f32)
    inv_query = rms_scale(query_raw)
    unit_query = query_raw * inv_query
    query_rot = rotate(unit_query * gain_query_f, cosine_all, sine_all).astype(low)
    inv_key = rms_scale(key_raw)
    unit_key = key_raw * inv_key
    key_rot = rotate(unit_key * gain_key_f, cosine_all, sine_all).astype(low)
    scores = contract(query_rot, key_rot, "btd,bud->btu") * score_scale
    masked = jnp.where(allowed, scores, masked_fill)
    row_top = jnp.max(masked, axis=-1, keepdims=True)
    exponent = jnp.exp(masked - row_top)
    probs = exponent / jnp.sum(exponent, axis=-1, keepdims=True)
    probs_low = probs.astype(low)
    mixed = contract(probs_low, value_rows, "btu,bud->btd").astype(low).reshape(all_count, head_dim)
    largest_own = jnp.max(row_top)
    branch, fall_own = scatter_sum(mixed, w_out, devices, 2, riders=(("line", w_down),))
    resid_mid = resid_in + branch

    inv_two = rms_scale(resid_mid)
    unit_two = resid_mid * inv_two
    normed_mid = (unit_two * gain_two).astype(low)
    logits = jnp.dot(normed_mid, router_full.astype(low), preferred_element_type=f32)
    choose = (expert_ids[:row_count, :, None] == jnp.arange(experts, dtype=jnp.int32)[None, None, :]).any(axis=1)
    picked = jnp.where(choose, logits, masked_fill)
    gate_power = jnp.where(choose, jnp.exp(picked - jnp.max(picked, axis=1, keepdims=True)), 0.0)
    route = gate_power / jnp.sum(gate_power, axis=1, keepdims=True)
    note_two = jnp.pad(route.T, ((0, 0), (0, 128 - row_count)))
    normed_all, notes, w_rise_gate, fall_other = slab_gather(
        (normed_mid, note_two), devices, 3, (("cube", w_gate), ("across", fall_own))
    )
    w_rise_gate = w_rise_gate.reshape(width, hidden)
    w_fall = jnp.where(
        y == 0, jnp.stack([fall_own, fall_other], axis=1), jnp.stack([fall_other, fall_own], axis=1)
    )
    w_fall = w_fall.transpose(2, 0, 1, 3).reshape(hidden, width)

    mine = ep * exp_local + z
    slab_rows = slab * row_count
    weight = lax.dynamic_slice_in_dim(notes, mine, 1, axis=1)[..., :row_count].reshape(slab_rows, 1)
    flat_mid = normed_all.reshape(slab_rows, width)
    flat_grad = grad_all.reshape(slab_rows, width)
    gate_part = jnp.dot(flat_mid, w_rise_gate, preferred_element_type=f32)
    up_part = jnp.dot(flat_mid, w_rise_up, preferred_element_type=f32)
    grad_plain = contract(flat_grad, w_fall, "td,fd->tf")
    sigmoid_gate = jax.nn.sigmoid(gate_part)
    silu_gate = gate_part * sigmoid_gate
    hidden_mid = silu_gate * up_part
    grad_route = jnp.sum(hidden_mid * grad_plain, axis=1, keepdims=True)
    weighted_mid = (hidden_mid * weight).astype(low)
    grad_hidden = grad_plain * weight
    grad_gate_part = (
        grad_hidden * up_part * sigmoid_gate * (1.0 + gate_part * (1.0 - sigmoid_gate))
    ).astype(low)
    grad_up_part = (grad_hidden * silu_gate).astype(low)
    lane = lax.broadcasted_iota(jnp.int32, (1, 128), 1)
    beside = jnp.where(lane == mine, grad_route, 0.0).astype(low)

    def for_each_y(grads):
        return grads.astype(low).reshape(lines, 2, wide_own, hidden)

    gate_halves = for_each_y(contract(flat_mid, grad_gate_part, "td,tf->df"))
    up_halves = for_each_y(contract(flat_mid, grad_up_part, "td,tf->df"))
    fall_halves = for_each_y(contract(flat_grad, weighted_mid, "td,tf->df"))
    summed, gate_come, up_come = slab_scatter(
        (grad_gate_part, grad_up_part),
        (w_rise_gate, w_rise_up),
        devices,
        4,
        turned=True,
        beside=beside,
        riders=(("half", gate_halves), ("half", up_halves)),
    )

    def add_halves(halves, come):
        kept = lax.dynamic_index_in_dim(halves, y, axis=1, keepdims=False)
        return (kept.astype(f32) + come.astype(f32)).astype(low)

    grad_gates = summed[:, width : width + experts]
    mean_term = jnp.sum(route * grad_gates, axis=1, keepdims=True)
    grad_logits = (route * (grad_gates - mean_term)).astype(low)
    grad_normed_mid = summed[:, :width] + contract(grad_logits, router_full.astype(low), "te,de->td")
    gain_part = jnp.sum(grad_normed_mid * unit_two, axis=0)
    grad_mid = grad_mid_out + norm_back(grad_normed_mid * gain_two, unit_two, inv_two)
    grad_branch = grad_mid.astype(low)
    router_part = contract(normed_mid, grad_logits, "td,te->de").reshape(devices, -1, 128)
    note_three = jnp.concatenate(
        [
            gain_part.reshape(-1, 128),
            jnp.full((8, 128), largest_own, f32),
        ],
        axis=0,
    )
    branch_all, notes, back_up = gather_rows(
        (grad_branch, note_three), devices, 6, (("line", add_halves(up_halves, up_come)),)
    )
    clip_factor = jnp.sqrt(clip_threshold / jnp.maximum(notes[:, -1, 0], clip_threshold))
    gain_sum = jnp.sum(notes[:, :-8], axis=0).reshape(-1)
    grad_gain_moe = lax.dynamic_slice_in_dim(gain_sum, me * rows_own, rows_own)

    flat_branch = branch_all.reshape(all_count, width)
    grad_out = contract(mixed, flat_branch, "tq,td->qd")
    grad_mixed = (
        contract(flat_branch, w_out, "td,qd->tq").astype(low).reshape(devices, row_count, head_dim)
    )
    grad_value = contract(probs_low, grad_mixed, "btu,btd->bud").astype(low)
    grad_probs = contract(grad_mixed, value_rows, "btd,bud->btu")
    grad_scores = (
        probs * (grad_probs - jnp.sum(probs * grad_probs, axis=-1, keepdims=True))
    ).astype(low)
    grad_query_rot = contract(grad_scores, key_rot, "btu,bud->btd") * score_scale
    grad_key_rot = contract(grad_scores, query_rot, "btu,btd->bud") * score_scale
    grad_query_normed = rotate_back(grad_query_rot, cosine_all, sine_all)
    grad_key_normed = rotate_back(grad_key_rot, cosine_all, sine_all)
    gain_pair = jnp.stack(
        [
            jnp.sum(grad_query_normed * unit_query, axis=(0, 1)),
            jnp.sum(grad_key_normed * unit_key, axis=(0, 1)),
        ]
    )
    grad_query_raw = norm_back(grad_query_normed * gain_query_f, unit_query, inv_query).astype(low)
    grad_key_raw = norm_back(grad_key_normed * gain_key_f, unit_key, inv_key).astype(low)
    grad_heads = jnp.concatenate([grad_query_raw, grad_key_raw, grad_value], axis=2).reshape(
        all_count, 3 * head_dim
    )
    grad_heads_w = contract(flat_unit, grad_heads, "td,tq->dq").astype(low)
    moe_rows, back_gate, fall_come = slab_scatter(
        (weighted_mid,),
        (w_fall,),
        devices,
        5,
        riders=(("line", add_halves(gate_halves, gate_come)), ("half", fall_halves)),
    )
    resid_out = resid_mid + moe_rows
    undeal = (jnp.arange(tok_count, dtype=jnp.int32)[:, None] == local_order[None, :]).astype(low)
    undeal = undeal[:, :row_count]
    block_out = jnp.dot(undeal, resid_out.astype(low), preferred_element_type=f32).astype(low)
    grad_unit_one, back_heads, back_fall, gain_pairs, router_parts = scatter_sum(
        grad_heads,
        w_heads,
        devices,
        7,
        turned=True,
        riders=(
            ("all", grad_heads_w.reshape(devices, rows_own, 3 * head_dim)),
            ("line", add_halves(fall_halves, fall_come)),
            ("same", jnp.pad(gain_pair, ((0, 6), (0, 0)))),
            ("all", router_part),
        ),
    )
    back_heads = back_heads.astype(f32)
    grad_gate = back_gate.astype(f32)
    grad_up = back_up.astype(f32)
    grad_down = back_fall.transpose(0, 2, 1).astype(f32)
    grad_router = jnp.sum(router_parts, axis=0).reshape(rows_own, experts)
    gain_pair = jnp.sum(gain_pairs, axis=0)
    plain_query = back_heads[..., :head_dim].transpose(1, 0, 2).reshape(rows_own, -1)

    def of_group(grads):
        grads = jnp.sum(grads.reshape(kv_count, group_size, rows_own, head_dim), axis=1)
        return grads.transpose(1, 0, 2).reshape(rows_own, -1)

    plain_key = of_group(back_heads[..., head_dim : 2 * head_dim])
    plain_value = of_group(back_heads[..., 2 * head_dim :])
    grad_gain_attn = (
        jnp.sum(plain_query * w_query.astype(f32), axis=1)
        + jnp.sum(plain_key * w_key.astype(f32), axis=1)
        + jnp.sum(plain_value * w_value.astype(f32), axis=1)
    )
    grad_resid_in = grad_mid + norm_back(grad_unit_one, unit_one, inv_one)
    grad_input = exact_dot(undeal.astype(f32), grad_resid_in)
    return (
        block_out,
        grad_input,
        plain_query * gain_col,
        plain_key * gain_col,
        plain_value * gain_col,
        grad_out,
        grad_router,
        grad_gain_attn,
        grad_gain_moe,
        gain_pair[0],
        gain_pair[1],
        grad_gate,
        grad_up,
        grad_down,
        clip_factor,
    )


def solution(mesh):
    placed = (
        P(("dp", "ep"), None),
        P(("dp", "ep"), None),
        P(("dp", "ep")),
        P(("dp", "ep"), None),
        P(("dp", "ep"), None),
        P(("dp", "ep"), None),
        P(("dp", "ep"), None),
        P(("dp", "ep"), None),
        P(("dp", "ep"), None),
        P(("dp", "ep"), None),
        P(("dp", "ep")),
        P(("dp", "ep")),
        P(),
        P(),
        P("ep", "dp", None),
        P("ep", "dp", None),
        P("ep", None, "dp"),
        P(),
    )
    return jax.shard_map(
        per_device if not whole_rows(mesh) else by_experts,
        mesh=mesh,
        in_specs=placed,
        out_specs=(
            P(("dp", "ep"), None),
            P(("dp", "ep"), None),
            P(("dp", "ep"), None),
            P(("dp", "ep"), None),
            P(("dp", "ep"), None),
            P(("dp", "ep"), None),
            P(("dp", "ep"), None),
            P(("dp", "ep")),
            P(("dp", "ep")),
            P(),
            P(),
            P("ep", "dp", None),
            P("ep", "dp", None),
            P("ep", None, "dp"),
            P(),
        ),
        check_vma=False,
    )
```

```python
import functools

import jax
import jax.numpy as jnp
from jax import lax
from jax.experimental import pallas as pl
from jax.experimental.pallas import tpu as pltpu
from jax.sharding import PartitionSpec as P

epsilon = 1e-06
theta_base = 1000000.0
masked_fill = -1e30


def rms_scale(values):
    return lax.rsqrt(jnp.mean(values * values, axis=-1, keepdims=True) + epsilon)


def rotate_half(values):
    half_dim = values.shape[-1] // 2
    return jnp.concatenate([-values[..., half_dim:], values[..., :half_dim]], axis=-1)


def rotate(values, cosine_table, sine_table):
    return values * cosine_table + rotate_half(values) * sine_table


def rotate_back(values, cosine_table, sine_table):
    scaled = values * sine_table
    half_dim = values.shape[-1] // 2
    turned = jnp.concatenate([scaled[..., half_dim:], -scaled[..., :half_dim]], axis=-1)
    return values * cosine_table + turned


def norm_back(grad_unit, unit_rows, inv_root):
    return inv_root * (
        grad_unit - unit_rows * jnp.mean(grad_unit * unit_rows, axis=-1, keepdims=True)
    )


def contract(left_side, right_side, pattern):
    return jnp.einsum(pattern, left_side, right_side, preferred_element_type=jnp.float32)


def layout(lens_row, tok_count):
    seq_ends = jnp.cumsum(lens_row)
    row_index = jnp.arange(tok_count, dtype=jnp.int32)
    segment = jnp.sum((row_index[:, None] >= seq_ends[None, :]).astype(jnp.int32), axis=1)
    starts_all = jnp.concatenate([jnp.zeros((1,), jnp.int32), seq_ends])
    seg_hot = segment[:, None] == jnp.arange(starts_all.shape[0], dtype=jnp.int32)[None, :]
    first_row = jnp.sum(jnp.where(seg_hot, starts_all[None, :], 0), axis=1)
    position = row_index - first_row
    valid_row = segment < lens_row.shape[0]
    allowed = (segment[:, None] == segment[None, :]) & (row_index[None, :] <= row_index[:, None])
    return (position, valid_row, allowed)


def rotary_tables(position, head_dim):
    half_dim = head_dim // 2
    frequency = theta_base ** (-(jnp.arange(half_dim, dtype=jnp.float32) * 2.0) / head_dim)
    angles = position.astype(jnp.float32)[:, None] * frequency[None, :]
    angles = jnp.concatenate([angles, angles], axis=-1)
    return (jnp.cos(angles), jnp.sin(angles))


def per_device(
    hidden_in,
    cotangent,
    deal_order,
    seq_lengths,
    expert_ids,
    w_query,
    w_key,
    w_value,
    w_out,
    w_router,
    gain_attn,
    gain_moe,
    gain_query,
    gain_key,
    w_gate,
    w_up,
    w_down,
    clip_threshold,
):
    tok_count = hidden_in.shape[0]
    model_width = hidden_in.shape[1]
    head_dim = gain_query.shape[0]
    local_order = deal_order % tok_count
    position, valid_row, allowed = layout(seq_lengths[0], tok_count)
    valid_col = valid_row.astype(jnp.float32)[:, None]
    cosine_table, sine_table = rotary_tables(position, head_dim)
    cosine_query = cosine_table[:, None, None, :]
    sine_query = sine_table[:, None, None, :]
    cosine_key = cosine_table[:, None, :]
    sine_key = sine_table[:, None, :]
    attn_params = (
        lax.all_gather(w_query, ("dp", "ep"), axis=0, tiled=True),
        lax.all_gather(w_key, ("dp", "ep"), axis=0, tiled=True),
        lax.all_gather(w_value, ("dp", "ep"), axis=0, tiled=True),
        lax.all_gather(w_out, ("dp", "ep"), axis=0, tiled=True),
        lax.all_gather(w_router, ("dp", "ep"), axis=0, tiled=True),
        lax.all_gather(gain_attn, ("dp", "ep"), axis=0, tiled=True),
        lax.all_gather(gain_moe, ("dp", "ep"), axis=0, tiled=True),
    )
    expert_params = (
        lax.all_gather(w_gate, "dp", axis=1, tiled=True),
        lax.all_gather(w_up, "dp", axis=1, tiled=True),
        lax.all_gather(w_down, "dp", axis=2, tiled=True),
    )
    query_full, key_full, value_full, out_full, router_full, gain_attn_full, gain_moe_full = (
        attn_params
    )
    gate_full, up_full, down_full = expert_params
    head_count = query_full.shape[1] // head_dim
    kv_count = key_full.shape[1] // head_dim
    group_size = head_count // kv_count
    experts = router_full.shape[1]
    top_count = expert_ids.shape[1]
    exp_local = w_gate.shape[0]
    ep_count = lax.axis_size("ep")
    capacity = (tok_count * top_count * 5 + 4 * experts - 1) // (4 * experts)
    score_scale = head_dim ** (-0.5)
    resid_in = hidden_in[local_order].astype(jnp.float32)
    inv_one = rms_scale(resid_in)
    unit_one = resid_in * inv_one
    gain_one = gain_attn_full.astype(jnp.float32)
    normed_in = (unit_one * gain_one).astype(jnp.bfloat16)
    query_raw = jnp.dot(normed_in, query_full, preferred_element_type=jnp.float32).reshape(
        tok_count, kv_count, group_size, head_dim
    )
    key_raw = jnp.dot(normed_in, key_full, preferred_element_type=jnp.float32).reshape(
        tok_count, kv_count, head_dim
    )
    value_rows = (
        jnp.dot(normed_in, value_full, preferred_element_type=jnp.float32)
        .astype(jnp.bfloat16)
        .reshape(tok_count, kv_count, head_dim)
    )
    inv_query = rms_scale(query_raw)
    unit_query = query_raw * inv_query
    gain_query_f = gain_query.astype(jnp.float32)
    query_rot = rotate(unit_query * gain_query_f, cosine_query, sine_query).astype(jnp.bfloat16)
    inv_key = rms_scale(key_raw)
    unit_key = key_raw * inv_key
    gain_key_f = gain_key.astype(jnp.float32)
    key_rot = rotate(unit_key * gain_key_f, cosine_key, sine_key).astype(jnp.bfloat16)
    scores = contract(query_rot, key_rot, "tkgd,ukd->kgtu") * score_scale
    masked = jnp.where(allowed, scores, masked_fill)
    row_top = jnp.max(masked, axis=-1, keepdims=True)
    exponent = jnp.exp(masked - row_top)
    row_total = jnp.sum(exponent, axis=-1, keepdims=True)
    log_total = row_top + jnp.log(row_total)
    probs_low = (exponent / row_total).astype(jnp.bfloat16)
    mixed_heads = (
        contract(probs_low, value_rows, "kgtu,ukd->tkgd")
        .astype(jnp.bfloat16)
        .reshape(tok_count, head_count * head_dim)
    )
    resid_mid = resid_in + jnp.dot(mixed_heads, out_full, preferred_element_type=jnp.float32)
    largest_local = jnp.max(
        jnp.where(allowed & valid_row[:, None], scores, masked_fill), axis=(2, 3)
    ).reshape(head_count)
    largest = lax.pmax(largest_local, ("dp", "ep"))
    clip_factor = jnp.sqrt(clip_threshold / jnp.maximum(largest, clip_threshold))
    inv_two = rms_scale(resid_mid)
    unit_two = resid_mid * inv_two
    gain_two = gain_moe_full.astype(jnp.float32)
    normed_mid = (unit_two * gain_two).astype(jnp.bfloat16)
    logits = jnp.dot(normed_mid, router_full, preferred_element_type=jnp.float32)
    choose = expert_ids[:, :, None] == jnp.arange(experts, dtype=jnp.int32)[None, None, :]
    picked = jnp.sum(jnp.where(choose, logits[:, None, :], 0.0), axis=2)
    gate_weights = jax.nn.softmax(picked, axis=-1)
    flat_ids = expert_ids.reshape(-1)
    flat_hot = (flat_ids[:, None] == jnp.arange(experts, dtype=jnp.int32)[None, :]).astype(
        jnp.int32
    )
    slot_rank = jnp.sum((jnp.cumsum(flat_hot, axis=0) - 1) * flat_hot, axis=1)
    slot_index = flat_ids * capacity + slot_rank
    pair_token = jnp.arange(tok_count * top_count, dtype=jnp.int32) // top_count
    send_rows = (
        jnp.zeros((experts * capacity, model_width), jnp.bfloat16)
        .at[slot_index]
        .set(normed_mid[pair_token])
    )
    send_rows = send_rows.reshape(ep_count, exp_local, capacity, model_width)
    arrived = lax.all_to_all(send_rows, "ep", split_axis=0, concat_axis=0, tiled=True)
    gate_part = contract(arrived, gate_full, "secd,edf->secf")
    up_part = contract(arrived, up_full, "secd,edf->secf")
    hidden_mid = (jax.nn.silu(gate_part) * up_part).astype(jnp.bfloat16)
    produced = contract(hidden_mid, down_full, "secf,efd->secd").astype(jnp.bfloat16)
    returned = lax.all_to_all(produced, "ep", split_axis=0, concat_axis=0, tiled=True)
    returned, arrived, gate_part, up_part = (returned, arrived, gate_part, up_part)
    pair_out = (
        returned.reshape(experts * capacity, model_width)[slot_index]
        .reshape(tok_count, top_count, model_width)
        .astype(jnp.float32)
    )
    resid_out = resid_mid + jnp.sum(gate_weights[:, :, None] * pair_out, axis=1)
    out_rows = (resid_out * valid_col).astype(jnp.bfloat16)
    block_out = jnp.zeros_like(out_rows).at[local_order].set(out_rows)
    attn_params = (
        lax.all_gather(w_query, ("dp", "ep"), axis=0, tiled=True),
        lax.all_gather(w_key, ("dp", "ep"), axis=0, tiled=True),
        lax.all_gather(w_value, ("dp", "ep"), axis=0, tiled=True),
        lax.all_gather(w_out, ("dp", "ep"), axis=0, tiled=True),
        lax.all_gather(w_router, ("dp", "ep"), axis=0, tiled=True),
        lax.all_gather(gain_attn, ("dp", "ep"), axis=0, tiled=True),
        lax.all_gather(gain_moe, ("dp", "ep"), axis=0, tiled=True),
    )
    expert_params = (
        lax.all_gather(w_gate, "dp", axis=1, tiled=True),
        lax.all_gather(w_up, "dp", axis=1, tiled=True),
        lax.all_gather(w_down, "dp", axis=2, tiled=True),
    )
    query_full, key_full, value_full, out_full, router_full, gain_attn_full, gain_moe_full = (
        attn_params
    )
    gate_full, up_full, down_full = expert_params
    grad_mid_out = cotangent[local_order].astype(jnp.float32) * valid_col
    grad_gates = jnp.sum(grad_mid_out[:, None, :] * pair_out, axis=2)
    grad_pair = (gate_weights[:, :, None] * grad_mid_out[:, None, :]).astype(jnp.bfloat16)
    send_grads = (
        jnp.zeros((experts * capacity, model_width), jnp.bfloat16)
        .at[slot_index]
        .set(grad_pair.reshape(-1, model_width))
    )
    send_grads = send_grads.reshape(ep_count, exp_local, capacity, model_width)
    grad_arrived = lax.all_to_all(send_grads, "ep", split_axis=0, concat_axis=0, tiled=True)
    grad_hidden = contract(grad_arrived, down_full, "secd,efd->secf")
    sigmoid_gate = jax.nn.sigmoid(gate_part)
    silu_gate = jax.nn.silu(gate_part)
    grad_gate_part = (
        grad_hidden * up_part * sigmoid_gate * (1.0 + gate_part * (1.0 - sigmoid_gate))
    ).astype(jnp.bfloat16)
    grad_up_part = (grad_hidden * silu_gate).astype(jnp.bfloat16)
    grad_rows = (
        contract(grad_gate_part, gate_full, "secf,edf->secd")
        + contract(grad_up_part, up_full, "secf,edf->secd")
    ).astype(jnp.bfloat16)
    grad_back = lax.all_to_all(grad_rows, "ep", split_axis=0, concat_axis=0, tiled=True)
    hidden_mid = (silu_gate * up_part).astype(jnp.bfloat16)
    grad_gate_w = contract(arrived, grad_gate_part, "secd,secf->edf")
    grad_up_w = contract(arrived, grad_up_part, "secd,secf->edf")
    grad_down_w = contract(hidden_mid, grad_arrived, "secf,secd->efd")
    grad_gate, grad_up, grad_down = (
        lax.psum_scatter(
            grad_gate_w.astype(jnp.bfloat16), "dp", scatter_dimension=1, tiled=True
        ).astype(jnp.float32),
        lax.psum_scatter(
            grad_up_w.astype(jnp.bfloat16), "dp", scatter_dimension=1, tiled=True
        ).astype(jnp.float32),
        lax.psum_scatter(
            grad_down_w.astype(jnp.bfloat16), "dp", scatter_dimension=2, tiled=True
        ).astype(jnp.float32),
    )
    mean_term = jnp.sum(gate_weights * grad_gates, axis=1, keepdims=True)
    grad_picked = gate_weights * (grad_gates - mean_term)
    grad_logits = jnp.sum(jnp.where(choose, grad_picked[:, :, None], 0.0), axis=1).astype(
        jnp.bfloat16
    )
    grad_router_w = contract(normed_mid, grad_logits, "td,te->de")
    pair_grads = (
        grad_back.reshape(experts * capacity, model_width)[slot_index]
        .reshape(tok_count, top_count, model_width)
        .astype(jnp.float32)
    )
    grad_normed_mid = jnp.sum(pair_grads, axis=1) + contract(grad_logits, router_full, "te,de->td")
    grad_gain_moe_w = jnp.sum(grad_normed_mid * unit_two, axis=0)
    grad_mid = grad_mid_out + norm_back(grad_normed_mid * gain_two, unit_two, inv_two)
    grad_branch = grad_mid.astype(jnp.bfloat16)
    grad_out_w = contract(mixed_heads, grad_branch, "tq,td->qd")
    grad_mixed = (
        contract(grad_branch, out_full, "td,qd->tq")
        .astype(jnp.bfloat16)
        .reshape(tok_count, kv_count, group_size, head_dim)
    )
    scores_again = contract(query_rot, key_rot, "tkgd,ukd->kgtu") * score_scale
    probs_back = jnp.exp(jnp.where(allowed, scores_again, masked_fill) - log_total)
    grad_value_rows = contract(
        probs_back.astype(jnp.bfloat16), grad_mixed, "kgtu,tkgd->ukd"
    ).astype(jnp.bfloat16)
    grad_probs = contract(grad_mixed, value_rows, "tkgd,ukd->kgtu")
    grad_scores = (
        probs_back * (grad_probs - jnp.sum(probs_back * grad_probs, axis=-1, keepdims=True))
    ).astype(jnp.bfloat16)
    grad_query_rot = contract(grad_scores, key_rot, "kgtu,ukd->tkgd") * score_scale
    grad_key_rot = contract(grad_scores, query_rot, "kgtu,tkgd->ukd") * score_scale
    grad_query_normed = rotate_back(grad_query_rot, cosine_query, sine_query)
    grad_key_normed = rotate_back(grad_key_rot, cosine_key, sine_key)
    grad_gain_q = jnp.sum(grad_query_normed * unit_query, axis=(0, 1, 2))
    grad_gain_k = jnp.sum(grad_key_normed * unit_key, axis=(0, 1))
    grad_query_raw = (
        norm_back(grad_query_normed * gain_query_f, unit_query, inv_query)
        .astype(jnp.bfloat16)
        .reshape(tok_count, head_count * head_dim)
    )
    grad_key_raw = (
        norm_back(grad_key_normed * gain_key_f, unit_key, inv_key)
        .astype(jnp.bfloat16)
        .reshape(tok_count, kv_count * head_dim)
    )
    grad_value_flat = grad_value_rows.reshape(tok_count, kv_count * head_dim)
    grad_query_w = contract(normed_in, grad_query_raw, "td,tq->dq")
    grad_key_w = contract(normed_in, grad_key_raw, "td,tq->dq")
    grad_value_w = contract(normed_in, grad_value_flat, "td,tq->dq")
    grad_normed_in = (
        contract(grad_query_raw, query_full, "tq,dq->td")
        + contract(grad_key_raw, key_full, "tq,dq->td")
        + contract(grad_value_flat, value_full, "tq,dq->td")
    )
    grad_gain_attn_w = jnp.sum(grad_normed_in * unit_one, axis=0)
    grad_resid_in = grad_mid + norm_back(grad_normed_in * gain_one, unit_one, inv_one)
    grad_input = jnp.zeros_like(grad_resid_in).at[local_order].set(grad_resid_in)
    grad_sums = (
        lax.psum_scatter(grad_query_w, ("dp", "ep"), scatter_dimension=0, tiled=True),
        lax.psum_scatter(grad_key_w, ("dp", "ep"), scatter_dimension=0, tiled=True),
        lax.psum_scatter(grad_value_w, ("dp", "ep"), scatter_dimension=0, tiled=True),
        lax.psum_scatter(grad_out_w, ("dp", "ep"), scatter_dimension=0, tiled=True),
        lax.psum_scatter(grad_router_w, ("dp", "ep"), scatter_dimension=0, tiled=True),
        lax.psum_scatter(grad_gain_attn_w, ("dp", "ep"), scatter_dimension=0, tiled=True),
        lax.psum_scatter(grad_gain_moe_w, ("dp", "ep"), scatter_dimension=0, tiled=True),
    )
    gain_sums = lax.psum((grad_gain_q, grad_gain_k), ("dp", "ep"))
    return (
        block_out,
        grad_input,
        grad_sums[0],
        grad_sums[1],
        grad_sums[2],
        grad_sums[3],
        grad_sums[4],
        grad_sums[5],
        grad_sums[6],
        gain_sums[0],
        gain_sums[1],
        grad_gate,
        grad_up,
        grad_down,
        clip_factor,
    )


MESH = pl.DeviceIdType.MESH


def place():
    dp = lax.axis_index("dp")
    ep = lax.axis_index("ep")
    z, y = dp // 2, dp % 2
    x, c = ep // 2, ep % 2
    first = (1 - c) * y + c * x
    second = (1 - c) * x + c * y
    return dp, ep, z, y, x, c, first, second


def targets(dp, ep, z, y, x, c, nz):
    up = (jnp.where(z < nz - 1, dp + 2, dp), ep)
    down = (jnp.where(z > 0, dp - 2, dp), ep)
    turn_y, turn_x = 1 - 2 * y, 2 - 4 * x
    near = (dp + (1 - c) * turn_y, ep + c * turn_x)
    far = (dp + c * turn_y, ep + (1 - c) * turn_x)
    twin = (dp, ep + 1 - 2 * c)
    return up, down, near, far, twin


def slot(z, first, second, c):
    return z * 8 + first * (4 - 2 * c) + second * (2 + 2 * c) + c


def greet(nz, z, dp, ep, ways, everyone):
    barrier = pltpu.get_barrier_semaphore()
    if everyone:
        total = nz * 8
        me = dp * 4 + ep

        def hello(step, carry):
            other = (me + step) % total
            pl.semaphore_signal(
                barrier, inc=1, device_id=(other // 4, other % 4), device_id_type=MESH
            )
            return carry

        lax.fori_loop(1, total, hello, 0)
        pl.semaphore_wait(barrier, total - 1)
        return
    for step in range(1, nz):
        other = ((z + step) % nz) * 2 + dp % 2
        pl.semaphore_signal(barrier, inc=1, device_id=(other, ep), device_id_type=MESH)
    for other in ways[2:]:
        pl.semaphore_signal(barrier, inc=1, device_id=other, device_id_type=MESH)
    pl.semaphore_wait(barrier, nz + 2)


class Riders:
    def __init__(self, kinds, nz, spot, refs):
        count = len(kinds)
        self.kinds, self.nz = kinds, nz
        self.dp, self.ep, self.z, self.y = spot
        self.me = self.dp * 4 + self.ep
        self.over_y = (self.dp + 1 - 2 * self.y, self.ep)
        self.ins, self.outs = refs[:count], refs[count : 2 * count]
        self.send, self.onward, self.recv, self.own = refs[2 * count :] if count else (None,) * 4
        self.spans = []
        for kind in kinds:
            if kind in ("all", "same"):
                self.spans.append((1, 8 * nz))
            else:
                self.spans.append((1 if kind in ("line", "cube") else 0, nz))
        self.steps = [(r, k) for r in range(count) for k in range(*self.spans[r])]
        self.steps.sort(key=lambda step: step[1] / self.spans[step[0]][1])
        self.cubes = [r for r in range(count) if kinds[r] == "cube"]

    def remote(self, source, target, send, recv, device):
        return pltpu.make_async_remote_copy(
            src_ref=source, dst_ref=target, send_sem=send, recv_sem=recv,
            device_id=device, device_id_type=MESH)

    def copy(self, r, step):
        kind, source, target = self.kinds[r], self.ins[r], self.outs[r]
        if kind in ("all", "same"):
            other = (self.me + step) % (8 * self.nz)
            source = source if kind == "same" else source.at[other]
            target, key, device = target.at[self.me], self.me, (other // 4, other % 4)
        elif kind in ("line", "cube"):
            other = (self.z + step) % self.nz
            source, key, device = source.at[other], self.z, (other * 2 + self.y, self.ep)
            target = target.at[self.z] if kind == "line" else target.at[self.z, self.y]
        else:
            source = source.at[step, 1 - self.y] if kind == "half" else source.at[step]
            target, key, device = target.at[step], step, self.over_y
        return self.remote(source, target, self.send.at[r, step], self.recv.at[r, key], device)

    def arrival(self, r, step):
        kind, target = self.kinds[r], self.outs[r]
        if kind in ("all", "same"):
            key = (self.me + step) % (8 * self.nz)
            target = target.at[key]
        elif kind in ("line", "cube"):
            key = (self.z + self.nz - step) % self.nz
            target = target.at[key] if kind == "line" else target.at[key, self.y]
        else:
            key, target = step, target.at[step]
        return self.remote(target, target, self.send.at[r, step], self.recv.at[r, key], self.over_y)

    def passing(self, r, step, first=False):
        key = (self.z + self.nz - step) % self.nz
        target = self.outs[r].at[key, self.y]
        source = self.ins[r].at[key] if first else target
        return self.remote(
            source, target, self.onward.at[r, step], self.recv.at[r, self.nz + key], self.over_y)

    def passed(self, r, step):
        key = (self.z + self.nz - step) % self.nz
        target = self.outs[r].at[key, 1 - self.y]
        return self.remote(
            target, target, self.onward.at[r, step], self.recv.at[r, self.nz + key], self.over_y)

    def own_copy(self, r):
        kind, source, target = self.kinds[r], self.ins[r], self.outs[r]
        if kind in ("all", "same"):
            source = source if kind == "same" else source.at[self.me]
            target = target.at[self.me]
        else:
            source = source.at[self.z]
            target = target.at[self.z] if kind == "line" else target.at[self.z, self.y]
        return pltpu.make_async_copy(source, target, self.own.at[r])

    def begin(self):
        for r, kind in enumerate(self.kinds):
            if kind not in ("half", "across"):
                self.own_copy(r).start()
            if kind == "cube":
                self.passing(r, 0, True).start()

    def some(self, share, shares):
        total = len(self.steps)
        for r, k in self.steps[total * share // shares : total * (share + 1) // shares]:
            self.copy(r, k).start()

    def onwards(self, step):
        for r in self.cubes:
            self.arrival(r, step).wait_recv()
            self.passing(r, step).start()

    def looped(self, step, steps):
        for r in range(len(self.kinds)):
            first, last = self.spans[r]
            per = -(-(last - first) // steps)
            for k in range(per):
                piece = first + step * per + k

                @pl.when(piece < last)
                def _():
                    self.copy(r, piece).start()

    def finish(self):
        for r, kind in enumerate(self.kinds):

            def settle(step, carry):
                if kind != "cube":
                    self.arrival(r, step).wait_recv()
                self.copy(r, step).wait_send()
                return carry

            lax.fori_loop(*self.spans[r], settle, 0)
            if kind == "cube":

                def settle_y(step, carry):
                    self.passed(r, step).wait_recv()
                    self.passing(r, step).wait_send()
                    return carry

                lax.fori_loop(0, self.nz, settle_y, 0)
            if kind not in ("half", "across"):
                self.own_copy(r).wait()


def rider_shapes(riders, devices):
    kinds = tuple(kind for kind, _ in riders)
    arrays = tuple(array for _, array in riders)
    outs = []
    for kind, v in riders:
        shape = v.shape
        if kind == "same":
            shape = (devices,) + shape
        elif kind == "cube":
            shape = shape[:1] + (2,) + shape[1:]
        elif kind == "half":
            shape = shape[:1] + shape[2:]
        outs.append(jax.ShapeDtypeStruct(shape, v.dtype))
    dma = pltpu.SemaphoreType.DMA
    count = len(riders)
    sems = [dma((count, devices))] * 3 + [dma((count,))] if count else []
    return kinds, arrays, tuple(outs), sems


def rider_specs(kinds):
    return [
        pl.BlockSpec(memory_space=pl.ANY if kind in ("half", "across") else pltpu.VMEM)
        for kind in kinds
    ]


def wide_greeting(kinds):
    return "all" in kinds or "same" in kinds


def on(allowed, action):
    if allowed is None:
        action()
    else:
        pl.when(allowed)(action)


def along(z, nz, step):
    if step == 0:
        yield None, z
    else:
        yield z >= step, jnp.maximum(z - step, 0)
        yield z + step < nz, jnp.minimum(z + step, nz - 1)


class Mover:
    def __init__(self, ins, outs, ways, sems):
        self.ins, self.outs, self.ways = ins, outs, ways
        self.send, self.recv, self.own = sems
        self.pending, self.own_copies = [], []

    def push(self, way, where, allowed=None, own=False):
        for k, out in enumerate(self.outs):
            copy = pltpu.make_async_remote_copy(
                src_ref=self.ins[k] if own else out.at[where],
                dst_ref=out.at[where],
                send_sem=self.send.at[k, way, where],
                recv_sem=self.recv.at[k, where],
                device_id=self.ways[way],
                device_id_type=MESH,
            )
            on(allowed, copy.start)
            self.pending.append((allowed, copy))

    def arrive(self, where):
        for k, out in enumerate(self.outs):
            pltpu.make_async_remote_copy(
                src_ref=out.at[where],
                dst_ref=out.at[where],
                send_sem=self.send.at[k, 0, where],
                recv_sem=self.recv.at[k, where],
                device_id=self.ways[-1],
                device_id_type=MESH,
            ).wait_recv()

    def keep(self, mine):
        for k, out in enumerate(self.outs):
            copy = pltpu.make_async_copy(self.ins[k], out.at[mine], self.own.at[k])
            copy.start()
            self.own_copies.append(copy)

    def settle(self):
        for allowed, copy in self.pending:
            on(allowed, copy.wait_send)
        for copy in self.own_copies:
            copy.wait()


class WholeGather(Mover):
    def begin(self, nz, z, a, b, c):
        self.nz, self.z, self.a, self.b, self.c = nz, z, a, b, c
        mine = slot(z, a, b, c)
        self.push(0, mine, z < nz - 1, True)
        self.push(1, mine, z > 0, True)
        for way in (2, 3, 4):
            self.push(way, mine, None, True)
        self.keep(mine)

    def turn(self, turn):
        nz, z, a, b, c = self.nz, self.z, self.a, self.b, self.c
        if turn < nz:
            for index, (allowed, zz) in enumerate(along(z, nz, turn)):
                where = slot(zz, a, b, c)
                on(allowed, functools.partial(self.arrive, where))
                self.push(index, where, allowed & ((z > 0) if index else (z < nz - 1)))
                for way in (2, 3, 4):
                    self.push(way, where, allowed)
        if turn - 1 < nz:
            for allowed, zz in along(z, nz, turn - 1):
                where = slot(zz, 1 - a, b, c)
                on(allowed, functools.partial(self.arrive, where))
                for way in (3, 4):
                    self.push(way, where, allowed)
            for allowed, zz in along(z, nz, turn - 1):
                where = slot(zz, a, 1 - b, c)
                on(allowed, functools.partial(self.arrive, where))
                self.push(4, where, allowed)
        if turn >= 2:
            for allowed, zz in along(z, nz, turn - 2):
                where = slot(zz, 1 - a, 1 - b, c)
                on(allowed, functools.partial(self.arrive, where))
                self.push(4, where, allowed)

    def end(self):
        for zz in range(self.nz):
            for aa in range(2):
                for bb in range(2):
                    self.arrive(slot(zz, aa, bb, 1 - self.c))
        self.settle()


class SlabGather(Mover):
    def begin(self, nz, z, ep, x, c):
        self.nz, self.z, self.ep, self.c = nz, z, ep, c
        self.other = ep + 2 - 4 * x
        mine = z * 4 + ep
        self.push(0, mine, z < nz - 1, True)
        self.push(1, mine, z > 0, True)
        for way in (2, 3):
            self.push(way, mine, None, True)
        self.keep(mine)

    def turn(self, turn):
        nz, z = self.nz, self.z
        if turn < nz:
            for index, (allowed, zz) in enumerate(along(z, nz, turn)):
                where = zz * 4 + self.ep
                on(allowed, functools.partial(self.arrive, where))
                self.push(index, where, allowed & ((z > 0) if index else (z < nz - 1)))
                for way in (2, 3):
                    self.push(way, where, allowed)
        if turn - 1 < nz:
            for allowed, zz in along(z, nz, turn - 1):
                where = zz * 4 + self.other
                on(allowed, functools.partial(self.arrive, where))
                self.push(3, where, allowed)

    def end(self):
        for where in range(4 * self.nz):
            pl.when(where % 2 != self.c)(functools.partial(self.arrive, where))
        self.settle()


def gather_kernel(nz, counts, kinds, *refs):
    whole, slabs = counts
    count, extra = whole + slabs, len(kinds)
    ins = refs[:count]
    outs = refs[count + extra : 2 * count + extra]
    sems = refs[2 * (count + extra) :]
    dp, ep, z, y, x, c, a, b = place()
    ways = targets(dp, ep, z, y, x, c, nz)
    up, down, near, far, twin = ways
    side = (dp, ep + 2 - 4 * x)
    movers = []
    if whole:
        movers.append(WholeGather(ins[:whole], outs[:whole], ways, sems[:3]))
        sems = sems[3:]
    if slabs:
        movers.append(SlabGather(ins[whole:], outs[whole:], (up, down, side, twin), sems[:3]))
        sems = sems[3:]
    riders = Riders(
        kinds, nz, (dp, ep, z, y),
        refs[count : count + extra] + refs[2 * count + extra : 2 * (count + extra)] + sems,
    )
    greet(nz, z, dp, ep, ways, wide_greeting(kinds))
    for mover in movers:
        if isinstance(mover, WholeGather):
            mover.begin(nz, z, a, b, c)
        else:
            mover.begin(nz, z, ep, x, c)
    riders.begin()
    riders.some(0, 1)
    for turn in range(1, nz + 2):
        for mover in movers:
            mover.turn(turn)
        if 2 <= turn <= nz:
            riders.onwards(turn - 1)
    for mover in movers:
        mover.end()
    riders.finish()


def gather_rows(whole, slabs, devices, ident, riders=()):
    arrays = whole + slabs
    nz = devices // 8
    kinds, ridden, rider_outs, rider_sems = rider_shapes(riders, devices)
    blocks = (devices,) * len(whole) + (4 * nz,) * len(slabs)
    dma = pltpu.SemaphoreType.DMA
    sems = []
    for count, ways, total in ((len(whole), 5, devices), (len(slabs), 4, 4 * nz)):
        if count:
            sems += [dma((count, ways, total)), dma((count, total)), dma((count,))]
    return pl.pallas_call(
        functools.partial(gather_kernel, nz, (len(whole), len(slabs)), kinds),
        out_shape=tuple(
            jax.ShapeDtypeStruct((total,) + v.shape, v.dtype) for total, v in zip(blocks, arrays)
        )
        + rider_outs,
        in_specs=[pl.BlockSpec(memory_space=pltpu.VMEM)] * len(arrays) + rider_specs(kinds),
        out_specs=tuple(pl.BlockSpec(memory_space=pl.ANY) for v in arrays + ridden),
        scratch_shapes=sems + rider_sems,
        compiler_params=pltpu.CompilerParams(collective_id=ident, has_side_effects=True),
        name="gather_rows_%d" % ident,
    )(*arrays, *ridden)


def scatter_kernel(nz, turned, kinds, *refs):
    extra = len(kinds)
    left_ref, right_ref = refs[:2]
    refs = refs[2:]
    out_ref = refs[extra]
    sent, got, from_far, from_near, rising, falling = refs[2 * extra + 1 : 2 * extra + 7]
    (twin_send, twin_recv, far_send, far_recv, near_send, near_recv, line_send, up_recv,
     down_recv) = refs[2 * extra + 7 : 2 * extra + 16]
    dp, ep, z, y, x, c, a, b = place()
    ways = targets(dp, ep, z, y, x, c, nz)
    up, down, near, far, twin = ways
    riders = Riders(
        kinds, nz, (dp, ep, z, y),
        refs[:extra] + refs[extra + 1 : 2 * extra + 1] + refs[2 * extra + 16 :]
    )
    greet(nz, z, dp, ep, ways, wide_greeting(kinds))
    riders.begin()
    per = 4 * nz

    def zed(step):
        if nz == 4:
            far_one = jnp.where(z < 2, 3, 0)
            second = jnp.where(z < 2, 2 - 2 * z, 7 - 2 * z)
            third = 1 + z % 2
            return jnp.where(step == 0, far_one, jnp.where(step == 1, second, jnp.where(step == 2, third, z)))
        return (z + 1 + step) % nz

    def term(where):
        sides = (((1,), (1 if turned else 0,)), ((), ()))
        return lax.dot_general(
            left_ref[where], right_ref[...], sides, preferred_element_type=jnp.float32
        )

    def order(index, aa, bb, cc):
        part = index // nz
        flip_b = 1 - part // 2
        flip_a = 1 - part % 2
        return slot(zed(index % nz), aa + flip_a * (1 - 2 * aa), bb + flip_b * (1 - 2 * bb), cc)

    def twin_copy(index):
        return pltpu.make_async_remote_copy(
            src_ref=sent.at[index], dst_ref=got.at[index], send_sem=twin_send.at[index],
            recv_sem=twin_recv.at[index], device_id=twin, device_id_type=MESH)

    def far_copy(index):
        return pltpu.make_async_remote_copy(
            src_ref=got.at[index], dst_ref=from_far.at[index], send_sem=far_send.at[index],
            recv_sem=far_recv.at[index], device_id=far, device_id_type=MESH)

    def near_copy(index):
        return pltpu.make_async_remote_copy(
            src_ref=got.at[2 * nz + index], dst_ref=from_near.at[index], send_sem=near_send.at[index],
            recv_sem=near_recv.at[index], device_id=near, device_id_type=MESH)

    def up_copy(index, zz):
        return pltpu.make_async_remote_copy(
            src_ref=got.at[3 * nz + index], dst_ref=rising.at[zz], send_sem=line_send.at[index],
            recv_sem=up_recv.at[zz], device_id=up, device_id_type=MESH)

    def down_copy(index, zz):
        return pltpu.make_async_remote_copy(
            src_ref=got.at[3 * nz + index], dst_ref=falling.at[zz], send_sem=line_send.at[index],
            recv_sem=down_recv.at[zz], device_id=down, device_id_type=MESH)

    def give(index):
        sent[index] = term(order(index, b, a, 1 - c)).astype(sent.dtype)
        twin_copy(index).start()

    def taken(index):
        value = term(order(index, a, b, c))
        twin_copy(index).wait_recv()
        return value + got[index].astype(jnp.float32)

    def far_step(step, carry):
        give(2 * step)
        give(2 * step + 1)
        got[step] = taken(step).astype(got.dtype)
        far_copy(step).start()
        riders.looped(step, 2 * nz)
        return carry

    lax.fori_loop(0, 2 * nz, far_step, 0)

    def near_step(step, carry):
        value = taken(2 * nz + step)
        far_copy(step).wait_recv()
        value = value + from_far[step].astype(jnp.float32)
        got[2 * nz + step] = value.astype(got.dtype)
        near_copy(step).start()
        return carry

    lax.fori_loop(0, nz, near_step, 0)

    def line_step(step, carry):
        zz = zed(step)
        value = taken(3 * nz + step)
        far_copy(nz + step).wait_recv()
        near_copy(step).wait_recv()
        out_ref[...] = value + from_far[nz + step].astype(jnp.float32) + from_near[step].astype(jnp.float32)

        @pl.when((zz >= z) & (z > 0))
        def _():
            up_copy(step, zz).wait_recv()
            out_ref[...] += rising[zz].astype(jnp.float32)

        @pl.when((zz <= z) & (z < nz - 1))
        def _():
            down_copy(step, zz).wait_recv()
            out_ref[...] += falling[zz].astype(jnp.float32)

        @pl.when(zz > z)
        def _():
            got[3 * nz + step] = out_ref[...].astype(got.dtype)
            up_copy(step, zz).start()

        @pl.when(zz < z)
        def _():
            got[3 * nz + step] = out_ref[...].astype(got.dtype)
            down_copy(step, zz).start()

        return carry

    lax.fori_loop(0, nz, line_step, 0)

    def finish(step, carry):
        twin_copy(step).wait_send()
        return carry

    lax.fori_loop(0, per, finish, 0)

    def finish_far(step, carry):
        far_copy(step).wait_send()
        return carry

    lax.fori_loop(0, 2 * nz, finish_far, 0)

    def finish_near(step, carry):
        near_copy(step).wait_send()

        @pl.when(step < nz - 1)
        def _():
            up_copy(step, 0).wait_send()

        return carry

    lax.fori_loop(0, nz, finish_near, 0)
    riders.finish()


def scatter_sum(left, right, devices, ident, turned=False, riders=()):
    nz = devices // 8
    rows = left.shape[0] // devices
    depth, wide = right.shape[::-1] if turned else right.shape
    kinds, ridden, rider_outs, rider_sems = rider_shapes(riders, devices)
    block = (rows, wide)
    low = jnp.bfloat16
    dma = pltpu.SemaphoreType.DMA
    result = pl.pallas_call(
        functools.partial(scatter_kernel, nz, turned, kinds),
        out_shape=(jax.ShapeDtypeStruct(block, jnp.float32),) + rider_outs,
        in_specs=[pl.BlockSpec(memory_space=pltpu.VMEM)] * 2 + rider_specs(kinds),
        out_specs=(pl.BlockSpec(memory_space=pltpu.VMEM),)
        + (pl.BlockSpec(memory_space=pl.ANY),) * len(riders),
        scratch_shapes=[
            pltpu.VMEM((4 * nz,) + block, low),
            pltpu.VMEM((4 * nz,) + block, low),
            pltpu.VMEM((2 * nz,) + block, low),
            pltpu.VMEM((nz,) + block, low),
            pltpu.VMEM((nz,) + block, low),
            pltpu.VMEM((nz,) + block, low),
            dma((4 * nz,)), dma((4 * nz,)), dma((2 * nz,)), dma((2 * nz,)),
            dma((nz,)), dma((nz,)), dma((nz,)), dma((nz,)), dma((nz,)),
        ]
        + rider_sems,
        compiler_params=pltpu.CompilerParams(
            collective_id=ident, has_side_effects=True, vmem_limit_bytes=58 * 2**20),
        name="scatter_sum_%d" % ident,
    )(left.reshape(devices, rows, depth), right, *ridden)
    return result if riders else result[0]


class SlabSum:
    def __init__(self, nz, turned, spot, ways, refs, buffers):
        self.nz, self.turned = nz, turned
        self.z, self.x, self.c = spot
        self.up, self.down, self.side, self.twin = ways
        self.lefts, self.rights, self.beside, self.out = refs
        (self.sent, self.got, self.from_side, self.rising, self.falling, self.held,
         self.twin_send, self.twin_recv, self.side_send, self.side_recv, self.line_send,
         self.up_recv, self.down_recv) = buffers
        self.plain = self.rights[0].shape[0 if turned else 1]
        self.span = 512 if self.plain % 512 == 0 else self.plain

    def zed(self, step):
        z, nz = self.z, self.nz
        if nz == 4:
            far_one = jnp.where(z < 2, 3, 0)
            second = jnp.where(z < 2, 2 - 2 * z, 7 - 2 * z)
            third = 1 + z % 2
            return jnp.where(step == 0, far_one, jnp.where(step == 1, second, jnp.where(step == 2, third, z)))
        return (z + 1 + step) % nz

    def order(self, index, cc):
        flip = 1 - index // self.nz
        return self.zed(index % self.nz) * 4 + (self.x + flip * (1 - 2 * self.x)) * 2 + cc

    def combine(self, targets_, wheres, added):
        rows = self.lefts[0].shape[1]

        def put(which, at, total):
            for ref in added[which]:
                total = total + ref[:, at].astype(jnp.float32)
            targets_[which][:, at] = total.astype(targets_[which].dtype)

        def fill(chunk, carry):
            at = pl.ds(pl.multiple_of(chunk * self.span, self.span), self.span)
            total = None
            for left_ref, right_ref in zip(self.lefts, self.rights):
                value = lax.dot_general(
                    jnp.concatenate([left_ref[where] for where in wheres], axis=0),
                    right_ref[at, :] if self.turned else right_ref[:, at],
                    (((1,), (1 if self.turned else 0,)), ((), ())),
                    preferred_element_type=jnp.float32,
                )
                total = value if total is None else total + value
            for which in range(len(wheres)):
                put(which, at, total[which * rows : (which + 1) * rows])
            return carry

        lax.fori_loop(0, self.plain // self.span, fill, 0)
        if self.beside is not None:
            at = pl.ds(self.plain, self.beside.shape[2])
            for which, where in enumerate(wheres):
                put(which, at, self.beside[where].astype(jnp.float32))

    def remote(self, source, target, send, recv, device):
        return pltpu.make_async_remote_copy(
            src_ref=source, dst_ref=target, send_sem=send, recv_sem=recv,
            device_id=device, device_id_type=MESH)

    def twin_copy(self, index):
        return self.remote(
            self.sent.at[index], self.got.at[index], self.twin_send.at[index],
            self.twin_recv.at[index], self.twin)

    def side_copy(self, index):
        return self.remote(
            self.got.at[index], self.from_side.at[index], self.side_send.at[index],
            self.side_recv.at[index], self.side)

    def line_copy(self, index, zz, rise):
        place_, recv = (self.rising, self.up_recv) if rise else (self.falling, self.down_recv)
        return self.remote(
            self.got.at[self.nz + index], place_.at[zz], self.line_send.at[index], recv.at[zz],
            self.up if rise else self.down)

    def give(self, pair, carry):
        both = (2 * pair, 2 * pair + 1)
        self.combine(
            [self.sent.at[index] for index in both],
            [self.order(index, 1 - self.c) for index in both], [(), ()])
        for index in both:
            self.twin_copy(index).start()
        return carry

    def to_side(self, pair):
        lax.fori_loop(2 * pair, 2 * pair + 2, self.give, 0)
        both = (2 * pair, 2 * pair + 1)
        for index in both:
            self.twin_copy(index).wait_recv()
        self.combine(
            [self.got.at[index] for index in both],
            [self.order(index, self.c) for index in both],
            [(self.got.at[index],) for index in both])
        for index in both:
            self.side_copy(index).start()

    def to_line(self, pair):
        both = (2 * pair, 2 * pair + 1)
        for step in both:
            self.twin_copy(self.nz + step).wait_recv()
            self.side_copy(step).wait_recv()
        self.combine(
            [self.held.at[0], self.held.at[1]],
            [self.order(self.nz + step, self.c) for step in both],
            [(self.got.at[self.nz + step], self.from_side.at[step]) for step in both])
        for which, step in enumerate(both):
            self.along_line(self.held.at[which], step)

    def along_line(self, held, step):
        z, zz = self.z, self.zed(step)

        @pl.when((zz >= z) & (z > 0))
        def _():
            self.line_copy(step, zz, True).wait_recv()
            held[...] += self.rising[zz].astype(jnp.float32)

        @pl.when((zz <= z) & (z < self.nz - 1))
        def _():
            self.line_copy(step, zz, False).wait_recv()
            held[...] += self.falling[zz].astype(jnp.float32)

        @pl.when(zz != z)
        def _():
            self.got[self.nz + step] = held[...].astype(self.got.dtype)

        pl.when(zz > z)(lambda: self.line_copy(step, zz, True).start())
        pl.when(zz < z)(lambda: self.line_copy(step, zz, False).start())

    def end(self):
        self.out[...] = self.held[1]

        def finish(step, carry):
            self.twin_copy(step).wait_send()
            return carry

        lax.fori_loop(0, 2 * self.nz, finish, 0)

        def finish_side(step, carry):
            self.side_copy(step).wait_send()

            @pl.when(step < self.nz - 1)
            def _():
                self.line_copy(step, 0, True).wait_send()

            return carry

        lax.fori_loop(0, self.nz, finish_side, 0)


def slab_scatter_kernel(nz, forms, kinds, *refs):
    extra, parts = len(kinds), len(forms)
    refs = list(refs)

    def take(count):
        taken = tuple(refs[:count])
        del refs[:count]
        return taken

    operands = []
    for pairs, turned, beside in forms:
        operands.append((take(pairs), take(pairs), take(1)[0] if beside else None))
    rider_ins = take(extra)
    outs = take(parts)
    rider_outs = take(extra)
    dp, ep, z, y, x, c, _, _ = place()
    up, down, near, far, twin = targets(dp, ep, z, y, x, c, nz)
    side = (dp, ep + 2 - 4 * x)
    sums = [
        SlabSum(nz, form[1], (z, x, c), (up, down, side, twin), held + (out,), take(13))
        for form, held, out in zip(forms, operands, outs)
    ]
    riders = Riders(kinds, nz, (dp, ep, z, y), rider_ins + rider_outs + tuple(refs))
    greet(nz, z, dp, ep, (up, down, near, far, twin), wide_greeting(kinds))
    riders.begin()

    def side_step(pair, carry):
        for part in sums:
            part.to_side(pair)
        riders.looped(pair, nz // 2)
        return carry

    lax.fori_loop(0, nz // 2, side_step, 0)

    def line_step(pair, carry):
        for part in sums:
            part.to_line(pair)
        return carry

    lax.fori_loop(0, nz // 2, line_step, 0)
    for part in sums:
        part.end()
    riders.finish()


def slab_scatter(parts, devices, ident, riders=()):
    nz = devices // 8
    blocks = 4 * nz
    rows = parts[0][0][0].shape[0] // blocks
    kinds, ridden, rider_outs, rider_sems = rider_shapes(riders, devices)
    low, dma = jnp.bfloat16, pltpu.SemaphoreType.DMA
    operands, outs, scratch, forms = (), (), [], []
    for lefts, rights, turned, beside in parts:
        held = () if beside is None else (beside.reshape(blocks, rows, -1),)
        wide = rights[0].shape[0 if turned else 1] + sum(v.shape[2] for v in held)
        block = (rows, wide)
        operands += tuple(v.reshape(blocks, rows, -1) for v in lefts) + tuple(rights) + held
        outs += (jax.ShapeDtypeStruct(block, jnp.float32),)
        scratch += [pltpu.VMEM((count * nz,) + block, low) for count in (2, 2, 1, 1, 1)]
        scratch += [pltpu.VMEM((2,) + block, jnp.float32)]
        scratch += [dma((2 * nz,))] * 2 + [dma((nz,))] * 5
        forms.append((len(lefts), turned, len(held)))
    return pl.pallas_call(
        functools.partial(slab_scatter_kernel, nz, tuple(forms), kinds),
        out_shape=outs + rider_outs,
        in_specs=[pl.BlockSpec(memory_space=pltpu.VMEM)] * len(operands) + rider_specs(kinds),
        out_specs=(pl.BlockSpec(memory_space=pltpu.VMEM),) * len(outs)
        + (pl.BlockSpec(memory_space=pl.ANY),) * len(riders),
        scratch_shapes=scratch + rider_sems,
        compiler_params=pltpu.CompilerParams(
            collective_id=ident, has_side_effects=True, vmem_limit_bytes=63 * 2**20),
        name="slab_scatter_%d" % ident,
    )(*operands, *ridden)


def whole_rows(mesh):
    return mesh.shape["ep"] == 4 and mesh.shape["dp"] in (4, 8)


def exact_dot(left_side, right_side):
    return jnp.dot(
        left_side, right_side, precision=lax.Precision.HIGHEST, preferred_element_type=jnp.float32
    )


def block_layout(lens, tok_count):
    ends = [lens[:, :1]]
    for at in range(1, lens.shape[1]):
        ends.append(ends[-1] + lens[:, at : at + 1])
    row_index = lax.broadcasted_iota(jnp.int32, (lens.shape[0], tok_count), 1)
    segment = jnp.zeros_like(row_index)
    first_row = jnp.zeros_like(row_index)
    for end in ends:
        passed = row_index >= end
        segment = segment + passed.astype(jnp.int32)
        first_row = jnp.where(passed, end, first_row)
    return (segment, row_index - first_row)


def by_experts(
    hidden_in,
    cotangent,
    deal_order,
    seq_lengths,
    expert_ids,
    w_query,
    w_key,
    w_value,
    w_out,
    w_router,
    gain_attn,
    gain_moe,
    gain_query,
    gain_key,
    w_gate,
    w_up,
    w_down,
    clip_threshold,
):
    f32, low = jnp.float32, jnp.bfloat16
    dp_count, ep_count = lax.axis_size("dp"), lax.axis_size("ep")
    devices = dp_count * ep_count
    dp, ep = lax.axis_index("dp"), lax.axis_index("ep")
    me = dp * ep_count + ep
    tok_count, width = hidden_in.shape
    row_count = tok_count * 7 // 8
    all_count = devices * row_count
    head_dim = gain_query.shape[0]
    half_dim = head_dim // 2
    rows_own = w_query.shape[0]
    head_count = w_query.shape[1] // head_dim
    kv_count = w_key.shape[1] // head_dim
    group_size = head_count // kv_count
    experts = w_router.shape[1]
    exp_local, wide_own, hidden = w_gate.shape
    lines = dp_count // 2
    slab = lines * ep_count
    z, y = dp // 2, dp % 2
    score_scale = head_dim ** (-0.5)

    gain_col = gain_attn.astype(f32)[:, None]
    heads_in = (w_query.astype(f32) * gain_col).astype(low).reshape(rows_own, head_count, head_dim)
    keys_in = (w_key.astype(f32) * gain_col).astype(low).reshape(rows_own, kv_count, head_dim)
    values_in = (w_value.astype(f32) * gain_col).astype(low).reshape(rows_own, kv_count, head_dim)
    sent_heads = jnp.concatenate(
        [heads_in, jnp.repeat(keys_in, group_size, axis=1), jnp.repeat(values_in, group_size, axis=1)],
        axis=2,
    ).transpose(1, 0, 2)

    local_order = deal_order % tok_count
    deal = (local_order[:, None] == jnp.arange(tok_count, dtype=jnp.int32)[None, :]).astype(low)
    deal = deal[:row_count]
    resid_in = jnp.dot(deal, hidden_in, preferred_element_type=f32)
    grad_mid_out = jnp.dot(deal, cotangent, preferred_element_type=f32)
    inv_one = rms_scale(resid_in)
    unit_one = resid_in * inv_one
    lens_row = jnp.pad(seq_lengths.astype(f32), ((0, 0), (0, 128 - seq_lengths.shape[1])))
    gain_row = jnp.pad(gain_moe.astype(f32)[None, :], ((0, 0), (0, 128 - rows_own)))
    router_rows = w_router.astype(f32).reshape(-1, 128)
    note_one = jnp.concatenate([lens_row, gain_row, router_rows], axis=0)
    note_one = jnp.pad(note_one, ((0, -note_one.shape[0] % 8), (0, 0)))
    unit_all, notes, grad_all, w_heads, w_rise_up = gather_rows(
        (unit_one.astype(low), note_one),
        (grad_mid_out.astype(low),),
        devices,
        1,
        (("all", sent_heads), ("cube", w_up)),
    )
    w_heads = w_heads.reshape(width, 3 * head_dim)
    w_rise_up = w_rise_up.reshape(width, hidden)
    lens_all = notes[:, 0, : seq_lengths.shape[1]].astype(jnp.int32)
    gain_two = notes[:, 1, :rows_own].reshape(1, width)
    router_full = notes[:, 2 : 2 + router_rows.shape[0]].reshape(width, experts)

    segment, position = block_layout(lens_all, row_count)
    step_down = lax.broadcasted_iota(jnp.int32, (1, row_count, row_count), 1)
    step_across = lax.broadcasted_iota(jnp.int32, (1, row_count, row_count), 2)
    allowed = (segment[:, :, None] == segment[:, None, :]) & (step_across <= step_down)
    cosine_rows, sine_rows = rotary_tables(jnp.arange(tok_count, dtype=jnp.int32), head_dim)
    place_hot = (position.reshape(-1)[:, None] == jnp.arange(tok_count)[None, :]).astype(f32)
    cosine_all = exact_dot(place_hot, cosine_rows).reshape(devices, row_count, head_dim)
    sine_all = exact_dot(place_hot, sine_rows).reshape(devices, row_count, head_dim)
    flat_unit = unit_all.reshape(all_count, width)
    projected = jnp.dot(flat_unit, w_heads, preferred_element_type=f32).reshape(
        devices, row_count, 3 * head_dim
    )
    query_raw = projected[..., :head_dim]
    key_raw = projected[..., head_dim : 2 * head_dim]
    value_rows = projected[..., 2 * head_dim :].astype(low)
    gain_query_f = gain_query.astype(f32)
    gain_key_f = gain_key.astype(f32)
    inv_query = rms_scale(query_raw)
    unit_query = query_raw * inv_query
    query_rot = rotate(unit_query * gain_query_f, cosine_all, sine_all).astype(low)
    inv_key = rms_scale(key_raw)
    unit_key = key_raw * inv_key
    key_rot = rotate(unit_key * gain_key_f, cosine_all, sine_all).astype(low)
    scores = contract(query_rot, key_rot, "btd,bud->btu") * score_scale
    masked = jnp.where(allowed, scores, masked_fill)
    row_top = jnp.max(masked, axis=-1, keepdims=True)
    exponent = jnp.exp(masked - row_top)
    probs = exponent / jnp.sum(exponent, axis=-1, keepdims=True)
    probs_low = probs.astype(low)
    mixed = contract(probs_low, value_rows, "btu,bud->btd").astype(low).reshape(all_count, head_dim)
    largest_own = jnp.max(row_top)
    branch, fall_own = scatter_sum(mixed, w_out, devices, 2, riders=(("line", w_down),))
    resid_mid = resid_in + branch

    inv_two = rms_scale(resid_mid)
    unit_two = resid_mid * inv_two
    normed_mid = (unit_two * gain_two).astype(low)
    logits = jnp.dot(normed_mid, router_full.astype(low), preferred_element_type=f32)
    choose = (expert_ids[:row_count, :, None] == jnp.arange(experts, dtype=jnp.int32)[None, None, :]).any(axis=1)
    picked = jnp.where(choose, logits, masked_fill)
    gate_power = jnp.where(choose, jnp.exp(picked - jnp.max(picked, axis=1, keepdims=True)), 0.0)
    route = gate_power / jnp.sum(gate_power, axis=1, keepdims=True)
    note_two = jnp.pad(route.T, ((0, 0), (0, 128 - row_count)))
    normed_all, notes, w_rise_gate, fall_other = gather_rows(
        (), (normed_mid, note_two), devices, 3, (("cube", w_gate), ("across", fall_own))
    )
    w_rise_gate = w_rise_gate.reshape(width, hidden)
    w_fall = jnp.where(
        y == 0, jnp.stack([fall_own, fall_other], axis=1), jnp.stack([fall_other, fall_own], axis=1)
    )
    w_fall = w_fall.transpose(2, 0, 1, 3).reshape(hidden, width)

    mine = ep * exp_local + z
    slab_rows = slab * row_count
    weight = lax.dynamic_slice_in_dim(notes, mine, 1, axis=1)[..., :row_count].reshape(slab_rows, 1)
    flat_mid = normed_all.reshape(slab_rows, width)
    flat_grad = grad_all.reshape(slab_rows, width)
    gate_part = jnp.dot(flat_mid, w_rise_gate, preferred_element_type=f32)
    up_part = jnp.dot(flat_mid, w_rise_up, preferred_element_type=f32)
    grad_plain = contract(flat_grad, w_fall, "td,fd->tf")
    sigmoid_gate = jax.nn.sigmoid(gate_part)
    silu_gate = gate_part * sigmoid_gate
    hidden_mid = silu_gate * up_part
    grad_route = jnp.sum(hidden_mid * grad_plain, axis=1, keepdims=True)
    weighted_mid = (hidden_mid * weight).astype(low)
    grad_hidden = grad_plain * weight
    grad_gate_part = (
        grad_hidden * up_part * sigmoid_gate * (1.0 + gate_part * (1.0 - sigmoid_gate))
    ).astype(low)
    grad_up_part = (grad_hidden * silu_gate).astype(low)
    lane = lax.broadcasted_iota(jnp.int32, (1, 128), 1)
    beside = jnp.where(lane == mine, grad_route, 0.0).astype(low)

    def for_each_y(grads):
        return grads.astype(low).reshape(lines, 2, wide_own, hidden)

    gate_halves = for_each_y(contract(flat_mid, grad_gate_part, "td,tf->df"))
    up_halves = for_each_y(contract(flat_mid, grad_up_part, "td,tf->df"))
    fall_halves = for_each_y(contract(flat_grad, weighted_mid, "td,tf->df"))
    summed, moe_rows, gate_come, up_come, fall_come = slab_scatter(
        (
            ((grad_gate_part, grad_up_part), (w_rise_gate, w_rise_up), True, beside),
            ((weighted_mid,), (w_fall,), False, None),
        ),
        devices,
        4,
        (("half", gate_halves), ("half", up_halves), ("half", fall_halves)),
    )

    def add_halves(halves, come):
        kept = lax.dynamic_index_in_dim(halves, y, axis=1, keepdims=False)
        return (kept.astype(f32) + come.astype(f32)).astype(low)

    grad_gates = summed[:, width : width + experts]
    mean_term = jnp.sum(route * grad_gates, axis=1, keepdims=True)
    grad_logits = (route * (grad_gates - mean_term)).astype(low)
    grad_normed_mid = summed[:, :width] + contract(grad_logits, router_full.astype(low), "te,de->td")
    gain_part = jnp.sum(grad_normed_mid * unit_two, axis=0)
    grad_mid = grad_mid_out + norm_back(grad_normed_mid * gain_two, unit_two, inv_two)
    grad_branch = grad_mid.astype(low)
    router_part = contract(normed_mid, grad_logits, "td,te->de").reshape(devices, -1, 128)
    note_three = jnp.concatenate(
        [
            gain_part.reshape(-1, 128),
            jnp.full((8, 128), largest_own, f32),
        ],
        axis=0,
    )
    branch_all, notes, back_gate, back_up = gather_rows(
        (grad_branch, note_three),
        (),
        devices,
        6,
        (
            ("line", add_halves(gate_halves, gate_come)),
            ("line", add_halves(up_halves, up_come)),
        ),
    )
    clip_factor = jnp.sqrt(clip_threshold / jnp.maximum(notes[:, -1, 0], clip_threshold))
    gain_sum = jnp.sum(notes[:, :-8], axis=0).reshape(-1)
    grad_gain_moe = lax.dynamic_slice_in_dim(gain_sum, me * rows_own, rows_own)

    flat_branch = branch_all.reshape(all_count, width)
    grad_out = contract(mixed, flat_branch, "tq,td->qd")
    grad_mixed = (
        contract(flat_branch, w_out, "td,qd->tq").astype(low).reshape(devices, row_count, head_dim)
    )
    grad_value = contract(probs_low, grad_mixed, "btu,btd->bud").astype(low)
    grad_probs = contract(grad_mixed, value_rows, "btd,bud->btu")
    grad_scores = (
        probs * (grad_probs - jnp.sum(probs * grad_probs, axis=-1, keepdims=True))
    ).astype(low)
    grad_query_rot = contract(grad_scores, key_rot, "btu,bud->btd") * score_scale
    grad_key_rot = contract(grad_scores, query_rot, "btu,btd->bud") * score_scale
    grad_query_normed = rotate_back(grad_query_rot, cosine_all, sine_all)
    grad_key_normed = rotate_back(grad_key_rot, cosine_all, sine_all)
    gain_pair = jnp.stack(
        [
            jnp.sum(grad_query_normed * unit_query, axis=(0, 1)),
            jnp.sum(grad_key_normed * unit_key, axis=(0, 1)),
        ]
    )
    grad_query_raw = norm_back(grad_query_normed * gain_query_f, unit_query, inv_query).astype(low)
    grad_key_raw = norm_back(grad_key_normed * gain_key_f, unit_key, inv_key).astype(low)
    grad_heads = jnp.concatenate([grad_query_raw, grad_key_raw, grad_value], axis=2).reshape(
        all_count, 3 * head_dim
    )
    grad_heads_w = contract(flat_unit, grad_heads, "td,tq->dq").astype(low)
    resid_out = resid_mid + moe_rows
    undeal = (jnp.arange(tok_count, dtype=jnp.int32)[:, None] == local_order[None, :]).astype(low)
    undeal = undeal[:, :row_count]
    block_out = jnp.dot(undeal, resid_out.astype(low), preferred_element_type=f32).astype(low)
    grad_unit_one, back_heads, back_fall, gain_pairs, router_parts = scatter_sum(
        grad_heads,
        w_heads,
        devices,
        7,
        turned=True,
        riders=(
            ("all", grad_heads_w.reshape(devices, rows_own, 3 * head_dim)),
            ("line", add_halves(fall_halves, fall_come)),
            ("same", jnp.pad(gain_pair, ((0, 6), (0, 0)))),
            ("all", router_part),
        ),
    )
    back_heads = back_heads.astype(f32)
    grad_gate = back_gate.astype(f32)
    grad_up = back_up.astype(f32)
    grad_down = back_fall.transpose(0, 2, 1).astype(f32)
    grad_router = jnp.sum(router_parts, axis=0).reshape(rows_own, experts)
    gain_pair = jnp.sum(gain_pairs, axis=0)
    plain_query = back_heads[..., :head_dim].transpose(1, 0, 2).reshape(rows_own, -1)

    def of_group(grads):
        grads = jnp.sum(grads.reshape(kv_count, group_size, rows_own, head_dim), axis=1)
        return grads.transpose(1, 0, 2).reshape(rows_own, -1)

    plain_key = of_group(back_heads[..., head_dim : 2 * head_dim])
    plain_value = of_group(back_heads[..., 2 * head_dim :])
    grad_gain_attn = (
        jnp.sum(plain_query * w_query.astype(f32), axis=1)
        + jnp.sum(plain_key * w_key.astype(f32), axis=1)
        + jnp.sum(plain_value * w_value.astype(f32), axis=1)
    )
    grad_resid_in = grad_mid + norm_back(grad_unit_one, unit_one, inv_one)
    grad_input = exact_dot(undeal.astype(f32), grad_resid_in)
    return (
        block_out,
        grad_input,
        plain_query * gain_col,
        plain_key * gain_col,
        plain_value * gain_col,
        grad_out,
        grad_router,
        grad_gain_attn,
        grad_gain_moe,
        gain_pair[0],
        gain_pair[1],
        grad_gate,
        grad_up,
        grad_down,
        clip_factor,
    )


def solution(mesh):
    placed = (
        P(("dp", "ep"), None),
        P(("dp", "ep"), None),
        P(("dp", "ep")),
        P(("dp", "ep"), None),
        P(("dp", "ep"), None),
        P(("dp", "ep"), None),
        P(("dp", "ep"), None),
        P(("dp", "ep"), None),
        P(("dp", "ep"), None),
        P(("dp", "ep"), None),
        P(("dp", "ep")),
        P(("dp", "ep")),
        P(),
        P(),
        P("ep", "dp", None),
        P("ep", "dp", None),
        P("ep", None, "dp"),
        P(),
    )
    return jax.shard_map(
        per_device if not whole_rows(mesh) else by_experts,
        mesh=mesh,
        in_specs=placed,
        out_specs=(
            P(("dp", "ep"), None),
            P(("dp", "ep"), None),
            P(("dp", "ep"), None),
            P(("dp", "ep"), None),
            P(("dp", "ep"), None),
            P(("dp", "ep"), None),
            P(("dp", "ep"), None),
            P(("dp", "ep")),
            P(("dp", "ep")),
            P(),
            P(),
            P("ep", "dp", None),
            P("ep", "dp", None),
            P("ep", None, "dp"),
            P(),
        ),
        check_vma=False,
    )
```

```python
import functools

import jax
import jax.numpy as jnp
from jax import lax
from jax.experimental import pallas as pl
from jax.experimental.pallas import tpu as pltpu
from jax.sharding import PartitionSpec as P

epsilon = 1e-06
theta_base = 1000000.0
masked_fill = -1e30


def rms_scale(values):
    return lax.rsqrt(jnp.mean(values * values, axis=-1, keepdims=True) + epsilon)


def rotate_half(values):
    half_dim = values.shape[-1] // 2
    return jnp.concatenate([-values[..., half_dim:], values[..., :half_dim]], axis=-1)


def rotate(values, cosine_table, sine_table):
    return values * cosine_table + rotate_half(values) * sine_table


def rotate_back(values, cosine_table, sine_table):
    scaled = values * sine_table
    half_dim = values.shape[-1] // 2
    turned = jnp.concatenate([scaled[..., half_dim:], -scaled[..., :half_dim]], axis=-1)
    return values * cosine_table + turned


def norm_back(grad_unit, unit_rows, inv_root):
    return inv_root * (
        grad_unit - unit_rows * jnp.mean(grad_unit * unit_rows, axis=-1, keepdims=True)
    )


def contract(left_side, right_side, pattern):
    return jnp.einsum(pattern, left_side, right_side, preferred_element_type=jnp.float32)


def layout(lens_row, tok_count):
    seq_ends = jnp.cumsum(lens_row)
    row_index = jnp.arange(tok_count, dtype=jnp.int32)
    segment = jnp.sum((row_index[:, None] >= seq_ends[None, :]).astype(jnp.int32), axis=1)
    starts_all = jnp.concatenate([jnp.zeros((1,), jnp.int32), seq_ends])
    seg_hot = segment[:, None] == jnp.arange(starts_all.shape[0], dtype=jnp.int32)[None, :]
    first_row = jnp.sum(jnp.where(seg_hot, starts_all[None, :], 0), axis=1)
    position = row_index - first_row
    valid_row = segment < lens_row.shape[0]
    allowed = (segment[:, None] == segment[None, :]) & (row_index[None, :] <= row_index[:, None])
    return (position, valid_row, allowed)


def rotary_tables(position, head_dim):
    half_dim = head_dim // 2
    frequency = theta_base ** (-(jnp.arange(half_dim, dtype=jnp.float32) * 2.0) / head_dim)
    angles = position.astype(jnp.float32)[:, None] * frequency[None, :]
    angles = jnp.concatenate([angles, angles], axis=-1)
    return (jnp.cos(angles), jnp.sin(angles))


def per_device(
    hidden_in,
    cotangent,
    deal_order,
    seq_lengths,
    expert_ids,
    w_query,
    w_key,
    w_value,
    w_out,
    w_router,
    gain_attn,
    gain_moe,
    gain_query,
    gain_key,
    w_gate,
    w_up,
    w_down,
    clip_threshold,
):
    tok_count = hidden_in.shape[0]
    model_width = hidden_in.shape[1]
    head_dim = gain_query.shape[0]
    local_order = deal_order % tok_count
    position, valid_row, allowed = layout(seq_lengths[0], tok_count)
    valid_col = valid_row.astype(jnp.float32)[:, None]
    cosine_table, sine_table = rotary_tables(position, head_dim)
    cosine_query = cosine_table[:, None, None, :]
    sine_query = sine_table[:, None, None, :]
    cosine_key = cosine_table[:, None, :]
    sine_key = sine_table[:, None, :]
    attn_params = (
        lax.all_gather(w_query, ("dp", "ep"), axis=0, tiled=True),
        lax.all_gather(w_key, ("dp", "ep"), axis=0, tiled=True),
        lax.all_gather(w_value, ("dp", "ep"), axis=0, tiled=True),
        lax.all_gather(w_out, ("dp", "ep"), axis=0, tiled=True),
        lax.all_gather(w_router, ("dp", "ep"), axis=0, tiled=True),
        lax.all_gather(gain_attn, ("dp", "ep"), axis=0, tiled=True),
        lax.all_gather(gain_moe, ("dp", "ep"), axis=0, tiled=True),
    )
    expert_params = (
        lax.all_gather(w_gate, "dp", axis=1, tiled=True),
        lax.all_gather(w_up, "dp", axis=1, tiled=True),
        lax.all_gather(w_down, "dp", axis=2, tiled=True),
    )
    query_full, key_full, value_full, out_full, router_full, gain_attn_full, gain_moe_full = (
        attn_params
    )
    gate_full, up_full, down_full = expert_params
    head_count = query_full.shape[1] // head_dim
    kv_count = key_full.shape[1] // head_dim
    group_size = head_count // kv_count
    experts = router_full.shape[1]
    top_count = expert_ids.shape[1]
    exp_local = w_gate.shape[0]
    ep_count = lax.axis_size("ep")
    capacity = (tok_count * top_count * 5 + 4 * experts - 1) // (4 * experts)
    score_scale = head_dim ** (-0.5)
    resid_in = hidden_in[local_order].astype(jnp.float32)
    inv_one = rms_scale(resid_in)
    unit_one = resid_in * inv_one
    gain_one = gain_attn_full.astype(jnp.float32)
    normed_in = (unit_one * gain_one).astype(jnp.bfloat16)
    query_raw = jnp.dot(normed_in, query_full, preferred_element_type=jnp.float32).reshape(
        tok_count, kv_count, group_size, head_dim
    )
    key_raw = jnp.dot(normed_in, key_full, preferred_element_type=jnp.float32).reshape(
        tok_count, kv_count, head_dim
    )
    value_rows = (
        jnp.dot(normed_in, value_full, preferred_element_type=jnp.float32)
        .astype(jnp.bfloat16)
        .reshape(tok_count, kv_count, head_dim)
    )
    inv_query = rms_scale(query_raw)
    unit_query = query_raw * inv_query
    gain_query_f = gain_query.astype(jnp.float32)
    query_rot = rotate(unit_query * gain_query_f, cosine_query, sine_query).astype(jnp.bfloat16)
    inv_key = rms_scale(key_raw)
    unit_key = key_raw * inv_key
    gain_key_f = gain_key.astype(jnp.float32)
    key_rot = rotate(unit_key * gain_key_f, cosine_key, sine_key).astype(jnp.bfloat16)
    scores = contract(query_rot, key_rot, "tkgd,ukd->kgtu") * score_scale
    masked = jnp.where(allowed, scores, masked_fill)
    row_top = jnp.max(masked, axis=-1, keepdims=True)
    exponent = jnp.exp(masked - row_top)
    row_total = jnp.sum(exponent, axis=-1, keepdims=True)
    log_total = row_top + jnp.log(row_total)
    probs_low = (exponent / row_total).astype(jnp.bfloat16)
    mixed_heads = (
        contract(probs_low, value_rows, "kgtu,ukd->tkgd")
        .astype(jnp.bfloat16)
        .reshape(tok_count, head_count * head_dim)
    )
    resid_mid = resid_in + jnp.dot(mixed_heads, out_full, preferred_element_type=jnp.float32)
    largest_local = jnp.max(
        jnp.where(allowed & valid_row[:, None], scores, masked_fill), axis=(2, 3)
    ).reshape(head_count)
    largest = lax.pmax(largest_local, ("dp", "ep"))
    clip_factor = jnp.sqrt(clip_threshold / jnp.maximum(largest, clip_threshold))
    inv_two = rms_scale(resid_mid)
    unit_two = resid_mid * inv_two
    gain_two = gain_moe_full.astype(jnp.float32)
    normed_mid = (unit_two * gain_two).astype(jnp.bfloat16)
    logits = jnp.dot(normed_mid, router_full, preferred_element_type=jnp.float32)
    choose = expert_ids[:, :, None] == jnp.arange(experts, dtype=jnp.int32)[None, None, :]
    picked = jnp.sum(jnp.where(choose, logits[:, None, :], 0.0), axis=2)
    gate_weights = jax.nn.softmax(picked, axis=-1)
    flat_ids = expert_ids.reshape(-1)
    flat_hot = (flat_ids[:, None] == jnp.arange(experts, dtype=jnp.int32)[None, :]).astype(
        jnp.int32
    )
    slot_rank = jnp.sum((jnp.cumsum(flat_hot, axis=0) - 1) * flat_hot, axis=1)
    slot_index = flat_ids * capacity + slot_rank
    pair_token = jnp.arange(tok_count * top_count, dtype=jnp.int32) // top_count
    send_rows = (
        jnp.zeros((experts * capacity, model_width), jnp.bfloat16)
        .at[slot_index]
        .set(normed_mid[pair_token])
    )
    send_rows = send_rows.reshape(ep_count, exp_local, capacity, model_width)
    arrived = lax.all_to_all(send_rows, "ep", split_axis=0, concat_axis=0, tiled=True)
    gate_part = contract(arrived, gate_full, "secd,edf->secf")
    up_part = contract(arrived, up_full, "secd,edf->secf")
    hidden_mid = (jax.nn.silu(gate_part) * up_part).astype(jnp.bfloat16)
    produced = contract(hidden_mid, down_full, "secf,efd->secd").astype(jnp.bfloat16)
    returned = lax.all_to_all(produced, "ep", split_axis=0, concat_axis=0, tiled=True)
    returned, arrived, gate_part, up_part = (returned, arrived, gate_part, up_part)
    pair_out = (
        returned.reshape(experts * capacity, model_width)[slot_index]
        .reshape(tok_count, top_count, model_width)
        .astype(jnp.float32)
    )
    resid_out = resid_mid + jnp.sum(gate_weights[:, :, None] * pair_out, axis=1)
    out_rows = (resid_out * valid_col).astype(jnp.bfloat16)
    block_out = jnp.zeros_like(out_rows).at[local_order].set(out_rows)
    attn_params = (
        lax.all_gather(w_query, ("dp", "ep"), axis=0, tiled=True),
        lax.all_gather(w_key, ("dp", "ep"), axis=0, tiled=True),
        lax.all_gather(w_value, ("dp", "ep"), axis=0, tiled=True),
        lax.all_gather(w_out, ("dp", "ep"), axis=0, tiled=True),
        lax.all_gather(w_router, ("dp", "ep"), axis=0, tiled=True),
        lax.all_gather(gain_attn, ("dp", "ep"), axis=0, tiled=True),
        lax.all_gather(gain_moe, ("dp", "ep"), axis=0, tiled=True),
    )
    expert_params = (
        lax.all_gather(w_gate, "dp", axis=1, tiled=True),
        lax.all_gather(w_up, "dp", axis=1, tiled=True),
        lax.all_gather(w_down, "dp", axis=2, tiled=True),
    )
    query_full, key_full, value_full, out_full, router_full, gain_attn_full, gain_moe_full = (
        attn_params
    )
    gate_full, up_full, down_full = expert_params
    grad_mid_out = cotangent[local_order].astype(jnp.float32) * valid_col
    grad_gates = jnp.sum(grad_mid_out[:, None, :] * pair_out, axis=2)
    grad_pair = (gate_weights[:, :, None] * grad_mid_out[:, None, :]).astype(jnp.bfloat16)
    send_grads = (
        jnp.zeros((experts * capacity, model_width), jnp.bfloat16)
        .at[slot_index]
        .set(grad_pair.reshape(-1, model_width))
    )
    send_grads = send_grads.reshape(ep_count, exp_local, capacity, model_width)
    grad_arrived = lax.all_to_all(send_grads, "ep", split_axis=0, concat_axis=0, tiled=True)
    grad_hidden = contract(grad_arrived, down_full, "secd,efd->secf")
    sigmoid_gate = jax.nn.sigmoid(gate_part)
    silu_gate = jax.nn.silu(gate_part)
    grad_gate_part = (
        grad_hidden * up_part * sigmoid_gate * (1.0 + gate_part * (1.0 - sigmoid_gate))
    ).astype(jnp.bfloat16)
    grad_up_part = (grad_hidden * silu_gate).astype(jnp.bfloat16)
    grad_rows = (
        contract(grad_gate_part, gate_full, "secf,edf->secd")
        + contract(grad_up_part, up_full, "secf,edf->secd")
    ).astype(jnp.bfloat16)
    grad_back = lax.all_to_all(grad_rows, "ep", split_axis=0, concat_axis=0, tiled=True)
    hidden_mid = (silu_gate * up_part).astype(jnp.bfloat16)
    grad_gate_w = contract(arrived, grad_gate_part, "secd,secf->edf")
    grad_up_w = contract(arrived, grad_up_part, "secd,secf->edf")
    grad_down_w = contract(hidden_mid, grad_arrived, "secf,secd->efd")
    grad_gate, grad_up, grad_down = (
        lax.psum_scatter(
            grad_gate_w.astype(jnp.bfloat16), "dp", scatter_dimension=1, tiled=True
        ).astype(jnp.float32),
        lax.psum_scatter(
            grad_up_w.astype(jnp.bfloat16), "dp", scatter_dimension=1, tiled=True
        ).astype(jnp.float32),
        lax.psum_scatter(
            grad_down_w.astype(jnp.bfloat16), "dp", scatter_dimension=2, tiled=True
        ).astype(jnp.float32),
    )
    mean_term = jnp.sum(gate_weights * grad_gates, axis=1, keepdims=True)
    grad_picked = gate_weights * (grad_gates - mean_term)
    grad_logits = jnp.sum(jnp.where(choose, grad_picked[:, :, None], 0.0), axis=1).astype(
        jnp.bfloat16
    )
    grad_router_w = contract(normed_mid, grad_logits, "td,te->de")
    pair_grads = (
        grad_back.reshape(experts * capacity, model_width)[slot_index]
        .reshape(tok_count, top_count, model_width)
        .astype(jnp.float32)
    )
    grad_normed_mid = jnp.sum(pair_grads, axis=1) + contract(grad_logits, router_full, "te,de->td")
    grad_gain_moe_w = jnp.sum(grad_normed_mid * unit_two, axis=0)
    grad_mid = grad_mid_out + norm_back(grad_normed_mid * gain_two, unit_two, inv_two)
    grad_branch = grad_mid.astype(jnp.bfloat16)
    grad_out_w = contract(mixed_heads, grad_branch, "tq,td->qd")
    grad_mixed = (
        contract(grad_branch, out_full, "td,qd->tq")
        .astype(jnp.bfloat16)
        .reshape(tok_count, kv_count, group_size, head_dim)
    )
    scores_again = contract(query_rot, key_rot, "tkgd,ukd->kgtu") * score_scale
    probs_back = jnp.exp(jnp.where(allowed, scores_again, masked_fill) - log_total)
    grad_value_rows = contract(
        probs_back.astype(jnp.bfloat16), grad_mixed, "kgtu,tkgd->ukd"
    ).astype(jnp.bfloat16)
    grad_probs = contract(grad_mixed, value_rows, "tkgd,ukd->kgtu")
    grad_scores = (
        probs_back * (grad_probs - jnp.sum(probs_back * grad_probs, axis=-1, keepdims=True))
    ).astype(jnp.bfloat16)
    grad_query_rot = contract(grad_scores, key_rot, "kgtu,ukd->tkgd") * score_scale
    grad_key_rot = contract(grad_scores, query_rot, "kgtu,tkgd->ukd") * score_scale
    grad_query_normed = rotate_back(grad_query_rot, cosine_query, sine_query)
    grad_key_normed = rotate_back(grad_key_rot, cosine_key, sine_key)
    grad_gain_q = jnp.sum(grad_query_normed * unit_query, axis=(0, 1, 2))
    grad_gain_k = jnp.sum(grad_key_normed * unit_key, axis=(0, 1))
    grad_query_raw = (
        norm_back(grad_query_normed * gain_query_f, unit_query, inv_query)
        .astype(jnp.bfloat16)
        .reshape(tok_count, head_count * head_dim)
    )
    grad_key_raw = (
        norm_back(grad_key_normed * gain_key_f, unit_key, inv_key)
        .astype(jnp.bfloat16)
        .reshape(tok_count, kv_count * head_dim)
    )
    grad_value_flat = grad_value_rows.reshape(tok_count, kv_count * head_dim)
    grad_query_w = contract(normed_in, grad_query_raw, "td,tq->dq")
    grad_key_w = contract(normed_in, grad_key_raw, "td,tq->dq")
    grad_value_w = contract(normed_in, grad_value_flat, "td,tq->dq")
    grad_normed_in = (
        contract(grad_query_raw, query_full, "tq,dq->td")
        + contract(grad_key_raw, key_full, "tq,dq->td")
        + contract(grad_value_flat, value_full, "tq,dq->td")
    )
    grad_gain_attn_w = jnp.sum(grad_normed_in * unit_one, axis=0)
    grad_resid_in = grad_mid + norm_back(grad_normed_in * gain_one, unit_one, inv_one)
    grad_input = jnp.zeros_like(grad_resid_in).at[local_order].set(grad_resid_in)
    grad_sums = (
        lax.psum_scatter(grad_query_w, ("dp", "ep"), scatter_dimension=0, tiled=True),
        lax.psum_scatter(grad_key_w, ("dp", "ep"), scatter_dimension=0, tiled=True),
        lax.psum_scatter(grad_value_w, ("dp", "ep"), scatter_dimension=0, tiled=True),
        lax.psum_scatter(grad_out_w, ("dp", "ep"), scatter_dimension=0, tiled=True),
        lax.psum_scatter(grad_router_w, ("dp", "ep"), scatter_dimension=0, tiled=True),
        lax.psum_scatter(grad_gain_attn_w, ("dp", "ep"), scatter_dimension=0, tiled=True),
        lax.psum_scatter(grad_gain_moe_w, ("dp", "ep"), scatter_dimension=0, tiled=True),
    )
    gain_sums = lax.psum((grad_gain_q, grad_gain_k), ("dp", "ep"))
    return (
        block_out,
        grad_input,
        grad_sums[0],
        grad_sums[1],
        grad_sums[2],
        grad_sums[3],
        grad_sums[4],
        grad_sums[5],
        grad_sums[6],
        gain_sums[0],
        gain_sums[1],
        grad_gate,
        grad_up,
        grad_down,
        clip_factor,
    )


MESH = pl.DeviceIdType.MESH


def place():
    dp = lax.axis_index("dp")
    ep = lax.axis_index("ep")
    z, y = dp // 2, dp % 2
    x, c = ep // 2, ep % 2
    first = (1 - c) * y + c * x
    second = (1 - c) * x + c * y
    return dp, ep, z, y, x, c, first, second


def targets(dp, ep, z, y, x, c, nz):
    up = (jnp.where(z < nz - 1, dp + 2, dp), ep)
    down = (jnp.where(z > 0, dp - 2, dp), ep)
    turn_y, turn_x = 1 - 2 * y, 2 - 4 * x
    near = (dp + (1 - c) * turn_y, ep + c * turn_x)
    far = (dp + c * turn_y, ep + (1 - c) * turn_x)
    twin = (dp, ep + 1 - 2 * c)
    return up, down, near, far, twin


def slot(z, first, second, c):
    return z * 8 + first * (4 - 2 * c) + second * (2 + 2 * c) + c


def greet(nz, z, dp, ep, ways, everyone):
    barrier = pltpu.get_barrier_semaphore()
    if everyone:
        total = nz * 8
        me = dp * 4 + ep

        def hello(step, carry):
            other = (me + step) % total
            pl.semaphore_signal(
                barrier, inc=1, device_id=(other // 4, other % 4), device_id_type=MESH
            )
            return carry

        lax.fori_loop(1, total, hello, 0)
        pl.semaphore_wait(barrier, total - 1)
        return
    for step in range(1, nz):
        other = ((z + step) % nz) * 2 + dp % 2
        pl.semaphore_signal(barrier, inc=1, device_id=(other, ep), device_id_type=MESH)
    for other in ways[2:]:
        pl.semaphore_signal(barrier, inc=1, device_id=other, device_id_type=MESH)
    pl.semaphore_wait(barrier, nz + 2)


class Riders:
    def __init__(self, kinds, nz, spot, refs):
        count = len(kinds)
        self.kinds, self.nz = kinds, nz
        self.dp, self.ep, self.z, self.y = spot
        self.me = self.dp * 4 + self.ep
        self.over_y = (self.dp + 1 - 2 * self.y, self.ep)
        self.ins, self.outs = refs[:count], refs[count : 2 * count]
        self.send, self.onward, self.recv, self.own = refs[2 * count :] if count else (None,) * 4
        self.spans = []
        for kind in kinds:
            if kind in ("all", "same"):
                self.spans.append((1, 8 * nz))
            else:
                self.spans.append((1 if kind in ("line", "cube") else 0, nz))
        self.cubes = [r for r in range(count) if kinds[r] == "cube"]

    def remote(self, source, target, send, recv, device):
        return pltpu.make_async_remote_copy(
            src_ref=source, dst_ref=target, send_sem=send, recv_sem=recv,
            device_id=device, device_id_type=MESH)

    def copy(self, r, step):
        kind, source, target = self.kinds[r], self.ins[r], self.outs[r]
        if kind in ("all", "same"):
            other = (self.me + step) % (8 * self.nz)
            source = source if kind == "same" else source.at[other]
            target, key, device = target.at[self.me], self.me, (other // 4, other % 4)
        elif kind in ("line", "cube"):
            other = (self.z + step) % self.nz
            source, key, device = source.at[other], self.z, (other * 2 + self.y, self.ep)
            target = target.at[self.z] if kind == "line" else target.at[self.z, self.y]
        else:
            source = source.at[step, 1 - self.y] if kind == "half" else source.at[step]
            target = target.at[step] if kind == "half" else target.at[step, self.y]
            key, device = step, self.over_y
        return self.remote(source, target, self.send.at[r, step], self.recv.at[r, key], device)

    def arrival(self, r, step):
        kind, target = self.kinds[r], self.outs[r]
        if kind in ("all", "same"):
            key = (self.me + step) % (8 * self.nz)
            target = target.at[key]
        elif kind in ("line", "cube"):
            key = (self.z + self.nz - step) % self.nz
            target = target.at[key] if kind == "line" else target.at[key, self.y]
        else:
            key = step
            target = target.at[step] if kind == "half" else target.at[step, 1 - self.y]
        return self.remote(target, target, self.send.at[r, step], self.recv.at[r, key], self.over_y)

    def passing(self, r, step, first=False):
        key = (self.z + self.nz - step) % self.nz
        target = self.outs[r].at[key, self.y]
        source = self.ins[r].at[key] if first else target
        return self.remote(
            source, target, self.onward.at[r, step], self.recv.at[r, self.nz + key], self.over_y)

    def passed(self, r, step):
        key = (self.z + self.nz - step) % self.nz
        target = self.outs[r].at[key, 1 - self.y]
        return self.remote(
            target, target, self.onward.at[r, step], self.recv.at[r, self.nz + key], self.over_y)

    def own_copies(self, r):
        kind, source, target = self.kinds[r], self.ins[r], self.outs[r]
        if kind in ("all", "same"):
            ends = [(source if kind == "same" else source.at[self.me], target.at[self.me])]
        elif kind == "half":
            ends = []
        elif kind == "pair":
            ends = [(source.at[k], target.at[k, self.y]) for k in range(self.nz)]
        else:
            target = target.at[self.z] if kind == "line" else target.at[self.z, self.y]
            ends = [(source.at[self.z], target)]
        return [pltpu.make_async_copy(here, there, self.own.at[r]) for here, there in ends]

    def begin(self, early=("half", "pair")):
        for r, kind in enumerate(self.kinds):
            for copy in self.own_copies(r):
                copy.start()
            if kind == "cube":
                self.passing(r, 0, True).start()
        self.steps = []
        for r, kind in enumerate(self.kinds):
            for k in range(*self.spans[r]):
                if kind in early:
                    self.copy(r, k).start()
                else:
                    self.steps.append((r, k))
        self.steps.sort(key=lambda step: step[1] / self.spans[step[0]][1])
        self.later = [r for r, kind in enumerate(self.kinds) if kind not in early]

    def some(self, share, shares):
        total = len(self.steps)
        for r, k in self.steps[total * share // shares : total * (share + 1) // shares]:
            self.copy(r, k).start()

    def onwards(self, step):
        for r in self.cubes:
            self.arrival(r, step).wait_recv()
            self.passing(r, step).start()

    def looped(self, step, steps):
        for r in self.later:
            first, last = self.spans[r]
            per = -(-(last - first) // steps)
            for k in range(per):
                piece = first + step * per + k

                @pl.when(piece < last)
                def _():
                    self.copy(r, piece).start()

    def finish(self):
        for r, kind in enumerate(self.kinds):

            def settle(step, carry):
                if kind != "cube":
                    self.arrival(r, step).wait_recv()
                self.copy(r, step).wait_send()
                return carry

            lax.fori_loop(*self.spans[r], settle, 0)
            if kind == "cube":

                def settle_y(step, carry):
                    self.passed(r, step).wait_recv()
                    self.passing(r, step).wait_send()
                    return carry

                lax.fori_loop(0, self.nz, settle_y, 0)
            for copy in self.own_copies(r):
                copy.wait()


def rider_shapes(riders, devices):
    kinds = tuple(kind for kind, _ in riders)
    arrays = tuple(array for _, array in riders)
    outs = []
    for kind, v in riders:
        shape = v.shape
        if kind == "same":
            shape = (devices,) + shape
        elif kind in ("cube", "pair"):
            shape = shape[:1] + (2,) + shape[1:]
        elif kind == "half":
            shape = shape[:1] + shape[2:]
        outs.append(jax.ShapeDtypeStruct(shape, v.dtype))
    dma = pltpu.SemaphoreType.DMA
    count = len(riders)
    sems = [dma((count, devices))] * 3 + [dma((count,))] if count else []
    return kinds, arrays, tuple(outs), sems


def rider_specs(kinds):
    return [
        pl.BlockSpec(memory_space=pl.ANY if kind == "half" else pltpu.VMEM)
        for kind in kinds
    ]


def wide_greeting(kinds):
    return "all" in kinds or "same" in kinds


def on(allowed, action):
    if allowed is None:
        action()
    else:
        pl.when(allowed)(action)


def along(z, nz, step):
    if step == 0:
        yield None, z
    else:
        yield z >= step, jnp.maximum(z - step, 0)
        yield z + step < nz, jnp.minimum(z + step, nz - 1)


class Mover:
    def __init__(self, ins, outs, ways, sems):
        self.ins, self.outs, self.ways = ins, outs, ways
        self.send, self.recv, self.own = sems
        self.pending, self.own_copies = [], []

    def push(self, way, where, allowed=None, own=False):
        for k, out in enumerate(self.outs):
            copy = pltpu.make_async_remote_copy(
                src_ref=self.ins[k] if own else out.at[where],
                dst_ref=out.at[where],
                send_sem=self.send.at[k, way, where],
                recv_sem=self.recv.at[k, where],
                device_id=self.ways[way],
                device_id_type=MESH,
            )
            on(allowed, copy.start)
            self.pending.append((allowed, copy))

    def arrive(self, where):
        for k, out in enumerate(self.outs):
            pltpu.make_async_remote_copy(
                src_ref=out.at[where],
                dst_ref=out.at[where],
                send_sem=self.send.at[k, 0, where],
                recv_sem=self.recv.at[k, where],
                device_id=self.ways[-1],
                device_id_type=MESH,
            ).wait_recv()

    def keep(self, mine):
        for k, out in enumerate(self.outs):
            copy = pltpu.make_async_copy(self.ins[k], out.at[mine], self.own.at[k])
            copy.start()
            self.own_copies.append(copy)

    def settle(self):
        for allowed, copy in self.pending:
            on(allowed, copy.wait_send)
        for copy in self.own_copies:
            copy.wait()


class WholeGather(Mover):
    def begin(self, nz, z, a, b, c):
        self.nz, self.z, self.a, self.b, self.c = nz, z, a, b, c
        mine = slot(z, a, b, c)
        self.push(0, mine, z < nz - 1, True)
        self.push(1, mine, z > 0, True)
        for way in (2, 3, 4):
            self.push(way, mine, None, True)
        self.keep(mine)

    def turn_z(self, turn):
        nz, z, a, b, c = self.nz, self.z, self.a, self.b, self.c
        if turn < nz:
            for index, (allowed, zz) in enumerate(along(z, nz, turn)):
                where = slot(zz, a, b, c)
                on(allowed, functools.partial(self.arrive, where))
                self.push(index, where, allowed & ((z > 0) if index else (z < nz - 1)))
                for way in (2, 3, 4):
                    self.push(way, where, allowed)

    def turn_xy(self, turn):
        nz, z, a, b, c = self.nz, self.z, self.a, self.b, self.c
        if turn - 1 < nz:
            for allowed, zz in along(z, nz, turn - 1):
                where = slot(zz, 1 - a, b, c)
                on(allowed, functools.partial(self.arrive, where))
                for way in (3, 4):
                    self.push(way, where, allowed)
            for allowed, zz in along(z, nz, turn - 1):
                where = slot(zz, a, 1 - b, c)
                on(allowed, functools.partial(self.arrive, where))
                self.push(4, where, allowed)
        if turn >= 2:
            for allowed, zz in along(z, nz, turn - 2):
                where = slot(zz, 1 - a, 1 - b, c)
                on(allowed, functools.partial(self.arrive, where))
                self.push(4, where, allowed)

    def end(self):
        for zz in range(self.nz):
            for aa in range(2):
                for bb in range(2):
                    self.arrive(slot(zz, aa, bb, 1 - self.c))
        self.settle()


class SlabGather(Mover):
    def begin(self, nz, z, ep, x, c):
        self.nz, self.z, self.ep, self.c = nz, z, ep, c
        self.other = ep + 2 - 4 * x
        mine = z * 4 + ep
        self.push(0, mine, z < nz - 1, True)
        self.push(1, mine, z > 0, True)
        for way in (2, 3):
            self.push(way, mine, None, True)
        self.keep(mine)

    def turn_z(self, turn):
        nz, z = self.nz, self.z
        if turn < nz:
            for index, (allowed, zz) in enumerate(along(z, nz, turn)):
                where = zz * 4 + self.ep
                on(allowed, functools.partial(self.arrive, where))
                self.push(index, where, allowed & ((z > 0) if index else (z < nz - 1)))
                for way in (2, 3):
                    self.push(way, where, allowed)

    def turn_xy(self, turn):
        nz, z = self.nz, self.z
        if turn - 1 < nz:
            for allowed, zz in along(z, nz, turn - 1):
                where = zz * 4 + self.other
                on(allowed, functools.partial(self.arrive, where))
                self.push(3, where, allowed)

    def end(self):
        for where in range(4 * self.nz):
            pl.when(where % 2 != self.c)(functools.partial(self.arrive, where))
        self.settle()


def gather_kernel(nz, counts, kinds, *refs):
    whole, slabs = counts
    count, extra = whole + slabs, len(kinds)
    ins = refs[:count]
    outs = refs[count + extra : 2 * count + extra]
    sems = refs[2 * (count + extra) :]
    dp, ep, z, y, x, c, a, b = place()
    ways = targets(dp, ep, z, y, x, c, nz)
    up, down, near, far, twin = ways
    side = (dp, ep + 2 - 4 * x)
    movers = []
    if whole:
        movers.append(WholeGather(ins[:whole], outs[:whole], ways, sems[:3]))
        sems = sems[3:]
    if slabs:
        movers.append(SlabGather(ins[whole:], outs[whole:], (up, down, side, twin), sems[:3]))
        sems = sems[3:]
    riders = Riders(
        kinds, nz, (dp, ep, z, y),
        refs[count : count + extra] + refs[2 * count + extra : 2 * (count + extra)] + sems,
    )
    greet(nz, z, dp, ep, ways, wide_greeting(kinds))
    for mover in movers:
        if isinstance(mover, WholeGather):
            mover.begin(nz, z, a, b, c)
        else:
            mover.begin(nz, z, ep, x, c)
    riders.begin()
    for turn in range(1, nz + 2):
        if turn <= nz:
            riders.some(turn - 1, nz)
        for mover in movers:
            mover.turn_z(turn)
            mover.turn_xy(turn)
        if 2 <= turn <= nz:
            riders.onwards(turn - 1)
    for mover in movers:
        mover.end()
    riders.finish()


def gather_rows(whole, slabs, devices, ident, riders=()):
    arrays = whole + slabs
    nz = devices // 8
    kinds, ridden, rider_outs, rider_sems = rider_shapes(riders, devices)
    blocks = (devices,) * len(whole) + (4 * nz,) * len(slabs)
    dma = pltpu.SemaphoreType.DMA
    sems = []
    for count, ways, total in ((len(whole), 5, devices), (len(slabs), 4, 4 * nz)):
        if count:
            sems += [dma((count, ways, total)), dma((count, total)), dma((count,))]
    return pl.pallas_call(
        functools.partial(gather_kernel, nz, (len(whole), len(slabs)), kinds),
        out_shape=tuple(
            jax.ShapeDtypeStruct((total,) + v.shape, v.dtype) for total, v in zip(blocks, arrays)
        )
        + rider_outs,
        in_specs=[pl.BlockSpec(memory_space=pltpu.VMEM)] * len(arrays) + rider_specs(kinds),
        out_specs=tuple(pl.BlockSpec(memory_space=pl.ANY) for v in arrays + ridden),
        scratch_shapes=sems + rider_sems,
        compiler_params=pltpu.CompilerParams(collective_id=ident, has_side_effects=True),
        name="gather_rows_%d" % ident,
    )(*arrays, *ridden)


def scatter_kernel(nz, turned, kinds, *refs):
    extra = len(kinds)
    left_ref, right_ref = refs[:2]
    refs = refs[2:]
    out_ref = refs[extra]
    sent, got, from_far, from_near, rising, falling = refs[2 * extra + 1 : 2 * extra + 7]
    (twin_send, twin_recv, far_send, far_recv, near_send, near_recv, line_send, up_recv,
     down_recv) = refs[2 * extra + 7 : 2 * extra + 16]
    dp, ep, z, y, x, c, a, b = place()
    ways = targets(dp, ep, z, y, x, c, nz)
    up, down, near, far, twin = ways
    riders = Riders(
        kinds, nz, (dp, ep, z, y),
        refs[:extra] + refs[extra + 1 : 2 * extra + 1] + refs[2 * extra + 16 :]
    )
    greet(nz, z, dp, ep, ways, wide_greeting(kinds))
    riders.begin(("half", "line"))
    per = 4 * nz

    def zed(step):
        if nz == 4:
            far_one = jnp.where(z < 2, 3, 0)
            second = jnp.where(z < 2, 2 - 2 * z, 7 - 2 * z)
            third = 1 + z % 2
            return jnp.where(step == 0, far_one, jnp.where(step == 1, second, jnp.where(step == 2, third, z)))
        return (z + 1 + step) % nz

    def term(where):
        sides = (((1,), (1 if turned else 0,)), ((), ()))
        return lax.dot_general(
            left_ref[where], right_ref[...], sides, preferred_element_type=jnp.float32
        )

    def order(index, aa, bb, cc):
        part = index // nz
        flip_b = 1 - part // 2
        flip_a = 1 - part % 2
        return slot(zed(index % nz), aa + flip_a * (1 - 2 * aa), bb + flip_b * (1 - 2 * bb), cc)

    def twin_copy(index):
        return pltpu.make_async_remote_copy(
            src_ref=sent.at[index], dst_ref=got.at[index], send_sem=twin_send.at[index],
            recv_sem=twin_recv.at[index], device_id=twin, device_id_type=MESH)

    def far_copy(index):
        return pltpu.make_async_remote_copy(
            src_ref=got.at[index], dst_ref=from_far.at[index], send_sem=far_send.at[index],
            recv_sem=far_recv.at[index], device_id=far, device_id_type=MESH)

    def near_copy(index):
        return pltpu.make_async_remote_copy(
            src_ref=got.at[2 * nz + index], dst_ref=from_near.at[index], send_sem=near_send.at[index],
            recv_sem=near_recv.at[index], device_id=near, device_id_type=MESH)

    def up_copy(index, zz):
        return pltpu.make_async_remote_copy(
            src_ref=got.at[3 * nz + index], dst_ref=rising.at[zz], send_sem=line_send.at[index],
            recv_sem=up_recv.at[zz], device_id=up, device_id_type=MESH)

    def down_copy(index, zz):
        return pltpu.make_async_remote_copy(
            src_ref=got.at[3 * nz + index], dst_ref=falling.at[zz], send_sem=line_send.at[index],
            recv_sem=down_recv.at[zz], device_id=down, device_id_type=MESH)

    def give(index):
        sent[index] = term(order(index, b, a, 1 - c)).astype(sent.dtype)
        twin_copy(index).start()

    def taken(index):
        value = term(order(index, a, b, c))
        twin_copy(index).wait_recv()
        return value + got[index].astype(jnp.float32)

    def far_step(step, carry):
        give(2 * step)
        give(2 * step + 1)
        got[step] = taken(step).astype(got.dtype)
        far_copy(step).start()
        riders.looped(step, 2 * nz)
        return carry

    lax.fori_loop(0, 2 * nz, far_step, 0)

    def near_step(step, carry):
        value = taken(2 * nz + step)
        far_copy(step).wait_recv()
        value = value + from_far[step].astype(jnp.float32)
        got[2 * nz + step] = value.astype(got.dtype)
        near_copy(step).start()
        return carry

    lax.fori_loop(0, nz, near_step, 0)

    def line_step(step, carry):
        zz = zed(step)
        value = taken(3 * nz + step)
        far_copy(nz + step).wait_recv()
        near_copy(step).wait_recv()
        out_ref[...] = value + from_far[nz + step].astype(jnp.float32) + from_near[step].astype(jnp.float32)

        @pl.when((zz >= z) & (z > 0))
        def _():
            up_copy(step, zz).wait_recv()
            out_ref[...] += rising[zz].astype(jnp.float32)

        @pl.when((zz <= z) & (z < nz - 1))
        def _():
            down_copy(step, zz).wait_recv()
            out_ref[...] += falling[zz].astype(jnp.float32)

        @pl.when(zz > z)
        def _():
            got[3 * nz + step] = out_ref[...].astype(got.dtype)
            up_copy(step, zz).start()

        @pl.when(zz < z)
        def _():
            got[3 * nz + step] = out_ref[...].astype(got.dtype)
            down_copy(step, zz).start()

        return carry

    lax.fori_loop(0, nz, line_step, 0)

    def finish(step, carry):
        twin_copy(step).wait_send()
        return carry

    lax.fori_loop(0, per, finish, 0)

    def finish_far(step, carry):
        far_copy(step).wait_send()
        return carry

    lax.fori_loop(0, 2 * nz, finish_far, 0)

    def finish_near(step, carry):
        near_copy(step).wait_send()

        @pl.when(step < nz - 1)
        def _():
            up_copy(step, 0).wait_send()

        return carry

    lax.fori_loop(0, nz, finish_near, 0)
    riders.finish()


def scatter_sum(left, right, devices, ident, turned=False, riders=()):
    nz = devices // 8
    rows = left.shape[0] // devices
    depth, wide = right.shape[::-1] if turned else right.shape
    kinds, ridden, rider_outs, rider_sems = rider_shapes(riders, devices)
    block = (rows, wide)
    low = jnp.bfloat16
    dma = pltpu.SemaphoreType.DMA
    result = pl.pallas_call(
        functools.partial(scatter_kernel, nz, turned, kinds),
        out_shape=(jax.ShapeDtypeStruct(block, jnp.float32),) + rider_outs,
        in_specs=[pl.BlockSpec(memory_space=pltpu.VMEM)] * 2 + rider_specs(kinds),
        out_specs=(pl.BlockSpec(memory_space=pltpu.VMEM),)
        + (pl.BlockSpec(memory_space=pl.ANY),) * len(riders),
        scratch_shapes=[
            pltpu.VMEM((4 * nz,) + block, low),
            pltpu.VMEM((4 * nz,) + block, low),
            pltpu.VMEM((2 * nz,) + block, low),
            pltpu.VMEM((nz,) + block, low),
            pltpu.VMEM((nz,) + block, low),
            pltpu.VMEM((nz,) + block, low),
            dma((4 * nz,)), dma((4 * nz,)), dma((2 * nz,)), dma((2 * nz,)),
            dma((nz,)), dma((nz,)), dma((nz,)), dma((nz,)), dma((nz,)),
        ]
        + rider_sems,
        compiler_params=pltpu.CompilerParams(
            collective_id=ident, has_side_effects=True, vmem_limit_bytes=58 * 2**20),
        name="scatter_sum_%d" % ident,
    )(left.reshape(devices, rows, depth), right, *ridden)
    return result if riders else result[0]


class SlabSum:
    def __init__(self, nz, turned, spot, ways, refs, buffers):
        self.nz, self.turned = nz, turned
        self.z, self.x, self.c = spot
        self.up, self.down, self.side, self.twin = ways
        self.lefts, self.rights, self.beside, self.out = refs
        (self.sent, self.got, self.from_side, self.rising, self.falling, self.held,
         self.twin_send, self.twin_recv, self.side_send, self.side_recv, self.line_send,
         self.up_recv, self.down_recv) = buffers
        self.plain = self.rights[0].shape[0 if turned else 1]
        self.span = 512 if self.plain % 512 == 0 else self.plain

    def zed(self, step):
        z, nz = self.z, self.nz
        if nz == 4:
            far_one = jnp.where(z < 2, 3, 0)
            second = jnp.where(z < 2, 2 - 2 * z, 7 - 2 * z)
            third = 1 + z % 2
            return jnp.where(step == 0, far_one, jnp.where(step == 1, second, jnp.where(step == 2, third, z)))
        return (z + 1 + step) % nz

    def order(self, index, cc):
        flip = 1 - index // self.nz
        return self.zed(index % self.nz) * 4 + (self.x + flip * (1 - 2 * self.x)) * 2 + cc

    def combine(self, targets_, wheres, added):
        rows = self.lefts[0].shape[1]

        def put(which, at, total):
            for ref in added[which]:
                total = total + ref[:, at].astype(jnp.float32)
            targets_[which][:, at] = total.astype(targets_[which].dtype)

        def fill(chunk, carry):
            at = pl.ds(pl.multiple_of(chunk * self.span, self.span), self.span)
            total = None
            for left_ref, right_ref in zip(self.lefts, self.rights):
                value = lax.dot_general(
                    jnp.concatenate([left_ref[where] for where in wheres], axis=0),
                    right_ref[at, :] if self.turned else right_ref[:, at],
                    (((1,), (1 if self.turned else 0,)), ((), ())),
                    preferred_element_type=jnp.float32,
                )
                total = value if total is None else total + value
            for which in range(len(wheres)):
                put(which, at, total[which * rows : (which + 1) * rows])
            return carry

        lax.fori_loop(0, self.plain // self.span, fill, 0)
        if self.beside is not None:
            at = pl.ds(self.plain, self.beside.shape[2])
            for which, where in enumerate(wheres):
                put(which, at, self.beside[where].astype(jnp.float32))

    def remote(self, source, target, send, recv, device):
        return pltpu.make_async_remote_copy(
            src_ref=source, dst_ref=target, send_sem=send, recv_sem=recv,
            device_id=device, device_id_type=MESH)

    def twin_copy(self, index):
        return self.remote(
            self.sent.at[index], self.got.at[index], self.twin_send.at[index],
            self.twin_recv.at[index], self.twin)

    def side_copy(self, index):
        return self.remote(
            self.got.at[index], self.from_side.at[index], self.side_send.at[index],
            self.side_recv.at[index], self.side)

    def line_copy(self, index, zz, rise):
        place_, recv = (self.rising, self.up_recv) if rise else (self.falling, self.down_recv)
        return self.remote(
            self.got.at[self.nz + index], place_.at[zz], self.line_send.at[index], recv.at[zz],
            self.up if rise else self.down)

    def give(self, pair, carry):
        both = (2 * pair, 2 * pair + 1)
        self.combine(
            [self.sent.at[index] for index in both],
            [self.order(index, 1 - self.c) for index in both], [(), ()])
        for index in both:
            self.twin_copy(index).start()
        return carry

    def to_side(self, pair):
        lax.fori_loop(2 * pair, 2 * pair + 2, self.give, 0)
        both = (2 * pair, 2 * pair + 1)
        for index in both:
            self.twin_copy(index).wait_recv()
        self.combine(
            [self.got.at[index] for index in both],
            [self.order(index, self.c) for index in both],
            [(self.got.at[index],) for index in both])
        for index in both:
            self.side_copy(index).start()

    def to_line(self, pair):
        both = (2 * pair, 2 * pair + 1)
        for step in both:
            self.twin_copy(self.nz + step).wait_recv()
            self.side_copy(step).wait_recv()
        self.combine(
            [self.held.at[0], self.held.at[1]],
            [self.order(self.nz + step, self.c) for step in both],
            [(self.got.at[self.nz + step], self.from_side.at[step]) for step in both])
        for which, step in enumerate(both):
            self.along_line(self.held.at[which], step)

    def along_line(self, held, step):
        z, zz = self.z, self.zed(step)

        @pl.when((zz >= z) & (z > 0))
        def _():
            self.line_copy(step, zz, True).wait_recv()
            held[...] += self.rising[zz].astype(jnp.float32)

        @pl.when((zz <= z) & (z < self.nz - 1))
        def _():
            self.line_copy(step, zz, False).wait_recv()
            held[...] += self.falling[zz].astype(jnp.float32)

        @pl.when(zz != z)
        def _():
            self.got[self.nz + step] = held[...].astype(self.got.dtype)

        pl.when(zz > z)(lambda: self.line_copy(step, zz, True).start())
        pl.when(zz < z)(lambda: self.line_copy(step, zz, False).start())

    def end(self):
        self.out[...] = self.held[1]

        def finish(step, carry):
            self.twin_copy(step).wait_send()
            return carry

        lax.fori_loop(0, 2 * self.nz, finish, 0)

        def finish_side(step, carry):
            self.side_copy(step).wait_send()

            @pl.when(step < self.nz - 1)
            def _():
                self.line_copy(step, 0, True).wait_send()

            return carry

        lax.fori_loop(0, self.nz, finish_side, 0)


def slab_scatter_kernel(nz, forms, kinds, *refs):
    extra, parts = len(kinds), len(forms)
    refs = list(refs)

    def take(count):
        taken = tuple(refs[:count])
        del refs[:count]
        return taken

    operands = []
    for pairs, turned, beside in forms:
        operands.append((take(pairs), take(pairs), take(1)[0] if beside else None))
    rider_ins = take(extra)
    outs = take(parts)
    rider_outs = take(extra)
    dp, ep, z, y, x, c, _, _ = place()
    up, down, near, far, twin = targets(dp, ep, z, y, x, c, nz)
    side = (dp, ep + 2 - 4 * x)
    sums = [
        SlabSum(nz, form[1], (z, x, c), (up, down, side, twin), held + (out,), take(13))
        for form, held, out in zip(forms, operands, outs)
    ]
    riders = Riders(kinds, nz, (dp, ep, z, y), rider_ins + rider_outs + tuple(refs))
    greet(nz, z, dp, ep, (up, down, near, far, twin), wide_greeting(kinds))
    riders.begin(("half", "line"))

    def side_step(pair, carry):
        for part in sums:
            part.to_side(pair)
        riders.looped(pair, nz // 2)
        return carry

    lax.fori_loop(0, nz // 2, side_step, 0)

    def line_step(pair, carry):
        for part in sums:
            part.to_line(pair)
        return carry

    lax.fori_loop(0, nz // 2, line_step, 0)
    for part in sums:
        part.end()
    riders.finish()


def slab_scatter(parts, devices, ident, riders=()):
    nz = devices // 8
    blocks = 4 * nz
    rows = parts[0][0][0].shape[0] // blocks
    kinds, ridden, rider_outs, rider_sems = rider_shapes(riders, devices)
    low, dma = jnp.bfloat16, pltpu.SemaphoreType.DMA
    operands, outs, scratch, forms = (), (), [], []
    for lefts, rights, turned, beside in parts:
        held = () if beside is None else (beside.reshape(blocks, rows, -1),)
        wide = rights[0].shape[0 if turned else 1] + sum(v.shape[2] for v in held)
        block = (rows, wide)
        operands += tuple(v.reshape(blocks, rows, -1) for v in lefts) + tuple(rights) + held
        outs += (jax.ShapeDtypeStruct(block, jnp.float32),)
        scratch += [pltpu.VMEM((count * nz,) + block, low) for count in (2, 2, 1, 1, 1)]
        scratch += [pltpu.VMEM((2,) + block, jnp.float32)]
        scratch += [dma((2 * nz,))] * 2 + [dma((nz,))] * 5
        forms.append((len(lefts), turned, len(held)))
    return pl.pallas_call(
        functools.partial(slab_scatter_kernel, nz, tuple(forms), kinds),
        out_shape=outs + rider_outs,
        in_specs=[pl.BlockSpec(memory_space=pltpu.VMEM)] * len(operands) + rider_specs(kinds),
        out_specs=(pl.BlockSpec(memory_space=pltpu.VMEM),) * len(outs)
        + (pl.BlockSpec(memory_space=pl.ANY),) * len(riders),
        scratch_shapes=scratch + rider_sems,
        compiler_params=pltpu.CompilerParams(
            collective_id=ident, has_side_effects=True, vmem_limit_bytes=63 * 2**20),
        name="slab_scatter_%d" % ident,
    )(*operands, *ridden)


def whole_rows(mesh):
    return mesh.shape["ep"] == 4 and mesh.shape["dp"] in (4, 8)


def exact_dot(left_side, right_side):
    return jnp.dot(
        left_side, right_side, precision=lax.Precision.HIGHEST, preferred_element_type=jnp.float32
    )


def block_layout(lens, tok_count):
    ends = [lens[:, :1]]
    for at in range(1, lens.shape[1]):
        ends.append(ends[-1] + lens[:, at : at + 1])
    row_index = lax.broadcasted_iota(jnp.int32, (lens.shape[0], tok_count), 1)
    segment = jnp.zeros_like(row_index)
    first_row = jnp.zeros_like(row_index)
    for end in ends:
        passed = row_index >= end
        segment = segment + passed.astype(jnp.int32)
        first_row = jnp.where(passed, end, first_row)
    return (segment, row_index - first_row)


def by_experts(
    hidden_in,
    cotangent,
    deal_order,
    seq_lengths,
    expert_ids,
    w_query,
    w_key,
    w_value,
    w_out,
    w_router,
    gain_attn,
    gain_moe,
    gain_query,
    gain_key,
    w_gate,
    w_up,
    w_down,
    clip_threshold,
):
    f32, low = jnp.float32, jnp.bfloat16
    dp_count, ep_count = lax.axis_size("dp"), lax.axis_size("ep")
    devices = dp_count * ep_count
    dp, ep = lax.axis_index("dp"), lax.axis_index("ep")
    me = dp * ep_count + ep
    tok_count, width = hidden_in.shape
    row_count = tok_count * 7 // 8
    all_count = devices * row_count
    head_dim = gain_query.shape[0]
    half_dim = head_dim // 2
    rows_own = w_query.shape[0]
    head_count = w_query.shape[1] // head_dim
    kv_count = w_key.shape[1] // head_dim
    group_size = head_count // kv_count
    experts = w_router.shape[1]
    exp_local, wide_own, hidden = w_gate.shape
    lines = dp_count // 2
    slab = lines * ep_count
    z, y = dp // 2, dp % 2
    score_scale = head_dim ** (-0.5)

    gain_col = gain_attn.astype(f32)[:, None]
    heads_in = (w_query.astype(f32) * gain_col).astype(low).reshape(rows_own, head_count, head_dim)
    keys_in = (w_key.astype(f32) * gain_col).astype(low).reshape(rows_own, kv_count, head_dim)
    values_in = (w_value.astype(f32) * gain_col).astype(low).reshape(rows_own, kv_count, head_dim)
    sent_heads = jnp.concatenate(
        [heads_in, jnp.repeat(keys_in, group_size, axis=1), jnp.repeat(values_in, group_size, axis=1)],
        axis=2,
    ).transpose(1, 0, 2)

    local_order = deal_order % tok_count
    deal = (local_order[:, None] == jnp.arange(tok_count, dtype=jnp.int32)[None, :]).astype(low)
    deal = deal[:row_count]
    resid_in = jnp.dot(deal, hidden_in, preferred_element_type=f32)
    grad_mid_out = jnp.dot(deal, cotangent, preferred_element_type=f32)
    inv_one = rms_scale(resid_in)
    unit_one = resid_in * inv_one
    lens_row = jnp.pad(seq_lengths.astype(f32), ((0, 0), (0, 128 - seq_lengths.shape[1])))
    gain_row = jnp.pad(gain_moe.astype(f32)[None, :], ((0, 0), (0, 128 - rows_own)))
    router_rows = w_router.astype(f32).reshape(-1, 128)
    note_one = jnp.concatenate([lens_row, gain_row, router_rows], axis=0)
    note_one = jnp.pad(note_one, ((0, -note_one.shape[0] % 8), (0, 0)))
    unit_all, notes, grad_all, w_heads, w_rise_up = gather_rows(
        (unit_one.astype(low), note_one),
        (grad_mid_out.astype(low),),
        devices,
        1,
        (("all", sent_heads), ("cube", w_up)),
    )
    w_heads = w_heads.reshape(width, 3 * head_dim)
    w_rise_up = w_rise_up.reshape(width, hidden)
    lens_all = notes[:, 0, : seq_lengths.shape[1]].astype(jnp.int32)
    gain_two = notes[:, 1, :rows_own].reshape(1, width)
    router_full = notes[:, 2 : 2 + router_rows.shape[0]].reshape(width, experts)

    segment, position = block_layout(lens_all, row_count)
    step_down = lax.broadcasted_iota(jnp.int32, (1, row_count, row_count), 1)
    step_across = lax.broadcasted_iota(jnp.int32, (1, row_count, row_count), 2)
    allowed = (segment[:, :, None] == segment[:, None, :]) & (step_across <= step_down)
    cosine_rows, sine_rows = rotary_tables(jnp.arange(tok_count, dtype=jnp.int32), head_dim)
    place_hot = (position.reshape(-1)[:, None] == jnp.arange(tok_count)[None, :]).astype(f32)
    cosine_all = exact_dot(place_hot, cosine_rows).reshape(devices, row_count, head_dim)
    sine_all = exact_dot(place_hot, sine_rows).reshape(devices, row_count, head_dim)
    flat_unit = unit_all.reshape(all_count, width)
    projected = jnp.dot(flat_unit, w_heads, preferred_element_type=f32).reshape(
        devices, row_count, 3 * head_dim
    )
    query_raw = projected[..., :head_dim]
    key_raw = projected[..., head_dim : 2 * head_dim]
    value_rows = projected[..., 2 * head_dim :].astype(low)
    gain_query_f = gain_query.astype(f32)
    gain_key_f = gain_key.astype(f32)
    inv_query = rms_scale(query_raw)
    unit_query = query_raw * inv_query
    query_rot = rotate(unit_query * gain_query_f, cosine_all, sine_all).astype(low)
    inv_key = rms_scale(key_raw)
    unit_key = key_raw * inv_key
    key_rot = rotate(unit_key * gain_key_f, cosine_all, sine_all).astype(low)
    scores = contract(query_rot, key_rot, "btd,bud->btu") * score_scale
    masked = jnp.where(allowed, scores, masked_fill)
    row_top = jnp.max(masked, axis=-1, keepdims=True)
    exponent = jnp.exp(masked - row_top)
    probs = exponent / jnp.sum(exponent, axis=-1, keepdims=True)
    probs_low = probs.astype(low)
    mixed = contract(probs_low, value_rows, "btu,bud->btd").astype(low).reshape(all_count, head_dim)
    largest_own = jnp.max(row_top)
    branch, fall_own = scatter_sum(mixed, w_out, devices, 2, riders=(("line", w_down.transpose(0, 2, 1)),))
    resid_mid = resid_in + branch

    inv_two = rms_scale(resid_mid)
    unit_two = resid_mid * inv_two
    normed_mid = (unit_two * gain_two).astype(low)
    logits = jnp.dot(normed_mid, router_full.astype(low), preferred_element_type=f32)
    choose = (expert_ids[:row_count, :, None] == jnp.arange(experts, dtype=jnp.int32)[None, None, :]).any(axis=1)
    picked = jnp.where(choose, logits, masked_fill)
    gate_power = jnp.where(choose, jnp.exp(picked - jnp.max(picked, axis=1, keepdims=True)), 0.0)
    route = gate_power / jnp.sum(gate_power, axis=1, keepdims=True)
    note_two = jnp.pad(route.T, ((0, 0), (0, 128 - row_count)))
    normed_all, notes, w_rise_gate, w_fall = gather_rows(
        (), (normed_mid, note_two), devices, 3, (("cube", w_gate), ("pair", fall_own))
    )
    w_rise_gate = w_rise_gate.reshape(width, hidden)
    w_fall = w_fall.reshape(width, hidden)

    mine = ep * exp_local + z
    slab_rows = slab * row_count
    weight = lax.dynamic_slice_in_dim(notes, mine, 1, axis=1)[..., :row_count].reshape(slab_rows, 1)
    flat_mid = normed_all.reshape(slab_rows, width)
    flat_grad = grad_all.reshape(slab_rows, width)
    gate_part = jnp.dot(flat_mid, w_rise_gate, preferred_element_type=f32)
    up_part = jnp.dot(flat_mid, w_rise_up, preferred_element_type=f32)
    grad_plain = jnp.dot(flat_grad, w_fall, preferred_element_type=f32)
    sigmoid_gate = jax.nn.sigmoid(gate_part)
    silu_gate = gate_part * sigmoid_gate
    hidden_mid = silu_gate * up_part
    grad_route = jnp.sum(hidden_mid * grad_plain, axis=1, keepdims=True)
    weighted_mid = (hidden_mid * weight).astype(low)
    grad_hidden = grad_plain * weight
    grad_gate_part = (
        grad_hidden * up_part * sigmoid_gate * (1.0 + gate_part * (1.0 - sigmoid_gate))
    ).astype(low)
    grad_up_part = (grad_hidden * silu_gate).astype(low)
    lane = lax.broadcasted_iota(jnp.int32, (1, 128), 1)
    beside = jnp.where(lane == mine, grad_route, 0.0).astype(low)

    def for_each_y(grads):
        return grads.astype(low).reshape(lines, 2, wide_own, hidden)

    gate_halves = for_each_y(contract(flat_mid, grad_gate_part, "td,tf->df"))
    up_halves = for_each_y(contract(flat_mid, grad_up_part, "td,tf->df"))
    fall_halves = for_each_y(contract(flat_grad, weighted_mid, "td,tf->df"))
    summed, moe_rows, gate_come, up_come, fall_come = slab_scatter(
        (
            ((grad_gate_part, grad_up_part), (w_rise_gate, w_rise_up), True, beside),
            ((weighted_mid,), (w_fall,), True, None),
        ),
        devices,
        4,
        (("half", gate_halves), ("half", up_halves), ("half", fall_halves)),
    )

    def add_halves(halves, come):
        kept = lax.dynamic_index_in_dim(halves, y, axis=1, keepdims=False)
        return (kept.astype(f32) + come.astype(f32)).astype(low)

    grad_gates = summed[:, width : width + experts]
    mean_term = jnp.sum(route * grad_gates, axis=1, keepdims=True)
    grad_logits = (route * (grad_gates - mean_term)).astype(low)
    grad_normed_mid = summed[:, :width] + contract(grad_logits, router_full.astype(low), "te,de->td")
    gain_part = jnp.sum(grad_normed_mid * unit_two, axis=0)
    grad_mid = grad_mid_out + norm_back(grad_normed_mid * gain_two, unit_two, inv_two)
    grad_branch = grad_mid.astype(low)
    router_part = contract(normed_mid, grad_logits, "td,te->de").reshape(devices, -1, 128)
    note_three = jnp.concatenate(
        [
            gain_part.reshape(-1, 128),
            jnp.full((8, 128), largest_own, f32),
        ],
        axis=0,
    )
    branch_all, notes, back_gate, back_up = gather_rows(
        (grad_branch, note_three),
        (),
        devices,
        6,
        (
            ("line", add_halves(gate_halves, gate_come)),
            ("line", add_halves(up_halves, up_come)),
        ),
    )
    clip_factor = jnp.sqrt(clip_threshold / jnp.maximum(notes[:, -1, 0], clip_threshold))
    gain_sum = jnp.sum(notes[:, :-8], axis=0).reshape(-1)
    grad_gain_moe = lax.dynamic_slice_in_dim(gain_sum, me * rows_own, rows_own)

    flat_branch = branch_all.reshape(all_count, width)
    grad_out = contract(mixed, flat_branch, "tq,td->qd")
    grad_mixed = (
        contract(flat_branch, w_out, "td,qd->tq").astype(low).reshape(devices, row_count, head_dim)
    )
    grad_value = contract(probs_low, grad_mixed, "btu,btd->bud").astype(low)
    grad_probs = contract(grad_mixed, value_rows, "btd,bud->btu")
    grad_scores = (
        probs * (grad_probs - jnp.sum(probs * grad_probs, axis=-1, keepdims=True))
    ).astype(low)
    grad_query_rot = contract(grad_scores, key_rot, "btu,bud->btd") * score_scale
    grad_key_rot = contract(grad_scores, query_rot, "btu,btd->bud") * score_scale
    grad_query_normed = rotate_back(grad_query_rot, cosine_all, sine_all)
    grad_key_normed = rotate_back(grad_key_rot, cosine_all, sine_all)
    gain_pair = jnp.stack(
        [
            jnp.sum(grad_query_normed * unit_query, axis=(0, 1)),
            jnp.sum(grad_key_normed * unit_key, axis=(0, 1)),
        ]
    )
    grad_query_raw = norm_back(grad_query_normed * gain_query_f, unit_query, inv_query).astype(low)
    grad_key_raw = norm_back(grad_key_normed * gain_key_f, unit_key, inv_key).astype(low)
    grad_heads = jnp.concatenate([grad_query_raw, grad_key_raw, grad_value], axis=2).reshape(
        all_count, 3 * head_dim
    )
    grad_heads_w = contract(flat_unit, grad_heads, "td,tq->dq").astype(low)
    resid_out = resid_mid + moe_rows
    undeal = (jnp.arange(tok_count, dtype=jnp.int32)[:, None] == local_order[None, :]).astype(low)
    undeal = undeal[:, :row_count]
    block_out = jnp.dot(undeal, resid_out.astype(low), preferred_element_type=f32).astype(low)
    grad_unit_one, back_heads, back_fall, gain_pairs, router_parts = scatter_sum(
        grad_heads,
        w_heads,
        devices,
        7,
        turned=True,
        riders=(
            ("all", grad_heads_w.reshape(devices, rows_own, 3 * head_dim)),
            ("line", add_halves(fall_halves, fall_come)),
            ("same", jnp.pad(gain_pair, ((0, 6), (0, 0)))),
            ("all", router_part),
        ),
    )
    back_heads = back_heads.astype(f32)
    grad_gate = back_gate.astype(f32)
    grad_up = back_up.astype(f32)
    grad_down = back_fall.transpose(0, 2, 1).astype(f32)
    grad_router = jnp.sum(router_parts, axis=0).reshape(rows_own, experts)
    gain_pair = jnp.sum(gain_pairs, axis=0)
    plain_query = back_heads[..., :head_dim].transpose(1, 0, 2).reshape(rows_own, -1)

    def of_group(grads):
        grads = jnp.sum(grads.reshape(kv_count, group_size, rows_own, head_dim), axis=1)
        return grads.transpose(1, 0, 2).reshape(rows_own, -1)

    plain_key = of_group(back_heads[..., head_dim : 2 * head_dim])
    plain_value = of_group(back_heads[..., 2 * head_dim :])
    grad_gain_attn = (
        jnp.sum(plain_query * w_query.astype(f32), axis=1)
        + jnp.sum(plain_key * w_key.astype(f32), axis=1)
        + jnp.sum(plain_value * w_value.astype(f32), axis=1)
    )
    grad_resid_in = grad_mid + norm_back(grad_unit_one, unit_one, inv_one)
    grad_input = exact_dot(undeal.astype(f32), grad_resid_in)
    return (
        block_out,
        grad_input,
        plain_query * gain_col,
        plain_key * gain_col,
        plain_value * gain_col,
        grad_out,
        grad_router,
        grad_gain_attn,
        grad_gain_moe,
        gain_pair[0],
        gain_pair[1],
        grad_gate,
        grad_up,
        grad_down,
        clip_factor,
    )


def solution(mesh):
    placed = (
        P(("dp", "ep"), None),
        P(("dp", "ep"), None),
        P(("dp", "ep")),
        P(("dp", "ep"), None),
        P(("dp", "ep"), None),
        P(("dp", "ep"), None),
        P(("dp", "ep"), None),
        P(("dp", "ep"), None),
        P(("dp", "ep"), None),
        P(("dp", "ep"), None),
        P(("dp", "ep")),
        P(("dp", "ep")),
        P(),
        P(),
        P("ep", "dp", None),
        P("ep", "dp", None),
        P("ep", None, "dp"),
        P(),
    )
    return jax.shard_map(
        per_device if not whole_rows(mesh) else by_experts,
        mesh=mesh,
        in_specs=placed,
        out_specs=(
            P(("dp", "ep"), None),
            P(("dp", "ep"), None),
            P(("dp", "ep"), None),
            P(("dp", "ep"), None),
            P(("dp", "ep"), None),
            P(("dp", "ep"), None),
            P(("dp", "ep"), None),
            P(("dp", "ep")),
            P(("dp", "ep")),
            P(),
            P(),
            P("ep", "dp", None),
            P("ep", "dp", None),
            P("ep", None, "dp"),
            P(),
        ),
        check_vma=False,
    )
```

```python
import functools

import jax
import jax.numpy as jnp
from jax import lax
from jax.experimental import pallas as pl
from jax.experimental.pallas import tpu as pltpu
from jax.sharding import PartitionSpec as P

epsilon = 1e-06
theta_base = 1000000.0
masked_fill = -1e30


def rms_scale(values):
    return lax.rsqrt(jnp.mean(values * values, axis=-1, keepdims=True) + epsilon)


def rotate_half(values):
    half_dim = values.shape[-1] // 2
    return jnp.concatenate([-values[..., half_dim:], values[..., :half_dim]], axis=-1)


def rotate(values, cosine_table, sine_table):
    return values * cosine_table + rotate_half(values) * sine_table


def rotate_back(values, cosine_table, sine_table):
    scaled = values * sine_table
    half_dim = values.shape[-1] // 2
    turned = jnp.concatenate([scaled[..., half_dim:], -scaled[..., :half_dim]], axis=-1)
    return values * cosine_table + turned


def norm_back(grad_unit, unit_rows, inv_root):
    return inv_root * (
        grad_unit - unit_rows * jnp.mean(grad_unit * unit_rows, axis=-1, keepdims=True)
    )


def contract(left_side, right_side, pattern):
    return jnp.einsum(pattern, left_side, right_side, preferred_element_type=jnp.float32)


def layout(lens_row, tok_count):
    seq_ends = jnp.cumsum(lens_row)
    row_index = jnp.arange(tok_count, dtype=jnp.int32)
    segment = jnp.sum((row_index[:, None] >= seq_ends[None, :]).astype(jnp.int32), axis=1)
    starts_all = jnp.concatenate([jnp.zeros((1,), jnp.int32), seq_ends])
    seg_hot = segment[:, None] == jnp.arange(starts_all.shape[0], dtype=jnp.int32)[None, :]
    first_row = jnp.sum(jnp.where(seg_hot, starts_all[None, :], 0), axis=1)
    position = row_index - first_row
    valid_row = segment < lens_row.shape[0]
    allowed = (segment[:, None] == segment[None, :]) & (row_index[None, :] <= row_index[:, None])
    return (position, valid_row, allowed)


def rotary_tables(position, head_dim):
    half_dim = head_dim // 2
    frequency = theta_base ** (-(jnp.arange(half_dim, dtype=jnp.float32) * 2.0) / head_dim)
    angles = position.astype(jnp.float32)[:, None] * frequency[None, :]
    angles = jnp.concatenate([angles, angles], axis=-1)
    return (jnp.cos(angles), jnp.sin(angles))


def per_device(
    hidden_in,
    cotangent,
    deal_order,
    seq_lengths,
    expert_ids,
    w_query,
    w_key,
    w_value,
    w_out,
    w_router,
    gain_attn,
    gain_moe,
    gain_query,
    gain_key,
    w_gate,
    w_up,
    w_down,
    clip_threshold,
):
    tok_count = hidden_in.shape[0]
    model_width = hidden_in.shape[1]
    head_dim = gain_query.shape[0]
    local_order = deal_order % tok_count
    position, valid_row, allowed = layout(seq_lengths[0], tok_count)
    valid_col = valid_row.astype(jnp.float32)[:, None]
    cosine_table, sine_table = rotary_tables(position, head_dim)
    cosine_query = cosine_table[:, None, None, :]
    sine_query = sine_table[:, None, None, :]
    cosine_key = cosine_table[:, None, :]
    sine_key = sine_table[:, None, :]
    attn_params = (
        lax.all_gather(w_query, ("dp", "ep"), axis=0, tiled=True),
        lax.all_gather(w_key, ("dp", "ep"), axis=0, tiled=True),
        lax.all_gather(w_value, ("dp", "ep"), axis=0, tiled=True),
        lax.all_gather(w_out, ("dp", "ep"), axis=0, tiled=True),
        lax.all_gather(w_router, ("dp", "ep"), axis=0, tiled=True),
        lax.all_gather(gain_attn, ("dp", "ep"), axis=0, tiled=True),
        lax.all_gather(gain_moe, ("dp", "ep"), axis=0, tiled=True),
    )
    expert_params = (
        lax.all_gather(w_gate, "dp", axis=1, tiled=True),
        lax.all_gather(w_up, "dp", axis=1, tiled=True),
        lax.all_gather(w_down, "dp", axis=2, tiled=True),
    )
    query_full, key_full, value_full, out_full, router_full, gain_attn_full, gain_moe_full = (
        attn_params
    )
    gate_full, up_full, down_full = expert_params
    head_count = query_full.shape[1] // head_dim
    kv_count = key_full.shape[1] // head_dim
    group_size = head_count // kv_count
    experts = router_full.shape[1]
    top_count = expert_ids.shape[1]
    exp_local = w_gate.shape[0]
    ep_count = lax.axis_size("ep")
    capacity = (tok_count * top_count * 5 + 4 * experts - 1) // (4 * experts)
    score_scale = head_dim ** (-0.5)
    resid_in = hidden_in[local_order].astype(jnp.float32)
    inv_one = rms_scale(resid_in)
    unit_one = resid_in * inv_one
    gain_one = gain_attn_full.astype(jnp.float32)
    normed_in = (unit_one * gain_one).astype(jnp.bfloat16)
    query_raw = jnp.dot(normed_in, query_full, preferred_element_type=jnp.float32).reshape(
        tok_count, kv_count, group_size, head_dim
    )
    key_raw = jnp.dot(normed_in, key_full, preferred_element_type=jnp.float32).reshape(
        tok_count, kv_count, head_dim
    )
    value_rows = (
        jnp.dot(normed_in, value_full, preferred_element_type=jnp.float32)
        .astype(jnp.bfloat16)
        .reshape(tok_count, kv_count, head_dim)
    )
    inv_query = rms_scale(query_raw)
    unit_query = query_raw * inv_query
    gain_query_f = gain_query.astype(jnp.float32)
    query_rot = rotate(unit_query * gain_query_f, cosine_query, sine_query).astype(jnp.bfloat16)
    inv_key = rms_scale(key_raw)
    unit_key = key_raw * inv_key
    gain_key_f = gain_key.astype(jnp.float32)
    key_rot = rotate(unit_key * gain_key_f, cosine_key, sine_key).astype(jnp.bfloat16)
    scores = contract(query_rot, key_rot, "tkgd,ukd->kgtu") * score_scale
    masked = jnp.where(allowed, scores, masked_fill)
    row_top = jnp.max(masked, axis=-1, keepdims=True)
    exponent = jnp.exp(masked - row_top)
    row_total = jnp.sum(exponent, axis=-1, keepdims=True)
    log_total = row_top + jnp.log(row_total)
    probs_low = (exponent / row_total).astype(jnp.bfloat16)
    mixed_heads = (
        contract(probs_low, value_rows, "kgtu,ukd->tkgd")
        .astype(jnp.bfloat16)
        .reshape(tok_count, head_count * head_dim)
    )
    resid_mid = resid_in + jnp.dot(mixed_heads, out_full, preferred_element_type=jnp.float32)
    largest_local = jnp.max(
        jnp.where(allowed & valid_row[:, None], scores, masked_fill), axis=(2, 3)
    ).reshape(head_count)
    largest = lax.pmax(largest_local, ("dp", "ep"))
    clip_factor = jnp.sqrt(clip_threshold / jnp.maximum(largest, clip_threshold))
    inv_two = rms_scale(resid_mid)
    unit_two = resid_mid * inv_two
    gain_two = gain_moe_full.astype(jnp.float32)
    normed_mid = (unit_two * gain_two).astype(jnp.bfloat16)
    logits = jnp.dot(normed_mid, router_full, preferred_element_type=jnp.float32)
    choose = expert_ids[:, :, None] == jnp.arange(experts, dtype=jnp.int32)[None, None, :]
    picked = jnp.sum(jnp.where(choose, logits[:, None, :], 0.0), axis=2)
    gate_weights = jax.nn.softmax(picked, axis=-1)
    flat_ids = expert_ids.reshape(-1)
    flat_hot = (flat_ids[:, None] == jnp.arange(experts, dtype=jnp.int32)[None, :]).astype(
        jnp.int32
    )
    slot_rank = jnp.sum((jnp.cumsum(flat_hot, axis=0) - 1) * flat_hot, axis=1)
    slot_index = flat_ids * capacity + slot_rank
    pair_token = jnp.arange(tok_count * top_count, dtype=jnp.int32) // top_count
    send_rows = (
        jnp.zeros((experts * capacity, model_width), jnp.bfloat16)
        .at[slot_index]
        .set(normed_mid[pair_token])
    )
    send_rows = send_rows.reshape(ep_count, exp_local, capacity, model_width)
    arrived = lax.all_to_all(send_rows, "ep", split_axis=0, concat_axis=0, tiled=True)
    gate_part = contract(arrived, gate_full, "secd,edf->secf")
    up_part = contract(arrived, up_full, "secd,edf->secf")
    hidden_mid = (jax.nn.silu(gate_part) * up_part).astype(jnp.bfloat16)
    produced = contract(hidden_mid, down_full, "secf,efd->secd").astype(jnp.bfloat16)
    returned = lax.all_to_all(produced, "ep", split_axis=0, concat_axis=0, tiled=True)
    returned, arrived, gate_part, up_part = (returned, arrived, gate_part, up_part)
    pair_out = (
        returned.reshape(experts * capacity, model_width)[slot_index]
        .reshape(tok_count, top_count, model_width)
        .astype(jnp.float32)
    )
    resid_out = resid_mid + jnp.sum(gate_weights[:, :, None] * pair_out, axis=1)
    out_rows = (resid_out * valid_col).astype(jnp.bfloat16)
    block_out = jnp.zeros_like(out_rows).at[local_order].set(out_rows)
    attn_params = (
        lax.all_gather(w_query, ("dp", "ep"), axis=0, tiled=True),
        lax.all_gather(w_key, ("dp", "ep"), axis=0, tiled=True),
        lax.all_gather(w_value, ("dp", "ep"), axis=0, tiled=True),
        lax.all_gather(w_out, ("dp", "ep"), axis=0, tiled=True),
        lax.all_gather(w_router, ("dp", "ep"), axis=0, tiled=True),
        lax.all_gather(gain_attn, ("dp", "ep"), axis=0, tiled=True),
        lax.all_gather(gain_moe, ("dp", "ep"), axis=0, tiled=True),
    )
    expert_params = (
        lax.all_gather(w_gate, "dp", axis=1, tiled=True),
        lax.all_gather(w_up, "dp", axis=1, tiled=True),
        lax.all_gather(w_down, "dp", axis=2, tiled=True),
    )
    query_full, key_full, value_full, out_full, router_full, gain_attn_full, gain_moe_full = (
        attn_params
    )
    gate_full, up_full, down_full = expert_params
    grad_mid_out = cotangent[local_order].astype(jnp.float32) * valid_col
    grad_gates = jnp.sum(grad_mid_out[:, None, :] * pair_out, axis=2)
    grad_pair = (gate_weights[:, :, None] * grad_mid_out[:, None, :]).astype(jnp.bfloat16)
    send_grads = (
        jnp.zeros((experts * capacity, model_width), jnp.bfloat16)
        .at[slot_index]
        .set(grad_pair.reshape(-1, model_width))
    )
    send_grads = send_grads.reshape(ep_count, exp_local, capacity, model_width)
    grad_arrived = lax.all_to_all(send_grads, "ep", split_axis=0, concat_axis=0, tiled=True)
    grad_hidden = contract(grad_arrived, down_full, "secd,efd->secf")
    sigmoid_gate = jax.nn.sigmoid(gate_part)
    silu_gate = jax.nn.silu(gate_part)
    grad_gate_part = (
        grad_hidden * up_part * sigmoid_gate * (1.0 + gate_part * (1.0 - sigmoid_gate))
    ).astype(jnp.bfloat16)
    grad_up_part = (grad_hidden * silu_gate).astype(jnp.bfloat16)
    grad_rows = (
        contract(grad_gate_part, gate_full, "secf,edf->secd")
        + contract(grad_up_part, up_full, "secf,edf->secd")
    ).astype(jnp.bfloat16)
    grad_back = lax.all_to_all(grad_rows, "ep", split_axis=0, concat_axis=0, tiled=True)
    hidden_mid = (silu_gate * up_part).astype(jnp.bfloat16)
    grad_gate_w = contract(arrived, grad_gate_part, "secd,secf->edf")
    grad_up_w = contract(arrived, grad_up_part, "secd,secf->edf")
    grad_down_w = contract(hidden_mid, grad_arrived, "secf,secd->efd")
    grad_gate, grad_up, grad_down = (
        lax.psum_scatter(
            grad_gate_w.astype(jnp.bfloat16), "dp", scatter_dimension=1, tiled=True
        ).astype(jnp.float32),
        lax.psum_scatter(
            grad_up_w.astype(jnp.bfloat16), "dp", scatter_dimension=1, tiled=True
        ).astype(jnp.float32),
        lax.psum_scatter(
            grad_down_w.astype(jnp.bfloat16), "dp", scatter_dimension=2, tiled=True
        ).astype(jnp.float32),
    )
    mean_term = jnp.sum(gate_weights * grad_gates, axis=1, keepdims=True)
    grad_picked = gate_weights * (grad_gates - mean_term)
    grad_logits = jnp.sum(jnp.where(choose, grad_picked[:, :, None], 0.0), axis=1).astype(
        jnp.bfloat16
    )
    grad_router_w = contract(normed_mid, grad_logits, "td,te->de")
    pair_grads = (
        grad_back.reshape(experts * capacity, model_width)[slot_index]
        .reshape(tok_count, top_count, model_width)
        .astype(jnp.float32)
    )
    grad_normed_mid = jnp.sum(pair_grads, axis=1) + contract(grad_logits, router_full, "te,de->td")
    grad_gain_moe_w = jnp.sum(grad_normed_mid * unit_two, axis=0)
    grad_mid = grad_mid_out + norm_back(grad_normed_mid * gain_two, unit_two, inv_two)
    grad_branch = grad_mid.astype(jnp.bfloat16)
    grad_out_w = contract(mixed_heads, grad_branch, "tq,td->qd")
    grad_mixed = (
        contract(grad_branch, out_full, "td,qd->tq")
        .astype(jnp.bfloat16)
        .reshape(tok_count, kv_count, group_size, head_dim)
    )
    scores_again = contract(query_rot, key_rot, "tkgd,ukd->kgtu") * score_scale
    probs_back = jnp.exp(jnp.where(allowed, scores_again, masked_fill) - log_total)
    grad_value_rows = contract(
        probs_back.astype(jnp.bfloat16), grad_mixed, "kgtu,tkgd->ukd"
    ).astype(jnp.bfloat16)
    grad_probs = contract(grad_mixed, value_rows, "tkgd,ukd->kgtu")
    grad_scores = (
        probs_back * (grad_probs - jnp.sum(probs_back * grad_probs, axis=-1, keepdims=True))
    ).astype(jnp.bfloat16)
    grad_query_rot = contract(grad_scores, key_rot, "kgtu,ukd->tkgd") * score_scale
    grad_key_rot = contract(grad_scores, query_rot, "kgtu,tkgd->ukd") * score_scale
    grad_query_normed = rotate_back(grad_query_rot, cosine_query, sine_query)
    grad_key_normed = rotate_back(grad_key_rot, cosine_key, sine_key)
    grad_gain_q = jnp.sum(grad_query_normed * unit_query, axis=(0, 1, 2))
    grad_gain_k = jnp.sum(grad_key_normed * unit_key, axis=(0, 1))
    grad_query_raw = (
        norm_back(grad_query_normed * gain_query_f, unit_query, inv_query)
        .astype(jnp.bfloat16)
        .reshape(tok_count, head_count * head_dim)
    )
    grad_key_raw = (
        norm_back(grad_key_normed * gain_key_f, unit_key, inv_key)
        .astype(jnp.bfloat16)
        .reshape(tok_count, kv_count * head_dim)
    )
    grad_value_flat = grad_value_rows.reshape(tok_count, kv_count * head_dim)
    grad_query_w = contract(normed_in, grad_query_raw, "td,tq->dq")
    grad_key_w = contract(normed_in, grad_key_raw, "td,tq->dq")
    grad_value_w = contract(normed_in, grad_value_flat, "td,tq->dq")
    grad_normed_in = (
        contract(grad_query_raw, query_full, "tq,dq->td")
        + contract(grad_key_raw, key_full, "tq,dq->td")
        + contract(grad_value_flat, value_full, "tq,dq->td")
    )
    grad_gain_attn_w = jnp.sum(grad_normed_in * unit_one, axis=0)
    grad_resid_in = grad_mid + norm_back(grad_normed_in * gain_one, unit_one, inv_one)
    grad_input = jnp.zeros_like(grad_resid_in).at[local_order].set(grad_resid_in)
    grad_sums = (
        lax.psum_scatter(grad_query_w, ("dp", "ep"), scatter_dimension=0, tiled=True),
        lax.psum_scatter(grad_key_w, ("dp", "ep"), scatter_dimension=0, tiled=True),
        lax.psum_scatter(grad_value_w, ("dp", "ep"), scatter_dimension=0, tiled=True),
        lax.psum_scatter(grad_out_w, ("dp", "ep"), scatter_dimension=0, tiled=True),
        lax.psum_scatter(grad_router_w, ("dp", "ep"), scatter_dimension=0, tiled=True),
        lax.psum_scatter(grad_gain_attn_w, ("dp", "ep"), scatter_dimension=0, tiled=True),
        lax.psum_scatter(grad_gain_moe_w, ("dp", "ep"), scatter_dimension=0, tiled=True),
    )
    gain_sums = lax.psum((grad_gain_q, grad_gain_k), ("dp", "ep"))
    return (
        block_out,
        grad_input,
        grad_sums[0],
        grad_sums[1],
        grad_sums[2],
        grad_sums[3],
        grad_sums[4],
        grad_sums[5],
        grad_sums[6],
        gain_sums[0],
        gain_sums[1],
        grad_gate,
        grad_up,
        grad_down,
        clip_factor,
    )


MESH = pl.DeviceIdType.MESH


def place():
    dp = lax.axis_index("dp")
    ep = lax.axis_index("ep")
    z, y = dp // 2, dp % 2
    x, c = ep // 2, ep % 2
    first = (1 - c) * y + c * x
    second = (1 - c) * x + c * y
    return dp, ep, z, y, x, c, first, second


def targets(dp, ep, z, y, x, c, nz):
    up = (jnp.where(z < nz - 1, dp + 2, dp), ep)
    down = (jnp.where(z > 0, dp - 2, dp), ep)
    turn_y, turn_x = 1 - 2 * y, 2 - 4 * x
    near = (dp + (1 - c) * turn_y, ep + c * turn_x)
    far = (dp + c * turn_y, ep + (1 - c) * turn_x)
    twin = (dp, ep + 1 - 2 * c)
    return up, down, near, far, twin


def slot(z, first, second, c):
    return z * 8 + first * (4 - 2 * c) + second * (2 + 2 * c) + c


def greet(nz, z, dp, ep, ways, everyone):
    barrier = pltpu.get_barrier_semaphore()
    if everyone:
        total = nz * 8
        me = dp * 4 + ep

        def hello(step, carry):
            other = (me + step) % total
            pl.semaphore_signal(
                barrier, inc=1, device_id=(other // 4, other % 4), device_id_type=MESH
            )
            return carry

        lax.fori_loop(1, total, hello, 0)
        pl.semaphore_wait(barrier, total - 1)
        return
    for step in range(1, nz):
        other = ((z + step) % nz) * 2 + dp % 2
        pl.semaphore_signal(barrier, inc=1, device_id=(other, ep), device_id_type=MESH)
    for other in ways[2:]:
        pl.semaphore_signal(barrier, inc=1, device_id=other, device_id_type=MESH)
    pl.semaphore_wait(barrier, nz + 2)


class Riders:
    def __init__(self, kinds, nz, spot, refs):
        count = len(kinds)
        self.kinds, self.nz = kinds, nz
        self.dp, self.ep, self.z, self.y = spot
        self.me = self.dp * 4 + self.ep
        self.over_y = (self.dp + 1 - 2 * self.y, self.ep)
        self.ins, self.outs = refs[:count], refs[count : 2 * count]
        self.send, self.onward, self.recv, self.own = refs[2 * count :] if count else (None,) * 4
        self.spans = []
        for kind in kinds:
            if kind in ("all", "same"):
                self.spans.append((1, 8 * nz))
            else:
                self.spans.append((1 if kind in ("line", "cube") else 0, nz))
        self.cubes = [r for r in range(count) if kinds[r] == "cube"]

    def remote(self, source, target, send, recv, device):
        return pltpu.make_async_remote_copy(
            src_ref=source, dst_ref=target, send_sem=send, recv_sem=recv,
            device_id=device, device_id_type=MESH)

    def copy(self, r, step):
        kind, source, target = self.kinds[r], self.ins[r], self.outs[r]
        if kind in ("all", "same"):
            other = (self.me + step) % (8 * self.nz)
            source = source if kind == "same" else source.at[other]
            target, key, device = target.at[self.me], self.me, (other // 4, other % 4)
        elif kind in ("line", "cube"):
            other = (self.z + step) % self.nz
            source, key, device = source.at[other], self.z, (other * 2 + self.y, self.ep)
            target = target.at[self.z] if kind == "line" else target.at[self.z, self.y]
        else:
            source = source.at[step, 1 - self.y] if kind == "half" else source.at[step]
            target = target.at[step] if kind == "half" else target.at[step, self.y]
            key, device = step, self.over_y
        return self.remote(source, target, self.send.at[r, step], self.recv.at[r, key], device)

    def arrival(self, r, step):
        kind, target = self.kinds[r], self.outs[r]
        if kind in ("all", "same"):
            key = (self.me + step) % (8 * self.nz)
            target = target.at[key]
        elif kind in ("line", "cube"):
            key = (self.z + self.nz - step) % self.nz
            target = target.at[key] if kind == "line" else target.at[key, self.y]
        else:
            key = step
            target = target.at[step] if kind == "half" else target.at[step, 1 - self.y]
        return self.remote(target, target, self.send.at[r, step], self.recv.at[r, key], self.over_y)

    def passing(self, r, step, first=False):
        key = (self.z + self.nz - step) % self.nz
        target = self.outs[r].at[key, self.y]
        source = self.ins[r].at[key] if first else target
        return self.remote(
            source, target, self.onward.at[r, step], self.recv.at[r, self.nz + key], self.over_y)

    def passed(self, r, step):
        key = (self.z + self.nz - step) % self.nz
        target = self.outs[r].at[key, 1 - self.y]
        return self.remote(
            target, target, self.onward.at[r, step], self.recv.at[r, self.nz + key], self.over_y)

    def own_copies(self, r):
        kind, source, target = self.kinds[r], self.ins[r], self.outs[r]
        if kind in ("all", "same"):
            ends = [(source if kind == "same" else source.at[self.me], target.at[self.me])]
        elif kind == "half":
            ends = []
        elif kind == "pair":
            ends = [(source.at[k], target.at[k, self.y]) for k in range(self.nz)]
        else:
            target = target.at[self.z] if kind == "line" else target.at[self.z, self.y]
            ends = [(source.at[self.z], target)]
        return [pltpu.make_async_copy(here, there, self.own.at[r]) for here, there in ends]

    def begin(self, early=("half", "pair")):
        for r, kind in enumerate(self.kinds):
            for copy in self.own_copies(r):
                copy.start()
            if kind == "cube":
                self.passing(r, 0, True).start()
        self.steps = []
        for r, kind in enumerate(self.kinds):
            for k in range(*self.spans[r]):
                if kind in early:
                    self.copy(r, k).start()
                else:
                    self.steps.append((r, k))
        self.steps.sort(key=lambda step: step[1] / self.spans[step[0]][1])
        self.later = [r for r, kind in enumerate(self.kinds) if kind not in early]

    def some(self, share, shares):
        total = len(self.steps)
        for r, k in self.steps[total * share // shares : total * (share + 1) // shares]:
            self.copy(r, k).start()

    def onwards(self, step):
        for r in self.cubes:
            self.arrival(r, step).wait_recv()
            self.passing(r, step).start()

    def looped(self, step, steps):
        for r in self.later:
            first, last = self.spans[r]
            per = -(-(last - first) // steps)
            for k in range(per):
                piece = first + step * per + k

                @pl.when(piece < last)
                def _():
                    self.copy(r, piece).start()

    def finish(self):
        for r, kind in enumerate(self.kinds):

            def settle(step, carry):
                if kind != "cube":
                    self.arrival(r, step).wait_recv()
                self.copy(r, step).wait_send()
                return carry

            lax.fori_loop(*self.spans[r], settle, 0)
            if kind == "cube":

                def settle_y(step, carry):
                    self.passed(r, step).wait_recv()
                    self.passing(r, step).wait_send()
                    return carry

                lax.fori_loop(0, self.nz, settle_y, 0)
            for copy in self.own_copies(r):
                copy.wait()


def rider_shapes(riders, devices):
    kinds = tuple(kind for kind, _ in riders)
    arrays = tuple(array for _, array in riders)
    outs = []
    for kind, v in riders:
        shape = v.shape
        if kind == "same":
            shape = (devices,) + shape
        elif kind in ("cube", "pair"):
            shape = shape[:1] + (2,) + shape[1:]
        elif kind == "half":
            shape = shape[:1] + shape[2:]
        outs.append(jax.ShapeDtypeStruct(shape, v.dtype))
    dma = pltpu.SemaphoreType.DMA
    count = len(riders)
    sems = [dma((count, devices))] * 3 + [dma((count,))] if count else []
    return kinds, arrays, tuple(outs), sems


def rider_specs(kinds):
    return [
        pl.BlockSpec(memory_space=pl.ANY if kind == "half" else pltpu.VMEM)
        for kind in kinds
    ]


def wide_greeting(kinds):
    return "all" in kinds or "same" in kinds


def on(allowed, action):
    if allowed is None:
        action()
    else:
        pl.when(allowed)(action)


def along(z, nz, step):
    if step == 0:
        yield None, z
    else:
        yield z >= step, jnp.maximum(z - step, 0)
        yield z + step < nz, jnp.minimum(z + step, nz - 1)


class Mover:
    def __init__(self, ins, outs, ways, sems):
        self.ins, self.outs, self.ways = ins, outs, ways
        self.send, self.recv, self.own = sems
        self.pending, self.own_copies = [], []

    def push(self, way, where, allowed=None, own=False):
        for k, out in enumerate(self.outs):
            copy = pltpu.make_async_remote_copy(
                src_ref=self.ins[k] if own else out.at[where],
                dst_ref=out.at[where],
                send_sem=self.send.at[k, way, where],
                recv_sem=self.recv.at[k, where],
                device_id=self.ways[way],
                device_id_type=MESH,
            )
            on(allowed, copy.start)
            self.pending.append((allowed, copy))

    def arrive(self, where):
        for k, out in enumerate(self.outs):
            pltpu.make_async_remote_copy(
                src_ref=out.at[where],
                dst_ref=out.at[where],
                send_sem=self.send.at[k, 0, where],
                recv_sem=self.recv.at[k, where],
                device_id=self.ways[-1],
                device_id_type=MESH,
            ).wait_recv()

    def keep(self, mine):
        for k, out in enumerate(self.outs):
            copy = pltpu.make_async_copy(self.ins[k], out.at[mine], self.own.at[k])
            copy.start()
            self.own_copies.append(copy)

    def settle(self):
        for allowed, copy in self.pending:
            on(allowed, copy.wait_send)
        for copy in self.own_copies:
            copy.wait()


class WholeGather(Mover):
    def begin(self, nz, z, a, b, c):
        self.nz, self.z, self.a, self.b, self.c = nz, z, a, b, c
        mine = slot(z, a, b, c)
        self.push(0, mine, z < nz - 1, True)
        self.push(1, mine, z > 0, True)
        for way in (2, 3, 4):
            self.push(way, mine, None, True)
        self.keep(mine)

    def turn_z(self, turn):
        nz, z, a, b, c = self.nz, self.z, self.a, self.b, self.c
        if turn < nz:
            for index, (allowed, zz) in enumerate(along(z, nz, turn)):
                where = slot(zz, a, b, c)
                on(allowed, functools.partial(self.arrive, where))
                self.push(index, where, allowed & ((z > 0) if index else (z < nz - 1)))
                for way in (2, 3, 4):
                    self.push(way, where, allowed)

    def turn_xy(self, turn):
        nz, z, a, b, c = self.nz, self.z, self.a, self.b, self.c
        if turn - 1 < nz:
            for allowed, zz in along(z, nz, turn - 1):
                where = slot(zz, 1 - a, b, c)
                on(allowed, functools.partial(self.arrive, where))
                for way in (3, 4):
                    self.push(way, where, allowed)
            for allowed, zz in along(z, nz, turn - 1):
                where = slot(zz, a, 1 - b, c)
                on(allowed, functools.partial(self.arrive, where))
                self.push(4, where, allowed)
        if turn >= 2:
            for allowed, zz in along(z, nz, turn - 2):
                where = slot(zz, 1 - a, 1 - b, c)
                on(allowed, functools.partial(self.arrive, where))
                self.push(4, where, allowed)

    def end(self):
        for zz in range(self.nz):
            for aa in range(2):
                for bb in range(2):
                    self.arrive(slot(zz, aa, bb, 1 - self.c))
        self.settle()


class SlabGather(Mover):
    def begin(self, nz, z, ep, x, c):
        self.nz, self.z, self.ep, self.c = nz, z, ep, c
        self.other = ep + 2 - 4 * x
        mine = z * 4 + ep
        self.push(0, mine, z < nz - 1, True)
        self.push(1, mine, z > 0, True)
        for way in (2, 3):
            self.push(way, mine, None, True)
        self.keep(mine)

    def turn_z(self, turn):
        nz, z = self.nz, self.z
        if turn < nz:
            for index, (allowed, zz) in enumerate(along(z, nz, turn)):
                where = zz * 4 + self.ep
                on(allowed, functools.partial(self.arrive, where))
                self.push(index, where, allowed & ((z > 0) if index else (z < nz - 1)))
                for way in (2, 3):
                    self.push(way, where, allowed)

    def turn_xy(self, turn):
        nz, z = self.nz, self.z
        if turn - 1 < nz:
            for allowed, zz in along(z, nz, turn - 1):
                where = zz * 4 + self.other
                on(allowed, functools.partial(self.arrive, where))
                self.push(3, where, allowed)

    def end(self):
        for where in range(4 * self.nz):
            pl.when(where % 2 != self.c)(functools.partial(self.arrive, where))
        self.settle()


def gather_kernel(nz, counts, kinds, *refs):
    whole, slabs = counts
    count, extra = whole + slabs, len(kinds)
    ins = refs[:count]
    outs = refs[count + extra : 2 * count + extra]
    sems = refs[2 * (count + extra) :]
    dp, ep, z, y, x, c, a, b = place()
    ways = targets(dp, ep, z, y, x, c, nz)
    up, down, near, far, twin = ways
    side = (dp, ep + 2 - 4 * x)
    movers = []
    if whole:
        movers.append(WholeGather(ins[:whole], outs[:whole], ways, sems[:3]))
        sems = sems[3:]
    if slabs:
        movers.append(SlabGather(ins[whole:], outs[whole:], (up, down, side, twin), sems[:3]))
        sems = sems[3:]
    riders = Riders(
        kinds, nz, (dp, ep, z, y),
        refs[count : count + extra] + refs[2 * count + extra : 2 * (count + extra)] + sems,
    )
    greet(nz, z, dp, ep, ways, wide_greeting(kinds))
    for mover in movers:
        if isinstance(mover, WholeGather):
            mover.begin(nz, z, a, b, c)
        else:
            mover.begin(nz, z, ep, x, c)
    riders.begin()
    for turn in range(1, nz + 2):
        if turn <= nz:
            riders.some(turn - 1, nz)
        for mover in movers:
            mover.turn_z(turn)
            mover.turn_xy(turn)
        if 2 <= turn <= nz:
            riders.onwards(turn - 1)
    for mover in movers:
        mover.end()
    riders.finish()


def gather_rows(whole, slabs, devices, ident, riders=()):
    arrays = whole + slabs
    nz = devices // 8
    kinds, ridden, rider_outs, rider_sems = rider_shapes(riders, devices)
    blocks = (devices,) * len(whole) + (4 * nz,) * len(slabs)
    dma = pltpu.SemaphoreType.DMA
    sems = []
    for count, ways, total in ((len(whole), 5, devices), (len(slabs), 4, 4 * nz)):
        if count:
            sems += [dma((count, ways, total)), dma((count, total)), dma((count,))]
    return pl.pallas_call(
        functools.partial(gather_kernel, nz, (len(whole), len(slabs)), kinds),
        out_shape=tuple(
            jax.ShapeDtypeStruct((total,) + v.shape, v.dtype) for total, v in zip(blocks, arrays)
        )
        + rider_outs,
        in_specs=[pl.BlockSpec(memory_space=pltpu.VMEM)] * len(arrays) + rider_specs(kinds),
        out_specs=tuple(pl.BlockSpec(memory_space=pl.ANY) for v in arrays + ridden),
        scratch_shapes=sems + rider_sems,
        compiler_params=pltpu.CompilerParams(collective_id=ident, has_side_effects=True),
        name="gather_rows_%d" % ident,
    )(*arrays, *ridden)


class Job:
    def __init__(self, held, stream, out, chunk, arrived):
        self.held, self.stream, self.out = held, stream, out
        self.chunk, self.arrived = chunk, arrived
        self.span = chunk.shape[2]
        self.count = stream.shape[1] // self.span

    def columns(self, index):
        return pl.ds(pl.multiple_of(index * self.span, self.span), self.span)

    def load(self, index):
        return pltpu.make_async_copy(
            self.stream.at[:, self.columns(index)], self.chunk.at[index % 2],
            self.arrived.at[index % 2])

    def begin(self):
        self.load(0).start()
        self.load(1).start()

    def run(self, index):
        self.load(index).wait()
        value = jnp.dot(
            self.held[...], self.chunk[index % 2], preferred_element_type=jnp.float32
        ).astype(self.out.dtype)
        if len(self.out.shape) == 3:
            self.out[index] = value
        else:
            self.out[:, self.columns(index)] = value

        @pl.when(index + 2 < self.count)
        def _():
            self.load(index + 2).start()


def job_shapes(job, blocked):
    if job is None:
        return (), (), [], []
    held, stream = job
    span = 256
    if blocked:
        shape, dtype = (stream.shape[1] // span, held.shape[0], span), jnp.bfloat16
    else:
        shape, dtype = (held.shape[0], stream.shape[1]), jnp.float32
    specs = [pl.BlockSpec(memory_space=pltpu.VMEM), pl.BlockSpec(memory_space=pl.ANY)]
    scratch = [pltpu.VMEM((2, stream.shape[0], span), stream.dtype), pltpu.SemaphoreType.DMA((2,))]
    return job, (jax.ShapeDtypeStruct(shape, dtype),), specs, scratch


def scatter_kernel(nz, turned, jobs, kinds, *refs):
    extra = len(kinds)
    left_ref, right_ref = refs[:2]
    held = refs[2 : 2 + 2 * jobs]
    refs = refs[2 + 2 * jobs :]
    out_ref = refs[extra]
    held += refs[extra + 1 : extra + 1 + jobs]
    refs = refs[: extra + 1] + refs[extra + 1 + jobs :]
    held += refs[2 * extra + 16 : 2 * extra + 16 + 2 * jobs]
    refs = refs[: 2 * extra + 16] + refs[2 * extra + 16 + 2 * jobs :]
    job = Job(*held) if jobs else None
    sent, got, from_far, from_near, rising, falling = refs[2 * extra + 1 : 2 * extra + 7]
    (twin_send, twin_recv, far_send, far_recv, near_send, near_recv, line_send, up_recv,
     down_recv) = refs[2 * extra + 7 : 2 * extra + 16]
    dp, ep, z, y, x, c, a, b = place()
    ways = targets(dp, ep, z, y, x, c, nz)
    up, down, near, far, twin = ways
    riders = Riders(
        kinds, nz, (dp, ep, z, y),
        refs[:extra] + refs[extra + 1 : 2 * extra + 1] + refs[2 * extra + 16 :]
    )
    greet(nz, z, dp, ep, ways, wide_greeting(kinds))
    riders.begin(("half", "line"))
    if jobs:
        job.begin()
    per = 4 * nz

    def zed(step):
        if nz == 4:
            far_one = jnp.where(z < 2, 3, 0)
            second = jnp.where(z < 2, 2 - 2 * z, 7 - 2 * z)
            third = 1 + z % 2
            return jnp.where(step == 0, far_one, jnp.where(step == 1, second, jnp.where(step == 2, third, z)))
        return (z + 1 + step) % nz

    def term(where):
        sides = (((1,), (1 if turned else 0,)), ((), ()))
        return lax.dot_general(
            left_ref[where], right_ref[...], sides, preferred_element_type=jnp.float32
        )

    def order(index, aa, bb, cc):
        part = index // nz
        flip_b = 1 - part // 2
        flip_a = 1 - part % 2
        return slot(zed(index % nz), aa + flip_a * (1 - 2 * aa), bb + flip_b * (1 - 2 * bb), cc)

    def twin_copy(index):
        return pltpu.make_async_remote_copy(
            src_ref=sent.at[index], dst_ref=got.at[index], send_sem=twin_send.at[index],
            recv_sem=twin_recv.at[index], device_id=twin, device_id_type=MESH)

    def far_copy(index):
        return pltpu.make_async_remote_copy(
            src_ref=got.at[index], dst_ref=from_far.at[index], send_sem=far_send.at[index],
            recv_sem=far_recv.at[index], device_id=far, device_id_type=MESH)

    def near_copy(index):
        return pltpu.make_async_remote_copy(
            src_ref=got.at[2 * nz + index], dst_ref=from_near.at[index], send_sem=near_send.at[index],
            recv_sem=near_recv.at[index], device_id=near, device_id_type=MESH)

    def up_copy(index, zz):
        return pltpu.make_async_remote_copy(
            src_ref=got.at[3 * nz + index], dst_ref=rising.at[zz], send_sem=line_send.at[index],
            recv_sem=up_recv.at[zz], device_id=up, device_id_type=MESH)

    def down_copy(index, zz):
        return pltpu.make_async_remote_copy(
            src_ref=got.at[3 * nz + index], dst_ref=falling.at[zz], send_sem=line_send.at[index],
            recv_sem=down_recv.at[zz], device_id=down, device_id_type=MESH)

    def give(index):
        sent[index] = term(order(index, b, a, 1 - c)).astype(sent.dtype)
        twin_copy(index).start()

    def taken(index):
        value = term(order(index, a, b, c))
        twin_copy(index).wait_recv()
        return value + got[index].astype(jnp.float32)

    def far_step(step, carry):
        give(2 * step)
        give(2 * step + 1)
        got[step] = taken(step).astype(got.dtype)
        far_copy(step).start()
        riders.looped(step, 2 * nz)
        return carry

    lax.fori_loop(0, 2 * nz, far_step, 0)

    def work(index, carry):
        job.run(index)
        return carry

    def near_step(step, carry):
        value = taken(2 * nz + step)
        far_copy(step).wait_recv()
        value = value + from_far[step].astype(jnp.float32)
        got[2 * nz + step] = value.astype(got.dtype)
        near_copy(step).start()
        if jobs:
            share = job.count // nz
            lax.fori_loop(step * share, step * share + share, work, 0)
        return carry

    lax.fori_loop(0, nz, near_step, 0)

    def line_step(step, carry):
        zz = zed(step)
        value = taken(3 * nz + step)
        far_copy(nz + step).wait_recv()
        near_copy(step).wait_recv()
        out_ref[...] = value + from_far[nz + step].astype(jnp.float32) + from_near[step].astype(jnp.float32)

        @pl.when((zz >= z) & (z > 0))
        def _():
            up_copy(step, zz).wait_recv()
            out_ref[...] += rising[zz].astype(jnp.float32)

        @pl.when((zz <= z) & (z < nz - 1))
        def _():
            down_copy(step, zz).wait_recv()
            out_ref[...] += falling[zz].astype(jnp.float32)

        @pl.when(zz > z)
        def _():
            got[3 * nz + step] = out_ref[...].astype(got.dtype)
            up_copy(step, zz).start()

        @pl.when(zz < z)
        def _():
            got[3 * nz + step] = out_ref[...].astype(got.dtype)
            down_copy(step, zz).start()

        return carry

    lax.fori_loop(0, nz, line_step, 0)

    def finish(step, carry):
        twin_copy(step).wait_send()
        return carry

    lax.fori_loop(0, per, finish, 0)

    def finish_far(step, carry):
        far_copy(step).wait_send()
        return carry

    lax.fori_loop(0, 2 * nz, finish_far, 0)

    def finish_near(step, carry):
        near_copy(step).wait_send()

        @pl.when(step < nz - 1)
        def _():
            up_copy(step, 0).wait_send()

        return carry

    lax.fori_loop(0, nz, finish_near, 0)
    riders.finish()


def scatter_sum(left, right, devices, ident, turned=False, riders=(), job=None):
    nz = devices // 8
    rows = left.shape[0] // devices
    depth, wide = right.shape[::-1] if turned else right.shape
    kinds, ridden, rider_outs, rider_sems = rider_shapes(riders, devices)
    job_ins, job_outs, job_specs, job_scratch = job_shapes(job, False)
    block = (rows, wide)
    low = jnp.bfloat16
    dma = pltpu.SemaphoreType.DMA
    result = pl.pallas_call(
        functools.partial(scatter_kernel, nz, turned, len(job_outs), kinds),
        out_shape=(jax.ShapeDtypeStruct(block, jnp.float32),) + job_outs + rider_outs,
        in_specs=[pl.BlockSpec(memory_space=pltpu.VMEM)] * 2 + job_specs + rider_specs(kinds),
        out_specs=(pl.BlockSpec(memory_space=pltpu.VMEM),) * (1 + len(job_outs))
        + (pl.BlockSpec(memory_space=pl.ANY),) * len(riders),
        scratch_shapes=[
            pltpu.VMEM((4 * nz,) + block, low),
            pltpu.VMEM((4 * nz,) + block, low),
            pltpu.VMEM((2 * nz,) + block, low),
            pltpu.VMEM((nz,) + block, low),
            pltpu.VMEM((nz,) + block, low),
            pltpu.VMEM((nz,) + block, low),
            dma((4 * nz,)), dma((4 * nz,)), dma((2 * nz,)), dma((2 * nz,)),
            dma((nz,)), dma((nz,)), dma((nz,)), dma((nz,)), dma((nz,)),
        ]
        + job_scratch
        + rider_sems,
        compiler_params=pltpu.CompilerParams(
            collective_id=ident, has_side_effects=True, vmem_limit_bytes=58 * 2**20),
        name="scatter_sum_%d" % ident,
    )(left.reshape(devices, rows, depth), right, *job_ins, *ridden)
    return result if riders else result[0]


class SlabSum:
    def __init__(self, nz, turned, spot, ways, refs, buffers):
        self.nz, self.turned = nz, turned
        self.z, self.x, self.c = spot
        self.up, self.down, self.side, self.twin = ways
        self.lefts, self.rights, self.beside, self.out = refs
        (self.sent, self.got, self.from_side, self.rising, self.falling, self.held,
         self.twin_send, self.twin_recv, self.side_send, self.side_recv, self.line_send,
         self.up_recv, self.down_recv) = buffers
        self.plain = self.rights[0].shape[0 if turned else 1]
        self.span = 512 if self.plain % 512 == 0 else self.plain

    def zed(self, step):
        z, nz = self.z, self.nz
        if nz == 4:
            far_one = jnp.where(z < 2, 3, 0)
            second = jnp.where(z < 2, 2 - 2 * z, 7 - 2 * z)
            third = 1 + z % 2
            return jnp.where(step == 0, far_one, jnp.where(step == 1, second, jnp.where(step == 2, third, z)))
        return (z + 1 + step) % nz

    def order(self, index, cc):
        flip = 1 - index // self.nz
        return self.zed(index % self.nz) * 4 + (self.x + flip * (1 - 2 * self.x)) * 2 + cc

    def combine(self, targets_, wheres, added):
        rows = self.lefts[0].shape[1]

        def put(which, at, total):
            for ref in added[which]:
                total = total + ref[:, at].astype(jnp.float32)
            targets_[which][:, at] = total.astype(targets_[which].dtype)

        def fill(chunk, carry):
            at = pl.ds(pl.multiple_of(chunk * self.span, self.span), self.span)
            total = None
            for left_ref, right_ref in zip(self.lefts, self.rights):
                value = lax.dot_general(
                    jnp.concatenate([left_ref[where] for where in wheres], axis=0),
                    right_ref[at, :] if self.turned else right_ref[:, at],
                    (((1,), (1 if self.turned else 0,)), ((), ())),
                    preferred_element_type=jnp.float32,
                )
                total = value if total is None else total + value
            for which in range(len(wheres)):
                put(which, at, total[which * rows : (which + 1) * rows])
            return carry

        lax.fori_loop(0, self.plain // self.span, fill, 0)
        if self.beside is not None:
            at = pl.ds(self.plain, self.beside.shape[2])
            for which, where in enumerate(wheres):
                put(which, at, self.beside[where].astype(jnp.float32))

    def remote(self, source, target, send, recv, device):
        return pltpu.make_async_remote_copy(
            src_ref=source, dst_ref=target, send_sem=send, recv_sem=recv,
            device_id=device, device_id_type=MESH)

    def twin_copy(self, index):
        return self.remote(
            self.sent.at[index], self.got.at[index], self.twin_send.at[index],
            self.twin_recv.at[index], self.twin)

    def side_copy(self, index):
        return self.remote(
            self.got.at[index], self.from_side.at[index], self.side_send.at[index],
            self.side_recv.at[index], self.side)

    def line_copy(self, index, zz, rise):
        place_, recv = (self.rising, self.up_recv) if rise else (self.falling, self.down_recv)
        return self.remote(
            self.got.at[self.nz + index], place_.at[zz], self.line_send.at[index], recv.at[zz],
            self.up if rise else self.down)

    def give(self, pair, carry):
        both = (2 * pair, 2 * pair + 1)
        self.combine(
            [self.sent.at[index] for index in both],
            [self.order(index, 1 - self.c) for index in both], [(), ()])
        for index in both:
            self.twin_copy(index).start()
        return carry

    def to_side(self, pair):
        lax.fori_loop(2 * pair, 2 * pair + 2, self.give, 0)
        both = (2 * pair, 2 * pair + 1)
        for index in both:
            self.twin_copy(index).wait_recv()
        self.combine(
            [self.got.at[index] for index in both],
            [self.order(index, self.c) for index in both],
            [(self.got.at[index],) for index in both])
        for index in both:
            self.side_copy(index).start()

    def to_line(self, pair):
        both = (2 * pair, 2 * pair + 1)
        for step in both:
            self.twin_copy(self.nz + step).wait_recv()
            self.side_copy(step).wait_recv()
        self.combine(
            [self.held.at[0], self.held.at[1]],
            [self.order(self.nz + step, self.c) for step in both],
            [(self.got.at[self.nz + step], self.from_side.at[step]) for step in both])
        for which, step in enumerate(both):
            self.along_line(self.held.at[which], step)

    def along_line(self, held, step):
        z, zz = self.z, self.zed(step)

        @pl.when((zz >= z) & (z > 0))
        def _():
            self.line_copy(step, zz, True).wait_recv()
            held[...] += self.rising[zz].astype(jnp.float32)

        @pl.when((zz <= z) & (z < self.nz - 1))
        def _():
            self.line_copy(step, zz, False).wait_recv()
            held[...] += self.falling[zz].astype(jnp.float32)

        @pl.when(zz != z)
        def _():
            self.got[self.nz + step] = held[...].astype(self.got.dtype)

        pl.when(zz > z)(lambda: self.line_copy(step, zz, True).start())
        pl.when(zz < z)(lambda: self.line_copy(step, zz, False).start())

    def end(self):
        self.out[...] = self.held[1]

        def finish(step, carry):
            self.twin_copy(step).wait_send()
            return carry

        lax.fori_loop(0, 2 * self.nz, finish, 0)

        def finish_side(step, carry):
            self.side_copy(step).wait_send()

            @pl.when(step < self.nz - 1)
            def _():
                self.line_copy(step, 0, True).wait_send()

            return carry

        lax.fori_loop(0, self.nz, finish_side, 0)


def slab_scatter_kernel(nz, forms, jobs, kinds, *refs):
    extra, parts = len(kinds), len(forms)
    refs = list(refs)

    def take(count):
        taken = tuple(refs[:count])
        del refs[:count]
        return taken

    operands = []
    for pairs, turned, beside in forms:
        operands.append((take(pairs), take(pairs), take(1)[0] if beside else None))
    held = take(2 * jobs)
    rider_ins = take(extra)
    outs = take(parts)
    held += take(jobs)
    come = take(jobs)
    rider_outs = take(extra)
    dp, ep, z, y, x, c, _, _ = place()
    up, down, near, far, twin = targets(dp, ep, z, y, x, c, nz)
    side = (dp, ep + 2 - 4 * x)
    sums = [
        SlabSum(nz, form[1], (z, x, c), (up, down, side, twin), given + (out,), take(13))
        for form, given, out in zip(forms, operands, outs)
    ]
    if jobs:
        job = Job(*(held + take(2)))
        made_send, made_recv = take(2)
    riders = Riders(kinds, nz, (dp, ep, z, y), rider_ins + rider_outs + tuple(refs))
    greet(nz, z, dp, ep, (up, down, near, far, twin), wide_greeting(kinds))
    riders.begin(("half", "line"))
    if jobs:
        job.begin()

    def side_step(pair, carry):
        for part in sums:
            part.to_side(pair)
        riders.looped(pair, nz // 2)
        return carry

    lax.fori_loop(0, nz // 2, side_step, 0)

    def work(index, carry):
        job.run(index)
        return carry

    def made_copy(step):
        return pltpu.make_async_remote_copy(
            src_ref=job.out.at[2 * step + 1 - y], dst_ref=come[0].at[step],
            send_sem=made_send.at[step], recv_sem=made_recv.at[step],
            device_id=riders.over_y, device_id_type=MESH)

    def line_step(pair, carry):
        for part in sums:
            part.to_line(pair)
        if jobs:
            lax.fori_loop(0, jnp.where(pair == 0, job.count, 0), work, 0)

            @pl.when(pair == 0)
            def _():
                for step in range(nz):
                    made_copy(step).start()

        return carry

    lax.fori_loop(0, nz // 2, line_step, 0)
    for part in sums:
        part.end()
    if jobs:
        for step in range(nz):
            made_copy(step).wait()
    riders.finish()


def slab_scatter(parts, devices, ident, riders=(), job=None):
    nz = devices // 8
    blocks = 4 * nz
    rows = parts[0][0][0].shape[0] // blocks
    kinds, ridden, rider_outs, rider_sems = rider_shapes(riders, devices)
    job_ins, job_outs, job_specs, job_scratch = job_shapes(job, True)
    low, dma = jnp.bfloat16, pltpu.SemaphoreType.DMA
    come = tuple(jax.ShapeDtypeStruct((nz,) + v.shape[1:], v.dtype) for v in job_outs)
    job_scratch += [dma((nz,))] * (2 * len(come))
    operands, outs, scratch, forms = (), (), [], []
    for lefts, rights, turned, beside in parts:
        held = () if beside is None else (beside.reshape(blocks, rows, -1),)
        wide = rights[0].shape[0 if turned else 1] + sum(v.shape[2] for v in held)
        block = (rows, wide)
        operands += tuple(v.reshape(blocks, rows, -1) for v in lefts) + tuple(rights) + held
        outs += (jax.ShapeDtypeStruct(block, jnp.float32),)
        scratch += [pltpu.VMEM((count * nz,) + block, low) for count in (2, 2, 1, 1, 1)]
        scratch += [pltpu.VMEM((2,) + block, jnp.float32)]
        scratch += [dma((2 * nz,))] * 2 + [dma((nz,))] * 5
        forms.append((len(lefts), turned, len(held)))
    return pl.pallas_call(
        functools.partial(slab_scatter_kernel, nz, tuple(forms), len(job_outs), kinds),
        out_shape=outs + job_outs + come + rider_outs,
        in_specs=[pl.BlockSpec(memory_space=pltpu.VMEM)] * len(operands) + job_specs + rider_specs(kinds),
        out_specs=(pl.BlockSpec(memory_space=pltpu.VMEM),) * (len(outs) + len(job_outs))
        + (pl.BlockSpec(memory_space=pl.ANY),) * (len(come) + len(riders)),
        scratch_shapes=scratch + job_scratch + rider_sems,
        compiler_params=pltpu.CompilerParams(
            collective_id=ident, has_side_effects=True, vmem_limit_bytes=63 * 2**20),
        name="slab_scatter_%d" % ident,
    )(*operands, *job_ins, *ridden)


def whole_rows(mesh):
    return mesh.shape["ep"] == 4 and mesh.shape["dp"] in (4, 8)


def exact_dot(left_side, right_side):
    return jnp.dot(
        left_side, right_side, precision=lax.Precision.HIGHEST, preferred_element_type=jnp.float32
    )


def block_layout(lens, tok_count):
    ends = [lens[:, :1]]
    for at in range(1, lens.shape[1]):
        ends.append(ends[-1] + lens[:, at : at + 1])
    row_index = lax.broadcasted_iota(jnp.int32, (lens.shape[0], tok_count), 1)
    segment = jnp.zeros_like(row_index)
    first_row = jnp.zeros_like(row_index)
    for end in ends:
        passed = row_index >= end
        segment = segment + passed.astype(jnp.int32)
        first_row = jnp.where(passed, end, first_row)
    return (segment, row_index - first_row)


def by_experts(
    hidden_in,
    cotangent,
    deal_order,
    seq_lengths,
    expert_ids,
    w_query,
    w_key,
    w_value,
    w_out,
    w_router,
    gain_attn,
    gain_moe,
    gain_query,
    gain_key,
    w_gate,
    w_up,
    w_down,
    clip_threshold,
):
    f32, low = jnp.float32, jnp.bfloat16
    dp_count, ep_count = lax.axis_size("dp"), lax.axis_size("ep")
    devices = dp_count * ep_count
    dp, ep = lax.axis_index("dp"), lax.axis_index("ep")
    me = dp * ep_count + ep
    tok_count, width = hidden_in.shape
    row_count = tok_count * 7 // 8
    all_count = devices * row_count
    head_dim = gain_query.shape[0]
    half_dim = head_dim // 2
    rows_own = w_query.shape[0]
    head_count = w_query.shape[1] // head_dim
    kv_count = w_key.shape[1] // head_dim
    group_size = head_count // kv_count
    experts = w_router.shape[1]
    exp_local, wide_own, hidden = w_gate.shape
    lines = dp_count // 2
    slab = lines * ep_count
    z, y = dp // 2, dp % 2
    score_scale = head_dim ** (-0.5)

    gain_col = gain_attn.astype(f32)[:, None]
    heads_in = (w_query.astype(f32) * gain_col).astype(low).reshape(rows_own, head_count, head_dim)
    keys_in = (w_key.astype(f32) * gain_col).astype(low).reshape(rows_own, kv_count, head_dim)
    values_in = (w_value.astype(f32) * gain_col).astype(low).reshape(rows_own, kv_count, head_dim)
    sent_heads = jnp.concatenate(
        [heads_in, jnp.repeat(keys_in, group_size, axis=1), jnp.repeat(values_in, group_size, axis=1)],
        axis=2,
    ).transpose(1, 0, 2)

    local_order = deal_order % tok_count
    deal = (local_order[:, None] == jnp.arange(tok_count, dtype=jnp.int32)[None, :]).astype(low)
    deal = deal[:row_count]
    resid_in = jnp.dot(deal, hidden_in, preferred_element_type=f32)
    grad_mid_out = jnp.dot(deal, cotangent, preferred_element_type=f32)
    inv_one = rms_scale(resid_in)
    unit_one = resid_in * inv_one
    lens_row = jnp.pad(seq_lengths.astype(f32), ((0, 0), (0, 128 - seq_lengths.shape[1])))
    gain_row = jnp.pad(gain_moe.astype(f32)[None, :], ((0, 0), (0, 128 - rows_own)))
    router_rows = w_router.astype(f32).reshape(-1, 128)
    note_one = jnp.concatenate([lens_row, gain_row, router_rows], axis=0)
    note_one = jnp.pad(note_one, ((0, -note_one.shape[0] % 8), (0, 0)))
    unit_all, notes, grad_all, w_heads, w_rise_up = gather_rows(
        (unit_one.astype(low), note_one),
        (grad_mid_out.astype(low),),
        devices,
        1,
        (("all", sent_heads), ("cube", w_up)),
    )
    w_heads = w_heads.reshape(width, 3 * head_dim)
    w_rise_up = w_rise_up.reshape(width, hidden)
    lens_all = notes[:, 0, : seq_lengths.shape[1]].astype(jnp.int32)
    gain_two = notes[:, 1, :rows_own].reshape(1, width)
    router_full = notes[:, 2 : 2 + router_rows.shape[0]].reshape(width, experts)

    segment, position = block_layout(lens_all, row_count)
    step_down = lax.broadcasted_iota(jnp.int32, (1, row_count, row_count), 1)
    step_across = lax.broadcasted_iota(jnp.int32, (1, row_count, row_count), 2)
    allowed = (segment[:, :, None] == segment[:, None, :]) & (step_across <= step_down)
    cosine_rows, sine_rows = rotary_tables(jnp.arange(tok_count, dtype=jnp.int32), head_dim)
    place_hot = (position.reshape(-1)[:, None] == jnp.arange(tok_count)[None, :]).astype(f32)
    cosine_all = exact_dot(place_hot, cosine_rows).reshape(devices, row_count, head_dim)
    sine_all = exact_dot(place_hot, sine_rows).reshape(devices, row_count, head_dim)
    flat_unit = unit_all.reshape(all_count, width)
    projected = jnp.dot(flat_unit, w_heads, preferred_element_type=f32).reshape(
        devices, row_count, 3 * head_dim
    )
    query_raw = projected[..., :head_dim]
    key_raw = projected[..., head_dim : 2 * head_dim]
    value_rows = projected[..., 2 * head_dim :].astype(low)
    gain_query_f = gain_query.astype(f32)
    gain_key_f = gain_key.astype(f32)
    inv_query = rms_scale(query_raw)
    unit_query = query_raw * inv_query
    query_rot = rotate(unit_query * gain_query_f, cosine_all, sine_all).astype(low)
    inv_key = rms_scale(key_raw)
    unit_key = key_raw * inv_key
    key_rot = rotate(unit_key * gain_key_f, cosine_all, sine_all).astype(low)
    scores = contract(query_rot, key_rot, "btd,bud->btu") * score_scale
    masked = jnp.where(allowed, scores, masked_fill)
    row_top = jnp.max(masked, axis=-1, keepdims=True)
    exponent = jnp.exp(masked - row_top)
    probs = exponent / jnp.sum(exponent, axis=-1, keepdims=True)
    probs_low = probs.astype(low)
    mixed = contract(probs_low, value_rows, "btu,bud->btd").astype(low).reshape(all_count, head_dim)
    largest_own = jnp.max(row_top)
    branch, fall_own = scatter_sum(mixed, w_out, devices, 2, riders=(("line", w_down.transpose(0, 2, 1)),))
    resid_mid = resid_in + branch

    inv_two = rms_scale(resid_mid)
    unit_two = resid_mid * inv_two
    normed_mid = (unit_two * gain_two).astype(low)
    logits = jnp.dot(normed_mid, router_full.astype(low), preferred_element_type=f32)
    choose = (expert_ids[:row_count, :, None] == jnp.arange(experts, dtype=jnp.int32)[None, None, :]).any(axis=1)
    picked = jnp.where(choose, logits, masked_fill)
    gate_power = jnp.where(choose, jnp.exp(picked - jnp.max(picked, axis=1, keepdims=True)), 0.0)
    route = gate_power / jnp.sum(gate_power, axis=1, keepdims=True)
    note_two = jnp.pad(route.T, ((0, 0), (0, 128 - row_count)))
    normed_all, notes, w_rise_gate, w_fall = gather_rows(
        (), (normed_mid, note_two), devices, 3, (("cube", w_gate), ("pair", fall_own))
    )
    w_rise_gate = w_rise_gate.reshape(width, hidden)
    w_fall = w_fall.reshape(width, hidden)

    mine = ep * exp_local + z
    slab_rows = slab * row_count
    weight = lax.dynamic_slice_in_dim(notes, mine, 1, axis=1)[..., :row_count].reshape(slab_rows, 1)
    flat_mid = normed_all.reshape(slab_rows, width)
    flat_grad = grad_all.reshape(slab_rows, width)
    gate_part = jnp.dot(flat_mid, w_rise_gate, preferred_element_type=f32)
    up_part = jnp.dot(flat_mid, w_rise_up, preferred_element_type=f32)
    grad_plain = jnp.dot(flat_grad, w_fall, preferred_element_type=f32)
    sigmoid_gate = jax.nn.sigmoid(gate_part)
    silu_gate = gate_part * sigmoid_gate
    hidden_mid = silu_gate * up_part
    grad_route = jnp.sum(hidden_mid * grad_plain, axis=1, keepdims=True)
    weighted_mid = (hidden_mid * weight).astype(low)
    grad_hidden = grad_plain * weight
    grad_gate_part = (
        grad_hidden * up_part * sigmoid_gate * (1.0 + gate_part * (1.0 - sigmoid_gate))
    ).astype(low)
    grad_up_part = (grad_hidden * silu_gate).astype(low)
    lane = lax.broadcasted_iota(jnp.int32, (1, 128), 1)
    beside = jnp.where(lane == mine, grad_route, 0.0).astype(low)

    def for_each_y(grads):
        return grads.astype(low).reshape(lines, 2, wide_own, hidden)

    gate_halves = for_each_y(contract(flat_mid, grad_gate_part, "td,tf->df"))
    up_halves = for_each_y(contract(flat_mid, grad_up_part, "td,tf->df"))
    summed, moe_rows, fall_halves, fall_come, gate_come, up_come = slab_scatter(
        (
            ((grad_gate_part, grad_up_part), (w_rise_gate, w_rise_up), True, beside),
            ((weighted_mid,), (w_fall,), True, None),
        ),
        devices,
        4,
        (("half", gate_halves), ("half", up_halves)),
        (weighted_mid.T, flat_grad),
    )
    fall_halves = fall_halves.reshape(lines, 2, hidden, wide_own)

    def add_halves(halves, come):
        kept = lax.dynamic_index_in_dim(halves, y, axis=1, keepdims=False)
        return (kept.astype(f32) + come.astype(f32)).astype(low)

    grad_gates = summed[:, width : width + experts]
    mean_term = jnp.sum(route * grad_gates, axis=1, keepdims=True)
    grad_logits = (route * (grad_gates - mean_term)).astype(low)
    grad_normed_mid = summed[:, :width] + contract(grad_logits, router_full.astype(low), "te,de->td")
    gain_part = jnp.sum(grad_normed_mid * unit_two, axis=0)
    grad_mid = grad_mid_out + norm_back(grad_normed_mid * gain_two, unit_two, inv_two)
    grad_branch = grad_mid.astype(low)
    router_part = contract(normed_mid, grad_logits, "td,te->de").reshape(devices, -1, 128)
    note_three = jnp.concatenate(
        [
            gain_part.reshape(-1, 128),
            jnp.full((8, 128), largest_own, f32),
        ],
        axis=0,
    )
    branch_all, notes, back_gate, back_up = gather_rows(
        (grad_branch, note_three),
        (),
        devices,
        6,
        (
            ("line", add_halves(gate_halves, gate_come)),
            ("line", add_halves(up_halves, up_come)),
        ),
    )
    clip_factor = jnp.sqrt(clip_threshold / jnp.maximum(notes[:, -1, 0], clip_threshold))
    gain_sum = jnp.sum(notes[:, :-8], axis=0).reshape(-1)
    grad_gain_moe = lax.dynamic_slice_in_dim(gain_sum, me * rows_own, rows_own)

    flat_branch = branch_all.reshape(all_count, width)
    grad_mixed = (
        contract(flat_branch, w_out, "td,qd->tq").astype(low).reshape(devices, row_count, head_dim)
    )
    grad_value = contract(probs_low, grad_mixed, "btu,btd->bud").astype(low)
    grad_probs = contract(grad_mixed, value_rows, "btd,bud->btu")
    grad_scores = (
        probs * (grad_probs - jnp.sum(probs * grad_probs, axis=-1, keepdims=True))
    ).astype(low)
    grad_query_rot = contract(grad_scores, key_rot, "btu,bud->btd") * score_scale
    grad_key_rot = contract(grad_scores, query_rot, "btu,btd->bud") * score_scale
    grad_query_normed = rotate_back(grad_query_rot, cosine_all, sine_all)
    grad_key_normed = rotate_back(grad_key_rot, cosine_all, sine_all)
    gain_pair = jnp.stack(
        [
            jnp.sum(grad_query_normed * unit_query, axis=(0, 1)),
            jnp.sum(grad_key_normed * unit_key, axis=(0, 1)),
        ]
    )
    grad_query_raw = norm_back(grad_query_normed * gain_query_f, unit_query, inv_query).astype(low)
    grad_key_raw = norm_back(grad_key_normed * gain_key_f, unit_key, inv_key).astype(low)
    grad_heads = jnp.concatenate([grad_query_raw, grad_key_raw, grad_value], axis=2).reshape(
        all_count, 3 * head_dim
    )
    grad_heads_w = contract(flat_unit, grad_heads, "td,tq->dq").astype(low)
    resid_out = resid_mid + moe_rows
    undeal = (jnp.arange(tok_count, dtype=jnp.int32)[:, None] == local_order[None, :]).astype(low)
    undeal = undeal[:, :row_count]
    block_out = jnp.dot(undeal, resid_out.astype(low), preferred_element_type=f32).astype(low)
    grad_unit_one, grad_out, back_heads, back_fall, gain_pairs, router_parts = scatter_sum(
        grad_heads,
        w_heads,
        devices,
        7,
        turned=True,
        riders=(
            ("all", grad_heads_w.reshape(devices, rows_own, 3 * head_dim)),
            ("line", add_halves(fall_halves, fall_come)),
            ("same", jnp.pad(gain_pair, ((0, 6), (0, 0)))),
            ("all", router_part),
        ),
        job=(mixed.T, flat_branch),
    )
    back_heads = back_heads.astype(f32)
    grad_gate = back_gate.astype(f32)
    grad_up = back_up.astype(f32)
    grad_down = back_fall.astype(f32)
    grad_router = jnp.sum(router_parts, axis=0).reshape(rows_own, experts)
    gain_pair = jnp.sum(gain_pairs, axis=0)
    plain_query = back_heads[..., :head_dim].transpose(1, 0, 2).reshape(rows_own, -1)

    def of_group(grads):
        grads = jnp.sum(grads.reshape(kv_count, group_size, rows_own, head_dim), axis=1)
        return grads.transpose(1, 0, 2).reshape(rows_own, -1)

    plain_key = of_group(back_heads[..., head_dim : 2 * head_dim])
    plain_value = of_group(back_heads[..., 2 * head_dim :])
    grad_gain_attn = (
        jnp.sum(plain_query * w_query.astype(f32), axis=1)
        + jnp.sum(plain_key * w_key.astype(f32), axis=1)
        + jnp.sum(plain_value * w_value.astype(f32), axis=1)
    )
    grad_resid_in = grad_mid + norm_back(grad_unit_one, unit_one, inv_one)
    grad_input = exact_dot(undeal.astype(f32), grad_resid_in)
    return (
        block_out,
        grad_input,
        plain_query * gain_col,
        plain_key * gain_col,
        plain_value * gain_col,
        grad_out,
        grad_router,
        grad_gain_attn,
        grad_gain_moe,
        gain_pair[0],
        gain_pair[1],
        grad_gate,
        grad_up,
        grad_down,
        clip_factor,
    )


def solution(mesh):
    placed = (
        P(("dp", "ep"), None),
        P(("dp", "ep"), None),
        P(("dp", "ep")),
        P(("dp", "ep"), None),
        P(("dp", "ep"), None),
        P(("dp", "ep"), None),
        P(("dp", "ep"), None),
        P(("dp", "ep"), None),
        P(("dp", "ep"), None),
        P(("dp", "ep"), None),
        P(("dp", "ep")),
        P(("dp", "ep")),
        P(),
        P(),
        P("ep", "dp", None),
        P("ep", "dp", None),
        P("ep", None, "dp"),
        P(),
    )
    return jax.shard_map(
        per_device if not whole_rows(mesh) else by_experts,
        mesh=mesh,
        in_specs=placed,
        out_specs=(
            P(("dp", "ep"), None),
            P(("dp", "ep"), None),
            P(("dp", "ep"), None),
            P(("dp", "ep"), None),
            P(("dp", "ep"), None),
            P(("dp", "ep"), None),
            P(("dp", "ep"), None),
            P(("dp", "ep")),
            P(("dp", "ep")),
            P(),
            P(),
            P("ep", "dp", None),
            P("ep", "dp", None),
            P("ep", None, "dp"),
            P(),
        ),
        check_vma=False,
    )
```

```python
import functools

import jax
import jax.numpy as jnp
from jax import lax
from jax.experimental import pallas as pl
from jax.experimental.pallas import tpu as pltpu
from jax.sharding import PartitionSpec as P

epsilon = 1e-06
theta_base = 1000000.0
masked_fill = -1e30


def rms_scale(values):
    return lax.rsqrt(jnp.mean(values * values, axis=-1, keepdims=True) + epsilon)


def rotate_half(values):
    half_dim = values.shape[-1] // 2
    return jnp.concatenate([-values[..., half_dim:], values[..., :half_dim]], axis=-1)


def rotate(values, cosine_table, sine_table):
    return values * cosine_table + rotate_half(values) * sine_table


def rotate_back(values, cosine_table, sine_table):
    scaled = values * sine_table
    half_dim = values.shape[-1] // 2
    turned = jnp.concatenate([scaled[..., half_dim:], -scaled[..., :half_dim]], axis=-1)
    return values * cosine_table + turned


def norm_back(grad_unit, unit_rows, inv_root):
    return inv_root * (
        grad_unit - unit_rows * jnp.mean(grad_unit * unit_rows, axis=-1, keepdims=True)
    )


def contract(left_side, right_side, pattern):
    return jnp.einsum(pattern, left_side, right_side, preferred_element_type=jnp.float32)


def layout(lens_row, tok_count):
    seq_ends = jnp.cumsum(lens_row)
    row_index = jnp.arange(tok_count, dtype=jnp.int32)
    segment = jnp.sum((row_index[:, None] >= seq_ends[None, :]).astype(jnp.int32), axis=1)
    starts_all = jnp.concatenate([jnp.zeros((1,), jnp.int32), seq_ends])
    seg_hot = segment[:, None] == jnp.arange(starts_all.shape[0], dtype=jnp.int32)[None, :]
    first_row = jnp.sum(jnp.where(seg_hot, starts_all[None, :], 0), axis=1)
    position = row_index - first_row
    valid_row = segment < lens_row.shape[0]
    allowed = (segment[:, None] == segment[None, :]) & (row_index[None, :] <= row_index[:, None])
    return (position, valid_row, allowed)


def rotary_tables(position, head_dim):
    half_dim = head_dim // 2
    frequency = theta_base ** (-(jnp.arange(half_dim, dtype=jnp.float32) * 2.0) / head_dim)
    angles = position.astype(jnp.float32)[:, None] * frequency[None, :]
    angles = jnp.concatenate([angles, angles], axis=-1)
    return (jnp.cos(angles), jnp.sin(angles))


def per_device(
    hidden_in,
    cotangent,
    deal_order,
    seq_lengths,
    expert_ids,
    w_query,
    w_key,
    w_value,
    w_out,
    w_router,
    gain_attn,
    gain_moe,
    gain_query,
    gain_key,
    w_gate,
    w_up,
    w_down,
    clip_threshold,
):
    tok_count = hidden_in.shape[0]
    model_width = hidden_in.shape[1]
    head_dim = gain_query.shape[0]
    local_order = deal_order % tok_count
    position, valid_row, allowed = layout(seq_lengths[0], tok_count)
    valid_col = valid_row.astype(jnp.float32)[:, None]
    cosine_table, sine_table = rotary_tables(position, head_dim)
    cosine_query = cosine_table[:, None, None, :]
    sine_query = sine_table[:, None, None, :]
    cosine_key = cosine_table[:, None, :]
    sine_key = sine_table[:, None, :]
    attn_params = (
        lax.all_gather(w_query, ("dp", "ep"), axis=0, tiled=True),
        lax.all_gather(w_key, ("dp", "ep"), axis=0, tiled=True),
        lax.all_gather(w_value, ("dp", "ep"), axis=0, tiled=True),
        lax.all_gather(w_out, ("dp", "ep"), axis=0, tiled=True),
        lax.all_gather(w_router, ("dp", "ep"), axis=0, tiled=True),
        lax.all_gather(gain_attn, ("dp", "ep"), axis=0, tiled=True),
        lax.all_gather(gain_moe, ("dp", "ep"), axis=0, tiled=True),
    )
    expert_params = (
        lax.all_gather(w_gate, "dp", axis=1, tiled=True),
        lax.all_gather(w_up, "dp", axis=1, tiled=True),
        lax.all_gather(w_down, "dp", axis=2, tiled=True),
    )
    query_full, key_full, value_full, out_full, router_full, gain_attn_full, gain_moe_full = (
        attn_params
    )
    gate_full, up_full, down_full = expert_params
    head_count = query_full.shape[1] // head_dim
    kv_count = key_full.shape[1] // head_dim
    group_size = head_count // kv_count
    experts = router_full.shape[1]
    top_count = expert_ids.shape[1]
    exp_local = w_gate.shape[0]
    ep_count = lax.axis_size("ep")
    capacity = (tok_count * top_count * 5 + 4 * experts - 1) // (4 * experts)
    score_scale = head_dim ** (-0.5)
    resid_in = hidden_in[local_order].astype(jnp.float32)
    inv_one = rms_scale(resid_in)
    unit_one = resid_in * inv_one
    gain_one = gain_attn_full.astype(jnp.float32)
    normed_in = (unit_one * gain_one).astype(jnp.bfloat16)
    query_raw = jnp.dot(normed_in, query_full, preferred_element_type=jnp.float32).reshape(
        tok_count, kv_count, group_size, head_dim
    )
    key_raw = jnp.dot(normed_in, key_full, preferred_element_type=jnp.float32).reshape(
        tok_count, kv_count, head_dim
    )
    value_rows = (
        jnp.dot(normed_in, value_full, preferred_element_type=jnp.float32)
        .astype(jnp.bfloat16)
        .reshape(tok_count, kv_count, head_dim)
    )
    inv_query = rms_scale(query_raw)
    unit_query = query_raw * inv_query
    gain_query_f = gain_query.astype(jnp.float32)
    query_rot = rotate(unit_query * gain_query_f, cosine_query, sine_query).astype(jnp.bfloat16)
    inv_key = rms_scale(key_raw)
    unit_key = key_raw * inv_key
    gain_key_f = gain_key.astype(jnp.float32)
    key_rot = rotate(unit_key * gain_key_f, cosine_key, sine_key).astype(jnp.bfloat16)
    scores = contract(query_rot, key_rot, "tkgd,ukd->kgtu") * score_scale
    masked = jnp.where(allowed, scores, masked_fill)
    row_top = jnp.max(masked, axis=-1, keepdims=True)
    exponent = jnp.exp(masked - row_top)
    row_total = jnp.sum(exponent, axis=-1, keepdims=True)
    log_total = row_top + jnp.log(row_total)
    probs_low = (exponent / row_total).astype(jnp.bfloat16)
    mixed_heads = (
        contract(probs_low, value_rows, "kgtu,ukd->tkgd")
        .astype(jnp.bfloat16)
        .reshape(tok_count, head_count * head_dim)
    )
    resid_mid = resid_in + jnp.dot(mixed_heads, out_full, preferred_element_type=jnp.float32)
    largest_local = jnp.max(
        jnp.where(allowed & valid_row[:, None], scores, masked_fill), axis=(2, 3)
    ).reshape(head_count)
    largest = lax.pmax(largest_local, ("dp", "ep"))
    clip_factor = jnp.sqrt(clip_threshold / jnp.maximum(largest, clip_threshold))
    inv_two = rms_scale(resid_mid)
    unit_two = resid_mid * inv_two
    gain_two = gain_moe_full.astype(jnp.float32)
    normed_mid = (unit_two * gain_two).astype(jnp.bfloat16)
    logits = jnp.dot(normed_mid, router_full, preferred_element_type=jnp.float32)
    choose = expert_ids[:, :, None] == jnp.arange(experts, dtype=jnp.int32)[None, None, :]
    picked = jnp.sum(jnp.where(choose, logits[:, None, :], 0.0), axis=2)
    gate_weights = jax.nn.softmax(picked, axis=-1)
    flat_ids = expert_ids.reshape(-1)
    flat_hot = (flat_ids[:, None] == jnp.arange(experts, dtype=jnp.int32)[None, :]).astype(
        jnp.int32
    )
    slot_rank = jnp.sum((jnp.cumsum(flat_hot, axis=0) - 1) * flat_hot, axis=1)
    slot_index = flat_ids * capacity + slot_rank
    pair_token = jnp.arange(tok_count * top_count, dtype=jnp.int32) // top_count
    send_rows = (
        jnp.zeros((experts * capacity, model_width), jnp.bfloat16)
        .at[slot_index]
        .set(normed_mid[pair_token])
    )
    send_rows = send_rows.reshape(ep_count, exp_local, capacity, model_width)
    arrived = lax.all_to_all(send_rows, "ep", split_axis=0, concat_axis=0, tiled=True)
    gate_part = contract(arrived, gate_full, "secd,edf->secf")
    up_part = contract(arrived, up_full, "secd,edf->secf")
    hidden_mid = (jax.nn.silu(gate_part) * up_part).astype(jnp.bfloat16)
    produced = contract(hidden_mid, down_full, "secf,efd->secd").astype(jnp.bfloat16)
    returned = lax.all_to_all(produced, "ep", split_axis=0, concat_axis=0, tiled=True)
    returned, arrived, gate_part, up_part = (returned, arrived, gate_part, up_part)
    pair_out = (
        returned.reshape(experts * capacity, model_width)[slot_index]
        .reshape(tok_count, top_count, model_width)
        .astype(jnp.float32)
    )
    resid_out = resid_mid + jnp.sum(gate_weights[:, :, None] * pair_out, axis=1)
    out_rows = (resid_out * valid_col).astype(jnp.bfloat16)
    block_out = jnp.zeros_like(out_rows).at[local_order].set(out_rows)
    attn_params = (
        lax.all_gather(w_query, ("dp", "ep"), axis=0, tiled=True),
        lax.all_gather(w_key, ("dp", "ep"), axis=0, tiled=True),
        lax.all_gather(w_value, ("dp", "ep"), axis=0, tiled=True),
        lax.all_gather(w_out, ("dp", "ep"), axis=0, tiled=True),
        lax.all_gather(w_router, ("dp", "ep"), axis=0, tiled=True),
        lax.all_gather(gain_attn, ("dp", "ep"), axis=0, tiled=True),
        lax.all_gather(gain_moe, ("dp", "ep"), axis=0, tiled=True),
    )
    expert_params = (
        lax.all_gather(w_gate, "dp", axis=1, tiled=True),
        lax.all_gather(w_up, "dp", axis=1, tiled=True),
        lax.all_gather(w_down, "dp", axis=2, tiled=True),
    )
    query_full, key_full, value_full, out_full, router_full, gain_attn_full, gain_moe_full = (
        attn_params
    )
    gate_full, up_full, down_full = expert_params
    grad_mid_out = cotangent[local_order].astype(jnp.float32) * valid_col
    grad_gates = jnp.sum(grad_mid_out[:, None, :] * pair_out, axis=2)
    grad_pair = (gate_weights[:, :, None] * grad_mid_out[:, None, :]).astype(jnp.bfloat16)
    send_grads = (
        jnp.zeros((experts * capacity, model_width), jnp.bfloat16)
        .at[slot_index]
        .set(grad_pair.reshape(-1, model_width))
    )
    send_grads = send_grads.reshape(ep_count, exp_local, capacity, model_width)
    grad_arrived = lax.all_to_all(send_grads, "ep", split_axis=0, concat_axis=0, tiled=True)
    grad_hidden = contract(grad_arrived, down_full, "secd,efd->secf")
    sigmoid_gate = jax.nn.sigmoid(gate_part)
    silu_gate = jax.nn.silu(gate_part)
    grad_gate_part = (
        grad_hidden * up_part * sigmoid_gate * (1.0 + gate_part * (1.0 - sigmoid_gate))
    ).astype(jnp.bfloat16)
    grad_up_part = (grad_hidden * silu_gate).astype(jnp.bfloat16)
    grad_rows = (
        contract(grad_gate_part, gate_full, "secf,edf->secd")
        + contract(grad_up_part, up_full, "secf,edf->secd")
    ).astype(jnp.bfloat16)
    grad_back = lax.all_to_all(grad_rows, "ep", split_axis=0, concat_axis=0, tiled=True)
    hidden_mid = (silu_gate * up_part).astype(jnp.bfloat16)
    grad_gate_w = contract(arrived, grad_gate_part, "secd,secf->edf")
    grad_up_w = contract(arrived, grad_up_part, "secd,secf->edf")
    grad_down_w = contract(hidden_mid, grad_arrived, "secf,secd->efd")
    grad_gate, grad_up, grad_down = (
        lax.psum_scatter(
            grad_gate_w.astype(jnp.bfloat16), "dp", scatter_dimension=1, tiled=True
        ).astype(jnp.float32),
        lax.psum_scatter(
            grad_up_w.astype(jnp.bfloat16), "dp", scatter_dimension=1, tiled=True
        ).astype(jnp.float32),
        lax.psum_scatter(
            grad_down_w.astype(jnp.bfloat16), "dp", scatter_dimension=2, tiled=True
        ).astype(jnp.float32),
    )
    mean_term = jnp.sum(gate_weights * grad_gates, axis=1, keepdims=True)
    grad_picked = gate_weights * (grad_gates - mean_term)
    grad_logits = jnp.sum(jnp.where(choose, grad_picked[:, :, None], 0.0), axis=1).astype(
        jnp.bfloat16
    )
    grad_router_w = contract(normed_mid, grad_logits, "td,te->de")
    pair_grads = (
        grad_back.reshape(experts * capacity, model_width)[slot_index]
        .reshape(tok_count, top_count, model_width)
        .astype(jnp.float32)
    )
    grad_normed_mid = jnp.sum(pair_grads, axis=1) + contract(grad_logits, router_full, "te,de->td")
    grad_gain_moe_w = jnp.sum(grad_normed_mid * unit_two, axis=0)
    grad_mid = grad_mid_out + norm_back(grad_normed_mid * gain_two, unit_two, inv_two)
    grad_branch = grad_mid.astype(jnp.bfloat16)
    grad_out_w = contract(mixed_heads, grad_branch, "tq,td->qd")
    grad_mixed = (
        contract(grad_branch, out_full, "td,qd->tq")
        .astype(jnp.bfloat16)
        .reshape(tok_count, kv_count, group_size, head_dim)
    )
    scores_again = contract(query_rot, key_rot, "tkgd,ukd->kgtu") * score_scale
    probs_back = jnp.exp(jnp.where(allowed, scores_again, masked_fill) - log_total)
    grad_value_rows = contract(
        probs_back.astype(jnp.bfloat16), grad_mixed, "kgtu,tkgd->ukd"
    ).astype(jnp.bfloat16)
    grad_probs = contract(grad_mixed, value_rows, "tkgd,ukd->kgtu")
    grad_scores = (
        probs_back * (grad_probs - jnp.sum(probs_back * grad_probs, axis=-1, keepdims=True))
    ).astype(jnp.bfloat16)
    grad_query_rot = contract(grad_scores, key_rot, "kgtu,ukd->tkgd") * score_scale
    grad_key_rot = contract(grad_scores, query_rot, "kgtu,tkgd->ukd") * score_scale
    grad_query_normed = rotate_back(grad_query_rot, cosine_query, sine_query)
    grad_key_normed = rotate_back(grad_key_rot, cosine_key, sine_key)
    grad_gain_q = jnp.sum(grad_query_normed * unit_query, axis=(0, 1, 2))
    grad_gain_k = jnp.sum(grad_key_normed * unit_key, axis=(0, 1))
    grad_query_raw = (
        norm_back(grad_query_normed * gain_query_f, unit_query, inv_query)
        .astype(jnp.bfloat16)
        .reshape(tok_count, head_count * head_dim)
    )
    grad_key_raw = (
        norm_back(grad_key_normed * gain_key_f, unit_key, inv_key)
        .astype(jnp.bfloat16)
        .reshape(tok_count, kv_count * head_dim)
    )
    grad_value_flat = grad_value_rows.reshape(tok_count, kv_count * head_dim)
    grad_query_w = contract(normed_in, grad_query_raw, "td,tq->dq")
    grad_key_w = contract(normed_in, grad_key_raw, "td,tq->dq")
    grad_value_w = contract(normed_in, grad_value_flat, "td,tq->dq")
    grad_normed_in = (
        contract(grad_query_raw, query_full, "tq,dq->td")
        + contract(grad_key_raw, key_full, "tq,dq->td")
        + contract(grad_value_flat, value_full, "tq,dq->td")
    )
    grad_gain_attn_w = jnp.sum(grad_normed_in * unit_one, axis=0)
    grad_resid_in = grad_mid + norm_back(grad_normed_in * gain_one, unit_one, inv_one)
    grad_input = jnp.zeros_like(grad_resid_in).at[local_order].set(grad_resid_in)
    grad_sums = (
        lax.psum_scatter(grad_query_w, ("dp", "ep"), scatter_dimension=0, tiled=True),
        lax.psum_scatter(grad_key_w, ("dp", "ep"), scatter_dimension=0, tiled=True),
        lax.psum_scatter(grad_value_w, ("dp", "ep"), scatter_dimension=0, tiled=True),
        lax.psum_scatter(grad_out_w, ("dp", "ep"), scatter_dimension=0, tiled=True),
        lax.psum_scatter(grad_router_w, ("dp", "ep"), scatter_dimension=0, tiled=True),
        lax.psum_scatter(grad_gain_attn_w, ("dp", "ep"), scatter_dimension=0, tiled=True),
        lax.psum_scatter(grad_gain_moe_w, ("dp", "ep"), scatter_dimension=0, tiled=True),
    )
    gain_sums = lax.psum((grad_gain_q, grad_gain_k), ("dp", "ep"))
    return (
        block_out,
        grad_input,
        grad_sums[0],
        grad_sums[1],
        grad_sums[2],
        grad_sums[3],
        grad_sums[4],
        grad_sums[5],
        grad_sums[6],
        gain_sums[0],
        gain_sums[1],
        grad_gate,
        grad_up,
        grad_down,
        clip_factor,
    )


MESH = pl.DeviceIdType.MESH


def place():
    dp = lax.axis_index("dp")
    ep = lax.axis_index("ep")
    z, y = dp // 2, dp % 2
    x, c = ep // 2, ep % 2
    first = (1 - c) * y + c * x
    second = (1 - c) * x + c * y
    return dp, ep, z, y, x, c, first, second


def targets(dp, ep, z, y, x, c, nz):
    up = (jnp.where(z < nz - 1, dp + 2, dp), ep)
    down = (jnp.where(z > 0, dp - 2, dp), ep)
    turn_y, turn_x = 1 - 2 * y, 2 - 4 * x
    near = (dp + (1 - c) * turn_y, ep + c * turn_x)
    far = (dp + c * turn_y, ep + (1 - c) * turn_x)
    twin = (dp, ep + 1 - 2 * c)
    return up, down, near, far, twin


def slot(z, first, second, c):
    return z * 8 + first * (4 - 2 * c) + second * (2 + 2 * c) + c


def greet(nz, z, dp, ep, ways, everyone):
    barrier = pltpu.get_barrier_semaphore()
    if everyone:
        total = nz * 8
        me = dp * 4 + ep

        def hello(step, carry):
            other = (me + step) % total
            pl.semaphore_signal(
                barrier, inc=1, device_id=(other // 4, other % 4), device_id_type=MESH
            )
            return carry

        lax.fori_loop(1, total, hello, 0)
        pl.semaphore_wait(barrier, total - 1)
        return
    for step in range(1, nz):
        other = ((z + step) % nz) * 2 + dp % 2
        pl.semaphore_signal(barrier, inc=1, device_id=(other, ep), device_id_type=MESH)
    for other in ways[2:]:
        pl.semaphore_signal(barrier, inc=1, device_id=other, device_id_type=MESH)
    pl.semaphore_wait(barrier, nz + 2)


class Riders:
    def __init__(self, kinds, nz, spot, refs):
        count = len(kinds)
        self.kinds, self.nz = kinds, nz
        self.dp, self.ep, self.z, self.y = spot
        self.me = self.dp * 4 + self.ep
        self.over_y = (self.dp + 1 - 2 * self.y, self.ep)
        self.ins, self.outs = refs[:count], refs[count : 2 * count]
        self.send, self.onward, self.recv, self.own = refs[2 * count :] if count else (None,) * 4
        self.spans = []
        for kind in kinds:
            if kind in ("all", "same"):
                self.spans.append((1, 8 * nz))
            else:
                self.spans.append((1 if kind in ("line", "cube") else 0, nz))
        self.cubes = [r for r in range(count) if kinds[r] == "cube"]

    def remote(self, source, target, send, recv, device):
        return pltpu.make_async_remote_copy(
            src_ref=source, dst_ref=target, send_sem=send, recv_sem=recv,
            device_id=device, device_id_type=MESH)

    def copy(self, r, step):
        kind, source, target = self.kinds[r], self.ins[r], self.outs[r]
        if kind in ("all", "same"):
            other = (self.me + step) % (8 * self.nz)
            source = source if kind == "same" else source.at[other]
            target, key, device = target.at[self.me], self.me, (other // 4, other % 4)
        elif kind in ("line", "cube"):
            other = (self.z + step) % self.nz
            source, key, device = source.at[other], self.z, (other * 2 + self.y, self.ep)
            target = target.at[self.z] if kind == "line" else target.at[self.z, self.y]
        else:
            source = source.at[step, 1 - self.y] if kind == "half" else source.at[step]
            target = target.at[step] if kind == "half" else target.at[step, self.y]
            key, device = step, self.over_y
        return self.remote(source, target, self.send.at[r, step], self.recv.at[r, key], device)

    def arrival(self, r, step):
        kind, target = self.kinds[r], self.outs[r]
        if kind in ("all", "same"):
            key = (self.me + step) % (8 * self.nz)
            target = target.at[key]
        elif kind in ("line", "cube"):
            key = (self.z + self.nz - step) % self.nz
            target = target.at[key] if kind == "line" else target.at[key, self.y]
        else:
            key = step
            target = target.at[step] if kind == "half" else target.at[step, 1 - self.y]
        return self.remote(target, target, self.send.at[r, step], self.recv.at[r, key], self.over_y)

    def passing(self, r, step, first=False):
        key = (self.z + self.nz - step) % self.nz
        target = self.outs[r].at[key, self.y]
        source = self.ins[r].at[key] if first else target
        return self.remote(
            source, target, self.onward.at[r, step], self.recv.at[r, self.nz + key], self.over_y)

    def passed(self, r, step):
        key = (self.z + self.nz - step) % self.nz
        target = self.outs[r].at[key, 1 - self.y]
        return self.remote(
            target, target, self.onward.at[r, step], self.recv.at[r, self.nz + key], self.over_y)

    def own_copies(self, r):
        kind, source, target = self.kinds[r], self.ins[r], self.outs[r]
        if kind in ("all", "same"):
            ends = [(source if kind == "same" else source.at[self.me], target.at[self.me])]
        elif kind == "half":
            ends = []
        elif kind == "pair":
            ends = [(source.at[k], target.at[k, self.y]) for k in range(self.nz)]
        else:
            target = target.at[self.z] if kind == "line" else target.at[self.z, self.y]
            ends = [(source.at[self.z], target)]
        return [pltpu.make_async_copy(here, there, self.own.at[r]) for here, there in ends]

    def begin(self, early=("half", "pair")):
        for r, kind in enumerate(self.kinds):
            for copy in self.own_copies(r):
                copy.start()
            if kind == "cube":
                self.passing(r, 0, True).start()
        self.steps = []
        for r, kind in enumerate(self.kinds):
            for k in range(*self.spans[r]):
                if kind in early:
                    self.copy(r, k).start()
                else:
                    self.steps.append((r, k))
        self.steps.sort(key=lambda step: step[1] / self.spans[step[0]][1])
        self.later = [r for r, kind in enumerate(self.kinds) if kind not in early]

    def some(self, share, shares):
        total = len(self.steps)
        for r, k in self.steps[total * share // shares : total * (share + 1) // shares]:
            self.copy(r, k).start()

    def onwards(self, step):
        for r in self.cubes:
            self.arrival(r, step).wait_recv()
            self.passing(r, step).start()

    def looped(self, step, steps):
        for r in self.later:
            first, last = self.spans[r]
            per = -(-(last - first) // steps)
            for k in range(per):
                piece = first + step * per + k

                @pl.when(piece < last)
                def _():
                    self.copy(r, piece).start()

    def finish(self):
        for r, kind in enumerate(self.kinds):

            def settle(step, carry):
                if kind != "cube":
                    self.arrival(r, step).wait_recv()
                self.copy(r, step).wait_send()
                return carry

            lax.fori_loop(*self.spans[r], settle, 0)
            if kind == "cube":

                def settle_y(step, carry):
                    self.passed(r, step).wait_recv()
                    self.passing(r, step).wait_send()
                    return carry

                lax.fori_loop(0, self.nz, settle_y, 0)
            for copy in self.own_copies(r):
                copy.wait()


def rider_shapes(riders, devices):
    kinds = tuple(kind for kind, _ in riders)
    arrays = tuple(array for _, array in riders)
    outs = []
    for kind, v in riders:
        shape = v.shape
        if kind == "same":
            shape = (devices,) + shape
        elif kind in ("cube", "pair"):
            shape = shape[:1] + (2,) + shape[1:]
        elif kind == "half":
            shape = shape[:1] + shape[2:]
        outs.append(jax.ShapeDtypeStruct(shape, v.dtype))
    dma = pltpu.SemaphoreType.DMA
    count = len(riders)
    sems = [dma((count, devices))] * 3 + [dma((count,))] if count else []
    return kinds, arrays, tuple(outs), sems


def rider_specs(kinds):
    return [
        pl.BlockSpec(memory_space=pl.ANY if kind == "half" else pltpu.VMEM)
        for kind in kinds
    ]


def wide_greeting(kinds):
    return "all" in kinds or "same" in kinds


def on(allowed, action):
    if allowed is None:
        action()
    else:
        pl.when(allowed)(action)


def along(z, nz, step):
    if step == 0:
        yield None, z
    else:
        yield z >= step, jnp.maximum(z - step, 0)
        yield z + step < nz, jnp.minimum(z + step, nz - 1)


class Mover:
    def __init__(self, ins, outs, ways, sems):
        self.ins, self.outs, self.ways = ins, outs, ways
        self.send, self.recv, self.own = sems
        self.pending, self.own_copies = [], []

    def push(self, way, where, allowed=None, own=False):
        for k, out in enumerate(self.outs):
            copy = pltpu.make_async_remote_copy(
                src_ref=self.ins[k] if own else out.at[where],
                dst_ref=out.at[where],
                send_sem=self.send.at[k, way, where],
                recv_sem=self.recv.at[k, where],
                device_id=self.ways[way],
                device_id_type=MESH,
            )
            on(allowed, copy.start)
            self.pending.append((allowed, copy))

    def arrive(self, where):
        for k, out in enumerate(self.outs):
            pltpu.make_async_remote_copy(
                src_ref=out.at[where],
                dst_ref=out.at[where],
                send_sem=self.send.at[k, 0, where],
                recv_sem=self.recv.at[k, where],
                device_id=self.ways[-1],
                device_id_type=MESH,
            ).wait_recv()

    def keep(self, mine):
        for k, out in enumerate(self.outs):
            copy = pltpu.make_async_copy(self.ins[k], out.at[mine], self.own.at[k])
            copy.start()
            self.own_copies.append(copy)

    def settle(self):
        for allowed, copy in self.pending:
            on(allowed, copy.wait_send)
        for copy in self.own_copies:
            copy.wait()


class WholeGather(Mover):
    def begin(self, nz, z, a, b, c):
        self.nz, self.z, self.a, self.b, self.c = nz, z, a, b, c
        mine = slot(z, a, b, c)
        self.push(0, mine, z < nz - 1, True)
        self.push(1, mine, z > 0, True)
        for way in (2, 3, 4):
            self.push(way, mine, None, True)
        self.keep(mine)

    def turn_z(self, turn):
        nz, z, a, b, c = self.nz, self.z, self.a, self.b, self.c
        if turn < nz:
            for index, (allowed, zz) in enumerate(along(z, nz, turn)):
                where = slot(zz, a, b, c)
                on(allowed, functools.partial(self.arrive, where))
                self.push(index, where, allowed & ((z > 0) if index else (z < nz - 1)))
                for way in (2, 3, 4):
                    self.push(way, where, allowed)

    def turn_xy(self, turn):
        nz, z, a, b, c = self.nz, self.z, self.a, self.b, self.c
        if turn - 1 < nz:
            for allowed, zz in along(z, nz, turn - 1):
                where = slot(zz, 1 - a, b, c)
                on(allowed, functools.partial(self.arrive, where))
                for way in (3, 4):
                    self.push(way, where, allowed)
            for allowed, zz in along(z, nz, turn - 1):
                where = slot(zz, a, 1 - b, c)
                on(allowed, functools.partial(self.arrive, where))
                self.push(4, where, allowed)
        if turn >= 2:
            for allowed, zz in along(z, nz, turn - 2):
                where = slot(zz, 1 - a, 1 - b, c)
                on(allowed, functools.partial(self.arrive, where))
                self.push(4, where, allowed)

    def end(self):
        for zz in range(self.nz):
            for aa in range(2):
                for bb in range(2):
                    self.arrive(slot(zz, aa, bb, 1 - self.c))
        self.settle()


class SlabGather(Mover):
    def begin(self, nz, z, ep, x, c):
        self.nz, self.z, self.ep, self.c = nz, z, ep, c
        self.other = ep + 2 - 4 * x
        mine = z * 4 + ep
        self.push(0, mine, z < nz - 1, True)
        self.push(1, mine, z > 0, True)
        for way in (2, 3):
            self.push(way, mine, None, True)
        self.keep(mine)

    def turn_z(self, turn):
        nz, z = self.nz, self.z
        if turn < nz:
            for index, (allowed, zz) in enumerate(along(z, nz, turn)):
                where = zz * 4 + self.ep
                on(allowed, functools.partial(self.arrive, where))
                self.push(index, where, allowed & ((z > 0) if index else (z < nz - 1)))
                for way in (2, 3):
                    self.push(way, where, allowed)

    def turn_xy(self, turn):
        nz, z = self.nz, self.z
        if turn - 1 < nz:
            for allowed, zz in along(z, nz, turn - 1):
                where = zz * 4 + self.other
                on(allowed, functools.partial(self.arrive, where))
                self.push(3, where, allowed)

    def end(self):
        for where in range(4 * self.nz):
            pl.when(where % 2 != self.c)(functools.partial(self.arrive, where))
        self.settle()


def gather_kernel(nz, counts, kinds, *refs):
    whole, slabs = counts
    count, extra = whole + slabs, len(kinds)
    ins = refs[:count]
    outs = refs[count + extra : 2 * count + extra]
    sems = refs[2 * (count + extra) :]
    dp, ep, z, y, x, c, a, b = place()
    ways = targets(dp, ep, z, y, x, c, nz)
    up, down, near, far, twin = ways
    side = (dp, ep + 2 - 4 * x)
    movers = []
    if whole:
        movers.append(WholeGather(ins[:whole], outs[:whole], ways, sems[:3]))
        sems = sems[3:]
    if slabs:
        movers.append(SlabGather(ins[whole:], outs[whole:], (up, down, side, twin), sems[:3]))
        sems = sems[3:]
    riders = Riders(
        kinds, nz, (dp, ep, z, y),
        refs[count : count + extra] + refs[2 * count + extra : 2 * (count + extra)] + sems,
    )
    greet(nz, z, dp, ep, ways, wide_greeting(kinds))
    for mover in movers:
        if isinstance(mover, WholeGather):
            mover.begin(nz, z, a, b, c)
        else:
            mover.begin(nz, z, ep, x, c)
    riders.begin()
    for turn in range(1, nz + 2):
        if turn <= nz:
            riders.some(turn - 1, nz)
        for mover in movers:
            mover.turn_z(turn)
            mover.turn_xy(turn)
        if 2 <= turn <= nz:
            riders.onwards(turn - 1)
    for mover in movers:
        mover.end()
    riders.finish()


def gather_rows(whole, slabs, devices, ident, riders=()):
    arrays = whole + slabs
    nz = devices // 8
    kinds, ridden, rider_outs, rider_sems = rider_shapes(riders, devices)
    blocks = (devices,) * len(whole) + (4 * nz,) * len(slabs)
    dma = pltpu.SemaphoreType.DMA
    sems = []
    for count, ways, total in ((len(whole), 5, devices), (len(slabs), 4, 4 * nz)):
        if count:
            sems += [dma((count, ways, total)), dma((count, total)), dma((count,))]
    return pl.pallas_call(
        functools.partial(gather_kernel, nz, (len(whole), len(slabs)), kinds),
        out_shape=tuple(
            jax.ShapeDtypeStruct((total,) + v.shape, v.dtype) for total, v in zip(blocks, arrays)
        )
        + rider_outs,
        in_specs=[pl.BlockSpec(memory_space=pltpu.VMEM)] * len(arrays) + rider_specs(kinds),
        out_specs=tuple(pl.BlockSpec(memory_space=pl.ANY) for v in arrays + ridden),
        scratch_shapes=sems + rider_sems,
        compiler_params=pltpu.CompilerParams(collective_id=ident, has_side_effects=True),
        name="gather_rows_%d" % ident,
    )(*arrays, *ridden)


def scatter_kernel(nz, turned, kinds, *refs):
    extra = len(kinds)
    left_ref, right_ref = refs[:2]
    refs = refs[2:]
    out_ref = refs[extra]
    sent, got, from_far, from_near, rising, falling = refs[2 * extra + 1 : 2 * extra + 7]
    (twin_send, twin_recv, far_send, far_recv, near_send, near_recv, line_send, up_recv,
     down_recv) = refs[2 * extra + 7 : 2 * extra + 16]
    dp, ep, z, y, x, c, a, b = place()
    ways = targets(dp, ep, z, y, x, c, nz)
    up, down, near, far, twin = ways
    riders = Riders(
        kinds, nz, (dp, ep, z, y),
        refs[:extra] + refs[extra + 1 : 2 * extra + 1] + refs[2 * extra + 16 :]
    )
    greet(nz, z, dp, ep, ways, wide_greeting(kinds))
    riders.begin(("half", "line"))
    per = 4 * nz

    def zed(step):
        if nz == 4:
            far_one = jnp.where(z < 2, 3, 0)
            second = jnp.where(z < 2, 2 - 2 * z, 7 - 2 * z)
            third = 1 + z % 2
            return jnp.where(step == 0, far_one, jnp.where(step == 1, second, jnp.where(step == 2, third, z)))
        return (z + 1 + step) % nz

    def term(where):
        sides = (((1,), (1 if turned else 0,)), ((), ()))
        return lax.dot_general(
            left_ref[where], right_ref[...], sides, preferred_element_type=jnp.float32
        )

    def order(index, aa, bb, cc):
        part = index // nz
        flip_b = 1 - part // 2
        flip_a = 1 - part % 2
        return slot(zed(index % nz), aa + flip_a * (1 - 2 * aa), bb + flip_b * (1 - 2 * bb), cc)

    def twin_copy(index):
        return pltpu.make_async_remote_copy(
            src_ref=sent.at[index], dst_ref=got.at[index], send_sem=twin_send.at[index],
            recv_sem=twin_recv.at[index], device_id=twin, device_id_type=MESH)

    def far_copy(index):
        return pltpu.make_async_remote_copy(
            src_ref=got.at[index], dst_ref=from_far.at[index], send_sem=far_send.at[index],
            recv_sem=far_recv.at[index], device_id=far, device_id_type=MESH)

    def near_copy(index):
        return pltpu.make_async_remote_copy(
            src_ref=got.at[2 * nz + index], dst_ref=from_near.at[index], send_sem=near_send.at[index],
            recv_sem=near_recv.at[index], device_id=near, device_id_type=MESH)

    def up_copy(index, zz):
        return pltpu.make_async_remote_copy(
            src_ref=got.at[3 * nz + index], dst_ref=rising.at[zz], send_sem=line_send.at[index],
            recv_sem=up_recv.at[zz], device_id=up, device_id_type=MESH)

    def down_copy(index, zz):
        return pltpu.make_async_remote_copy(
            src_ref=got.at[3 * nz + index], dst_ref=falling.at[zz], send_sem=line_send.at[index],
            recv_sem=down_recv.at[zz], device_id=down, device_id_type=MESH)

    def give(index):
        sent[index] = term(order(index, b, a, 1 - c)).astype(sent.dtype)
        twin_copy(index).start()

    def taken(index):
        value = term(order(index, a, b, c))
        twin_copy(index).wait_recv()
        return value + got[index].astype(jnp.float32)

    def far_step(step, carry):
        give(2 * step)
        give(2 * step + 1)
        got[step] = taken(step).astype(got.dtype)
        far_copy(step).start()
        riders.looped(step, 2 * nz)
        return carry

    lax.fori_loop(0, 2 * nz, far_step, 0)

    def near_step(step, carry):
        value = taken(2 * nz + step)
        far_copy(step).wait_recv()
        value = value + from_far[step].astype(jnp.float32)
        got[2 * nz + step] = value.astype(got.dtype)
        near_copy(step).start()
        return carry

    lax.fori_loop(0, nz, near_step, 0)

    def line_step(step, carry):
        zz = zed(step)
        value = taken(3 * nz + step)
        far_copy(nz + step).wait_recv()
        near_copy(step).wait_recv()
        out_ref[...] = value + from_far[nz + step].astype(jnp.float32) + from_near[step].astype(jnp.float32)

        @pl.when((zz >= z) & (z > 0))
        def _():
            up_copy(step, zz).wait_recv()
            out_ref[...] += rising[zz].astype(jnp.float32)

        @pl.when((zz <= z) & (z < nz - 1))
        def _():
            down_copy(step, zz).wait_recv()
            out_ref[...] += falling[zz].astype(jnp.float32)

        @pl.when(zz > z)
        def _():
            got[3 * nz + step] = out_ref[...].astype(got.dtype)
            up_copy(step, zz).start()

        @pl.when(zz < z)
        def _():
            got[3 * nz + step] = out_ref[...].astype(got.dtype)
            down_copy(step, zz).start()

        return carry

    lax.fori_loop(0, nz, line_step, 0)

    def finish(step, carry):
        twin_copy(step).wait_send()
        return carry

    lax.fori_loop(0, per, finish, 0)

    def finish_far(step, carry):
        far_copy(step).wait_send()
        return carry

    lax.fori_loop(0, 2 * nz, finish_far, 0)

    def finish_near(step, carry):
        near_copy(step).wait_send()

        @pl.when(step < nz - 1)
        def _():
            up_copy(step, 0).wait_send()

        return carry

    lax.fori_loop(0, nz, finish_near, 0)
    riders.finish()


def scatter_sum(left, right, devices, ident, turned=False, riders=()):
    nz = devices // 8
    rows = left.shape[0] // devices
    depth, wide = right.shape[::-1] if turned else right.shape
    kinds, ridden, rider_outs, rider_sems = rider_shapes(riders, devices)
    block = (rows, wide)
    low = jnp.bfloat16
    dma = pltpu.SemaphoreType.DMA
    result = pl.pallas_call(
        functools.partial(scatter_kernel, nz, turned, kinds),
        out_shape=(jax.ShapeDtypeStruct(block, jnp.float32),) + rider_outs,
        in_specs=[pl.BlockSpec(memory_space=pltpu.VMEM)] * 2 + rider_specs(kinds),
        out_specs=(pl.BlockSpec(memory_space=pltpu.VMEM),)
        + (pl.BlockSpec(memory_space=pl.ANY),) * len(riders),
        scratch_shapes=[
            pltpu.VMEM((4 * nz,) + block, low),
            pltpu.VMEM((4 * nz,) + block, low),
            pltpu.VMEM((2 * nz,) + block, low),
            pltpu.VMEM((nz,) + block, low),
            pltpu.VMEM((nz,) + block, low),
            pltpu.VMEM((nz,) + block, low),
            dma((4 * nz,)), dma((4 * nz,)), dma((2 * nz,)), dma((2 * nz,)),
            dma((nz,)), dma((nz,)), dma((nz,)), dma((nz,)), dma((nz,)),
        ]
        + rider_sems,
        compiler_params=pltpu.CompilerParams(
            collective_id=ident, has_side_effects=True, vmem_limit_bytes=58 * 2**20),
        name="scatter_sum_%d" % ident,
    )(left.reshape(devices, rows, depth), right, *ridden)
    return result if riders else result[0]


class SlabSum:
    def __init__(self, nz, turned, spot, ways, refs, buffers):
        self.nz, self.turned = nz, turned
        self.z, self.x, self.c = spot
        self.up, self.down, self.side, self.twin = ways
        self.lefts, self.rights, self.beside, self.out = refs
        (self.sent, self.got, self.from_side, self.rising, self.falling,
         self.twin_send, self.twin_recv, self.side_send, self.side_recv, self.line_send,
         self.up_recv, self.down_recv) = buffers
        self.plain = self.rights[0].shape[0 if turned else 1]
        self.span = 512 if self.plain % 512 == 0 else self.plain

    def zed(self, step):
        z, nz = self.z, self.nz
        if nz == 4:
            far_one = jnp.where(z < 2, 3, 0)
            second = jnp.where(z < 2, 2 - 2 * z, 7 - 2 * z)
            third = 1 + z % 2
            return jnp.where(step == 0, far_one, jnp.where(step == 1, second, jnp.where(step == 2, third, z)))
        return (z + 1 + step) % nz

    def order(self, index, cc):
        flip = 1 - index // self.nz
        return self.zed(index % self.nz) * 4 + (self.x + flip * (1 - 2 * self.x)) * 2 + cc

    def combine(self, targets_, wheres, added):
        rows = self.lefts[0].shape[1]

        def put(which, at, total):
            for ref in added[which]:
                total = total + ref[:, at].astype(jnp.float32)
            targets_[which][:, at] = total.astype(targets_[which].dtype)

        def fill(chunk, carry):
            at = pl.ds(pl.multiple_of(chunk * self.span, self.span), self.span)
            total = None
            for left_ref, right_ref in zip(self.lefts, self.rights):
                value = lax.dot_general(
                    jnp.concatenate([left_ref[where] for where in wheres], axis=0),
                    right_ref[at, :] if self.turned else right_ref[:, at],
                    (((1,), (1 if self.turned else 0,)), ((), ())),
                    preferred_element_type=jnp.float32,
                )
                total = value if total is None else total + value
            for which in range(len(wheres)):
                put(which, at, total[which * rows : (which + 1) * rows])
            return carry

        lax.fori_loop(0, self.plain // self.span, fill, 0)
        if self.beside is not None:
            at = pl.ds(self.plain, self.beside.shape[2])
            for which, where in enumerate(wheres):
                put(which, at, self.beside[where].astype(jnp.float32))

    def remote(self, source, target, send, recv, device):
        return pltpu.make_async_remote_copy(
            src_ref=source, dst_ref=target, send_sem=send, recv_sem=recv,
            device_id=device, device_id_type=MESH)

    def twin_copy(self, index):
        return self.remote(
            self.sent.at[index], self.got.at[index], self.twin_send.at[index],
            self.twin_recv.at[index], self.twin)

    def side_copy(self, index):
        return self.remote(
            self.got.at[index], self.from_side.at[index], self.side_send.at[index],
            self.side_recv.at[index], self.side)

    def line_copy(self, index, zz, rise):
        place_, recv = (self.rising, self.up_recv) if rise else (self.falling, self.down_recv)
        return self.remote(
            self.got.at[self.nz + index], place_.at[zz], self.line_send.at[index], recv.at[zz],
            self.up if rise else self.down)

    def give(self, pair, carry):
        both = (2 * pair, 2 * pair + 1)
        self.combine(
            [self.sent.at[index] for index in both],
            [self.order(index, 1 - self.c) for index in both], [(), ()])
        for index in both:
            self.twin_copy(index).start()
        return carry

    def to_side(self, pair):
        lax.fori_loop(2 * pair, 2 * pair + 2, self.give, 0)
        both = (2 * pair, 2 * pair + 1)
        for index in both:
            self.twin_copy(index).wait_recv()
        self.combine(
            [self.got.at[index] for index in both],
            [self.order(index, self.c) for index in both],
            [(self.got.at[index],) for index in both])
        self.side_copy(both[0]).start()

    def to_line(self, step):
        self.twin_copy(self.nz + step).wait_recv()
        self.side_copy(step).wait_recv()
        self.combine(
            [self.out],
            [self.order(self.nz + step, self.c)],
            [(self.got.at[self.nz + step], self.from_side.at[step])])
        self.along_line(self.out, step)

    def along_line(self, held, step):
        z, zz = self.z, self.zed(step)

        @pl.when((zz >= z) & (z > 0))
        def _():
            self.line_copy(step, zz, True).wait_recv()
            held[...] += self.rising[zz].astype(jnp.float32)

        @pl.when((zz <= z) & (z < self.nz - 1))
        def _():
            self.line_copy(step, zz, False).wait_recv()
            held[...] += self.falling[zz].astype(jnp.float32)

        @pl.when(zz != z)
        def _():
            self.got[self.nz + step] = held[...].astype(self.got.dtype)

        pl.when(zz > z)(lambda: self.line_copy(step, zz, True).start())
        pl.when(zz < z)(lambda: self.line_copy(step, zz, False).start())

    def end(self):
        def finish(step, carry):
            self.twin_copy(step).wait_send()
            return carry

        lax.fori_loop(0, 2 * self.nz, finish, 0)

        def finish_side(step, carry):
            self.side_copy(step).wait_send()

            @pl.when(step < self.nz - 1)
            def _():
                self.line_copy(step, 0, True).wait_send()

            return carry

        lax.fori_loop(0, self.nz, finish_side, 0)


def slab_scatter_kernel(nz, forms, kinds, *refs):
    extra, parts = len(kinds), len(forms)
    refs = list(refs)

    def take(count):
        taken = tuple(refs[:count])
        del refs[:count]
        return taken

    operands = []
    for pairs, turned, beside in forms:
        operands.append((take(pairs), take(pairs), take(1)[0] if beside else None))
    rider_ins = take(extra)
    outs = take(parts)
    rider_outs = take(extra)
    dp, ep, z, y, x, c, _, _ = place()
    up, down, near, far, twin = targets(dp, ep, z, y, x, c, nz)
    side = (dp, ep + 2 - 4 * x)
    sums = [
        SlabSum(nz, form[1], (z, x, c), (up, down, side, twin), held + (out,), take(12))
        for form, held, out in zip(forms, operands, outs)
    ]
    riders = Riders(kinds, nz, (dp, ep, z, y), rider_ins + rider_outs + tuple(refs))
    greet(nz, z, dp, ep, (up, down, near, far, twin), wide_greeting(kinds))
    riders.begin(("half", "line"))

    def side_step(pair, carry):
        for part in sums:
            part.to_side(pair)
        for part in sums:
            part.side_copy(2 * pair + 1).start()
        riders.looped(pair, nz // 2)
        return carry

    lax.fori_loop(0, nz // 2, side_step, 0)

    def line_step(step, carry):
        for part in sums:
            part.to_line(step)
        return carry

    lax.fori_loop(0, nz, line_step, 0)
    for part in sums:
        part.end()
    riders.finish()


def slab_scatter(parts, devices, ident, riders=()):
    nz = devices // 8
    blocks = 4 * nz
    rows = parts[0][0][0].shape[0] // blocks
    kinds, ridden, rider_outs, rider_sems = rider_shapes(riders, devices)
    low, dma = jnp.bfloat16, pltpu.SemaphoreType.DMA
    operands, outs, scratch, forms = (), (), [], []
    for lefts, rights, turned, beside in parts:
        held = () if beside is None else (beside.reshape(blocks, rows, -1),)
        wide = rights[0].shape[0 if turned else 1] + sum(v.shape[2] for v in held)
        block = (rows, wide)
        operands += tuple(v.reshape(blocks, rows, -1) for v in lefts) + tuple(rights) + held
        outs += (jax.ShapeDtypeStruct(block, jnp.float32),)
        scratch += [pltpu.VMEM((count * nz,) + block, low) for count in (2, 2, 1, 1, 1)]
        scratch += [dma((2 * nz,))] * 2 + [dma((nz,))] * 5
        forms.append((len(lefts), turned, len(held)))
    return pl.pallas_call(
        functools.partial(slab_scatter_kernel, nz, tuple(forms), kinds),
        out_shape=outs + rider_outs,
        in_specs=[pl.BlockSpec(memory_space=pltpu.VMEM)] * len(operands) + rider_specs(kinds),
        out_specs=(pl.BlockSpec(memory_space=pltpu.VMEM),) * len(outs)
        + (pl.BlockSpec(memory_space=pl.ANY),) * len(riders),
        scratch_shapes=scratch + rider_sems,
        compiler_params=pltpu.CompilerParams(
            collective_id=ident, has_side_effects=True, vmem_limit_bytes=63 * 2**20),
        name="slab_scatter_%d" % ident,
    )(*operands, *ridden)


def whole_rows(mesh):
    return mesh.shape["ep"] == 4 and mesh.shape["dp"] in (4, 8)


def exact_dot(left_side, right_side):
    return jnp.dot(
        left_side, right_side, precision=lax.Precision.HIGHEST, preferred_element_type=jnp.float32
    )


def block_layout(lens, tok_count):
    ends = [lens[:, :1]]
    for at in range(1, lens.shape[1]):
        ends.append(ends[-1] + lens[:, at : at + 1])
    row_index = lax.broadcasted_iota(jnp.int32, (lens.shape[0], tok_count), 1)
    segment = jnp.zeros_like(row_index)
    first_row = jnp.zeros_like(row_index)
    for end in ends:
        passed = row_index >= end
        segment = segment + passed.astype(jnp.int32)
        first_row = jnp.where(passed, end, first_row)
    return (segment, row_index - first_row)


def by_experts(
    hidden_in,
    cotangent,
    deal_order,
    seq_lengths,
    expert_ids,
    w_query,
    w_key,
    w_value,
    w_out,
    w_router,
    gain_attn,
    gain_moe,
    gain_query,
    gain_key,
    w_gate,
    w_up,
    w_down,
    clip_threshold,
):
    f32, low = jnp.float32, jnp.bfloat16
    dp_count, ep_count = lax.axis_size("dp"), lax.axis_size("ep")
    devices = dp_count * ep_count
    dp, ep = lax.axis_index("dp"), lax.axis_index("ep")
    me = dp * ep_count + ep
    tok_count, width = hidden_in.shape
    row_count = tok_count * 7 // 8
    all_count = devices * row_count
    head_dim = gain_query.shape[0]
    half_dim = head_dim // 2
    rows_own = w_query.shape[0]
    head_count = w_query.shape[1] // head_dim
    kv_count = w_key.shape[1] // head_dim
    group_size = head_count // kv_count
    experts = w_router.shape[1]
    exp_local, wide_own, hidden = w_gate.shape
    lines = dp_count // 2
    slab = lines * ep_count
    z, y = dp // 2, dp % 2
    score_scale = head_dim ** (-0.5)

    gain_col = gain_attn.astype(f32)[:, None]
    heads_in = (w_query.astype(f32) * gain_col).astype(low).reshape(rows_own, head_count, head_dim)
    keys_in = (w_key.astype(f32) * gain_col).astype(low).reshape(rows_own, kv_count, head_dim)
    values_in = (w_value.astype(f32) * gain_col).astype(low).reshape(rows_own, kv_count, head_dim)
    sent_heads = jnp.concatenate(
        [heads_in, jnp.repeat(keys_in, group_size, axis=1), jnp.repeat(values_in, group_size, axis=1)],
        axis=2,
    ).transpose(1, 0, 2)

    local_order = deal_order % tok_count
    deal = (local_order[:, None] == jnp.arange(tok_count, dtype=jnp.int32)[None, :]).astype(low)
    deal = deal[:row_count]
    resid_in = jnp.dot(deal, hidden_in, preferred_element_type=f32)
    grad_mid_out = jnp.dot(deal, cotangent, preferred_element_type=f32)
    inv_one = rms_scale(resid_in)
    unit_one = resid_in * inv_one
    lens_row = jnp.pad(seq_lengths.astype(f32), ((0, 0), (0, 128 - seq_lengths.shape[1])))
    gain_row = jnp.pad(gain_moe.astype(f32)[None, :], ((0, 0), (0, 128 - rows_own)))
    router_rows = w_router.astype(f32).reshape(-1, 128)
    note_one = jnp.concatenate([lens_row, gain_row, router_rows], axis=0)
    note_one = jnp.pad(note_one, ((0, -note_one.shape[0] % 8), (0, 0)))
    unit_all, notes, grad_all, w_heads, w_rise_up = gather_rows(
        (unit_one.astype(low), note_one),
        (grad_mid_out.astype(low),),
        devices,
        1,
        (("all", sent_heads), ("cube", w_up)),
    )
    w_heads = w_heads.reshape(width, 3 * head_dim)
    w_rise_up = w_rise_up.reshape(width, hidden)
    lens_all = notes[:, 0, : seq_lengths.shape[1]].astype(jnp.int32)
    gain_two = notes[:, 1, :rows_own].reshape(1, width)
    router_full = notes[:, 2 : 2 + router_rows.shape[0]].reshape(width, experts)

    segment, position = block_layout(lens_all, row_count)
    step_down = lax.broadcasted_iota(jnp.int32, (1, row_count, row_count), 1)
    step_across = lax.broadcasted_iota(jnp.int32, (1, row_count, row_count), 2)
    allowed = (segment[:, :, None] == segment[:, None, :]) & (step_across <= step_down)
    cosine_rows, sine_rows = rotary_tables(jnp.arange(tok_count, dtype=jnp.int32), head_dim)
    place_hot = (position.reshape(-1)[:, None] == jnp.arange(tok_count)[None, :]).astype(f32)
    cosine_all = exact_dot(place_hot, cosine_rows).reshape(devices, row_count, head_dim)
    sine_all = exact_dot(place_hot, sine_rows).reshape(devices, row_count, head_dim)
    flat_unit = unit_all.reshape(all_count, width)
    projected = jnp.dot(flat_unit, w_heads, preferred_element_type=f32).reshape(
        devices, row_count, 3 * head_dim
    )
    query_raw = projected[..., :head_dim]
    key_raw = projected[..., head_dim : 2 * head_dim]
    value_rows = projected[..., 2 * head_dim :].astype(low)
    gain_query_f = gain_query.astype(f32)
    gain_key_f = gain_key.astype(f32)
    inv_query = rms_scale(query_raw)
    unit_query = query_raw * inv_query
    query_rot = rotate(unit_query * gain_query_f, cosine_all, sine_all).astype(low)
    inv_key = rms_scale(key_raw)
    unit_key = key_raw * inv_key
    key_rot = rotate(unit_key * gain_key_f, cosine_all, sine_all).astype(low)
    scores = contract(query_rot, key_rot, "btd,bud->btu") * score_scale
    masked = jnp.where(allowed, scores, masked_fill)
    row_top = jnp.max(masked, axis=-1, keepdims=True)
    exponent = jnp.exp(masked - row_top)
    probs = exponent / jnp.sum(exponent, axis=-1, keepdims=True)
    probs_low = probs.astype(low)
    mixed = contract(probs_low, value_rows, "btu,bud->btd").astype(low).reshape(all_count, head_dim)
    largest_own = jnp.max(row_top)
    branch, fall_own = scatter_sum(mixed, w_out, devices, 2, riders=(("line", w_down.transpose(0, 2, 1)),))
    resid_mid = resid_in + branch

    inv_two = rms_scale(resid_mid)
    unit_two = resid_mid * inv_two
    normed_mid = (unit_two * gain_two).astype(low)
    logits = jnp.dot(normed_mid, router_full.astype(low), preferred_element_type=f32)
    choose = (expert_ids[:row_count, :, None] == jnp.arange(experts, dtype=jnp.int32)[None, None, :]).any(axis=1)
    picked = jnp.where(choose, logits, masked_fill)
    gate_power = jnp.where(choose, jnp.exp(picked - jnp.max(picked, axis=1, keepdims=True)), 0.0)
    route = gate_power / jnp.sum(gate_power, axis=1, keepdims=True)
    note_two = jnp.pad(route.T, ((0, 0), (0, 128 - row_count)))
    normed_all, notes, w_rise_gate, w_fall = gather_rows(
        (), (normed_mid, note_two), devices, 3, (("cube", w_gate), ("pair", fall_own))
    )
    w_rise_gate = w_rise_gate.reshape(width, hidden)
    w_fall = w_fall.reshape(width, hidden)

    mine = ep * exp_local + z
    slab_rows = slab * row_count
    weight = lax.dynamic_slice_in_dim(notes, mine, 1, axis=1)[..., :row_count].reshape(slab_rows, 1)
    flat_mid = normed_all.reshape(slab_rows, width)
    flat_grad = grad_all.reshape(slab_rows, width)
    gate_part = jnp.dot(flat_mid, w_rise_gate, preferred_element_type=f32)
    up_part = jnp.dot(flat_mid, w_rise_up, preferred_element_type=f32)
    grad_plain = jnp.dot(flat_grad, w_fall, preferred_element_type=f32)
    sigmoid_gate = jax.nn.sigmoid(gate_part)
    silu_gate = gate_part * sigmoid_gate
    hidden_mid = silu_gate * up_part
    grad_route = jnp.sum(hidden_mid * grad_plain, axis=1, keepdims=True)
    weighted_mid = (hidden_mid * weight).astype(low)
    grad_hidden = grad_plain * weight
    grad_gate_part = (
        grad_hidden * up_part * sigmoid_gate * (1.0 + gate_part * (1.0 - sigmoid_gate))
    ).astype(low)
    grad_up_part = (grad_hidden * silu_gate).astype(low)
    lane = lax.broadcasted_iota(jnp.int32, (1, 128), 1)
    beside = jnp.where(lane == mine, grad_route, 0.0).astype(low)

    def for_each_y(grads):
        return grads.astype(low).reshape(lines, 2, wide_own, hidden)

    gate_halves = for_each_y(contract(flat_mid, grad_gate_part, "td,tf->df"))
    up_halves = for_each_y(contract(flat_mid, grad_up_part, "td,tf->df"))
    fall_halves = for_each_y(contract(flat_grad, weighted_mid, "td,tf->df"))
    summed, moe_rows, gate_come, up_come, fall_come = slab_scatter(
        (
            ((grad_gate_part, grad_up_part), (w_rise_gate, w_rise_up), True, beside),
            ((weighted_mid,), (w_fall,), True, None),
        ),
        devices,
        4,
        (("half", gate_halves), ("half", up_halves), ("half", fall_halves)),
    )

    def add_halves(halves, come):
        kept = lax.dynamic_index_in_dim(halves, y, axis=1, keepdims=False)
        return (kept.astype(f32) + come.astype(f32)).astype(low)

    grad_gates = summed[:, width : width + experts]
    mean_term = jnp.sum(route * grad_gates, axis=1, keepdims=True)
    grad_logits = (route * (grad_gates - mean_term)).astype(low)
    grad_normed_mid = summed[:, :width] + contract(grad_logits, router_full.astype(low), "te,de->td")
    gain_part = jnp.sum(grad_normed_mid * unit_two, axis=0)
    grad_mid = grad_mid_out + norm_back(grad_normed_mid * gain_two, unit_two, inv_two)
    grad_branch = grad_mid.astype(low)
    router_part = contract(normed_mid, grad_logits, "td,te->de").reshape(devices, -1, 128)
    note_three = jnp.concatenate(
        [
            gain_part.reshape(-1, 128),
            jnp.full((8, 128), largest_own, f32),
        ],
        axis=0,
    )
    branch_all, notes, back_gate, back_up = gather_rows(
        (grad_branch, note_three),
        (),
        devices,
        6,
        (
            ("line", add_halves(gate_halves, gate_come)),
            ("line", add_halves(up_halves, up_come)),
        ),
    )
    clip_factor = jnp.sqrt(clip_threshold / jnp.maximum(notes[:, -1, 0], clip_threshold))
    gain_sum = jnp.sum(notes[:, :-8], axis=0).reshape(-1)
    grad_gain_moe = lax.dynamic_slice_in_dim(gain_sum, me * rows_own, rows_own)

    flat_branch = branch_all.reshape(all_count, width)
    grad_out = contract(mixed, flat_branch, "tq,td->qd")
    grad_mixed = (
        contract(flat_branch, w_out, "td,qd->tq").astype(low).reshape(devices, row_count, head_dim)
    )
    grad_value = contract(probs_low, grad_mixed, "btu,btd->bud").astype(low)
    grad_probs = contract(grad_mixed, value_rows, "btd,bud->btu")
    grad_scores = (
        probs * (grad_probs - jnp.sum(probs * grad_probs, axis=-1, keepdims=True))
    ).astype(low)
    grad_query_rot = contract(grad_scores, key_rot, "btu,bud->btd") * score_scale
    grad_key_rot = contract(grad_scores, query_rot, "btu,btd->bud") * score_scale
    grad_query_normed = rotate_back(grad_query_rot, cosine_all, sine_all)
    grad_key_normed = rotate_back(grad_key_rot, cosine_all, sine_all)
    gain_pair = jnp.stack(
        [
            jnp.sum(grad_query_normed * unit_query, axis=(0, 1)),
            jnp.sum(grad_key_normed * unit_key, axis=(0, 1)),
        ]
    )
    grad_query_raw = norm_back(grad_query_normed * gain_query_f, unit_query, inv_query).astype(low)
    grad_key_raw = norm_back(grad_key_normed * gain_key_f, unit_key, inv_key).astype(low)
    grad_heads = jnp.concatenate([grad_query_raw, grad_key_raw, grad_value], axis=2).reshape(
        all_count, 3 * head_dim
    )
    grad_heads_w = contract(flat_unit, grad_heads, "td,tq->dq").astype(low)
    resid_out = resid_mid + moe_rows
    undeal = (jnp.arange(tok_count, dtype=jnp.int32)[:, None] == local_order[None, :]).astype(low)
    undeal = undeal[:, :row_count]
    block_out = jnp.dot(undeal, resid_out.astype(low), preferred_element_type=f32).astype(low)
    grad_unit_one, back_heads, back_fall, gain_pairs, router_parts = scatter_sum(
        grad_heads,
        w_heads,
        devices,
        7,
        turned=True,
        riders=(
            ("all", grad_heads_w.reshape(devices, rows_own, 3 * head_dim)),
            ("line", add_halves(fall_halves, fall_come)),
            ("same", jnp.pad(gain_pair, ((0, 6), (0, 0)))),
            ("all", router_part),
        ),
    )
    back_heads = back_heads.astype(f32)
    grad_gate = back_gate.astype(f32)
    grad_up = back_up.astype(f32)
    grad_down = back_fall.transpose(0, 2, 1).astype(f32)
    grad_router = jnp.sum(router_parts, axis=0).reshape(rows_own, experts)
    gain_pair = jnp.sum(gain_pairs, axis=0)
    plain_query = back_heads[..., :head_dim].transpose(1, 0, 2).reshape(rows_own, -1)

    def of_group(grads):
        grads = jnp.sum(grads.reshape(kv_count, group_size, rows_own, head_dim), axis=1)
        return grads.transpose(1, 0, 2).reshape(rows_own, -1)

    plain_key = of_group(back_heads[..., head_dim : 2 * head_dim])
    plain_value = of_group(back_heads[..., 2 * head_dim :])
    grad_gain_attn = (
        jnp.sum(plain_query * w_query.astype(f32), axis=1)
        + jnp.sum(plain_key * w_key.astype(f32), axis=1)
        + jnp.sum(plain_value * w_value.astype(f32), axis=1)
    )
    grad_resid_in = grad_mid + norm_back(grad_unit_one, unit_one, inv_one)
    grad_input = exact_dot(undeal.astype(f32), grad_resid_in)
    return (
        block_out,
        grad_input,
        plain_query * gain_col,
        plain_key * gain_col,
        plain_value * gain_col,
        grad_out,
        grad_router,
        grad_gain_attn,
        grad_gain_moe,
        gain_pair[0],
        gain_pair[1],
        grad_gate,
        grad_up,
        grad_down,
        clip_factor,
    )


def solution(mesh):
    placed = (
        P(("dp", "ep"), None),
        P(("dp", "ep"), None),
        P(("dp", "ep")),
        P(("dp", "ep"), None),
        P(("dp", "ep"), None),
        P(("dp", "ep"), None),
        P(("dp", "ep"), None),
        P(("dp", "ep"), None),
        P(("dp", "ep"), None),
        P(("dp", "ep"), None),
        P(("dp", "ep")),
        P(("dp", "ep")),
        P(),
        P(),
        P("ep", "dp", None),
        P("ep", "dp", None),
        P("ep", None, "dp"),
        P(),
    )
    return jax.shard_map(
        per_device if not whole_rows(mesh) else by_experts,
        mesh=mesh,
        in_specs=placed,
        out_specs=(
            P(("dp", "ep"), None),
            P(("dp", "ep"), None),
            P(("dp", "ep"), None),
            P(("dp", "ep"), None),
            P(("dp", "ep"), None),
            P(("dp", "ep"), None),
            P(("dp", "ep"), None),
            P(("dp", "ep")),
            P(("dp", "ep")),
            P(),
            P(),
            P("ep", "dp", None),
            P("ep", "dp", None),
            P("ep", None, "dp"),
            P(),
        ),
        check_vma=False,
    )
```
